32 devices in a mesh: px: 8 (over z, y), py: 4 (over x, core).
Axes of the slice: x: 2, y: 2, z: 4, core: 2. Of those that a mesh axis runs over, the one named last changes fastest.
Arguments:
- initial_field: float32 [1, 2048, 2048], P(None, ('px', 'py')), may hold values from -6 to 6
- target_field: float32 [1, 2048, 2048], P(None, ('px', 'py')), may hold values from -6 to 6
- forcing: float32 [2, 2048, 2048], P(None, ('px', 'py')), may hold values from -6 to 6
Outputs:
- next_field: float32 [1, 2048, 2048], P(None, ('px', 'py'))
- objective: float32 [], replicated
- field_grad: float32 [1, 2048, 2048], P(None, ('px', 'py'))
- forcing_grad: float32 [2, 2048, 2048], P(None, ('px', 'py'))
The draws below stay inside these ranges and needn't reach their ends.
All inputs are finite; a program needn't handle non-finite values.
Results may differ from the reference program's by a relative error of at most 0.00014.
Values sent between devices are 32-bit elements; how exact they have to be, the bound alone decides.
A program may use at most 128 MiB of HBM per device.

```python
import jax
import jax.numpy as jnp
from jax import lax

NX = 2048
NY = 2048
MEMBERS = 1


def block_scale(own_key, dims, shards, low, largest):
    def one(dim, shards_of):
        heights = jax.random.uniform(jax.random.fold_in(jax.random.fold_in(own_key, 6), dim), (shards_of,), jnp.float32, low / len(shards), largest / len(shards))
        return jnp.repeat(jnp.exp(heights), dims[dim] // shards_of).reshape((-1,) + (1,) * (len(dims) - dim - 1))

    level = one(*shards[0])
    for cut in shards[1:]:
        level = level * one(*cut)
    return level


def gaussian(key, extent, deviation, bound, cuts=(), held_as=jnp.bfloat16):
    values = deviation * jax.random.normal(key, extent, jnp.float32)
    if cuts:
        values = values * block_scale(key, extent, cuts, -0.22, 0.18)
    return jnp.clip(values, -bound, bound).astype(held_as)


def setup_inputs(seed: int = 0) -> dict:
    arg_keys = jax.random.split(jax.random.key(seed), 4)
    initial_field = gaussian(arg_keys[0], (MEMBERS, NX, NY), 1.0, 6.0, ((1, 32),), jnp.float32)
    target_field = gaussian(arg_keys[1], (MEMBERS, NX, NY), 1.0, 6.0, ((1, 32),), jnp.float32)
    forcing = gaussian(arg_keys[2], (2, NY, NX), 1.0, 6.0, ((1, 32),), jnp.float32)
    return {"initial_field": initial_field, "target_field": target_field, "forcing": forcing}


time_step = 0.25

def wavenumbers(count):
    position = jnp.arange(count, dtype=jnp.int32)
    signed = jnp.where(position < count // 2, position, position - count)
    waves = (4.0 * signed.astype(jnp.float32) / count).astype(jnp.float32)
    derive = jnp.where(position == count // 2, jnp.float32(0.0), waves).astype(jnp.float32)
    return (waves, derive)

def advance(field, forcing):
    wave_first, deriv_first = wavenumbers(NX)
    wave_second, deriv_second = wavenumbers(NY)
    wave_square = wave_first[:, None] ** 2 + wave_second[None, :] ** 2
    denominator = 1.0 + time_step * (wave_square * wave_square - wave_square)
    state_hat = jnp.fft.fft2(field, norm='ortho')
    grad_first = jnp.fft.ifft2(1j * deriv_first[:, None] * state_hat, norm='ortho').real
    grad_second = jnp.fft.ifft2(1j * deriv_second[None, :] * state_hat, norm='ortho').real
    nonlinear = -0.5 * (grad_first * grad_first + grad_second * grad_second)
    nonlinear_hat = jnp.fft.fft2(nonlinear, norm='ortho')
    forcing_hat = lax.complex(forcing[0].T, forcing[1].T)
    next_hat = (state_hat + time_step * (nonlinear_hat + forcing_hat)) / denominator
    return jnp.fft.ifft2(next_hat, norm='ortho').real

def reference(initial_field, target_field, forcing):

    def one_member(pair):
        field, goal = pair
        next_one, pullback = jax.vjp(advance, field, forcing)
        residual = next_one - goal
        grad_one, forcing_one = pullback(residual)
        return (next_one, jnp.sum(residual * residual), grad_one, forcing_one)
    next_field, squares, field_grad, forcing_parts = lax.map(one_member, (initial_field, target_field))
    objective = 0.5 * jnp.sum(squares) / (MEMBERS * NX * NY)
    forcing_grad = lax.optimization_barrier(jnp.sum(forcing_parts, axis=0))
    return (next_field, objective, field_grad, forcing_grad)
```

```python
import functools
import math

import jax
import jax.numpy as jnp
import numpy as np
from jax import lax
from jax.experimental import pallas as pl
from jax.experimental.pallas import tpu as pltpu
from jax.sharding import PartitionSpec as P

time_step = 0.25
axes = ("px", "py")
TILE = 128


def split_length(length):
    inner = 256 if length % 256 == 0 else TILE
    return (length // inner, inner)


def small_dft(items, sign):
    count = len(items)
    if count == 1:
        return items
    evens = small_dft(items[0::2], sign)
    odds = small_dft(items[1::2], sign)
    low, high = [], []
    for k in range(count // 2):
        odd_re, odd_im = odds[k]
        if 4 * k == count:
            odd_re, odd_im = (-odd_im, odd_re) if sign > 0 else (odd_im, -odd_re)
        elif k:
            c = math.cos(2.0 * math.pi * k / count)
            s = sign * math.sin(2.0 * math.pi * k / count)
            if abs(abs(c) - abs(s)) < 1e-12:
                sc, ss = math.copysign(1.0, c), math.copysign(1.0, s)
                odd_re, odd_im = (
                    c * (odd_re - sc * ss * odd_im),
                    c * (odd_im + sc * ss * odd_re),
                )
            else:
                odd_re, odd_im = (c * odd_re - s * odd_im, c * odd_im + s * odd_re)
        even_re, even_im = evens[k]
        low.append((even_re + odd_re, even_im + odd_im))
        high.append((even_re - odd_re, even_im - odd_im))
    return low + high


def halves(value):
    top = value.astype(jnp.bfloat16)
    return top, (value - top.astype(jnp.float32)).astype(jnp.bfloat16)


def orders(length, rows):
    inner = split_length(length)[1]
    half = rows // 2
    lane = np.arange(inner)
    natural = lane
    local = lane % (inner // 2)
    line = local % half
    kept = rows * (local // half) + np.where((lane >= inner // 2) & (line == 0), half, line)
    groups = TILE // rows
    tall = rows // groups
    within = lane % (inner // groups)
    lines = rows * (within // tall) + tall * (lane // (inner // groups)) + within % tall
    return natural, kept, lines


def twiddle_table(length, order):
    outer = split_length(length)[0]
    angle = 2.0 * np.pi * np.outer(np.arange(outer), order) / length
    return (np.stack([np.cos(angle), np.sin(angle)]) / math.sqrt(length)).astype(np.float32)


def matrix_table(length, sign, left, right):
    inner = split_length(length)[1]
    angle = 2.0 * np.pi * (np.outer(left, right) % inner) / inner
    c, s = np.cos(angle), np.sin(angle)
    full = np.block([[c, sign * s], [-sign * s, c]])
    top = full.astype(jnp.bfloat16)
    return np.stack([top, (full - top.astype(np.float64)).astype(jnp.bfloat16)])


def mirror_table(length):
    inner = split_length(length)[1]
    lane = np.arange(inner)
    both = np.zeros((2, inner, inner))
    both[0, (inner - lane) % inner, lane] = 1.0
    both[1, inner - 1 - lane, lane] = 1.0
    return both.astype(jnp.bfloat16)


class Pieces:
    def __init__(self, length, rows, turned=None, top=None, low=None, grid_out=None):
        self.length, self.rows, self.half = length, rows, rows // 2
        self.outer, self.inner = split_length(length)
        self.turned, self.top, self.low, self.z = turned, top, low, grid_out
        self.step = math.gcd(rows // 2, 16)

    def chunks(self, lines, body):
        def run(i, carry):
            body(pl.multiple_of(i * self.step, self.step))
            return carry

        lax.fori_loop(0, lines // self.step, run, 0)

    def put(self, k, at, part, value):
        lanes = pl.ds(part * self.inner, self.inner)
        top, low = halves(value)
        self.top[k, at, lanes] = top
        self.low[k, at, lanes] = low

    def get(self, k, at, part):
        return self.z[k, at, pl.ds(part * self.inner, self.inner)]

    def multiply(self, lines, matrix, real_in=False, real_out=False):
        deep = self.inner if real_in else 2 * self.inner
        wide = self.inner if real_out else 2 * self.inner
        count = self.outer * lines
        top = self.top[:, :lines, :deep].reshape(count, deep)
        low = self.low[:, :lines, :deep].reshape(count, deep)
        right_top = matrix[0, :deep, :wide]
        right_low = matrix[1, :deep, :wide]
        dot = functools.partial(jnp.dot, preferred_element_type=jnp.float32)
        total = dot(top, right_top) + dot(low, right_top) + dot(top, right_low)
        self.z[:, :lines, :wide] = total.reshape(self.outer, lines, wide)

    def twist(self, k, pair, sign, twiddle):
        c = twiddle[0, pl.ds(k, 1), :]
        s = twiddle[1, pl.ds(k, 1), :]
        s = s if sign > 0 else -s
        re, im = pair
        return (re * c - im * s, re * s + im * c)

    def turn_full(self, source):
        rows, blocks = self.rows, TILE // self.rows
        for t in range(self.length // TILE):
            tile = source[pl.ds(t * blocks, blocks), :rows, :].reshape(TILE, 2 * rows)
            self.turned[: 2 * rows, pl.ds(t * TILE, TILE)] = tile.T

    def turn_lines(self, source):
        rows = self.rows
        groups = TILE // rows
        blocks, wide = self.inner // rows, self.inner // groups
        for t in range(self.outer):
            tile = source[pl.ds(t * blocks, blocks), :, :].reshape(wide, TILE).T
            for h in range(groups):
                self.turned[:rows, pl.ds(t * self.inner + h * wide, wide)] = tile[h * rows : (h + 1) * rows]

    def kept_lanes(self, j):
        wide = self.inner // 2
        return j * self.inner + (wide if 2 * j >= self.outer else 0), wide

    def clear_other(self, j):
        at, wide = self.kept_lanes(j)
        other = j * self.inner + (0 if 2 * j >= self.outer else wide)
        self.turned[: 2 * self.rows, pl.ds(other, wide)] = jnp.zeros((2 * self.rows, wide), jnp.float32)

    def turn_kept(self, source):
        rows, half, blocks = self.rows, self.half, self.inner // self.rows
        for j in range(self.outer):
            at, wide = self.kept_lanes(j)
            tile = source[pl.ds(j * blocks, blocks), :, :].reshape(wide, 2 * rows)
            self.turned[: 2 * rows, pl.ds(at, wide)] = tile.T
            self.clear_other(j)

    def unpack_middle(self):
        rows, middle = self.rows, (self.outer // 2) * self.inner
        first = self.turned[rows : 2 * rows, :TILE]
        lane0 = lax.broadcasted_iota(jnp.int32, first.shape, 1) == 0
        zero = jnp.zeros_like(first)
        self.turned[:rows, pl.ds(middle, TILE)] += jnp.where(lane0, first, zero)
        self.turned[rows : 2 * rows, :TILE] = jnp.where(lane0, zero, first)

    def incoming(self, lines, sign, twiddle, matrix, real_out=False):
        def body(r0):
            items = []
            for j in range(self.outer):
                lanes = pl.ds(j * self.inner, self.inner)
                items.append((
                    self.turned[pl.ds(r0, self.step), lanes],
                    self.turned[pl.ds(lines + r0, self.step), lanes],
                ))
            for k, pair in enumerate(small_dft(items, sign)):
                re, im = self.twist(k, pair, sign, twiddle)
                self.put(k, pl.ds(r0, self.step), 0, re)
                self.put(k, pl.ds(r0, self.step), 1, im)

        self.chunks(lines, body)
        self.multiply(lines, matrix, real_out=real_out)

    def outgoing(self, lines, sign, twiddle, matrix, real_in, write):
        self.multiply(lines, matrix, real_in=real_in)

        def body(r0):
            at = pl.ds(r0, self.step)
            write(r0, small_dft([
                self.twist(k, (self.get(k, at, 0), self.get(k, at, 1)), sign, twiddle)
                for k in range(self.outer)
            ], sign))

        self.chunks(lines, body)

    def pack_middle(self, items):
        re, im = items[0]
        lane0 = lax.broadcasted_iota(jnp.int32, im.shape, 1) == 0
        return [(re, jnp.where(lane0, items[self.outer // 2][0], im))] + items[1:]

    def write_full(self, result, pack):
        rows = self.rows

        def write(r0, items):
            at = pl.ds(r0, self.step)
            for j, (re, im) in enumerate(self.pack_middle(items) if pack else items):
                for piece in range(self.inner // rows):
                    to = j * (self.inner // rows) + piece
                    lanes = slice(piece * rows, (piece + 1) * rows)
                    result[to, at, pl.ds(0, rows)] = re[:, lanes]
                    result[to, at, pl.ds(rows, rows)] = im[:, lanes]

        return write

    def outgoing_kept(self, twiddle, matrix, result):
        self.multiply(self.rows, matrix, real_in=True)
        rows, half, blocks = self.rows, self.half, self.inner // self.rows
        tall = rows * rows // TILE
        step = math.gcd(rows, 16)
        span = min(tall, step)
        for h in range(rows // max(tall, step)):

            def body(i, carry, h=h):
                r0 = i * step if isinstance(i, int) else pl.multiple_of(i * step, step)
                at = pl.ds(h * max(tall, step) + r0, step)
                items = self.pack_middle(small_dft([
                    self.twist(k, (self.get(k, at, 0), self.get(k, at, 1)), -1.0, twiddle)
                    for k in range(self.outer)
                ], -1.0))
                for j, pair in enumerate(items):
                    base = self.inner // 2 if 2 * j >= self.outer else 0
                    for piece in range(blocks):
                        lanes = slice(base + piece * half, base + (piece + 1) * half)
                        for part, value in enumerate(pair):
                            for sub in range(step // span):
                                group = h * (step // span) + sub
                                to = pl.ds(group * rows + part * half, half)
                                held = value[sub * span : (sub + 1) * span, lanes]
                                result[j * blocks + piece, pl.ds(r0, span), to] = held
                return carry

            if tall > step:
                lax.fori_loop(0, tall // step, body, 0)
            else:
                body(0, 0)

    def mirrored(self, blocks, mirror):
        dot = functools.partial(jnp.dot, preferred_element_type=jnp.float32)

        def flip(values, which):
            top, low = halves(jnp.concatenate(values, axis=0))
            return dot(top, mirror[which]) + dot(low, mirror[which])

        flat = [part for k in range(self.outer) for pair in blocks[k] for part in pair]
        per = 2 * len(blocks[0])
        low = flip(flat[:per], 0)
        high = flip(flat[per:], 1)
        out = []
        for k in range(self.outer):
            part, base = (low, 0) if k == 0 else (high, (self.outer - k - 1) * per)
            take = lambda i: part[(base + i) * 8 : (base + i + 1) * 8]
            out.append([(take(2 * i), -take(2 * i + 1)) for i in range(per // 2)])
        return out

    def pack_columns(self, slabs, result):
        rows, half, wide = self.rows, self.half, self.inner // 2
        blocks, groups = self.inner // rows, TILE // rows
        tall = rows // groups
        for k in range(self.outer):
            slab = slabs(k)
            for s in range(blocks):
                parts = []
                for group in range(groups):
                    for part in range(2):
                        at = part * wide + s * half
                        parts.append(slab[group * tall : (group + 1) * tall, at : at + half])
                result[k * blocks + s] = jnp.concatenate(parts, axis=1)

    def turn_columns(self, source, result):
        rows, wide, blocks = self.rows, self.inner // 2, self.inner // self.rows
        for j in range(self.outer):
            tile = source[pl.ds(j * blocks, blocks), :, :].reshape(wide, 2 * rows).T
            result[j, :, pl.ds(0, wide)] = tile[:rows]
            result[j, :, pl.ds(wide, wide)] = tile[rows:]

    def spread(self, first, second, strided, result):
        rows, fill = self.rows, TILE - 2 * self.rows
        for t in range(self.length // TILE):
            lanes = pl.ds(t * TILE, TILE)
            parts = [first[:, lanes], second[:, lanes]]
            if fill:
                parts.append(jnp.zeros((fill, TILE), jnp.float32))
            strided[pl.ds(t * TILE, TILE), :] = jnp.concatenate(parts, axis=0).T
        for k in range(self.outer):
            slab = strided[pl.ds(k, self.inner, stride=self.outer), :].T
            result[k] = slab[: 2 * rows, :]

    def collect(self, slabs, strided, results):
        rows = self.rows
        for k in range(self.outer):
            slab = slabs(k)
            fill = TILE - slab.shape[0]
            if fill:
                slab = jnp.concatenate([slab, jnp.zeros((fill, self.inner), jnp.float32)], axis=0)
            strided[pl.ds(k, self.inner, stride=self.outer), :] = slab.T
        for t in range(self.length // TILE):
            block = strided[pl.ds(t * TILE, TILE), :].T
            for i, result in enumerate(results):
                result[:, pl.ds(t * TILE, TILE)] = block[i * rows : (i + 1) * rows, :]


def signed_waves(position, count):
    signed = jnp.where(position < count // 2, position, position - count)
    waves = 4.0 * signed.astype(jnp.float32) / count
    return waves, jnp.where(position == count // 2, jnp.float32(0.0), waves)


def first_waves(piece, k):
    lanes = lax.broadcasted_iota(jnp.int32, (1, piece.inner), 1)
    return signed_waves(piece.outer * lanes + k, piece.length)


def inverse_denominator(wave_first, wave_second):
    square = wave_first * wave_first + wave_second * wave_second
    return 1.0 / (1.0 + time_step * (square * square - square))


def second_wave(piece, position):
    shape = (position.shape[0], piece.inner)
    return jnp.broadcast_to(signed_waves(position, piece.length)[0], shape)


def row_index(count, width):
    return lax.broadcasted_iota(jnp.int32, (count, width), 0)


def start_kernel(length, rows, field, target, out, both_p, *scratch):
    piece = Pieces(length, rows)
    piece.spread(field, target, scratch[0], both_p)
    piece.pack_columns(lambda k: both_p[k, pl.ds(0, rows), :], out)


def slope_second_kernel(length, rows, field_p, twiddle, out_matrix, in_matrix, kept, result, *scratch):
    piece = Pieces(length, rows, *scratch)

    def body(r0):
        at = pl.ds(r0, piece.step)
        for k in range(piece.outer):
            piece.put(k, at, 0, field_p[k, at, :])

    piece.chunks(rows, body)
    for j in range(piece.outer):
        piece.clear_other(j)

    def write(r0, items):
        for j, (re, im) in enumerate(items):
            at, wide = piece.kept_lanes(j)
            base = at - j * piece.inner
            position = j * piece.inner + kept[:, base : base + wide]
            slope = 2.0 * signed_waves(position, length)[1]
            piece.turned[pl.ds(r0, piece.step), pl.ds(at, wide)] = -slope * im[:, base : base + wide]
            piece.turned[pl.ds(rows + r0, piece.step), pl.ds(at, wide)] = slope * re[:, base : base + wide]

    piece.outgoing(rows, -1.0, twiddle, out_matrix, True, write)
    piece.incoming(rows, 1.0, twiddle, in_matrix, real_out=True)
    result[...] = piece.z[:, :, : piece.inner]


def spread_kernel(length, rows, forcing, result, strided):
    Pieces(length, rows).spread(forcing.at[0], forcing.at[1], strided, result)


def collect_kernel(length, rows, slabs, result, strided):
    piece = Pieces(length, rows)
    piece.collect(lambda k: slabs[k], strided, [result.at[i] for i in range(result.shape[0])])


def weight_of(device, r0, step, inner):
    alone = (row_index(step, inner) + r0 + device) == 0
    return jnp.where(alone, jnp.float32(1.0), jnp.float32(2.0))


def slope_first_kernel(length, rows, source, in_twiddle, in_matrix, out_twiddle, out_matrix, out, *scratch):
    piece = Pieces(length, rows, *scratch)
    half = piece.half
    piece.turn_lines(source)
    piece.incoming(half, -1.0, in_twiddle, in_matrix)

    def body(r0):
        at = pl.ds(r0, piece.step)
        for k in range(piece.outer):
            re, im = piece.get(k, at, 0), piece.get(k, at, 1)
            scale = first_waves(piece, k)[1]
            piece.put(k, at, 0, -scale * im)
            piece.put(k, at, 1, scale * re)

    piece.chunks(half, body)
    piece.outgoing(half, 1.0, out_twiddle, out_matrix, False, piece.write_full(out, False))


def edge_inverses(piece, k):
    wave_first = first_waves(piece, k)[0]
    middle = jnp.full((1, 1), piece.length // 2, jnp.int32)
    zero = jnp.zeros((1, 1), jnp.int32)
    return [inverse_denominator(wave_first, signed_waves(p, piece.length)[0]) for p in (zero, middle)]


def next_kernel(length, rows, device_ref, source, forcing, in_twiddle, in_matrix, out_twiddle, out_matrix, mirror, out, *scratch):
    device = device_ref[0]
    piece = Pieces(length, rows, *scratch)
    half, step, inner = piece.half, piece.step, piece.inner
    late = device >= (length // rows) // 2
    piece.turn_lines(source)
    piece.incoming(half, -1.0, in_twiddle, in_matrix)

    def body(r0):
        at, also = pl.ds(r0, step), pl.ds(half + r0, step)
        index = row_index(step, 1) + r0
        low_wave = second_wave(piece, device * rows + index)
        high_wave = second_wave(piece, device * rows + half + index)
        moved = jnp.logical_and(row_index(step, inner) + r0 == 0, late)
        weight = weight_of(device, r0, step, inner)
        for k in range(piece.outer):
            wave_first = first_waves(piece, k)[0]
            low = inverse_denominator(wave_first, low_wave)
            high = inverse_denominator(wave_first, high_wave)
            for part in range(2):
                own = weight * piece.get(k, at, part)
                f_low = time_step * forcing[k, pl.ds(part * rows + r0, step), :]
                f_high = time_step * forcing[k, pl.ds(part * rows + half + r0, step), :]
                piece.put(k, at, part, (f_low + jnp.where(moved, 0.0, own)) * low)
                piece.put(k, also, part, (f_high + jnp.where(moved, own, 0.0)) * high)

    piece.chunks(half, body)

    @pl.when(device == 0)
    def _():
        at = pl.ds(0, 8)
        blocks = []
        for k in range(piece.outer):
            own = tuple(piece.get(k, at, part) for part in range(2))
            full = tuple(
                own[part] + time_step * forcing[k, pl.ds(part * rows, 8), :] for part in range(2)
            )
            blocks.append([own, full])
        flipped = piece.mirrored(blocks, mirror)
        rest = pl.ds(0, 16)
        row0 = row_index(16, inner) == 0
        for k in range(piece.outer):
            zero, middle = edge_inverses(piece, k)
            for part in range(2):
                own, full = blocks[k][0][part], blocks[k][1][part]
                own_c, full_c = flipped[k][0][part], flipped[k][1][part]
                value = 0.5 * ((full + full_c) * zero + (own - own_c) * middle)
                replace(piece, k, part, value)

    piece.outgoing(rows, 1.0, out_twiddle, out_matrix, False, piece.write_full(out, False))


def replace(piece, k, part, value):
    lanes = pl.ds(part * piece.inner, piece.inner)
    row0 = row_index(16, piece.inner) == 0
    value = jnp.concatenate([value, value], axis=0)
    for held, new in zip((piece.top, piece.low), halves(value)):
        old = held[k, pl.ds(0, 16), lanes].astype(jnp.float32)
        held[k, pl.ds(0, 16), lanes] = jnp.where(row0, new.astype(jnp.float32), old).astype(jnp.bfloat16)


def misfit_kernel(length, rows, device_ref, source, in_twiddle, in_matrix, out_twiddle, out_matrix, mirror, out, full, total_out, *scratch):
    device = device_ref[0]
    piece = Pieces(length, rows, *scratch)
    half, step, inner = piece.half, piece.step, piece.inner
    late = device >= (length // rows) // 2
    piece.turn_full(source)
    piece.incoming(rows, -1.0, in_twiddle, in_matrix)

    def body(r0):
        at, also = pl.ds(r0, step), pl.ds(half + r0, step)
        index = row_index(step, 1) + r0
        low_wave = second_wave(piece, device * rows + index)
        high_wave = second_wave(piece, device * rows + half + index)
        moved = jnp.logical_and(row_index(step, inner) + r0 == 0, late)
        weight = weight_of(device, r0, step, inner)
        for k in range(piece.outer):
            wave_first = first_waves(piece, k)[0]
            low = time_step * inverse_denominator(wave_first, low_wave)
            high = time_step * inverse_denominator(wave_first, high_wave)
            for part in range(2):
                low_value = piece.get(k, at, part) * low
                high_value = piece.get(k, also, part) * high
                full[k, pl.ds(part * rows + r0, step), :] = low_value
                full[k, pl.ds(part * rows + half + r0, step), :] = high_value
                own = jnp.where(moved, high_value, low_value)
                piece.put(k, at, part, weight * own)

    piece.chunks(half, body)

    @pl.when(device == 0)
    def _():
        at = pl.ds(0, 8)
        blocks = [[(piece.get(k, at, 0), piece.get(k, at, 1))] for k in range(piece.outer)]
        flipped = piece.mirrored(blocks, mirror)
        row0 = row_index(8, inner) == 0
        for k in range(piece.outer):
            zero, middle = edge_inverses(piece, k)
            for part in range(2):
                own, own_c = blocks[k][0][part], flipped[k][0][part]
                first = (0.5 * time_step) * (own + own_c) * zero
                value = first + (0.5 * time_step) * (own - own_c) * middle
                at_full = pl.ds(part * rows, 8)
                full[k, at_full, :] = jnp.where(row0, first, full[k, at_full, :])
                replace(piece, k, part, value)

    piece.outgoing(half, 1.0, out_twiddle, out_matrix, False, piece.write_full(out, False))
    total_out[...] = jnp.sum(source[:, pl.ds(rows, 8), :], axis=0)


def nonlinear_kernel(length, rows, source, both_p, second, twiddle, out_matrix, out, first, *scratch):
    piece = Pieces(length, rows, *scratch)
    piece.turn_columns(source, first)

    def body(r0):
        at = pl.ds(r0, piece.step)
        for k in range(piece.outer):
            one, other = first[k, at, :], second[k, at, :]
            piece.put(k, at, 0, both_p[k, at, :] - (0.5 * time_step) * (one * one + other * other))

    piece.chunks(rows, body)
    piece.outgoing_kept(twiddle, out_matrix, out)


def joint_kernel(length, rows, source, first, second, twiddle, in_matrix, out, value_out, second_out, *scratch):
    piece = Pieces(length, rows, *scratch)
    piece.turn_kept(source)
    piece.unpack_middle()
    piece.incoming(rows, 1.0, twiddle, in_matrix, real_out=True)
    lanes = pl.ds(0, piece.inner)

    def body(r0):
        at = pl.ds(r0, piece.step)
        for k in range(piece.outer):
            value = piece.get(k, at, 0)
            value_out[k, at, :] = (1.0 / time_step) * value
            second_out[k, at, :] = value * second[k, at, :]
            piece.z[k, at, lanes] = value * first[k, at, :]

    piece.chunks(rows, body)
    piece.pack_columns(lambda k: piece.z[k, pl.ds(0, rows), lanes], out)


def residual_kernel(length, rows, source, both_p, twiddle, in_matrix, out_matrix, out, field_out, *scratch):
    piece = Pieces(length, rows, *scratch[:4])
    strided, total = scratch[4:]
    piece.turn_full(source)
    piece.unpack_middle()
    piece.incoming(rows, 1.0, twiddle, in_matrix, real_out=True)
    piece.collect(lambda k: piece.get(k, pl.ds(0, rows), 0), strided, [field_out])
    total[...] = jnp.zeros_like(total)

    def body(r0):
        at = pl.ds(r0, piece.step)
        for k in range(piece.outer):
            residual = piece.get(k, at, 0) - both_p[k, pl.ds(rows + r0, piece.step), :]
            total[...] += residual * residual
            piece.put(k, at, 0, residual)

    piece.chunks(rows, body)
    piece.outgoing(rows, -1.0, twiddle, out_matrix, True, piece.write_full(out, True))
    value = 0.5 * jnp.sum(total[...])
    out[:, pl.ds(rows, 8), :] = jnp.full((out.shape[0], 8, 2 * rows), value, jnp.float32)


def last_kernel(length, rows, source, value, second, field_out, strided, first):
    piece = Pieces(length, rows)
    piece.turn_columns(source, first)
    piece.collect(lambda k: first[k] + value[k] + second[k], strided, [field_out])


def member_step(device, field, target, forcing_p, devices, rows, length):
    outer, inner = split_length(length)
    half = rows // 2
    float32 = jnp.float32
    shape = lambda *dims: jax.ShapeDtypeStruct(dims, float32)
    kept_blocks = shape(devices, rows * rows // TILE, TILE)
    half_blocks = shape(devices, half, 2 * rows)
    blocks = shape(devices, rows, 2 * rows)
    longer = shape(devices, rows + 8, 2 * rows)
    pair, one = shape(outer, 2 * rows, inner), shape(outer, rows, inner)
    plain = shape(rows, length)
    step = math.gcd(half, 16)
    base = [
        pltpu.VMEM((2 * rows, length), float32),
        pltpu.VMEM((outer, rows, 2 * inner), jnp.bfloat16),
        pltpu.VMEM((outer, rows, 2 * inner), jnp.bfloat16),
        pltpu.VMEM((outer, rows, 2 * inner), float32),
    ]
    strided = pltpu.VMEM((length, TILE), float32)
    total = pltpu.VMEM((step, inner), float32)
    vmem = pl.BlockSpec(memory_space=pltpu.VMEM)
    smem = pl.BlockSpec(memory_space=pltpu.SMEM)

    natural, kept, lines = orders(length, rows)
    tw_natural, tw_kept, tw_lines = [jnp.asarray(twiddle_table(length, o)) for o in (natural, kept, lines)]
    matrix = lambda *args: matrix_table(length, *args)
    forward, backward = matrix(-1.0, natural, natural), matrix(1.0, natural, natural)
    kept_out, kept_in = matrix(-1.0, natural, kept)[:, :inner], matrix(1.0, kept, natural)[:, :, :inner]
    lines_in = matrix(-1.0, lines, natural)
    mirror = jnp.asarray(mirror_table(length))
    kept_lane = jnp.asarray(kept[None, :].astype(np.int32))

    def call(body, outs, scratch, *operands):
        return pl.pallas_call(
            functools.partial(body, length, rows),
            out_shape=outs,
            in_specs=[smem if operand is device else vmem for operand in operands],
            out_specs=jax.tree.map(lambda leaf: vmem, outs),
            scratch_shapes=scratch,
            compiler_params=pltpu.CompilerParams(vmem_limit_bytes=20 * 2**20),
            cost_estimate=pl.CostEstimate(flops=6 * 10**9, bytes_accessed=4 * 2**20, transcendentals=0),
        )(*operands)

    def move(value):
        return lax.all_to_all(value, axes, split_axis=0, concat_axis=0, tiled=True)

    spectral_tables = (tw_lines, lines_in, tw_natural, backward)
    slope_tables = (tw_kept, kept_out, kept_in, kept_lane)
    sent, both_p = call(start_kernel, (kept_blocks, pair), [strided], field, target)
    second = call(slope_second_kernel, one, base, both_p, *slope_tables)
    sent = call(slope_first_kernel, half_blocks, base, move(sent), *spectral_tables)
    sent, first = call(nonlinear_kernel, (kept_blocks, one), base, move(sent), both_p, second, tw_kept, kept_out)
    sent = call(next_kernel, blocks, base, device, move(sent), forcing_p, *spectral_tables, mirror)
    sent, next_field = call(
        residual_kernel, (longer, plain), base + [strided, total],
        move(sent), both_p, tw_natural, backward, forward,
    )
    sent, full, sums = call(
        misfit_kernel, (half_blocks, pair, shape(8, 2 * rows)), base,
        device, move(sent), tw_natural, forward, tw_natural, backward, mirror,
    )
    sent, value, product = call(
        joint_kernel, (kept_blocks, one, one), base, move(sent), first, second, tw_kept, kept_in
    )
    second_part = call(slope_second_kernel, one, base, product, *slope_tables)
    sent = call(slope_first_kernel, half_blocks, base, move(sent), *spectral_tables)
    field_grad = call(
        last_kernel, plain, [strided, pltpu.VMEM((outer, rows, inner), float32)], move(sent), value, second_part
    )
    return next_field, sums[0, 0], field_grad, full


def per_device(devices, initial_field, target_field, forcing):
    members, rows, length = initial_field.shape
    device = lax.axis_index(axes).astype(jnp.int32).reshape(1)
    outer, inner = split_length(length)
    vmem = pl.BlockSpec(memory_space=pltpu.VMEM)
    strided = pltpu.VMEM((length, TILE), jnp.float32)

    def reorder(body, shape, operand):
        return pl.pallas_call(
            functools.partial(body, length, rows),
            out_shape=jax.ShapeDtypeStruct(shape, jnp.float32),
            in_specs=[vmem],
            out_specs=vmem,
            scratch_shapes=[strided],
        )(operand)

    forcing_p = reorder(spread_kernel, (outer, 2 * rows, inner), forcing)
    results = [
        member_step(device, initial_field[m], target_field[m], forcing_p, devices, rows, length)
        for m in range(members)
    ]
    next_field = jnp.stack([one[0] for one in results])
    objective = sum(one[1] for one in results) / (members * length * length)
    field_grad = jnp.stack([one[2] for one in results])
    forcing_grad = reorder(collect_kernel, (2, rows, length), sum(one[3] for one in results))
    return (next_field, objective, field_grad, forcing_grad)


def solution(mesh):
    devices = mesh.shape["px"] * mesh.shape["py"]
    spec = P(None, axes, None)
    return jax.shard_map(
        functools.partial(per_device, devices),
        mesh=mesh,
        in_specs=(spec, spec, spec),
        out_specs=(spec, P(), spec, spec),
        check_vma=False,
    )
```

```python
import functools
import math
from types import SimpleNamespace

import jax
import jax.numpy as jnp
import numpy as np
from jax import lax
from jax.experimental import pallas as pl
from jax.experimental.pallas import tpu as pltpu
from jax.sharding import PartitionSpec as P

time_step = 0.25
axes = ("px", "py")
TILE = 128


def split_length(length):
    inner = 256 if length % 256 == 0 else TILE
    return (length // inner, inner)


def small_dft(items, sign):
    count = len(items)
    if count == 1:
        return items
    evens = small_dft(items[0::2], sign)
    odds = small_dft(items[1::2], sign)
    low, high = [], []
    for k in range(count // 2):
        odd_re, odd_im = odds[k]
        if 4 * k == count:
            odd_re, odd_im = (-odd_im, odd_re) if sign > 0 else (odd_im, -odd_re)
        elif k:
            c = math.cos(2.0 * math.pi * k / count)
            s = sign * math.sin(2.0 * math.pi * k / count)
            if abs(abs(c) - abs(s)) < 1e-12:
                sc, ss = math.copysign(1.0, c), math.copysign(1.0, s)
                odd_re, odd_im = (
                    c * (odd_re - sc * ss * odd_im),
                    c * (odd_im + sc * ss * odd_re),
                )
            else:
                odd_re, odd_im = (c * odd_re - s * odd_im, c * odd_im + s * odd_re)
        even_re, even_im = evens[k]
        low.append((even_re + odd_re, even_im + odd_im))
        high.append((even_re - odd_re, even_im - odd_im))
    return low + high


def halves(value):
    top = value.astype(jnp.bfloat16)
    return top, (value - top.astype(jnp.float32)).astype(jnp.bfloat16)


def orders(length, rows):
    inner = split_length(length)[1]
    half = rows // 2
    lane = np.arange(inner)
    natural = lane
    local = lane % (inner // 2)
    line = local % half
    kept = rows * (local // half) + np.where((lane >= inner // 2) & (line == 0), half, line)
    groups = TILE // rows
    tall = rows // groups
    within = lane % (inner // groups)
    lines = rows * (within // tall) + tall * (lane // (inner // groups)) + within % tall
    return natural, kept, lines


def twiddle_table(length, order):
    outer = split_length(length)[0]
    angle = 2.0 * np.pi * np.outer(np.arange(outer), order) / length
    return (np.stack([np.cos(angle), np.sin(angle)]) / math.sqrt(length)).astype(np.float32)


def matrix_table(length, sign, left, right):
    inner = split_length(length)[1]
    angle = 2.0 * np.pi * (np.outer(left, right) % inner) / inner
    c, s = np.cos(angle), np.sin(angle)
    full = np.block([[c, sign * s], [-sign * s, c]])
    top = full.astype(jnp.bfloat16)
    return np.stack([top, (full - top.astype(np.float64)).astype(jnp.bfloat16)])


def mirror_table(length):
    inner = split_length(length)[1]
    lane = np.arange(inner)
    both = np.zeros((2, inner, inner))
    both[0, (inner - lane) % inner, lane] = 1.0
    both[1, inner - 1 - lane, lane] = 1.0
    return both.astype(jnp.bfloat16)


class Pieces:
    def __init__(self, length, rows, turned=None, top=None, low=None, grid_out=None):
        self.length, self.rows, self.half = length, rows, rows // 2
        self.outer, self.inner = split_length(length)
        self.turned, self.top, self.low, self.z = turned, top, low, grid_out
        self.step = math.gcd(rows // 2, 16)

    def chunks(self, lines, body):
        def run(i, carry):
            body(pl.multiple_of(i * self.step, self.step))
            return carry

        lax.fori_loop(0, lines // self.step, run, 0)

    def put(self, k, at, part, value):
        lanes = pl.ds(part * self.inner, self.inner)
        top, low = halves(value)
        self.top[k, at, lanes] = top
        self.low[k, at, lanes] = low

    def get(self, k, at, part):
        return self.z[k, at, pl.ds(part * self.inner, self.inner)]

    def multiply(self, lines, matrix, real_in=False, real_out=False):
        deep = self.inner if real_in else 2 * self.inner
        wide = self.inner if real_out else 2 * self.inner
        count = self.outer * lines
        top = self.top[:, :lines, :deep].reshape(count, deep)
        low = self.low[:, :lines, :deep].reshape(count, deep)
        right_top = matrix[0, :deep, :wide]
        right_low = matrix[1, :deep, :wide]
        dot = functools.partial(jnp.dot, preferred_element_type=jnp.float32)
        total = dot(top, right_top) + dot(low, right_top) + dot(top, right_low)
        self.z[:, :lines, :wide] = total.reshape(self.outer, lines, wide)

    def twist(self, k, pair, sign, twiddle):
        c = twiddle[0, pl.ds(k, 1), :]
        s = twiddle[1, pl.ds(k, 1), :]
        s = s if sign > 0 else -s
        re, im = pair
        return (re * c - im * s, re * s + im * c)

    def turn_full(self, source):
        rows, blocks = self.rows, TILE // self.rows
        for t in range(self.length // TILE):
            tile = source[pl.ds(t * blocks, blocks), :rows, :].reshape(TILE, 2 * rows)
            self.turned[: 2 * rows, pl.ds(t * TILE, TILE)] = tile.T

    def turn_lines(self, source):
        rows = self.rows
        groups = TILE // rows
        blocks, wide = self.inner // rows, self.inner // groups
        for t in range(self.outer):
            tile = source[pl.ds(t * blocks, blocks), :, :].reshape(wide, TILE).T
            for h in range(groups):
                self.turned[:rows, pl.ds(t * self.inner + h * wide, wide)] = tile[h * rows : (h + 1) * rows]

    def kept_lanes(self, j):
        wide = self.inner // 2
        return j * self.inner + (wide if 2 * j >= self.outer else 0), wide

    def clear_other(self, j):
        at, wide = self.kept_lanes(j)
        other = j * self.inner + (0 if 2 * j >= self.outer else wide)
        self.turned[: 2 * self.rows, pl.ds(other, wide)] = jnp.zeros((2 * self.rows, wide), jnp.float32)

    def turn_kept(self, source):
        rows, half, blocks = self.rows, self.half, self.inner // self.rows
        for j in range(self.outer):
            at, wide = self.kept_lanes(j)
            tile = source[pl.ds(j * blocks, blocks), :, :].reshape(wide, 2 * rows)
            self.turned[: 2 * rows, pl.ds(at, wide)] = tile.T
            self.clear_other(j)

    def unpack_middle(self):
        rows, middle = self.rows, (self.outer // 2) * self.inner
        first = self.turned[rows : 2 * rows, :TILE]
        lane0 = lax.broadcasted_iota(jnp.int32, first.shape, 1) == 0
        zero = jnp.zeros_like(first)
        self.turned[:rows, pl.ds(middle, TILE)] += jnp.where(lane0, first, zero)
        self.turned[rows : 2 * rows, :TILE] = jnp.where(lane0, zero, first)

    def incoming(self, lines, sign, twiddle, matrix, real_out=False):
        def body(r0):
            items = []
            for j in range(self.outer):
                lanes = pl.ds(j * self.inner, self.inner)
                items.append((
                    self.turned[pl.ds(r0, self.step), lanes],
                    self.turned[pl.ds(lines + r0, self.step), lanes],
                ))
            for k, pair in enumerate(small_dft(items, sign)):
                re, im = self.twist(k, pair, sign, twiddle)
                self.put(k, pl.ds(r0, self.step), 0, re)
                self.put(k, pl.ds(r0, self.step), 1, im)

        self.chunks(lines, body)
        self.multiply(lines, matrix, real_out=real_out)

    def outgoing(self, lines, sign, twiddle, matrix, real_in, write):
        self.multiply(lines, matrix, real_in=real_in)

        def body(r0):
            at = pl.ds(r0, self.step)
            write(r0, small_dft([
                self.twist(k, (self.get(k, at, 0), self.get(k, at, 1)), sign, twiddle)
                for k in range(self.outer)
            ], sign))

        self.chunks(lines, body)

    def pack_middle(self, items):
        re, im = items[0]
        lane0 = lax.broadcasted_iota(jnp.int32, im.shape, 1) == 0
        return [(re, jnp.where(lane0, items[self.outer // 2][0], im))] + items[1:]

    def write_full(self, result, pack):
        rows = self.rows

        def write(r0, items):
            at = pl.ds(r0, self.step)
            for j, (re, im) in enumerate(self.pack_middle(items) if pack else items):
                for piece in range(self.inner // rows):
                    to = j * (self.inner // rows) + piece
                    lanes = slice(piece * rows, (piece + 1) * rows)
                    result[to, at, pl.ds(0, rows)] = re[:, lanes]
                    result[to, at, pl.ds(rows, rows)] = im[:, lanes]

        return write

    def outgoing_slots(self, twiddle, matrix, kept, other):
        self.multiply(self.rows, matrix, real_in=True)
        rows, half, blocks = self.rows, self.half, self.inner // self.rows
        tall, step = rows * rows // TILE, self.step
        for h in range(rows // tall):

            def body(i, carry, h=h):
                r0 = pl.multiple_of(i * step, step)
                at = pl.ds(h * tall + r0, step)
                items = self.pack_middle(small_dft([
                    self.twist(k, (self.get(k, at, 0), self.get(k, at, 1)), -1.0, twiddle)
                    for k in range(self.outer)
                ], -1.0))
                for j, pair in enumerate(items):
                    for part, value in enumerate(pair):
                        if 2 * j >= self.outer:
                            value = exchange_lanes(value, rows)
                        to = pl.ds(h * rows + part * half, half)
                        for piece in range(blocks):
                            for side, result in enumerate((kept, other)):
                                base = piece * rows + side * half
                                result[j * blocks + piece, pl.ds(r0, step), to] = value[:, base : base + half]
                return carry

            lax.fori_loop(0, tall // step, body, 0)

    def outgoing_kept(self, twiddle, matrix, result):
        self.multiply(self.rows, matrix, real_in=True)
        rows, half, blocks = self.rows, self.half, self.inner // self.rows
        tall = rows * rows // TILE
        step = math.gcd(rows, 16)
        span = min(tall, step)
        for h in range(rows // max(tall, step)):

            def body(i, carry, h=h):
                r0 = i * step if isinstance(i, int) else pl.multiple_of(i * step, step)
                at = pl.ds(h * max(tall, step) + r0, step)
                items = self.pack_middle(small_dft([
                    self.twist(k, (self.get(k, at, 0), self.get(k, at, 1)), -1.0, twiddle)
                    for k in range(self.outer)
                ], -1.0))
                for j, pair in enumerate(items):
                    base = self.inner // 2 if 2 * j >= self.outer else 0
                    for piece in range(blocks):
                        lanes = slice(base + piece * half, base + (piece + 1) * half)
                        for part, value in enumerate(pair):
                            for sub in range(step // span):
                                group = h * (step // span) + sub
                                to = pl.ds(group * rows + part * half, half)
                                held = value[sub * span : (sub + 1) * span, lanes]
                                result[j * blocks + piece, pl.ds(r0, span), to] = held
                return carry

            if tall > step:
                lax.fori_loop(0, tall // step, body, 0)
            else:
                body(0, 0)

    def mirrored(self, blocks, mirror):
        dot = functools.partial(jnp.dot, preferred_element_type=jnp.float32)

        def flip(values, which):
            top, low = halves(jnp.concatenate(values, axis=0))
            return dot(top, mirror[which]) + dot(low, mirror[which])

        flat = [part for k in range(self.outer) for pair in blocks[k] for part in pair]
        per = 2 * len(blocks[0])
        low = flip(flat[:per], 0)
        high = flip(flat[per:], 1)
        out = []
        for k in range(self.outer):
            part, base = (low, 0) if k == 0 else (high, (self.outer - k - 1) * per)
            take = lambda i: part[(base + i) * 8 : (base + i + 1) * 8]
            out.append([(take(2 * i), -take(2 * i + 1)) for i in range(per // 2)])
        return out

    def pack_columns(self, slabs, result):
        rows, half, wide = self.rows, self.half, self.inner // 2
        blocks, groups = self.inner // rows, TILE // rows
        tall = rows // groups
        for k in range(self.outer):
            slab = slabs(k)
            for s in range(blocks):
                parts = []
                for group in range(groups):
                    for part in range(2):
                        at = part * wide + s * half
                        parts.append(slab[group * tall : (group + 1) * tall, at : at + half])
                result[k * blocks + s] = jnp.concatenate(parts, axis=1)

    def turn_columns(self, source, result):
        rows, wide, blocks = self.rows, self.inner // 2, self.inner // self.rows
        for j in range(self.outer):
            tile = source[pl.ds(j * blocks, blocks), :, :].reshape(wide, 2 * rows).T
            result[j, :, pl.ds(0, wide)] = tile[:rows]
            result[j, :, pl.ds(wide, wide)] = tile[rows:]

    def spread(self, first, second, strided, result):
        rows, fill = self.rows, TILE - 2 * self.rows
        for t in range(self.length // TILE):
            lanes = pl.ds(t * TILE, TILE)
            parts = [first[:, lanes], second[:, lanes]]
            if fill:
                parts.append(jnp.zeros((fill, TILE), jnp.float32))
            strided[pl.ds(t * TILE, TILE), :] = jnp.concatenate(parts, axis=0).T
        for k in range(self.outer):
            slab = strided[pl.ds(k, self.inner, stride=self.outer), :].T
            result[k] = slab[: 2 * rows, :]

    def collect(self, slabs, strided, results):
        rows = self.rows
        for k in range(self.outer):
            slab = slabs(k)
            fill = TILE - slab.shape[0]
            if fill:
                slab = jnp.concatenate([slab, jnp.zeros((fill, self.inner), jnp.float32)], axis=0)
            strided[pl.ds(k, self.inner, stride=self.outer), :] = slab.T
        for t in range(self.length // TILE):
            block = strided[pl.ds(t * TILE, TILE), :].T
            for i, result in enumerate(results):
                result[:, pl.ds(t * TILE, TILE)] = block[i * rows : (i + 1) * rows, :]


def signed_waves(position, count):
    signed = jnp.where(position < count // 2, position, position - count)
    waves = 4.0 * signed.astype(jnp.float32) / count
    return waves, jnp.where(position == count // 2, jnp.float32(0.0), waves)


def first_waves(piece, k):
    lanes = lax.broadcasted_iota(jnp.int32, (1, piece.inner), 1)
    return signed_waves(piece.outer * lanes + k, piece.length)


def inverse_denominator(wave_first, wave_second):
    square = wave_first * wave_first + wave_second * wave_second
    return 1.0 / (1.0 + time_step * (square * square - square))


def second_wave(piece, position):
    shape = (position.shape[0], piece.inner)
    return jnp.broadcast_to(signed_waves(position, piece.length)[0], shape)


def row_index(count, width):
    return lax.broadcasted_iota(jnp.int32, (count, width), 0)


def exchange_lanes(value, rows):
    half, wide = rows // 2, value.shape[1]
    line = lax.broadcasted_iota(jnp.int32, value.shape, 1) % rows
    up, down = pltpu.roll(value, half, 1), pltpu.roll(value, wide - half, 1)
    return jnp.where(line == 0, down, jnp.where(line == half, up, value))


def exchange_rows(held, first, second, swapped):
    at, also = first, second
    one, other = held[at], held[also]
    top = lax.broadcasted_iota(jnp.int32, one.shape, one.ndim - 2) == 0
    moved = top if swapped is None else jnp.logical_and(top, swapped)
    held[at] = jnp.where(moved, other, one)
    held[also] = jnp.where(moved, one, other)


class Links:
    def __init__(self, devices, fast):
        self.devices, self.fast = devices, fast
        self.device = lax.axis_index(axes[0]) * fast + lax.axis_index(axes[1])

    def partner(self, i):
        total, bit = 0, 1
        while bit < self.devices:
            total += bit * lax.rem(lax.div(self.device, bit) + lax.div(i, bit), 2)
            bit *= 2
        return total

    def send(self, source, target, sems):
        send_sem, recv_sem, own_sem = sems

        def go(i, carry):
            peer = self.partner(self.devices - i)
            pltpu.make_async_remote_copy(
                src_ref=source(peer),
                dst_ref=target(self.device),
                send_sem=send_sem,
                recv_sem=recv_sem,
                device_id=(lax.div(peer, self.fast), lax.rem(peer, self.fast)),
                device_id_type=pl.DeviceIdType.MESH,
            ).start()
            return carry

        lax.fori_loop(1, self.devices, go, 0)
        pltpu.make_async_copy(source(self.device), target(self.device), own_sem).start()

    def whole(self, source, target, sems):
        others = pl.ds(0, self.devices - 1)
        return pltpu.make_async_remote_copy(
            src_ref=source(others),
            dst_ref=target(others),
            send_sem=sems[0],
            recv_sem=sems[1],
            device_id=(0, 0),
            device_id_type=pl.DeviceIdType.MESH,
        )

    def receive(self, source, target, sems):
        pltpu.make_async_copy(source(self.device), target(self.device), sems[2]).wait()
        self.whole(source, target, sems).wait_recv()

    def sent(self, source, target, sems):
        self.whole(source, target, sems).wait_send()


def start_kernel(length, rows, field, target, out, both_p, *scratch):
    piece = Pieces(length, rows)
    piece.spread(field, target, scratch[0], both_p)
    piece.pack_columns(lambda k: both_p[k, pl.ds(0, rows), :], out)


def slope_second_kernel(length, rows, field_p, twiddle, out_matrix, in_matrix, kept, result, *scratch):
    piece = Pieces(length, rows, *scratch)

    def body(r0):
        at = pl.ds(r0, piece.step)
        for k in range(piece.outer):
            piece.put(k, at, 0, field_p[k, at, :])

    piece.chunks(rows, body)
    for j in range(piece.outer):
        piece.clear_other(j)

    def write(r0, items):
        for j, (re, im) in enumerate(items):
            at, wide = piece.kept_lanes(j)
            base = at - j * piece.inner
            position = j * piece.inner + kept[:, base : base + wide]
            slope = 2.0 * signed_waves(position, length)[1]
            piece.turned[pl.ds(r0, piece.step), pl.ds(at, wide)] = -slope * im[:, base : base + wide]
            piece.turned[pl.ds(rows + r0, piece.step), pl.ds(at, wide)] = slope * re[:, base : base + wide]

    piece.outgoing(rows, -1.0, twiddle, out_matrix, True, write)
    piece.incoming(rows, 1.0, twiddle, in_matrix, real_out=True)
    result[...] = piece.z[:, :, : piece.inner]


def spread_kernel(length, rows, forcing, result, strided):
    Pieces(length, rows).spread(forcing.at[0], forcing.at[1], strided, result)


def collect_kernel(length, rows, slabs, result, strided):
    piece = Pieces(length, rows)
    piece.collect(lambda k: slabs[k], strided, [result.at[i] for i in range(result.shape[0])])


def weight_of(device, r0, step, inner):
    alone = (row_index(step, inner) + r0 + device) == 0
    return jnp.where(alone, jnp.float32(1.0), jnp.float32(2.0))


def slope_first_kernel(length, rows, source, in_twiddle, in_matrix, out_twiddle, out_matrix, out, *scratch):
    piece = Pieces(length, rows, *scratch)
    half = piece.half
    piece.turn_lines(source)
    piece.incoming(half, -1.0, in_twiddle, in_matrix)

    def body(r0):
        at = pl.ds(r0, piece.step)
        for k in range(piece.outer):
            re, im = piece.get(k, at, 0), piece.get(k, at, 1)
            scale = first_waves(piece, k)[1]
            piece.put(k, at, 0, -scale * im)
            piece.put(k, at, 1, scale * re)

    piece.chunks(half, body)
    piece.outgoing(half, 1.0, out_twiddle, out_matrix, False, piece.write_full(out, False))


def edge_inverses(piece, k):
    wave_first = first_waves(piece, k)[0]
    middle = jnp.full((1, 1), piece.length // 2, jnp.int32)
    zero = jnp.zeros((1, 1), jnp.int32)
    return [inverse_denominator(wave_first, signed_waves(p, piece.length)[0]) for p in (zero, middle)]


def next_kernel(length, rows, device_ref, source, forcing, in_twiddle, in_matrix, out_twiddle, out_matrix, mirror, out, *scratch):
    device = device_ref[0]
    piece = Pieces(length, rows, *scratch)
    half, step, inner = piece.half, piece.step, piece.inner
    late = device >= (length // rows) // 2
    piece.turn_lines(source)
    piece.incoming(half, -1.0, in_twiddle, in_matrix)

    def body(r0):
        at, also = pl.ds(r0, step), pl.ds(half + r0, step)
        index = row_index(step, 1) + r0
        low_wave = second_wave(piece, device * rows + index)
        high_wave = second_wave(piece, device * rows + half + index)
        moved = jnp.logical_and(row_index(step, inner) + r0 == 0, late)
        weight = weight_of(device, r0, step, inner)
        for k in range(piece.outer):
            wave_first = first_waves(piece, k)[0]
            low = inverse_denominator(wave_first, low_wave)
            high = inverse_denominator(wave_first, high_wave)
            for part in range(2):
                own = weight * piece.get(k, at, part)
                f_low = time_step * forcing[k, pl.ds(part * rows + r0, step), :]
                f_high = time_step * forcing[k, pl.ds(part * rows + half + r0, step), :]
                piece.put(k, at, part, (f_low + jnp.where(moved, 0.0, own)) * low)
                piece.put(k, also, part, (f_high + jnp.where(moved, own, 0.0)) * high)

    piece.chunks(half, body)

    @pl.when(device == 0)
    def _():
        at = pl.ds(0, 8)
        blocks = []
        for k in range(piece.outer):
            own = tuple(piece.get(k, at, part) for part in range(2))
            full = tuple(
                own[part] + time_step * forcing[k, pl.ds(part * rows, 8), :] for part in range(2)
            )
            blocks.append([own, full])
        flipped = piece.mirrored(blocks, mirror)
        rest = pl.ds(0, 16)
        row0 = row_index(16, inner) == 0
        for k in range(piece.outer):
            zero, middle = edge_inverses(piece, k)
            for part in range(2):
                own, full = blocks[k][0][part], blocks[k][1][part]
                own_c, full_c = flipped[k][0][part], flipped[k][1][part]
                value = 0.5 * ((full + full_c) * zero + (own - own_c) * middle)
                replace(piece, k, part, value)

    piece.outgoing(rows, 1.0, out_twiddle, out_matrix, False, piece.write_full(out, False))


def replace(piece, k, part, value):
    lanes = pl.ds(part * piece.inner, piece.inner)
    row0 = row_index(16, piece.inner) == 0
    value = jnp.concatenate([value, value], axis=0)
    for held, new in zip((piece.top, piece.low), halves(value)):
        old = held[k, pl.ds(0, 16), lanes].astype(jnp.float32)
        held[k, pl.ds(0, 16), lanes] = jnp.where(row0, new.astype(jnp.float32), old).astype(jnp.bfloat16)


def misfit_kernel(length, rows, device_ref, source, in_twiddle, in_matrix, out_twiddle, out_matrix, mirror, out, full, total_out, *scratch):
    device = device_ref[0]
    piece = Pieces(length, rows, *scratch)
    half, step, inner = piece.half, piece.step, piece.inner
    late = device >= (length // rows) // 2
    piece.turn_full(source)
    piece.incoming(rows, -1.0, in_twiddle, in_matrix)

    def body(r0):
        at, also = pl.ds(r0, step), pl.ds(half + r0, step)
        index = row_index(step, 1) + r0
        low_wave = second_wave(piece, device * rows + index)
        high_wave = second_wave(piece, device * rows + half + index)
        moved = jnp.logical_and(row_index(step, inner) + r0 == 0, late)
        weight = weight_of(device, r0, step, inner)
        for k in range(piece.outer):
            wave_first = first_waves(piece, k)[0]
            low = time_step * inverse_denominator(wave_first, low_wave)
            high = time_step * inverse_denominator(wave_first, high_wave)
            for part in range(2):
                low_value = piece.get(k, at, part) * low
                high_value = piece.get(k, also, part) * high
                full[k, pl.ds(part * rows + r0, step), :] = low_value
                full[k, pl.ds(part * rows + half + r0, step), :] = high_value
                own = jnp.where(moved, high_value, low_value)
                piece.put(k, at, part, weight * own)

    piece.chunks(half, body)

    @pl.when(device == 0)
    def _():
        at = pl.ds(0, 8)
        blocks = [[(piece.get(k, at, 0), piece.get(k, at, 1))] for k in range(piece.outer)]
        flipped = piece.mirrored(blocks, mirror)
        row0 = row_index(8, inner) == 0
        for k in range(piece.outer):
            zero, middle = edge_inverses(piece, k)
            for part in range(2):
                own, own_c = blocks[k][0][part], flipped[k][0][part]
                first = (0.5 * time_step) * (own + own_c) * zero
                value = first + (0.5 * time_step) * (own - own_c) * middle
                at_full = pl.ds(part * rows, 8)
                full[k, at_full, :] = jnp.where(row0, first, full[k, at_full, :])
                replace(piece, k, part, value)

    piece.outgoing(half, 1.0, out_twiddle, out_matrix, False, piece.write_full(out, False))
    total_out[...] = jnp.sum(source[:, pl.ds(rows, 8), :], axis=0)


def nonlinear_kernel(length, rows, source, both_p, second, twiddle, out_matrix, out, first, *scratch):
    piece = Pieces(length, rows, *scratch)
    piece.turn_columns(source, first)

    def body(r0):
        at = pl.ds(r0, piece.step)
        for k in range(piece.outer):
            one, other = first[k, at, :], second[k, at, :]
            piece.put(k, at, 0, both_p[k, at, :] - (0.5 * time_step) * (one * one + other * other))

    piece.chunks(rows, body)
    piece.outgoing_kept(twiddle, out_matrix, out)


def joint_kernel(length, rows, source, first, second, twiddle, in_matrix, out, value_out, second_out, *scratch):
    piece = Pieces(length, rows, *scratch)
    piece.turn_kept(source)
    piece.unpack_middle()
    piece.incoming(rows, 1.0, twiddle, in_matrix, real_out=True)
    lanes = pl.ds(0, piece.inner)

    def body(r0):
        at = pl.ds(r0, piece.step)
        for k in range(piece.outer):
            value = piece.get(k, at, 0)
            value_out[k, at, :] = (1.0 / time_step) * value
            second_out[k, at, :] = value * second[k, at, :]
            piece.z[k, at, lanes] = value * first[k, at, :]

    piece.chunks(rows, body)
    piece.pack_columns(lambda k: piece.z[k, pl.ds(0, rows), lanes], out)


def residual_kernel(length, rows, source, both_p, twiddle, in_matrix, out_matrix, out, field_out, *scratch):
    piece = Pieces(length, rows, *scratch[:4])
    strided, total = scratch[4:]
    piece.turn_full(source)
    piece.unpack_middle()
    piece.incoming(rows, 1.0, twiddle, in_matrix, real_out=True)
    piece.collect(lambda k: piece.get(k, pl.ds(0, rows), 0), strided, [field_out])
    total[...] = jnp.zeros_like(total)

    def body(r0):
        at = pl.ds(r0, piece.step)
        for k in range(piece.outer):
            residual = piece.get(k, at, 0) - both_p[k, pl.ds(rows + r0, piece.step), :]
            total[...] += residual * residual
            piece.put(k, at, 0, residual)

    piece.chunks(rows, body)
    piece.outgoing(rows, -1.0, twiddle, out_matrix, True, piece.write_full(out, True))
    value = 0.5 * jnp.sum(total[...])
    out[:, pl.ds(rows, 8), :] = jnp.full((out.shape[0], 8, 2 * rows), value, jnp.float32)


def last_kernel(length, rows, source, value, second, field_out, strided, first):
    piece = Pieces(length, rows)
    piece.turn_columns(source, first)
    piece.collect(lambda k: first[k] + value[k] + second[k], strided, [field_out])


def slots_of(device, late, index, rows, half, other):
    line = half + index if other else index
    special = jnp.where(late, 0, half) if other else jnp.where(late, half, 0)
    return device * rows + jnp.where(index == 0, special, line)


def step_kernel(length, rows, devices, fast, inputs, outs, box):
    links = Links(devices, fast)
    device, half = links.device, rows // 2
    late = device >= devices // 2
    copies, sems = box.copies, box.sems
    piece = Pieces(length, rows, box.turned, box.top, box.low, box.z)
    step, inner, outer = piece.step, piece.inner, piece.outer
    both_p, forcing_p, full = box.both_p, box.forcing_p, box.full
    first, second, value = box.first, box.second, box.value
    strided, total = box.strided, box.total

    loads = [
        pltpu.make_async_copy(ref, held, copies.at[i])
        for i, (ref, held) in enumerate(zip(inputs.refs, inputs.held))
    ]
    for copy in loads:
        copy.start()
    waiting = iter(loads)

    def load(count):
        for i in range(count):
            next(waiting).wait()

    at_all = lambda ref: lambda e: ref.at[e]
    at_lines = lambda ref, base, count: lambda e: ref.at[e, pl.ds(base, count)]
    order = []

    def send(source, target):
        i = len(order)
        order.append((source, target, (sems.at[i, 0], sems.at[i, 1], sems.at[i, 2])))
        links.send(*order[-1])
        return order[-1]

    def receive(*moves):
        for move in moves:
            links.receive(*move)

    def send_all(source, target):
        return send(at_all(source), at_all(target))

    tables = inputs.twiddles
    tw_natural, tw_kept, tw_lines = (tables.at[i] for i in range(3))
    forward, backward, lines_in = inputs.forward, inputs.backward, inputs.lines
    kept_out, kept_in, kept, mirror = inputs.kept_out, inputs.kept_in, inputs.kept, inputs.mirror

    def slope_first(source, out):
        slope_first_kernel(
            length, rows, source, tw_lines, lines_in, tw_natural, backward, out,
            piece.turned, piece.top, piece.low, piece.z,
        )

    def slope_second(source, out):
        slope_second_kernel(
            length, rows, source, tw_kept, kept_out, kept_in, kept, out,
            piece.turned, piece.top, piece.low, piece.z,
        )

    load(2)
    piece.spread(inputs.field, inputs.target, strided, both_p)
    piece.pack_columns(lambda k: both_p[k, pl.ds(0, rows), :], box.s_field)
    m_field = send_all(box.s_field, box.r_field)

    load(4)
    slope_second(both_p, second)
    load(1)
    piece.spread(inputs.forcing.at[0], inputs.forcing.at[1], strided, forcing_p)
    for k in range(outer):
        for part in range(2):
            at, also = (k, pl.ds(part * rows, 8)), (k, pl.ds(part * rows + half, 8))
            exchange_rows(forcing_p, at, also, late)
    load(4)

    def rest(r0):
        at = pl.ds(r0, step)
        wave = second_wave(piece, slots_of(device, late, row_index(step, 1) + r0, rows, half, True))
        for k in range(outer):
            scale = time_step * inverse_denominator(first_waves(piece, k)[0], wave)
            for part in range(2):
                piece.put(k, at, part, scale * forcing_p[k, pl.ds(part * rows + half + r0, step), :])

    piece.chunks(half, rest)
    piece.outgoing(half, 1.0, tw_natural, backward, False, piece.write_full(box.s_rest, False))

    def send_rest(base, count):
        target = at_lines(box.r_next, half + base, count)
        return send(at_lines(box.s_rest, base, count), target)

    quarter = half // 4
    m_rest0 = send_rest(0, quarter)

    receive(m_field)
    slope_first(box.r_field, box.s_slope)
    m_slope = send_all(box.s_slope, box.r_slope)
    m_rest1 = send_rest(quarter, quarter)

    receive(m_slope)
    nonlinear_kernel(
        length, rows, box.r_slope, both_p, second, tw_kept, kept_out, box.s_sum, first,
        piece.turned, piece.top, piece.low, piece.z,
    )
    m_sum = send_all(box.s_sum, box.r_sum)
    m_rest2 = send_rest(2 * quarter, half - 2 * quarter)

    receive(m_sum)
    piece.turn_lines(box.r_sum)
    piece.incoming(half, -1.0, tw_lines, lines_in)

    def divide(r0):
        at = pl.ds(r0, step)
        wave = second_wave(piece, slots_of(device, late, row_index(step, 1) + r0, rows, half, False))
        weight = weight_of(device, r0, step, inner)
        for k in range(outer):
            scale = inverse_denominator(first_waves(piece, k)[0], wave)
            for part in range(2):
                forced = time_step * forcing_p[k, pl.ds(part * rows + r0, step), :]
                piece.put(k, at, part, (weight * piece.get(k, at, part) + forced) * scale)

    piece.chunks(half, divide)

    @pl.when(device == 0)
    def _():
        at = pl.ds(0, 8)
        blocks = []
        for k in range(outer):
            own = tuple(piece.get(k, at, part) for part in range(2))
            joined = tuple(own[part] + time_step * forcing_p[k, pl.ds(part * rows, 8), :] for part in range(2))
            blocks.append([own, joined])
        flipped = piece.mirrored(blocks, mirror)
        for k in range(outer):
            zero, middle = edge_inverses(piece, k)
            for part in range(2):
                own, joined = blocks[k][0][part], blocks[k][1][part]
                own_c, joined_c = flipped[k][0][part], flipped[k][1][part]
                replace(piece, k, part, 0.5 * ((joined + joined_c) * zero + (own - own_c) * middle))

    piece.outgoing(half, 1.0, tw_natural, backward, False, piece.write_full(box.s_next, False))
    m_next = send(at_all(box.s_next), at_lines(box.r_next, 0, half))

    receive(m_rest0, m_rest1, m_rest2, m_next)
    turned_late = pl.ds(devices // 2, devices // 2)
    exchange_rows(box.r_next, (turned_late, pl.ds(0, 8)), (turned_late, pl.ds(half, 8)), None)
    piece.turn_full(box.r_next)
    piece.unpack_middle()
    piece.incoming(rows, 1.0, tw_natural, backward, real_out=True)
    total[...] = jnp.zeros_like(total)
    lanes = pl.ds(0, inner)

    def misfit(r0):
        at = pl.ds(r0, step)
        for k in range(outer):
            now = piece.get(k, at, 0)
            value[k, at, :] = now
            residual = now - both_p[k, pl.ds(rows + r0, step), :]
            total[...] += residual * residual
            piece.put(k, at, 0, residual)

    piece.chunks(rows, misfit)
    piece.outgoing_slots(tw_natural, forward, box.s_kept, box.s_other)
    m_kept = send_all(box.s_kept, box.r_kept)
    count = rows * rows // TILE
    eighth = count // 4

    def send_other(base, size):
        return send(at_lines(box.s_other, base, size), at_lines(box.r_other, base, size))

    m_other0 = send_other(0, eighth)
    box.s_total[...] = jnp.full(box.s_total.shape, 0.5 * jnp.sum(total[...]), jnp.float32)
    m_total = send(lambda e: box.s_total.at[e], lambda e: box.r_total.at[e])
    stores = []

    def store(ref, out):
        stores.append(pltpu.make_async_copy(ref, out, copies.at[len(loads) + len(stores)]))
        stores[-1].start()

    piece.collect(lambda k: value[k], strided, [box.o_next])
    store(box.o_next, outs.next)

    receive(m_kept)
    piece.turn_lines(box.r_kept)
    piece.incoming(half, -1.0, tw_lines, lines_in)

    def adjoint(r0):
        at = pl.ds(r0, step)
        wave = second_wave(piece, slots_of(device, late, row_index(step, 1) + r0, rows, half, False))
        weight = weight_of(device, r0, step, inner)
        for k in range(outer):
            scale = time_step * inverse_denominator(first_waves(piece, k)[0], wave)
            for part in range(2):
                own = piece.get(k, at, part) * scale
                full[k, pl.ds(part * rows + r0, step), :] = own
                piece.put(k, at, part, weight * own)

    piece.chunks(half, adjoint)

    @pl.when(device == 0)
    def _():
        at = pl.ds(0, 8)
        blocks = [[(piece.get(k, at, 0), piece.get(k, at, 1))] for k in range(outer)]
        flipped = piece.mirrored(blocks, mirror)
        row0 = row_index(8, inner) == 0
        for k in range(outer):
            zero, middle = edge_inverses(piece, k)
            for part in range(2):
                own, own_c = blocks[k][0][part], flipped[k][0][part]
                line = (0.5 * time_step) * (own + own_c) * zero
                at_full = pl.ds(part * rows, 8)
                full[k, at_full, :] = jnp.where(row0, line, full[k, at_full, :])
                replace(piece, k, part, line + (0.5 * time_step) * (own - own_c) * middle)

    piece.outgoing(half, 1.0, tw_natural, backward, False, piece.write_full(box.s_back, False))
    m_back = send_all(box.s_back, box.r_back)
    m_other1 = send_other(eighth, eighth)

    receive(m_back)
    joint_kernel(
        length, rows, box.r_back, first, second, tw_kept, kept_in, box.s_product, value, box.product,
        piece.turned, piece.top, piece.low, piece.z,
    )
    m_product = send_all(box.s_product, box.r_product)
    m_other2 = send_other(2 * eighth, count - 2 * eighth)

    slope_second(box.product, second)
    for k in range(outer):
        value[k] = value[k] + second[k]

    receive(m_product)
    slope_first(box.r_product, box.s_last)
    m_last = send_all(box.s_last, box.r_last)

    receive(m_other0, m_other1, m_other2, m_total)
    piece.turn_lines(box.r_other)
    piece.incoming(half, -1.0, tw_lines, lines_in)

    def others(r0):
        at = pl.ds(r0, step)
        wave = second_wave(piece, slots_of(device, late, row_index(step, 1) + r0, rows, half, True))
        for k in range(outer):
            scale = time_step * inverse_denominator(first_waves(piece, k)[0], wave)
            for part in range(2):
                full[k, pl.ds(part * rows + half + r0, step), :] = piece.get(k, at, part) * scale

    piece.chunks(half, others)
    for k in range(outer):
        for part in range(2):
            at, also = (k, pl.ds(part * rows, 8)), (k, pl.ds(part * rows + half, 8))
            exchange_rows(full, at, also, late)
    piece.collect(lambda k: full[k], strided, [box.o_forcing.at[i] for i in range(2)])
    store(box.o_forcing, outs.forcing)
    outs.total[...] = jnp.sum(box.r_total[...], axis=0)

    receive(m_last)
    piece.turn_columns(box.r_last, first)
    piece.collect(lambda k: first[k] + value[k], strided, [box.o_field])
    store(box.o_field, outs.field)
    for move in order:
        links.sent(*move)
    for copy in stores:
        copy.wait()


messages = 15


def joined_step(field, target, forcing, devices, fast, rows, length):
    outer, inner = split_length(length)
    half, step = rows // 2, math.gcd(rows // 2, 16)
    natural, kept, lines = orders(length, rows)
    matrix = lambda *args: matrix_table(length, *args)
    tables = dict(
        field=field, target=target,
        twiddles=np.stack([twiddle_table(length, o) for o in (natural, kept, lines)]),
        kept=kept[None, :].astype(np.int32),
        kept_out=matrix(-1.0, natural, kept)[:, :inner],
        kept_in=matrix(1.0, kept, natural)[:, :, :inner],
        forcing=forcing,
        backward=matrix(1.0, natural, natural),
        lines=matrix(-1.0, lines, natural),
        forward=matrix(-1.0, natural, natural),
        mirror=mirror_table(length),
    )
    operands = [jnp.asarray(table) for table in tables.values()]
    float32 = jnp.float32
    held = lambda *dims: pltpu.VMEM(dims, float32)
    packed, lined = held(devices, rows * rows // TILE, TILE), held(devices, half, 2 * rows)
    pair, one = held(outer, 2 * rows, inner), held(outer, rows, inner)
    plain, small = held(rows, length), held(devices, 8, TILE)
    halved = pltpu.VMEM((outer, rows, 2 * inner), jnp.bfloat16)
    shapes = dict(
        turned=held(2 * rows, length), top=halved, low=halved, z=held(outer, rows, 2 * inner),
        strided=held(length, TILE), total=held(step, inner),
        both_p=pair, forcing_p=pair, full=pair, first=one, second=one, value=one, product=one,
        o_next=plain, o_field=plain, o_forcing=held(2, rows, length),
        s_field=packed, r_field=packed, s_slope=lined, r_slope=lined, s_sum=packed, r_sum=packed,
        s_rest=lined, s_next=lined, r_next=held(devices, rows, 2 * rows),
        s_kept=packed, r_kept=packed, s_other=packed, r_other=packed, s_total=small, r_total=small,
        s_back=lined, r_back=lined, s_product=packed, r_product=packed, s_last=lined, r_last=lined,
        copies=pltpu.SemaphoreType.DMA((len(operands) + 3,)),
        sems=pltpu.SemaphoreType.DMA((messages, 3)),
    )
    inputs = [pltpu.VMEM(operand.shape, operand.dtype) for operand in operands]

    def body(*refs):
        a, b = len(operands), len(operands) + 4
        c = b + len(operands)
        given = SimpleNamespace(refs=refs[:a], held=refs[b:c], **dict(zip(tables, refs[b:c])))
        outs = SimpleNamespace(next=refs[a], field=refs[a + 1], forcing=refs[a + 2], total=refs[a + 3])
        step_kernel(length, rows, devices, fast, given, outs, SimpleNamespace(**dict(zip(shapes, refs[c:]))))

    anywhere = pl.BlockSpec(memory_space=pl.ANY)
    shape = lambda *dims: jax.ShapeDtypeStruct(dims, float32)
    next_field, field_grad, forcing_grad, total = pl.pallas_call(
        body,
        out_shape=(shape(rows, length), shape(rows, length), shape(2, rows, length), shape(8, TILE)),
        in_specs=[anywhere] * len(operands),
        out_specs=(anywhere, anywhere, anywhere, pl.BlockSpec(memory_space=pltpu.VMEM)),
        scratch_shapes=inputs + list(shapes.values()),
        compiler_params=pltpu.CompilerParams(vmem_limit_bytes=56 * 2**20, has_side_effects=True),
        cost_estimate=pl.CostEstimate(flops=6 * 10**10, bytes_accessed=4 * 2**20, transcendentals=0),
    )(*operands)
    return next_field, total[0, 0], field_grad, forcing_grad


def member_step(device, field, target, forcing_p, devices, rows, length):
    outer, inner = split_length(length)
    half = rows // 2
    float32 = jnp.float32
    shape = lambda *dims: jax.ShapeDtypeStruct(dims, float32)
    kept_blocks = shape(devices, rows * rows // TILE, TILE)
    half_blocks = shape(devices, half, 2 * rows)
    blocks = shape(devices, rows, 2 * rows)
    longer = shape(devices, rows + 8, 2 * rows)
    pair, one = shape(outer, 2 * rows, inner), shape(outer, rows, inner)
    plain = shape(rows, length)
    step = math.gcd(half, 16)
    base = [
        pltpu.VMEM((2 * rows, length), float32),
        pltpu.VMEM((outer, rows, 2 * inner), jnp.bfloat16),
        pltpu.VMEM((outer, rows, 2 * inner), jnp.bfloat16),
        pltpu.VMEM((outer, rows, 2 * inner), float32),
    ]
    strided = pltpu.VMEM((length, TILE), float32)
    total = pltpu.VMEM((step, inner), float32)
    vmem = pl.BlockSpec(memory_space=pltpu.VMEM)
    smem = pl.BlockSpec(memory_space=pltpu.SMEM)

    natural, kept, lines = orders(length, rows)
    tw_natural, tw_kept, tw_lines = [jnp.asarray(twiddle_table(length, o)) for o in (natural, kept, lines)]
    matrix = lambda *args: matrix_table(length, *args)
    forward, backward = matrix(-1.0, natural, natural), matrix(1.0, natural, natural)
    kept_out, kept_in = matrix(-1.0, natural, kept)[:, :inner], matrix(1.0, kept, natural)[:, :, :inner]
    lines_in = matrix(-1.0, lines, natural)
    mirror = jnp.asarray(mirror_table(length))
    kept_lane = jnp.asarray(kept[None, :].astype(np.int32))

    def call(body, outs, scratch, *operands):
        return pl.pallas_call(
            functools.partial(body, length, rows),
            out_shape=outs,
            in_specs=[smem if operand is device else vmem for operand in operands],
            out_specs=jax.tree.map(lambda leaf: vmem, outs),
            scratch_shapes=scratch,
            compiler_params=pltpu.CompilerParams(vmem_limit_bytes=20 * 2**20),
            cost_estimate=pl.CostEstimate(flops=6 * 10**9, bytes_accessed=4 * 2**20, transcendentals=0),
        )(*operands)

    def move(value):
        return lax.all_to_all(value, axes, split_axis=0, concat_axis=0, tiled=True)

    spectral_tables = (tw_lines, lines_in, tw_natural, backward)
    slope_tables = (tw_kept, kept_out, kept_in, kept_lane)
    sent, both_p = call(start_kernel, (kept_blocks, pair), [strided], field, target)
    second = call(slope_second_kernel, one, base, both_p, *slope_tables)
    sent = call(slope_first_kernel, half_blocks, base, move(sent), *spectral_tables)
    sent, first = call(nonlinear_kernel, (kept_blocks, one), base, move(sent), both_p, second, tw_kept, kept_out)
    sent = call(next_kernel, blocks, base, device, move(sent), forcing_p, *spectral_tables, mirror)
    sent, next_field = call(
        residual_kernel, (longer, plain), base + [strided, total],
        move(sent), both_p, tw_natural, backward, forward,
    )
    sent, full, sums = call(
        misfit_kernel, (half_blocks, pair, shape(8, 2 * rows)), base,
        device, move(sent), tw_natural, forward, tw_natural, backward, mirror,
    )
    sent, value, product = call(
        joint_kernel, (kept_blocks, one, one), base, move(sent), first, second, tw_kept, kept_in
    )
    second_part = call(slope_second_kernel, one, base, product, *slope_tables)
    sent = call(slope_first_kernel, half_blocks, base, move(sent), *spectral_tables)
    field_grad = call(
        last_kernel, plain, [strided, pltpu.VMEM((outer, rows, inner), float32)], move(sent), value, second_part
    )
    return next_field, sums[0, 0], field_grad, full


def per_device(devices, fast, initial_field, target_field, forcing):
    members, rows, length = initial_field.shape
    device = lax.axis_index(axes).astype(jnp.int32).reshape(1)
    outer, inner = split_length(length)
    vmem = pl.BlockSpec(memory_space=pltpu.VMEM)
    strided = pltpu.VMEM((length, TILE), jnp.float32)

    def reorder(body, shape, operand):
        return pl.pallas_call(
            functools.partial(body, length, rows),
            out_shape=jax.ShapeDtypeStruct(shape, jnp.float32),
            in_specs=[vmem],
            out_specs=vmem,
            scratch_shapes=[strided],
        )(operand)

    if rows * rows % (TILE * 32) == 0 and TILE % rows == 0:
        results = [
            joined_step(initial_field[m], target_field[m], forcing, devices, fast, rows, length)
            for m in range(members)
        ]
        next_field = jnp.stack([one[0] for one in results])
        objective = sum(one[1] for one in results) / (members * length * length)
        field_grad = jnp.stack([one[2] for one in results])
        return (next_field, objective, field_grad, sum(one[3] for one in results))
    forcing_p = reorder(spread_kernel, (outer, 2 * rows, inner), forcing)
    results = [
        member_step(device, initial_field[m], target_field[m], forcing_p, devices, rows, length)
        for m in range(members)
    ]
    next_field = jnp.stack([one[0] for one in results])
    objective = sum(one[1] for one in results) / (members * length * length)
    field_grad = jnp.stack([one[2] for one in results])
    forcing_grad = reorder(collect_kernel, (2, rows, length), sum(one[3] for one in results))
    return (next_field, objective, field_grad, forcing_grad)


def solution(mesh):
    devices = mesh.shape["px"] * mesh.shape["py"]
    spec = P(None, axes, None)
    return jax.shard_map(
        functools.partial(per_device, devices, mesh.shape["py"]),
        mesh=mesh,
        in_specs=(spec, spec, spec),
        out_specs=(spec, P(), spec, spec),
        check_vma=False,
    )
```

```python
import functools
import math
from types import SimpleNamespace

import jax
import jax.numpy as jnp
import numpy as np
from jax import lax
from jax.experimental import pallas as pl
from jax.experimental.pallas import tpu as pltpu
from jax.sharding import PartitionSpec as P

time_step = 0.25
axes = ("px", "py")
TILE = 128


def split_length(length):
    inner = 256 if length % 256 == 0 else TILE
    return (length // inner, inner)


def small_dft(items, sign):
    count = len(items)
    if count == 1:
        return items
    evens = small_dft(items[0::2], sign)
    odds = small_dft(items[1::2], sign)
    low, high = [], []
    for k in range(count // 2):
        odd_re, odd_im = odds[k]
        if 4 * k == count:
            odd_re, odd_im = (-odd_im, odd_re) if sign > 0 else (odd_im, -odd_re)
        elif k:
            c = math.cos(2.0 * math.pi * k / count)
            s = sign * math.sin(2.0 * math.pi * k / count)
            if abs(abs(c) - abs(s)) < 1e-12:
                sc, ss = math.copysign(1.0, c), math.copysign(1.0, s)
                odd_re, odd_im = (
                    c * (odd_re - sc * ss * odd_im),
                    c * (odd_im + sc * ss * odd_re),
                )
            else:
                odd_re, odd_im = (c * odd_re - s * odd_im, c * odd_im + s * odd_re)
        even_re, even_im = evens[k]
        low.append((even_re + odd_re, even_im + odd_im))
        high.append((even_re - odd_re, even_im - odd_im))
    return low + high


def halves(value):
    top = value.astype(jnp.bfloat16)
    return top, (value - top.astype(jnp.float32)).astype(jnp.bfloat16)


def orders(length, rows):
    inner = split_length(length)[1]
    half = rows // 2
    lane = np.arange(inner)
    natural = lane
    local = lane % (inner // 2)
    line = local % half
    kept = rows * (local // half) + np.where((lane >= inner // 2) & (line == 0), half, line)
    groups = TILE // rows
    tall = rows // groups
    within = lane % (inner // groups)
    lines = rows * (within // tall) + tall * (lane // (inner // groups)) + within % tall
    return natural, kept, lines


def twiddle_table(length, order):
    outer = split_length(length)[0]
    angle = 2.0 * np.pi * np.outer(np.arange(outer), order) / length
    return (np.stack([np.cos(angle), np.sin(angle)]) / math.sqrt(length)).astype(np.float32)


def matrix_table(length, sign, left, right):
    inner = split_length(length)[1]
    angle = 2.0 * np.pi * (np.outer(left, right) % inner) / inner
    c, s = np.cos(angle), np.sin(angle)
    full = np.block([[c, sign * s], [-sign * s, c]])
    top = full.astype(jnp.bfloat16)
    return np.stack([top, (full - top.astype(np.float64)).astype(jnp.bfloat16)])


def mirror_table(length):
    inner = split_length(length)[1]
    lane = np.arange(inner)
    both = np.zeros((2, inner, inner))
    both[0, (inner - lane) % inner, lane] = 1.0
    both[1, inner - 1 - lane, lane] = 1.0
    return both.astype(jnp.bfloat16)


class Pieces:
    def __init__(self, length, rows, turned=None, top=None, low=None, grid_out=None):
        self.length, self.rows, self.half = length, rows, rows // 2
        self.outer, self.inner = split_length(length)
        self.turned, self.top, self.low, self.z = turned, top, low, grid_out
        self.step = math.gcd(rows // 2, 16)

    def chunks(self, lines, body):
        def run(i, carry):
            body(pl.multiple_of(i * self.step, self.step))
            return carry

        lax.fori_loop(0, lines // self.step, run, 0)

    def put(self, k, at, part, value):
        lanes = pl.ds(part * self.inner, self.inner)
        top, low = halves(value)
        self.top[k, at, lanes] = top
        self.low[k, at, lanes] = low

    def get(self, k, at, part):
        return self.z[k, at, pl.ds(part * self.inner, self.inner)]

    def multiply(self, lines, matrix, real_in=False, real_out=False):
        deep = self.inner if real_in else 2 * self.inner
        wide = self.inner if real_out else 2 * self.inner
        count = self.outer * lines
        top = self.top[:, :lines, :deep].reshape(count, deep)
        low = self.low[:, :lines, :deep].reshape(count, deep)
        right_top = matrix[0, :deep, :wide]
        right_low = matrix[1, :deep, :wide]
        dot = functools.partial(jnp.dot, preferred_element_type=jnp.float32)
        total = dot(top, right_top) + dot(low, right_top) + dot(top, right_low)
        self.z[:, :lines, :wide] = total.reshape(self.outer, lines, wide)

    def twist(self, k, pair, sign, twiddle):
        c = twiddle[0, pl.ds(k, 1), :]
        s = twiddle[1, pl.ds(k, 1), :]
        s = s if sign > 0 else -s
        re, im = pair
        return (re * c - im * s, re * s + im * c)

    def turn_full(self, source):
        rows, blocks = self.rows, TILE // self.rows
        for t in range(self.length // TILE):
            tile = source[pl.ds(t * blocks, blocks), :rows, :].reshape(TILE, 2 * rows)
            self.turned[: 2 * rows, pl.ds(t * TILE, TILE)] = tile.T

    def turn_lines(self, source):
        rows = self.rows
        groups = TILE // rows
        blocks, wide = self.inner // rows, self.inner // groups
        for t in range(self.outer):
            tile = source[pl.ds(t * blocks, blocks), :, :].reshape(wide, TILE).T
            for h in range(groups):
                self.turned[:rows, pl.ds(t * self.inner + h * wide, wide)] = tile[h * rows : (h + 1) * rows]

    def kept_lanes(self, j):
        wide = self.inner // 2
        return j * self.inner + (wide if 2 * j >= self.outer else 0), wide

    def clear_other(self, j):
        at, wide = self.kept_lanes(j)
        other = j * self.inner + (0 if 2 * j >= self.outer else wide)
        self.turned[: 2 * self.rows, pl.ds(other, wide)] = jnp.zeros((2 * self.rows, wide), jnp.float32)

    def turn_kept(self, source):
        rows, half, blocks = self.rows, self.half, self.inner // self.rows
        for j in range(self.outer):
            at, wide = self.kept_lanes(j)
            tile = source[pl.ds(j * blocks, blocks), :, :].reshape(wide, 2 * rows)
            self.turned[: 2 * rows, pl.ds(at, wide)] = tile.T
            self.clear_other(j)

    def unpack_middle(self):
        rows, middle = self.rows, (self.outer // 2) * self.inner
        first = self.turned[rows : 2 * rows, :TILE]
        lane0 = lax.broadcasted_iota(jnp.int32, first.shape, 1) == 0
        zero = jnp.zeros_like(first)
        self.turned[:rows, pl.ds(middle, TILE)] += jnp.where(lane0, first, zero)
        self.turned[rows : 2 * rows, :TILE] = jnp.where(lane0, zero, first)

    def incoming(self, lines, sign, twiddle, matrix, real_out=False):
        def body(r0):
            items = []
            for j in range(self.outer):
                lanes = pl.ds(j * self.inner, self.inner)
                items.append((
                    self.turned[pl.ds(r0, self.step), lanes],
                    self.turned[pl.ds(lines + r0, self.step), lanes],
                ))
            for k, pair in enumerate(small_dft(items, sign)):
                re, im = self.twist(k, pair, sign, twiddle)
                self.put(k, pl.ds(r0, self.step), 0, re)
                self.put(k, pl.ds(r0, self.step), 1, im)

        self.chunks(lines, body)
        self.multiply(lines, matrix, real_out=real_out)

    def outgoing(self, lines, sign, twiddle, matrix, real_in, write):
        self.multiply(lines, matrix, real_in=real_in)

        def body(r0):
            at = pl.ds(r0, self.step)
            write(r0, small_dft([
                self.twist(k, (self.get(k, at, 0), self.get(k, at, 1)), sign, twiddle)
                for k in range(self.outer)
            ], sign))

        self.chunks(lines, body)

    def pack_middle(self, items):
        re, im = items[0]
        lane0 = lax.broadcasted_iota(jnp.int32, im.shape, 1) == 0
        return [(re, jnp.where(lane0, items[self.outer // 2][0], im))] + items[1:]

    def write_full(self, result, pack):
        rows = self.rows

        def write(r0, items):
            at = pl.ds(r0, self.step)
            for j, (re, im) in enumerate(self.pack_middle(items) if pack else items):
                for piece in range(self.inner // rows):
                    to = j * (self.inner // rows) + piece
                    lanes = slice(piece * rows, (piece + 1) * rows)
                    result[to, at, pl.ds(0, rows)] = re[:, lanes]
                    result[to, at, pl.ds(rows, rows)] = im[:, lanes]

        return write

    def outgoing_slots(self, twiddle, matrix, kept, other):
        self.multiply(self.rows, matrix, real_in=True)
        rows, half, blocks = self.rows, self.half, self.inner // self.rows
        tall, step = rows * rows // TILE, self.step
        for h in range(rows // tall):

            def body(i, carry, h=h):
                r0 = pl.multiple_of(i * step, step)
                at = pl.ds(h * tall + r0, step)
                items = self.pack_middle(small_dft([
                    self.twist(k, (self.get(k, at, 0), self.get(k, at, 1)), -1.0, twiddle)
                    for k in range(self.outer)
                ], -1.0))
                for j, pair in enumerate(items):
                    for part, value in enumerate(pair):
                        if 2 * j >= self.outer:
                            value = exchange_lanes(value, rows)
                        to = pl.ds(h * rows + part * half, half)
                        for piece in range(blocks):
                            for side, result in enumerate((kept, other)):
                                base = piece * rows + side * half
                                result[j * blocks + piece, pl.ds(r0, step), to] = value[:, base : base + half]
                return carry

            lax.fori_loop(0, tall // step, body, 0)

    def outgoing_kept(self, twiddle, matrix, result):
        self.multiply(self.rows, matrix, real_in=True)
        rows, half, blocks = self.rows, self.half, self.inner // self.rows
        tall = rows * rows // TILE
        step = math.gcd(rows, 16)
        span = min(tall, step)
        for h in range(rows // max(tall, step)):

            def body(i, carry, h=h):
                r0 = i * step if isinstance(i, int) else pl.multiple_of(i * step, step)
                at = pl.ds(h * max(tall, step) + r0, step)
                items = self.pack_middle(small_dft([
                    self.twist(k, (self.get(k, at, 0), self.get(k, at, 1)), -1.0, twiddle)
                    for k in range(self.outer)
                ], -1.0))
                for j, pair in enumerate(items):
                    base = self.inner // 2 if 2 * j >= self.outer else 0
                    for piece in range(blocks):
                        lanes = slice(base + piece * half, base + (piece + 1) * half)
                        for part, value in enumerate(pair):
                            for sub in range(step // span):
                                group = h * (step // span) + sub
                                to = pl.ds(group * rows + part * half, half)
                                held = value[sub * span : (sub + 1) * span, lanes]
                                result[j * blocks + piece, pl.ds(r0, span), to] = held
                return carry

            if tall > step:
                lax.fori_loop(0, tall // step, body, 0)
            else:
                body(0, 0)

    def mirrored(self, blocks, mirror):
        dot = functools.partial(jnp.dot, preferred_element_type=jnp.float32)

        def flip(values, which):
            top, low = halves(jnp.concatenate(values, axis=0))
            return dot(top, mirror[which]) + dot(low, mirror[which])

        flat = [part for k in range(self.outer) for pair in blocks[k] for part in pair]
        per = 2 * len(blocks[0])
        low = flip(flat[:per], 0)
        high = flip(flat[per:], 1)
        out = []
        for k in range(self.outer):
            part, base = (low, 0) if k == 0 else (high, (self.outer - k - 1) * per)
            take = lambda i: part[(base + i) * 8 : (base + i + 1) * 8]
            out.append([(take(2 * i), -take(2 * i + 1)) for i in range(per // 2)])
        return out

    def pack_columns(self, slabs, result):
        rows, half, wide = self.rows, self.half, self.inner // 2
        blocks, groups = self.inner // rows, TILE // rows
        tall = rows // groups
        for k in range(self.outer):
            slab = slabs(k)
            for s in range(blocks):
                parts = []
                for group in range(groups):
                    for part in range(2):
                        at = part * wide + s * half
                        parts.append(slab[group * tall : (group + 1) * tall, at : at + half])
                result[k * blocks + s] = jnp.concatenate(parts, axis=1)

    def turn_columns(self, source, result):
        rows, wide, blocks = self.rows, self.inner // 2, self.inner // self.rows
        for j in range(self.outer):
            tile = source[pl.ds(j * blocks, blocks), :, :].reshape(wide, 2 * rows).T
            result[j, :, pl.ds(0, wide)] = tile[:rows]
            result[j, :, pl.ds(wide, wide)] = tile[rows:]

    def spread(self, first, second, strided, result):
        rows, fill = self.rows, TILE - 2 * self.rows
        for t in range(self.length // TILE):
            lanes = pl.ds(t * TILE, TILE)
            parts = [first[:, lanes], second[:, lanes]]
            if fill:
                parts.append(jnp.zeros((fill, TILE), jnp.float32))
            strided[pl.ds(t * TILE, TILE), :] = jnp.concatenate(parts, axis=0).T
        for k in range(self.outer):
            slab = strided[pl.ds(k, self.inner, stride=self.outer), :].T
            result[k] = slab[: 2 * rows, :]

    def collect(self, slabs, strided, results):
        rows = self.rows
        for k in range(self.outer):
            slab = slabs(k)
            fill = TILE - slab.shape[0]
            if fill:
                slab = jnp.concatenate([slab, jnp.zeros((fill, self.inner), jnp.float32)], axis=0)
            strided[pl.ds(k, self.inner, stride=self.outer), :] = slab.T
        for t in range(self.length // TILE):
            block = strided[pl.ds(t * TILE, TILE), :].T
            for i, result in enumerate(results):
                result[:, pl.ds(t * TILE, TILE)] = block[i * rows : (i + 1) * rows, :]


def signed_waves(position, count):
    signed = jnp.where(position < count // 2, position, position - count)
    waves = 4.0 * signed.astype(jnp.float32) / count
    return waves, jnp.where(position == count // 2, jnp.float32(0.0), waves)


def first_waves(piece, k):
    lanes = lax.broadcasted_iota(jnp.int32, (1, piece.inner), 1)
    return signed_waves(piece.outer * lanes + k, piece.length)


def inverse_denominator(wave_first, wave_second):
    square = wave_first * wave_first + wave_second * wave_second
    return 1.0 / (1.0 + time_step * (square * square - square))


def second_wave(piece, position):
    shape = (position.shape[0], piece.inner)
    return jnp.broadcast_to(signed_waves(position, piece.length)[0], shape)


def row_index(count, width):
    return lax.broadcasted_iota(jnp.int32, (count, width), 0)


def exchange_lanes(value, rows):
    half, wide = rows // 2, value.shape[1]
    line = lax.broadcasted_iota(jnp.int32, value.shape, 1) % rows
    up, down = pltpu.roll(value, half, 1), pltpu.roll(value, wide - half, 1)
    return jnp.where(line == 0, down, jnp.where(line == half, up, value))


def exchange_rows(held, first, second, swapped):
    at, also = first, second
    one, other = held[at], held[also]
    top = lax.broadcasted_iota(jnp.int32, one.shape, one.ndim - 2) == 0
    moved = top if swapped is None else jnp.logical_and(top, swapped)
    held[at] = jnp.where(moved, other, one)
    held[also] = jnp.where(moved, one, other)


class Links:
    def __init__(self, devices, fast):
        self.devices, self.fast = devices, fast
        self.device = lax.axis_index(axes[0]) * fast + lax.axis_index(axes[1])

    def partner(self, i):
        total, bit = 0, 1
        while bit < self.devices:
            total += bit * lax.rem(lax.div(self.device, bit) + lax.div(i, bit), 2)
            bit *= 2
        return total

    def send(self, source, target, sems, share=0, shares=1):
        send_sem, recv_sem, own_sem = sems

        def go(i, carry):
            peer = self.partner(self.devices - i)
            pltpu.make_async_remote_copy(
                src_ref=source(peer),
                dst_ref=target(self.device),
                send_sem=send_sem,
                recv_sem=recv_sem,
                device_id=(lax.div(peer, self.fast), lax.rem(peer, self.fast)),
                device_id_type=pl.DeviceIdType.MESH,
            ).start()
            return carry

        far, near = self.devices // 2, self.devices // 2 - 1
        for base, count in ((1, far), (1 + far, near)):
            lax.fori_loop(base + count * share // shares, base + count * (share + 1) // shares, go, 0)
        if share == 0:
            pltpu.make_async_copy(source(self.device), target(self.device), own_sem).start()

    def whole(self, source, target, sems):
        others = pl.ds(0, self.devices - 1)
        return pltpu.make_async_remote_copy(
            src_ref=source(others),
            dst_ref=target(others),
            send_sem=sems[0],
            recv_sem=sems[1],
            device_id=(0, 0),
            device_id_type=pl.DeviceIdType.MESH,
        )

    def receive(self, source, target, sems):
        pltpu.make_async_copy(source(self.device), target(self.device), sems[2]).wait()
        self.whole(source, target, sems).wait_recv()

    def sent(self, source, target, sems):
        self.whole(source, target, sems).wait_send()


def start_kernel(length, rows, field, target, out, both_p, *scratch):
    piece = Pieces(length, rows)
    piece.spread(field, target, scratch[0], both_p)
    piece.pack_columns(lambda k: both_p[k, pl.ds(0, rows), :], out)


def slope_second_kernel(length, rows, field_p, twiddle, out_matrix, in_matrix, kept, result, *scratch):
    piece = Pieces(length, rows, *scratch)

    def body(r0):
        at = pl.ds(r0, piece.step)
        for k in range(piece.outer):
            piece.put(k, at, 0, field_p[k, at, :])

    piece.chunks(rows, body)
    for j in range(piece.outer):
        piece.clear_other(j)

    def write(r0, items):
        for j, (re, im) in enumerate(items):
            at, wide = piece.kept_lanes(j)
            base = at - j * piece.inner
            position = j * piece.inner + kept[:, base : base + wide]
            slope = 2.0 * signed_waves(position, length)[1]
            piece.turned[pl.ds(r0, piece.step), pl.ds(at, wide)] = -slope * im[:, base : base + wide]
            piece.turned[pl.ds(rows + r0, piece.step), pl.ds(at, wide)] = slope * re[:, base : base + wide]

    piece.outgoing(rows, -1.0, twiddle, out_matrix, True, write)
    piece.incoming(rows, 1.0, twiddle, in_matrix, real_out=True)
    result[...] = piece.z[:, :, : piece.inner]


def spread_kernel(length, rows, forcing, result, strided):
    Pieces(length, rows).spread(forcing.at[0], forcing.at[1], strided, result)


def collect_kernel(length, rows, slabs, result, strided):
    piece = Pieces(length, rows)
    piece.collect(lambda k: slabs[k], strided, [result.at[i] for i in range(result.shape[0])])


def weight_of(device, r0, step, inner):
    alone = (row_index(step, inner) + r0 + device) == 0
    return jnp.where(alone, jnp.float32(1.0), jnp.float32(2.0))


def slope_first_kernel(length, rows, source, in_twiddle, in_matrix, out_twiddle, out_matrix, out, *scratch):
    piece = Pieces(length, rows, *scratch)
    half = piece.half
    piece.turn_lines(source)
    piece.incoming(half, -1.0, in_twiddle, in_matrix)

    def body(r0):
        at = pl.ds(r0, piece.step)
        for k in range(piece.outer):
            re, im = piece.get(k, at, 0), piece.get(k, at, 1)
            scale = first_waves(piece, k)[1]
            piece.put(k, at, 0, -scale * im)
            piece.put(k, at, 1, scale * re)

    piece.chunks(half, body)
    piece.outgoing(half, 1.0, out_twiddle, out_matrix, False, piece.write_full(out, False))


def edge_inverses(piece, k):
    wave_first = first_waves(piece, k)[0]
    middle = jnp.full((1, 1), piece.length // 2, jnp.int32)
    zero = jnp.zeros((1, 1), jnp.int32)
    return [inverse_denominator(wave_first, signed_waves(p, piece.length)[0]) for p in (zero, middle)]


def next_kernel(length, rows, device_ref, source, forcing, in_twiddle, in_matrix, out_twiddle, out_matrix, mirror, out, *scratch):
    device = device_ref[0]
    piece = Pieces(length, rows, *scratch)
    half, step, inner = piece.half, piece.step, piece.inner
    late = device >= (length // rows) // 2
    piece.turn_lines(source)
    piece.incoming(half, -1.0, in_twiddle, in_matrix)

    def body(r0):
        at, also = pl.ds(r0, step), pl.ds(half + r0, step)
        index = row_index(step, 1) + r0
        low_wave = second_wave(piece, device * rows + index)
        high_wave = second_wave(piece, device * rows + half + index)
        moved = jnp.logical_and(row_index(step, inner) + r0 == 0, late)
        weight = weight_of(device, r0, step, inner)
        for k in range(piece.outer):
            wave_first = first_waves(piece, k)[0]
            low = inverse_denominator(wave_first, low_wave)
            high = inverse_denominator(wave_first, high_wave)
            for part in range(2):
                own = weight * piece.get(k, at, part)
                f_low = time_step * forcing[k, pl.ds(part * rows + r0, step), :]
                f_high = time_step * forcing[k, pl.ds(part * rows + half + r0, step), :]
                piece.put(k, at, part, (f_low + jnp.where(moved, 0.0, own)) * low)
                piece.put(k, also, part, (f_high + jnp.where(moved, own, 0.0)) * high)

    piece.chunks(half, body)

    @pl.when(device == 0)
    def _():
        at = pl.ds(0, 8)
        blocks = []
        for k in range(piece.outer):
            own = tuple(piece.get(k, at, part) for part in range(2))
            full = tuple(
                own[part] + time_step * forcing[k, pl.ds(part * rows, 8), :] for part in range(2)
            )
            blocks.append([own, full])
        flipped = piece.mirrored(blocks, mirror)
        rest = pl.ds(0, 16)
        row0 = row_index(16, inner) == 0
        for k in range(piece.outer):
            zero, middle = edge_inverses(piece, k)
            for part in range(2):
                own, full = blocks[k][0][part], blocks[k][1][part]
                own_c, full_c = flipped[k][0][part], flipped[k][1][part]
                value = 0.5 * ((full + full_c) * zero + (own - own_c) * middle)
                replace(piece, k, part, value)

    piece.outgoing(rows, 1.0, out_twiddle, out_matrix, False, piece.write_full(out, False))


def replace(piece, k, part, value):
    lanes = pl.ds(part * piece.inner, piece.inner)
    row0 = row_index(16, piece.inner) == 0
    value = jnp.concatenate([value, value], axis=0)
    for held, new in zip((piece.top, piece.low), halves(value)):
        old = held[k, pl.ds(0, 16), lanes].astype(jnp.float32)
        held[k, pl.ds(0, 16), lanes] = jnp.where(row0, new.astype(jnp.float32), old).astype(jnp.bfloat16)


def misfit_kernel(length, rows, device_ref, source, in_twiddle, in_matrix, out_twiddle, out_matrix, mirror, out, full, total_out, *scratch):
    device = device_ref[0]
    piece = Pieces(length, rows, *scratch)
    half, step, inner = piece.half, piece.step, piece.inner
    late = device >= (length // rows) // 2
    piece.turn_full(source)
    piece.incoming(rows, -1.0, in_twiddle, in_matrix)

    def body(r0):
        at, also = pl.ds(r0, step), pl.ds(half + r0, step)
        index = row_index(step, 1) + r0
        low_wave = second_wave(piece, device * rows + index)
        high_wave = second_wave(piece, device * rows + half + index)
        moved = jnp.logical_and(row_index(step, inner) + r0 == 0, late)
        weight = weight_of(device, r0, step, inner)
        for k in range(piece.outer):
            wave_first = first_waves(piece, k)[0]
            low = time_step * inverse_denominator(wave_first, low_wave)
            high = time_step * inverse_denominator(wave_first, high_wave)
            for part in range(2):
                low_value = piece.get(k, at, part) * low
                high_value = piece.get(k, also, part) * high
                full[k, pl.ds(part * rows + r0, step), :] = low_value
                full[k, pl.ds(part * rows + half + r0, step), :] = high_value
                own = jnp.where(moved, high_value, low_value)
                piece.put(k, at, part, weight * own)

    piece.chunks(half, body)

    @pl.when(device == 0)
    def _():
        at = pl.ds(0, 8)
        blocks = [[(piece.get(k, at, 0), piece.get(k, at, 1))] for k in range(piece.outer)]
        flipped = piece.mirrored(blocks, mirror)
        row0 = row_index(8, inner) == 0
        for k in range(piece.outer):
            zero, middle = edge_inverses(piece, k)
            for part in range(2):
                own, own_c = blocks[k][0][part], flipped[k][0][part]
                first = (0.5 * time_step) * (own + own_c) * zero
                value = first + (0.5 * time_step) * (own - own_c) * middle
                at_full = pl.ds(part * rows, 8)
                full[k, at_full, :] = jnp.where(row0, first, full[k, at_full, :])
                replace(piece, k, part, value)

    piece.outgoing(half, 1.0, out_twiddle, out_matrix, False, piece.write_full(out, False))
    total_out[...] = jnp.sum(source[:, pl.ds(rows, 8), :], axis=0)


def nonlinear_kernel(length, rows, source, both_p, second, twiddle, out_matrix, out, first, *scratch):
    piece = Pieces(length, rows, *scratch)
    piece.turn_columns(source, first)

    def body(r0):
        at = pl.ds(r0, piece.step)
        for k in range(piece.outer):
            one, other = first[k, at, :], second[k, at, :]
            piece.put(k, at, 0, both_p[k, at, :] - (0.5 * time_step) * (one * one + other * other))

    piece.chunks(rows, body)
    piece.outgoing_kept(twiddle, out_matrix, out)


def joint_kernel(length, rows, source, first, second, twiddle, in_matrix, out, value_out, second_out, *scratch):
    piece = Pieces(length, rows, *scratch)
    piece.turn_kept(source)
    piece.unpack_middle()
    piece.incoming(rows, 1.0, twiddle, in_matrix, real_out=True)
    lanes = pl.ds(0, piece.inner)

    def body(r0):
        at = pl.ds(r0, piece.step)
        for k in range(piece.outer):
            value = piece.get(k, at, 0)
            value_out[k, at, :] = (1.0 / time_step) * value
            second_out[k, at, :] = value * second[k, at, :]
            piece.z[k, at, lanes] = value * first[k, at, :]

    piece.chunks(rows, body)
    piece.pack_columns(lambda k: piece.z[k, pl.ds(0, rows), lanes], out)


def residual_kernel(length, rows, source, both_p, twiddle, in_matrix, out_matrix, out, field_out, *scratch):
    piece = Pieces(length, rows, *scratch[:4])
    strided, total = scratch[4:]
    piece.turn_full(source)
    piece.unpack_middle()
    piece.incoming(rows, 1.0, twiddle, in_matrix, real_out=True)
    piece.collect(lambda k: piece.get(k, pl.ds(0, rows), 0), strided, [field_out])
    total[...] = jnp.zeros_like(total)

    def body(r0):
        at = pl.ds(r0, piece.step)
        for k in range(piece.outer):
            residual = piece.get(k, at, 0) - both_p[k, pl.ds(rows + r0, piece.step), :]
            total[...] += residual * residual
            piece.put(k, at, 0, residual)

    piece.chunks(rows, body)
    piece.outgoing(rows, -1.0, twiddle, out_matrix, True, piece.write_full(out, True))
    value = 0.5 * jnp.sum(total[...])
    out[:, pl.ds(rows, 8), :] = jnp.full((out.shape[0], 8, 2 * rows), value, jnp.float32)


def last_kernel(length, rows, source, value, second, field_out, strided, first):
    piece = Pieces(length, rows)
    piece.turn_columns(source, first)
    piece.collect(lambda k: first[k] + value[k] + second[k], strided, [field_out])


def slots_of(device, late, index, rows, half, other):
    line = half + index if other else index
    special = jnp.where(late, 0, half) if other else jnp.where(late, half, 0)
    return device * rows + jnp.where(index == 0, special, line)


def step_kernel(length, rows, devices, fast, inputs, outs, box):
    links = Links(devices, fast)
    device, half = links.device, rows // 2
    late = device >= devices // 2
    copies, sems = box.copies, box.sems
    piece = Pieces(length, rows, box.turned, box.top, box.low, box.z)
    step, inner, outer = piece.step, piece.inner, piece.outer
    both_p, forcing_p, full = box.both_p, box.forcing_p, box.full
    first, second, value = box.first, box.second, box.value
    strided, total = box.strided, box.total

    loads = [
        pltpu.make_async_copy(ref, held, copies.at[i])
        for i, (ref, held) in enumerate(zip(inputs.refs, inputs.held))
    ]
    for copy in loads[:2]:
        copy.start()
    waiting = iter(loads)

    def load(count):
        for i in range(count):
            next(waiting).wait()

    at_all = lambda ref: lambda e: ref.at[e]
    at_lines = lambda ref, base, count: lambda e: ref.at[e, pl.ds(base, count)]
    order = []

    def plan(source, target):
        i = len(order)
        order.append((source, target, (sems.at[i, 0], sems.at[i, 1], sems.at[i, 2])))
        return order[-1]

    def send(source, target):
        move = plan(source, target)
        links.send(*move)
        return move

    def receive(*moves):
        for move in moves:
            links.receive(*move)

    def send_all(source, target):
        return send(at_all(source), at_all(target))

    tables = inputs.twiddles
    tw_natural, tw_kept, tw_lines = (tables.at[i] for i in range(3))
    forward, backward, lines_in = inputs.forward, inputs.backward, inputs.lines
    kept_out, kept_in, kept, mirror = inputs.kept_out, inputs.kept_in, inputs.kept, inputs.mirror

    def slope_first(source, out):
        slope_first_kernel(
            length, rows, source, tw_lines, lines_in, tw_natural, backward, out,
            piece.turned, piece.top, piece.low, piece.z,
        )

    def slope_second(source, out):
        slope_second_kernel(
            length, rows, source, tw_kept, kept_out, kept_in, kept, out,
            piece.turned, piece.top, piece.low, piece.z,
        )

    load(2)
    for copy in loads[2:]:
        copy.start()
    piece.spread(inputs.field, inputs.target, strided, both_p)
    piece.pack_columns(lambda k: both_p[k, pl.ds(0, rows), :], box.s_field)
    m_field = send_all(box.s_field, box.r_field)

    load(4)
    slope_second(both_p, second)
    load(1)
    piece.spread(inputs.forcing.at[0], inputs.forcing.at[1], strided, forcing_p)
    for k in range(outer):
        for part in range(2):
            at, also = (k, pl.ds(part * rows, 8)), (k, pl.ds(part * rows + half, 8))
            exchange_rows(forcing_p, at, also, late)
    load(4)

    def rest(r0):
        at = pl.ds(r0, step)
        wave = second_wave(piece, slots_of(device, late, row_index(step, 1) + r0, rows, half, True))
        for k in range(outer):
            scale = time_step * inverse_denominator(first_waves(piece, k)[0], wave)
            for part in range(2):
                piece.put(k, at, part, scale * forcing_p[k, pl.ds(part * rows + half + r0, step), :])

    piece.chunks(half, rest)
    piece.outgoing(half, 1.0, tw_natural, backward, False, piece.write_full(box.s_rest, False))

    m_rest = plan(at_all(box.s_rest), at_lines(box.r_next, half, half))

    receive(m_field)
    links.send(*m_rest, 0, 3)
    slope_first(box.r_field, box.s_slope)
    m_slope = send_all(box.s_slope, box.r_slope)

    receive(m_slope)
    links.send(*m_rest, 1, 3)
    nonlinear_kernel(
        length, rows, box.r_slope, both_p, second, tw_kept, kept_out, box.s_sum, first,
        piece.turned, piece.top, piece.low, piece.z,
    )
    m_sum = send_all(box.s_sum, box.r_sum)

    receive(m_sum)
    links.send(*m_rest, 2, 3)
    piece.turn_lines(box.r_sum)
    piece.incoming(half, -1.0, tw_lines, lines_in)

    def divide(r0):
        at = pl.ds(r0, step)
        wave = second_wave(piece, slots_of(device, late, row_index(step, 1) + r0, rows, half, False))
        weight = weight_of(device, r0, step, inner)
        for k in range(outer):
            scale = inverse_denominator(first_waves(piece, k)[0], wave)
            for part in range(2):
                forced = time_step * forcing_p[k, pl.ds(part * rows + r0, step), :]
                piece.put(k, at, part, (weight * piece.get(k, at, part) + forced) * scale)

    piece.chunks(half, divide)

    @pl.when(device == 0)
    def _():
        at = pl.ds(0, 8)
        blocks = []
        for k in range(outer):
            own = tuple(piece.get(k, at, part) for part in range(2))
            joined = tuple(own[part] + time_step * forcing_p[k, pl.ds(part * rows, 8), :] for part in range(2))
            blocks.append([own, joined])
        flipped = piece.mirrored(blocks, mirror)
        for k in range(outer):
            zero, middle = edge_inverses(piece, k)
            for part in range(2):
                own, joined = blocks[k][0][part], blocks[k][1][part]
                own_c, joined_c = flipped[k][0][part], flipped[k][1][part]
                replace(piece, k, part, 0.5 * ((joined + joined_c) * zero + (own - own_c) * middle))

    piece.outgoing(half, 1.0, tw_natural, backward, False, piece.write_full(box.s_next, False))
    m_next = send(at_all(box.s_next), at_lines(box.r_next, 0, half))

    receive(m_rest, m_next)
    turned_late = pl.ds(devices // 2, devices // 2)
    exchange_rows(box.r_next, (turned_late, pl.ds(0, 8)), (turned_late, pl.ds(half, 8)), None)
    piece.turn_full(box.r_next)
    piece.unpack_middle()
    piece.incoming(rows, 1.0, tw_natural, backward, real_out=True)
    total[...] = jnp.zeros_like(total)
    lanes = pl.ds(0, inner)

    def misfit(r0):
        at = pl.ds(r0, step)
        for k in range(outer):
            now = piece.get(k, at, 0)
            value[k, at, :] = now
            residual = now - both_p[k, pl.ds(rows + r0, step), :]
            total[...] += residual * residual
            piece.put(k, at, 0, residual)

    piece.chunks(rows, misfit)
    piece.outgoing_slots(tw_natural, forward, box.s_kept, box.s_other)
    m_kept = send_all(box.s_kept, box.r_kept)
    m_other = plan(at_all(box.s_other), at_all(box.r_other))
    box.s_total[...] = jnp.full(box.s_total.shape, 0.5 * jnp.sum(total[...]), jnp.float32)
    m_total = send(lambda e: box.s_total.at[e], lambda e: box.r_total.at[e])
    piece.collect(lambda k: value[k], strided, [outs.next])

    receive(m_kept)
    links.send(*m_other, 0, 3)
    piece.turn_lines(box.r_kept)
    piece.incoming(half, -1.0, tw_lines, lines_in)

    def adjoint(r0):
        at = pl.ds(r0, step)
        wave = second_wave(piece, slots_of(device, late, row_index(step, 1) + r0, rows, half, False))
        weight = weight_of(device, r0, step, inner)
        for k in range(outer):
            scale = time_step * inverse_denominator(first_waves(piece, k)[0], wave)
            for part in range(2):
                own = piece.get(k, at, part) * scale
                full[k, pl.ds(part * rows + r0, step), :] = own
                piece.put(k, at, part, weight * own)

    piece.chunks(half, adjoint)

    @pl.when(device == 0)
    def _():
        at = pl.ds(0, 8)
        blocks = [[(piece.get(k, at, 0), piece.get(k, at, 1))] for k in range(outer)]
        flipped = piece.mirrored(blocks, mirror)
        row0 = row_index(8, inner) == 0
        for k in range(outer):
            zero, middle = edge_inverses(piece, k)
            for part in range(2):
                own, own_c = blocks[k][0][part], flipped[k][0][part]
                line = (0.5 * time_step) * (own + own_c) * zero
                at_full = pl.ds(part * rows, 8)
                full[k, at_full, :] = jnp.where(row0, line, full[k, at_full, :])
                replace(piece, k, part, line + (0.5 * time_step) * (own - own_c) * middle)

    piece.outgoing(half, 1.0, tw_natural, backward, False, piece.write_full(box.s_back, False))
    m_back = send_all(box.s_back, box.r_back)

    receive(m_back)
    links.send(*m_other, 1, 3)
    joint_kernel(
        length, rows, box.r_back, first, second, tw_kept, kept_in, box.s_product, value, box.product,
        piece.turned, piece.top, piece.low, piece.z,
    )
    m_product = send_all(box.s_product, box.r_product)

    slope_second(box.product, second)
    for k in range(outer):
        value[k] = value[k] + second[k]

    receive(m_product)
    links.send(*m_other, 2, 3)
    slope_first(box.r_product, box.s_last)
    m_last = send_all(box.s_last, box.r_last)

    receive(m_other, m_total)
    piece.turn_lines(box.r_other)
    piece.incoming(half, -1.0, tw_lines, lines_in)

    def others(r0):
        at = pl.ds(r0, step)
        wave = second_wave(piece, slots_of(device, late, row_index(step, 1) + r0, rows, half, True))
        for k in range(outer):
            scale = time_step * inverse_denominator(first_waves(piece, k)[0], wave)
            for part in range(2):
                full[k, pl.ds(part * rows + half + r0, step), :] = piece.get(k, at, part) * scale

    piece.chunks(half, others)
    for k in range(outer):
        for part in range(2):
            at, also = (k, pl.ds(part * rows, 8)), (k, pl.ds(part * rows + half, 8))
            exchange_rows(full, at, also, late)
    piece.collect(lambda k: full[k], strided, [outs.forcing.at[i] for i in range(2)])
    outs.total[...] = jnp.sum(box.r_total[...], axis=0) / (length * length)

    receive(m_last)
    piece.turn_columns(box.r_last, first)
    for k in range(outer):
        outs.field[k] = first[k] + value[k]
    for move in order:
        links.sent(*move)


messages = 11


def joined_step(field, target, forcing, devices, fast, rows, length):
    outer, inner = split_length(length)
    half, step = rows // 2, math.gcd(rows // 2, 16)
    natural, kept, lines = orders(length, rows)
    matrix = lambda *args: matrix_table(length, *args)
    tables = dict(
        field=field, target=target,
        twiddles=np.stack([twiddle_table(length, o) for o in (natural, kept, lines)]),
        kept=kept[None, :].astype(np.int32),
        kept_out=matrix(-1.0, natural, kept)[:, :inner],
        kept_in=matrix(1.0, kept, natural)[:, :, :inner],
        forcing=forcing,
        backward=matrix(1.0, natural, natural),
        lines=matrix(-1.0, lines, natural),
        forward=matrix(-1.0, natural, natural),
        mirror=mirror_table(length),
    )
    operands = [jnp.asarray(table) for table in tables.values()]
    float32 = jnp.float32
    held = lambda *dims: pltpu.VMEM(dims, float32)
    packed, lined = held(devices, rows * rows // TILE, TILE), held(devices, half, 2 * rows)
    pair, one = held(outer, 2 * rows, inner), held(outer, rows, inner)
    small = held(devices, 8, TILE)
    halved = pltpu.VMEM((outer, rows, 2 * inner), jnp.bfloat16)
    shapes = dict(
        turned=held(2 * rows, length), top=halved, low=halved, z=held(outer, rows, 2 * inner),
        strided=held(length, TILE), total=held(step, inner),
        both_p=pair, forcing_p=pair, full=pair, first=one, second=one, value=one, product=one,
        s_field=packed, r_field=packed, s_slope=lined, r_slope=lined, s_sum=packed, r_sum=packed,
        s_rest=lined, s_next=lined, r_next=held(devices, rows, 2 * rows),
        s_kept=packed, r_kept=packed, s_other=packed, r_other=packed, s_total=small, r_total=small,
        s_back=lined, r_back=lined, s_product=packed, r_product=packed, s_last=lined, r_last=lined,
        copies=pltpu.SemaphoreType.DMA((len(operands),)),
        sems=pltpu.SemaphoreType.DMA((messages, 3)),
    )
    inputs = [pltpu.VMEM(operand.shape, operand.dtype) for operand in operands]

    def body(*refs):
        a, b = len(operands), len(operands) + 4
        c = b + len(operands)
        given = SimpleNamespace(refs=refs[:a], held=refs[b:c], **dict(zip(tables, refs[b:c])))
        outs = SimpleNamespace(next=refs[a], field=refs[a + 1], forcing=refs[a + 2], total=refs[a + 3])
        step_kernel(length, rows, devices, fast, given, outs, SimpleNamespace(**dict(zip(shapes, refs[c:]))))

    anywhere = pl.BlockSpec(memory_space=pl.ANY)
    vmem, smem = pl.BlockSpec(memory_space=pltpu.VMEM), pl.BlockSpec(memory_space=pltpu.SMEM)
    shape = lambda *dims: jax.ShapeDtypeStruct(dims, float32)
    next_field, slabs, forcing_grad, total = pl.pallas_call(
        body,
        out_shape=(shape(rows, length), shape(outer, rows, inner), shape(2, rows, length), shape(8, TILE)),
        in_specs=[pl.BlockSpec(memory_space=pltpu.HBM)] * len(operands),
        out_specs=(vmem, vmem, vmem, vmem),
        scratch_shapes=inputs + list(shapes.values()),
        compiler_params=pltpu.CompilerParams(vmem_limit_bytes=34 * 2**20, has_side_effects=True),
        cost_estimate=pl.CostEstimate(flops=6 * 10**10, bytes_accessed=4 * 2**20, transcendentals=0),
    )(*[pltpu.with_memory_space_constraint(one, pltpu.HBM) for one in operands])
    return pl.pallas_call(
        functools.partial(tail_kernel, length, rows),
        out_shape=(shape(rows, length), shape(rows, length), shape(2, rows, length), shape(1, 1)),
        in_specs=[vmem] * 4,
        out_specs=(anywhere, anywhere, anywhere, smem),
        scratch_shapes=[held(length, TILE), held(rows, length), pltpu.SemaphoreType.DMA((3,))],
        compiler_params=pltpu.CompilerParams(vmem_limit_bytes=8 * 2**20),
        cost_estimate=pl.CostEstimate(flops=10**9, bytes_accessed=4 * 2**20, transcendentals=0),
    )(next_field, slabs, forcing_grad, total)


def tail_kernel(length, rows, next_field, slabs, forcing_grad, total, next_out, field_out, forcing_out, total_out, strided, held, sems):
    piece = Pieces(length, rows)
    copies = [
        pltpu.make_async_copy(next_field, next_out, sems.at[0]),
        pltpu.make_async_copy(forcing_grad, forcing_out, sems.at[1]),
        pltpu.make_async_copy(held, field_out, sems.at[2]),
    ]
    copies[0].start()
    copies[1].start()
    total_out[0, 0] = jnp.sum(total[0:1, 0:1])
    piece.collect(lambda k: slabs[k], strided, [held])
    copies[2].start()
    for copy in copies:
        copy.wait()


def member_step(device, field, target, forcing_p, devices, rows, length):
    outer, inner = split_length(length)
    half = rows // 2
    float32 = jnp.float32
    shape = lambda *dims: jax.ShapeDtypeStruct(dims, float32)
    kept_blocks = shape(devices, rows * rows // TILE, TILE)
    half_blocks = shape(devices, half, 2 * rows)
    blocks = shape(devices, rows, 2 * rows)
    longer = shape(devices, rows + 8, 2 * rows)
    pair, one = shape(outer, 2 * rows, inner), shape(outer, rows, inner)
    plain = shape(rows, length)
    step = math.gcd(half, 16)
    base = [
        pltpu.VMEM((2 * rows, length), float32),
        pltpu.VMEM((outer, rows, 2 * inner), jnp.bfloat16),
        pltpu.VMEM((outer, rows, 2 * inner), jnp.bfloat16),
        pltpu.VMEM((outer, rows, 2 * inner), float32),
    ]
    strided = pltpu.VMEM((length, TILE), float32)
    total = pltpu.VMEM((step, inner), float32)
    vmem = pl.BlockSpec(memory_space=pltpu.VMEM)
    smem = pl.BlockSpec(memory_space=pltpu.SMEM)

    natural, kept, lines = orders(length, rows)
    tw_natural, tw_kept, tw_lines = [jnp.asarray(twiddle_table(length, o)) for o in (natural, kept, lines)]
    matrix = lambda *args: matrix_table(length, *args)
    forward, backward = matrix(-1.0, natural, natural), matrix(1.0, natural, natural)
    kept_out, kept_in = matrix(-1.0, natural, kept)[:, :inner], matrix(1.0, kept, natural)[:, :, :inner]
    lines_in = matrix(-1.0, lines, natural)
    mirror = jnp.asarray(mirror_table(length))
    kept_lane = jnp.asarray(kept[None, :].astype(np.int32))

    def call(body, outs, scratch, *operands):
        return pl.pallas_call(
            functools.partial(body, length, rows),
            out_shape=outs,
            in_specs=[smem if operand is device else vmem for operand in operands],
            out_specs=jax.tree.map(lambda leaf: vmem, outs),
            scratch_shapes=scratch,
            compiler_params=pltpu.CompilerParams(vmem_limit_bytes=20 * 2**20),
            cost_estimate=pl.CostEstimate(flops=6 * 10**9, bytes_accessed=4 * 2**20, transcendentals=0),
        )(*operands)

    def move(value):
        return lax.all_to_all(value, axes, split_axis=0, concat_axis=0, tiled=True)

    spectral_tables = (tw_lines, lines_in, tw_natural, backward)
    slope_tables = (tw_kept, kept_out, kept_in, kept_lane)
    sent, both_p = call(start_kernel, (kept_blocks, pair), [strided], field, target)
    second = call(slope_second_kernel, one, base, both_p, *slope_tables)
    sent = call(slope_first_kernel, half_blocks, base, move(sent), *spectral_tables)
    sent, first = call(nonlinear_kernel, (kept_blocks, one), base, move(sent), both_p, second, tw_kept, kept_out)
    sent = call(next_kernel, blocks, base, device, move(sent), forcing_p, *spectral_tables, mirror)
    sent, next_field = call(
        residual_kernel, (longer, plain), base + [strided, total],
        move(sent), both_p, tw_natural, backward, forward,
    )
    sent, full, sums = call(
        misfit_kernel, (half_blocks, pair, shape(8, 2 * rows)), base,
        device, move(sent), tw_natural, forward, tw_natural, backward, mirror,
    )
    sent, value, product = call(
        joint_kernel, (kept_blocks, one, one), base, move(sent), first, second, tw_kept, kept_in
    )
    second_part = call(slope_second_kernel, one, base, product, *slope_tables)
    sent = call(slope_first_kernel, half_blocks, base, move(sent), *spectral_tables)
    field_grad = call(
        last_kernel, plain, [strided, pltpu.VMEM((outer, rows, inner), float32)], move(sent), value, second_part
    )
    return next_field, sums[0, 0], field_grad, full


def per_device(devices, fast, initial_field, target_field, forcing):
    members, rows, length = initial_field.shape
    device = lax.axis_index(axes).astype(jnp.int32).reshape(1)
    outer, inner = split_length(length)
    vmem = pl.BlockSpec(memory_space=pltpu.VMEM)
    strided = pltpu.VMEM((length, TILE), jnp.float32)

    def reorder(body, shape, operand):
        return pl.pallas_call(
            functools.partial(body, length, rows),
            out_shape=jax.ShapeDtypeStruct(shape, jnp.float32),
            in_specs=[vmem],
            out_specs=vmem,
            scratch_shapes=[strided],
        )(operand)

    if rows * rows % (TILE * 32) == 0 and TILE % rows == 0:
        results = [
            joined_step(initial_field[m], target_field[m], forcing, devices, fast, rows, length)
            for m in range(members)
        ]
        next_field = jnp.stack([one[0] for one in results])
        field_grad = jnp.stack([one[1] for one in results])
        forcing_grad = sum(one[2] for one in results)
        objective = sum(one[3].reshape(()) for one in results) / members
        return (next_field, objective, field_grad, forcing_grad)
    forcing_p = reorder(spread_kernel, (outer, 2 * rows, inner), forcing)
    results = [
        member_step(device, initial_field[m], target_field[m], forcing_p, devices, rows, length)
        for m in range(members)
    ]
    next_field = jnp.stack([one[0] for one in results])
    objective = sum(one[1] for one in results) / (members * length * length)
    field_grad = jnp.stack([one[2] for one in results])
    forcing_grad = reorder(collect_kernel, (2, rows, length), sum(one[3] for one in results))
    return (next_field, objective, field_grad, forcing_grad)


def solution(mesh):
    devices = mesh.shape["px"] * mesh.shape["py"]
    spec = P(None, axes, None)
    return jax.shard_map(
        functools.partial(per_device, devices, mesh.shape["py"]),
        mesh=mesh,
        in_specs=(spec, spec, spec),
        out_specs=(spec, P(), spec, spec),
        check_vma=False,
    )
```

```python
import functools
import math
from types import SimpleNamespace

import jax
import jax.numpy as jnp
import numpy as np
from jax import lax
from jax.experimental import pallas as pl
from jax.experimental.pallas import tpu as pltpu
from jax.sharding import PartitionSpec as P

time_step = 0.25
axes = ("px", "py")
TILE = 128


def split_length(length):
    inner = 256 if length % 256 == 0 else TILE
    return (length // inner, inner)


def small_dft(items, sign):
    count = len(items)
    if count == 1:
        return items
    evens = small_dft(items[0::2], sign)
    odds = small_dft(items[1::2], sign)
    low, high = [], []
    for k in range(count // 2):
        odd_re, odd_im = odds[k]
        if 4 * k == count:
            odd_re, odd_im = (-odd_im, odd_re) if sign > 0 else (odd_im, -odd_re)
        elif k:
            c = math.cos(2.0 * math.pi * k / count)
            s = sign * math.sin(2.0 * math.pi * k / count)
            if abs(abs(c) - abs(s)) < 1e-12:
                sc, ss = math.copysign(1.0, c), math.copysign(1.0, s)
                odd_re, odd_im = (
                    c * (odd_re - sc * ss * odd_im),
                    c * (odd_im + sc * ss * odd_re),
                )
            else:
                odd_re, odd_im = (c * odd_re - s * odd_im, c * odd_im + s * odd_re)
        even_re, even_im = evens[k]
        low.append((even_re + odd_re, even_im + odd_im))
        high.append((even_re - odd_re, even_im - odd_im))
    return low + high


def half_dft(items, sign):
    count = 2 * len(items)
    turned = []
    for j, (re, im) in enumerate(items):
        c = math.cos(2.0 * math.pi * j / count)
        s = sign * math.sin(2.0 * math.pi * j / count)
        turned.append((re, im) if j == 0 else (c * re - s * im, c * im + s * re))
    pairs = zip(small_dft(items, sign), small_dft(turned, sign))
    return [one for pair in pairs for one in pair]


def halves(value):
    top = value.astype(jnp.bfloat16)
    return top, (value - top.astype(jnp.float32)).astype(jnp.bfloat16)


def orders(length, rows):
    inner = split_length(length)[1]
    half = rows // 2
    lane = np.arange(inner)
    natural = lane
    local = lane % (inner // 2)
    line = local % half
    kept = rows * (local // half) + np.where((lane >= inner // 2) & (line == 0), half, line)
    return natural, kept, line_order(inner, rows, TILE // rows)


def line_order(inner, rows, groups):
    lane = np.arange(inner)
    tall, wide = rows // groups, inner // groups
    within = lane % wide
    return rows * (within // tall) + tall * (lane // wide) + within % tall


def twiddle_table(length, order):
    outer = split_length(length)[0]
    angle = 2.0 * np.pi * np.outer(np.arange(outer), order) / length
    return (np.stack([np.cos(angle), np.sin(angle)]) / math.sqrt(length)).astype(np.float32)


def matrix_table(length, sign, left, right):
    inner = split_length(length)[1]
    angle = 2.0 * np.pi * (np.outer(left, right) % inner) / inner
    c, s = np.cos(angle), np.sin(angle)
    full = np.block([[c, sign * s], [-sign * s, c]])
    top = full.astype(jnp.bfloat16)
    return np.stack([top, (full - top.astype(np.float64)).astype(jnp.bfloat16)])


def mirror_table(length):
    inner = split_length(length)[1]
    lane = np.arange(inner)
    both = np.zeros((2, inner, inner))
    both[0, (inner - lane) % inner, lane] = 1.0
    both[1, inner - 1 - lane, lane] = 1.0
    return both.astype(jnp.bfloat16)


class Pieces:
    def __init__(self, length, rows, turned=None, top=None, low=None, grid_out=None):
        self.length, self.rows, self.half = length, rows, rows // 2
        self.outer, self.inner = split_length(length)
        self.turned, self.top, self.low, self.z = turned, top, low, grid_out
        self.step = math.gcd(rows // 2, 16)

    def chunks(self, lines, body):
        def run(i, carry):
            body(pl.multiple_of(i * self.step, self.step))
            return carry

        lax.fori_loop(0, lines // self.step, run, 0)

    def put(self, k, at, part, value):
        lanes = pl.ds(part * self.inner, self.inner)
        top, low = halves(value)
        self.top[k, at, lanes] = top
        self.low[k, at, lanes] = low

    def get(self, k, at, part):
        return self.z[k, at, pl.ds(part * self.inner, self.inner)]

    def multiply(self, lines, matrix, real_in=False, real_out=False):
        deep = self.inner if real_in else 2 * self.inner
        wide = self.inner if real_out else 2 * self.inner
        count = self.outer * lines
        top = self.top[:, :lines, :deep].reshape(count, deep)
        low = self.low[:, :lines, :deep].reshape(count, deep)
        right_top = matrix[0, :deep, :wide]
        right_low = matrix[1, :deep, :wide]
        dot = functools.partial(jnp.dot, preferred_element_type=jnp.float32)
        total = dot(top, right_top) + dot(low, right_top) + dot(top, right_low)
        self.z[:, :lines, :wide] = total.reshape(self.outer, lines, wide)

    def twist(self, k, pair, sign, twiddle, flip=None):
        c = twiddle[0, pl.ds(k, 1), :]
        s = twiddle[1, pl.ds(k, 1), :]
        if flip is not None and k % 2:
            c, s = flip * c, flip * s
        s = s if sign > 0 else -s
        re, im = pair
        return (re * c - im * s, re * s + im * c)

    def turn_full(self, source):
        rows, blocks = self.rows, TILE // self.rows
        for t in range(self.length // TILE):
            tile = source[pl.ds(t * blocks, blocks), :rows, :].reshape(TILE, 2 * rows)
            self.turned[: 2 * rows, pl.ds(t * TILE, TILE)] = tile.T

    def turn_lines(self, source):
        rows = self.rows
        groups = TILE // rows
        blocks, wide = self.inner // rows, self.inner // groups
        for t in range(self.outer):
            tile = source[pl.ds(t * blocks, blocks), :, :].reshape(wide, TILE).T
            for h in range(groups):
                self.turned[:rows, pl.ds(t * self.inner + h * wide, wide)] = tile[h * rows : (h + 1) * rows]

    def kept_lanes(self, j):
        wide = self.inner // 2
        return j * self.inner + (wide if 2 * j >= self.outer else 0), wide

    def clear_other(self, j):
        at, wide = self.kept_lanes(j)
        other = j * self.inner + (0 if 2 * j >= self.outer else wide)
        self.turned[: 2 * self.rows, pl.ds(other, wide)] = jnp.zeros((2 * self.rows, wide), jnp.float32)

    def turn_kept(self, source):
        rows, half, blocks = self.rows, self.half, self.inner // self.rows
        for j in range(self.outer):
            at, wide = self.kept_lanes(j)
            tile = source[pl.ds(j * blocks, blocks), :, :].reshape(wide, 2 * rows)
            self.turned[: 2 * rows, pl.ds(at, wide)] = tile.T
            self.clear_other(j)

    def unpack_middle(self):
        rows, middle = self.rows, (self.outer // 2) * self.inner
        first = self.turned[rows : 2 * rows, :TILE]
        lane0 = lax.broadcasted_iota(jnp.int32, first.shape, 1) == 0
        zero = jnp.zeros_like(first)
        self.turned[:rows, pl.ds(middle, TILE)] += jnp.where(lane0, first, zero)
        self.turned[rows : 2 * rows, :TILE] = jnp.where(lane0, zero, first)

    def incoming(self, lines, sign, twiddle, matrix, real_out=False):
        def body(r0):
            items = []
            for j in range(self.outer):
                lanes = pl.ds(j * self.inner, self.inner)
                items.append((
                    self.turned[pl.ds(r0, self.step), lanes],
                    self.turned[pl.ds(lines + r0, self.step), lanes],
                ))
            for k, pair in enumerate(small_dft(items, sign)):
                re, im = self.twist(k, pair, sign, twiddle)
                self.put(k, pl.ds(r0, self.step), 0, re)
                self.put(k, pl.ds(r0, self.step), 1, im)

        self.chunks(lines, body)
        self.multiply(lines, matrix, real_out=real_out)

    def outgoing(self, lines, sign, twiddle, matrix, real_in, write):
        self.multiply(lines, matrix, real_in=real_in)

        def body(r0):
            at = pl.ds(r0, self.step)
            write(r0, small_dft([
                self.twist(k, (self.get(k, at, 0), self.get(k, at, 1)), sign, twiddle)
                for k in range(self.outer)
            ], sign))

        self.chunks(lines, body)

    def pack_middle(self, items):
        re, im = items[0]
        lane0 = lax.broadcasted_iota(jnp.int32, im.shape, 1) == 0
        return [(re, jnp.where(lane0, items[self.outer // 2][0], im))] + items[1:]

    def write_full(self, result, pack):
        rows = self.rows

        def write(r0, items):
            at = pl.ds(r0, self.step)
            for j, (re, im) in enumerate(self.pack_middle(items) if pack else items):
                for piece in range(self.inner // rows):
                    to = j * (self.inner // rows) + piece
                    lanes = slice(piece * rows, (piece + 1) * rows)
                    result[to, at, pl.ds(0, rows)] = re[:, lanes]
                    result[to, at, pl.ds(rows, rows)] = im[:, lanes]

        return write

    def pack_cut(self, slabs, results):
        rows, half, wide = self.rows, self.half, self.inner // 2
        cuts, count = len(results), half // len(results)
        groups = TILE // (2 * count)
        tall = rows // groups
        for k in range(self.outer):
            slab = slabs(k)
            for s in range(self.inner // rows):
                for q, result in enumerate(results):
                    parts = []
                    for group in range(groups):
                        for part in range(2):
                            at = part * wide + s * half + q * count
                            parts.append(slab[group * tall : (group + 1) * tall, at : at + count])
                    result[k * (self.inner // rows) + s] = jnp.concatenate(parts, axis=1)

    def turn_cut(self, source, lines, spans):
        blocks = self.inner // self.rows
        groups = TILE // (2 * lines)
        wide = self.inner // groups
        for t in range(spans):
            tile = source[pl.ds(t * blocks, blocks), :, :].reshape(wide, TILE).T
            for h in range(groups):
                held = tile[h * 2 * lines : (h + 1) * 2 * lines]
                self.turned[: 2 * lines, pl.ds(t * self.inner + h * wide, wide)] = held

    def turn_whole(self, source, tiles):
        rows, blocks = self.rows, TILE // self.rows
        for t in range(tiles):
            tile = source[pl.ds(t * blocks, blocks), :rows, :].reshape(TILE, 2 * rows)
            self.turned[: 2 * rows, pl.ds(t * TILE, TILE)] = tile.T

    def first_imaginary(self, at):
        rows = self.rows
        part = self.turned[rows : 2 * rows, pl.ds(at, TILE)]
        lane0 = lax.broadcasted_iota(jnp.int32, part.shape, 1) == 0
        self.turned[rows : 2 * rows, pl.ds(at, TILE)] = jnp.where(lane0, 0.0, part)
        return jnp.where(lane0, part, 0.0)

    def incoming_half(self, lines, sign, twiddle, matrix, flip, extra=None, real_out=False):
        def body(r0):
            at = pl.ds(r0, self.step)
            items = []
            for j in range(self.outer // 2):
                lanes = pl.ds(j * self.inner, self.inner)
                items.append((self.turned[at, lanes], self.turned[pl.ds(lines + r0, self.step), lanes]))
            for k, (re, im) in enumerate(half_dft(items, sign)):
                if extra is not None:
                    re = re - extra[at, :] if k % 2 else re + extra[at, :]
                re, im = self.twist(k, (re, im), sign, twiddle, flip)
                self.put(k, at, 0, re)
                self.put(k, at, 1, im)

        self.chunks(lines, body)
        self.multiply(lines, matrix, real_out=real_out)

    def outgoing_half(self, lines, sign, twiddle, matrix, flip, write):
        self.multiply(lines, matrix)

        def body(r0):
            at = pl.ds(r0, self.step)
            write(r0, small_dft([
                self.twist(k, (self.get(k, at, 0), self.get(k, at, 1)), sign, twiddle, flip)
                for k in range(self.outer)
            ], sign)[: self.outer // 2])

        self.chunks(lines, body)

    def outgoing_sides(self, twiddle, matrix, sides, late=None):
        self.multiply(self.rows, matrix, real_in=True)
        rows, half, blocks, middle = self.rows, self.half, self.inner // self.rows, self.outer // 2
        tall, step = rows * rows // TILE, self.step
        for h in range(rows // tall):

            def body(i, carry, h=h):
                r0 = pl.multiple_of(i * step, step)
                at = pl.ds(h * tall + r0, step)
                items = small_dft([
                    self.twist(k, (self.get(k, at, 0), self.get(k, at, 1)), -1.0, twiddle)
                    for k in range(self.outer)
                ], -1.0)
                (low, low_im), (high, high_im) = items[0], items[middle]
                lane0 = lax.broadcasted_iota(jnp.int32, low.shape, 1) == 0
                items[0] = (low, jnp.where(lane0, high, low_im))
                items[middle] = (high, jnp.where(lane0, low, high_im))
                if late is not None:
                    items = [
                        tuple(jnp.where(late, one, other) for one, other in zip(items[middle + j], items[j]))
                        for j in range(middle)
                    ]
                for j, pair in enumerate(items):
                    for part, value in enumerate(pair):
                        to = pl.ds(h * rows + part * half, half)
                        for piece in range(blocks):
                            for side, result in enumerate(sides):
                                base = piece * rows + side * half
                                result[j * blocks + piece, pl.ds(r0, step), to] = value[:, base : base + half]
                return carry

            lax.fori_loop(0, tall // step, body, 0)

    def outgoing_kept(self, twiddle, matrix, result):
        self.multiply(self.rows, matrix, real_in=True)
        rows, half, blocks = self.rows, self.half, self.inner // self.rows
        tall = rows * rows // TILE
        step = math.gcd(rows, 16)
        span = min(tall, step)
        for h in range(rows // max(tall, step)):

            def body(i, carry, h=h):
                r0 = i * step if isinstance(i, int) else pl.multiple_of(i * step, step)
                at = pl.ds(h * max(tall, step) + r0, step)
                items = self.pack_middle(small_dft([
                    self.twist(k, (self.get(k, at, 0), self.get(k, at, 1)), -1.0, twiddle)
                    for k in range(self.outer)
                ], -1.0))
                for j, pair in enumerate(items):
                    base = self.inner // 2 if 2 * j >= self.outer else 0
                    for piece in range(blocks):
                        lanes = slice(base + piece * half, base + (piece + 1) * half)
                        for part, value in enumerate(pair):
                            for sub in range(step // span):
                                group = h * (step // span) + sub
                                to = pl.ds(group * rows + part * half, half)
                                held = value[sub * span : (sub + 1) * span, lanes]
                                result[j * blocks + piece, pl.ds(r0, span), to] = held
                return carry

            if tall > step:
                lax.fori_loop(0, tall // step, body, 0)
            else:
                body(0, 0)

    def mirrored(self, blocks, mirror):
        dot = functools.partial(jnp.dot, preferred_element_type=jnp.float32)

        def flip(values, which):
            top, low = halves(jnp.concatenate(values, axis=0))
            return dot(top, mirror[which]) + dot(low, mirror[which])

        flat = [part for k in range(self.outer) for pair in blocks[k] for part in pair]
        per = 2 * len(blocks[0])
        low = flip(flat[:per], 0)
        high = flip(flat[per:], 1)
        out = []
        for k in range(self.outer):
            part, base = (low, 0) if k == 0 else (high, (self.outer - k - 1) * per)
            take = lambda i: part[(base + i) * 8 : (base + i + 1) * 8]
            out.append([(take(2 * i), -take(2 * i + 1)) for i in range(per // 2)])
        return out

    def pack_columns(self, slabs, result):
        rows, half, wide = self.rows, self.half, self.inner // 2
        blocks, groups = self.inner // rows, TILE // rows
        tall = rows // groups
        for k in range(self.outer):
            slab = slabs(k)
            for s in range(blocks):
                parts = []
                for group in range(groups):
                    for part in range(2):
                        at = part * wide + s * half
                        parts.append(slab[group * tall : (group + 1) * tall, at : at + half])
                result[k * blocks + s] = jnp.concatenate(parts, axis=1)

    def turn_columns(self, source, result):
        rows, wide, blocks = self.rows, self.inner // 2, self.inner // self.rows
        for j in range(self.outer):
            tile = source[pl.ds(j * blocks, blocks), :, :].reshape(wide, 2 * rows).T
            result[j, :, pl.ds(0, wide)] = tile[:rows]
            result[j, :, pl.ds(wide, wide)] = tile[rows:]

    def spread(self, first, second, strided, result):
        rows, fill = self.rows, TILE - 2 * self.rows
        for t in range(self.length // TILE):
            lanes = pl.ds(t * TILE, TILE)
            parts = [first[:, lanes], second[:, lanes]]
            if fill:
                parts.append(jnp.zeros((fill, TILE), jnp.float32))
            strided[pl.ds(t * TILE, TILE), :] = jnp.concatenate(parts, axis=0).T
        for k in range(self.outer):
            slab = strided[pl.ds(k, self.inner, stride=self.outer), :].T
            result[k] = slab[: 2 * rows, :]

    def collect(self, slabs, strided, results):
        rows = self.rows
        for k in range(self.outer):
            slab = slabs(k)
            fill = TILE - slab.shape[0]
            if fill:
                slab = jnp.concatenate([slab, jnp.zeros((fill, self.inner), jnp.float32)], axis=0)
            strided[pl.ds(k, self.inner, stride=self.outer), :] = slab.T
        for t in range(self.length // TILE):
            block = strided[pl.ds(t * TILE, TILE), :].T
            for i, result in enumerate(results):
                result[:, pl.ds(t * TILE, TILE)] = block[i * rows : (i + 1) * rows, :]


def signed_waves(position, count):
    signed = jnp.where(position < count // 2, position, position - count)
    waves = 4.0 * signed.astype(jnp.float32) / count
    return waves, jnp.where(position == count // 2, jnp.float32(0.0), waves)


def first_waves(piece, k):
    lanes = lax.broadcasted_iota(jnp.int32, (1, piece.inner), 1)
    return signed_waves(piece.outer * lanes + k, piece.length)


def inverse_denominator(wave_first, wave_second):
    square = wave_first * wave_first + wave_second * wave_second
    return 1.0 / (1.0 + time_step * (square * square - square))


def second_wave(piece, position):
    shape = (position.shape[0], piece.inner)
    return jnp.broadcast_to(signed_waves(position, piece.length)[0], shape)


def row_index(count, width):
    return lax.broadcasted_iota(jnp.int32, (count, width), 0)


class Links:
    def __init__(self, devices, fast):
        self.devices, self.fast = devices, fast
        self.device = lax.axis_index(axes[0]) * fast + lax.axis_index(axes[1])

    def partner(self, i):
        total, bit = 0, 1
        while bit < self.devices:
            total += bit * lax.rem(lax.div(self.device, bit) + lax.div(i, bit), 2)
            bit *= 2
        return total

    def send(self, source, target, sems, count):
        send_sem, recv_sem, own_sem = sems
        own = lax.rem(self.device, count)

        def go(i, carry):
            peer = self.partner(count - i)
            pltpu.make_async_remote_copy(
                src_ref=source(lax.rem(peer, count)),
                dst_ref=target(own),
                send_sem=send_sem,
                recv_sem=recv_sem,
                device_id=(lax.div(peer, self.fast), lax.rem(peer, self.fast)),
                device_id_type=pl.DeviceIdType.MESH,
            ).start()
            return carry

        lax.fori_loop(1, count, go, 0)
        pltpu.make_async_copy(source(own), target(own), own_sem).start()

    def whole(self, source, target, sems, count):
        others = pl.ds(0, count - 1)
        return pltpu.make_async_remote_copy(
            src_ref=source(others),
            dst_ref=target(others),
            send_sem=sems[0],
            recv_sem=sems[1],
            device_id=(0, 0),
            device_id_type=pl.DeviceIdType.MESH,
        )

    def receive(self, source, target, sems, count):
        own = lax.rem(self.device, count)
        pltpu.make_async_copy(source(own), target(own), sems[2]).wait()
        self.whole(source, target, sems, count).wait_recv()

    def sent(self, source, target, sems, count):
        self.whole(source, target, sems, count).wait_send()


def start_kernel(length, rows, field, target, out, both_p, *scratch):
    piece = Pieces(length, rows)
    piece.spread(field, target, scratch[0], both_p)
    piece.pack_columns(lambda k: both_p[k, pl.ds(0, rows), :], out)


def slope_second_kernel(length, rows, field_p, twiddle, out_matrix, in_matrix, kept, result, *scratch):
    piece = Pieces(length, rows, *scratch)

    def body(r0):
        at = pl.ds(r0, piece.step)
        for k in range(piece.outer):
            piece.put(k, at, 0, field_p[k, at, :])

    piece.chunks(rows, body)
    for j in range(piece.outer):
        piece.clear_other(j)

    def write(r0, items):
        for j, (re, im) in enumerate(items):
            at, wide = piece.kept_lanes(j)
            base = at - j * piece.inner
            position = j * piece.inner + kept[:, base : base + wide]
            slope = 2.0 * signed_waves(position, length)[1]
            piece.turned[pl.ds(r0, piece.step), pl.ds(at, wide)] = -slope * im[:, base : base + wide]
            piece.turned[pl.ds(rows + r0, piece.step), pl.ds(at, wide)] = slope * re[:, base : base + wide]

    piece.outgoing(rows, -1.0, twiddle, out_matrix, True, write)
    piece.incoming(rows, 1.0, twiddle, in_matrix, real_out=True)
    result[...] = piece.z[:, :, : piece.inner]


def spread_kernel(length, rows, forcing, result, strided):
    Pieces(length, rows).spread(forcing.at[0], forcing.at[1], strided, result)


def collect_kernel(length, rows, slabs, result, strided):
    piece = Pieces(length, rows)
    piece.collect(lambda k: slabs[k], strided, [result.at[i] for i in range(result.shape[0])])


def weight_of(device, r0, step, inner):
    alone = (row_index(step, inner) + r0 + device) == 0
    return jnp.where(alone, jnp.float32(1.0), jnp.float32(2.0))


def slope_first_kernel(length, rows, source, in_twiddle, in_matrix, out_twiddle, out_matrix, out, *scratch):
    piece = Pieces(length, rows, *scratch)
    half = piece.half
    piece.turn_lines(source)
    piece.incoming(half, -1.0, in_twiddle, in_matrix)

    def body(r0):
        at = pl.ds(r0, piece.step)
        for k in range(piece.outer):
            re, im = piece.get(k, at, 0), piece.get(k, at, 1)
            scale = first_waves(piece, k)[1]
            piece.put(k, at, 0, -scale * im)
            piece.put(k, at, 1, scale * re)

    piece.chunks(half, body)
    piece.outgoing(half, 1.0, out_twiddle, out_matrix, False, piece.write_full(out, False))


def edge_inverses(piece, k):
    wave_first = first_waves(piece, k)[0]
    middle = jnp.full((1, 1), piece.length // 2, jnp.int32)
    zero = jnp.zeros((1, 1), jnp.int32)
    return [inverse_denominator(wave_first, signed_waves(p, piece.length)[0]) for p in (zero, middle)]


def next_kernel(length, rows, device_ref, source, forcing, in_twiddle, in_matrix, out_twiddle, out_matrix, mirror, out, *scratch):
    device = device_ref[0]
    piece = Pieces(length, rows, *scratch)
    half, step, inner = piece.half, piece.step, piece.inner
    late = device >= (length // rows) // 2
    piece.turn_lines(source)
    piece.incoming(half, -1.0, in_twiddle, in_matrix)

    def body(r0):
        at, also = pl.ds(r0, step), pl.ds(half + r0, step)
        index = row_index(step, 1) + r0
        low_wave = second_wave(piece, device * rows + index)
        high_wave = second_wave(piece, device * rows + half + index)
        moved = jnp.logical_and(row_index(step, inner) + r0 == 0, late)
        weight = weight_of(device, r0, step, inner)
        for k in range(piece.outer):
            wave_first = first_waves(piece, k)[0]
            low = inverse_denominator(wave_first, low_wave)
            high = inverse_denominator(wave_first, high_wave)
            for part in range(2):
                own = weight * piece.get(k, at, part)
                f_low = time_step * forcing[k, pl.ds(part * rows + r0, step), :]
                f_high = time_step * forcing[k, pl.ds(part * rows + half + r0, step), :]
                piece.put(k, at, part, (f_low + jnp.where(moved, 0.0, own)) * low)
                piece.put(k, also, part, (f_high + jnp.where(moved, own, 0.0)) * high)

    piece.chunks(half, body)

    @pl.when(device == 0)
    def _():
        at = pl.ds(0, 8)
        blocks = []
        for k in range(piece.outer):
            own = tuple(piece.get(k, at, part) for part in range(2))
            full = tuple(
                own[part] + time_step * forcing[k, pl.ds(part * rows, 8), :] for part in range(2)
            )
            blocks.append([own, full])
        flipped = piece.mirrored(blocks, mirror)
        rest = pl.ds(0, 16)
        row0 = row_index(16, inner) == 0
        for k in range(piece.outer):
            zero, middle = edge_inverses(piece, k)
            for part in range(2):
                own, full = blocks[k][0][part], blocks[k][1][part]
                own_c, full_c = flipped[k][0][part], flipped[k][1][part]
                value = 0.5 * ((full + full_c) * zero + (own - own_c) * middle)
                replace(piece, k, part, value)

    piece.outgoing(rows, 1.0, out_twiddle, out_matrix, False, piece.write_full(out, False))


def replace(piece, k, part, value):
    lanes = pl.ds(part * piece.inner, piece.inner)
    row0 = row_index(16, piece.inner) == 0
    value = jnp.concatenate([value, value], axis=0)
    for held, new in zip((piece.top, piece.low), halves(value)):
        old = held[k, pl.ds(0, 16), lanes].astype(jnp.float32)
        held[k, pl.ds(0, 16), lanes] = jnp.where(row0, new.astype(jnp.float32), old).astype(jnp.bfloat16)


def misfit_kernel(length, rows, device_ref, source, in_twiddle, in_matrix, out_twiddle, out_matrix, mirror, out, full, total_out, *scratch):
    device = device_ref[0]
    piece = Pieces(length, rows, *scratch)
    half, step, inner = piece.half, piece.step, piece.inner
    late = device >= (length // rows) // 2
    piece.turn_full(source)
    piece.incoming(rows, -1.0, in_twiddle, in_matrix)

    def body(r0):
        at, also = pl.ds(r0, step), pl.ds(half + r0, step)
        index = row_index(step, 1) + r0
        low_wave = second_wave(piece, device * rows + index)
        high_wave = second_wave(piece, device * rows + half + index)
        moved = jnp.logical_and(row_index(step, inner) + r0 == 0, late)
        weight = weight_of(device, r0, step, inner)
        for k in range(piece.outer):
            wave_first = first_waves(piece, k)[0]
            low = time_step * inverse_denominator(wave_first, low_wave)
            high = time_step * inverse_denominator(wave_first, high_wave)
            for part in range(2):
                low_value = piece.get(k, at, part) * low
                high_value = piece.get(k, also, part) * high
                full[k, pl.ds(part * rows + r0, step), :] = low_value
                full[k, pl.ds(part * rows + half + r0, step), :] = high_value
                own = jnp.where(moved, high_value, low_value)
                piece.put(k, at, part, weight * own)

    piece.chunks(half, body)

    @pl.when(device == 0)
    def _():
        at = pl.ds(0, 8)
        blocks = [[(piece.get(k, at, 0), piece.get(k, at, 1))] for k in range(piece.outer)]
        flipped = piece.mirrored(blocks, mirror)
        row0 = row_index(8, inner) == 0
        for k in range(piece.outer):
            zero, middle = edge_inverses(piece, k)
            for part in range(2):
                own, own_c = blocks[k][0][part], flipped[k][0][part]
                first = (0.5 * time_step) * (own + own_c) * zero
                value = first + (0.5 * time_step) * (own - own_c) * middle
                at_full = pl.ds(part * rows, 8)
                full[k, at_full, :] = jnp.where(row0, first, full[k, at_full, :])
                replace(piece, k, part, value)

    piece.outgoing(half, 1.0, out_twiddle, out_matrix, False, piece.write_full(out, False))
    total_out[...] = jnp.sum(source[:, pl.ds(rows, 8), :], axis=0)


def nonlinear_kernel(length, rows, source, both_p, second, twiddle, out_matrix, out, first, *scratch):
    piece = Pieces(length, rows, *scratch)
    piece.turn_columns(source, first)

    def body(r0):
        at = pl.ds(r0, piece.step)
        for k in range(piece.outer):
            one, other = first[k, at, :], second[k, at, :]
            piece.put(k, at, 0, both_p[k, at, :] - (0.5 * time_step) * (one * one + other * other))

    piece.chunks(rows, body)
    piece.outgoing_kept(twiddle, out_matrix, out)


def joint_kernel(length, rows, source, first, second, twiddle, in_matrix, out, value_out, second_out, *scratch):
    piece = Pieces(length, rows, *scratch)
    piece.turn_kept(source)
    piece.unpack_middle()
    piece.incoming(rows, 1.0, twiddle, in_matrix, real_out=True)
    lanes = pl.ds(0, piece.inner)

    def body(r0):
        at = pl.ds(r0, piece.step)
        for k in range(piece.outer):
            value = piece.get(k, at, 0)
            value_out[k, at, :] = (1.0 / time_step) * value
            second_out[k, at, :] = value * second[k, at, :]
            piece.z[k, at, lanes] = value * first[k, at, :]

    piece.chunks(rows, body)
    piece.pack_columns(lambda k: piece.z[k, pl.ds(0, rows), lanes], out)


def residual_kernel(length, rows, source, both_p, twiddle, in_matrix, out_matrix, out, field_out, *scratch):
    piece = Pieces(length, rows, *scratch[:4])
    strided, total = scratch[4:]
    piece.turn_full(source)
    piece.unpack_middle()
    piece.incoming(rows, 1.0, twiddle, in_matrix, real_out=True)
    piece.collect(lambda k: piece.get(k, pl.ds(0, rows), 0), strided, [field_out])
    total[...] = jnp.zeros_like(total)

    def body(r0):
        at = pl.ds(r0, piece.step)
        for k in range(piece.outer):
            residual = piece.get(k, at, 0) - both_p[k, pl.ds(rows + r0, piece.step), :]
            total[...] += residual * residual
            piece.put(k, at, 0, residual)

    piece.chunks(rows, body)
    piece.outgoing(rows, -1.0, twiddle, out_matrix, True, piece.write_full(out, True))
    value = 0.5 * jnp.sum(total[...])
    out[:, pl.ds(rows, 8), :] = jnp.full((out.shape[0], 8, 2 * rows), value, jnp.float32)


def last_kernel(length, rows, source, value, second, field_out, strided, first):
    piece = Pieces(length, rows)
    piece.turn_columns(source, first)
    piece.collect(lambda k: first[k] + value[k] + second[k], strided, [field_out])


def step_kernel(length, rows, devices, fast, cuts, inputs, outs, box):
    links = Links(devices, fast)
    device, half, part_devices = links.device, rows // 2, devices // 2
    late = device >= part_devices
    flip = jnp.where(late, -1.0, 1.0).astype(jnp.float32)
    sides = range(2)
    copies, sems = box.copies, box.sems
    work = (box.turned, box.top, box.low, box.z)
    piece = Pieces(length, rows, *work)
    step, inner, outer = piece.step, piece.inner, piece.outer
    both_p, forcing_p, full = box.both_p, box.forcing_p, box.full
    first, second, value = box.first, box.second, box.value
    strided, total = box.strided, box.total
    lanes = pl.ds(0, inner)

    loads = [
        pltpu.make_async_copy(ref, held, copies.at[i])
        for i, (ref, held) in enumerate(zip(inputs.refs, inputs.held))
    ]
    for copy in loads[:2]:
        copy.start()
    waiting = iter(loads)

    def load(count):
        for i in range(count):
            next(waiting).wait()

    at_all = lambda ref: lambda e: ref.at[e]
    at_lines = lambda ref, base, count: lambda e: ref.at[e, pl.ds(base, count)]
    order = []

    def send(source, target, count=devices):
        i = len(order)
        order.append((source, target, (sems.at[i, 0], sems.at[i, 1], sems.at[i, 2]), count))
        links.send(*order[-1])
        return order[-1]

    def receive(*moves):
        for move in moves:
            links.receive(*move)

    tw_natural, tw_kept, tw_lines, tw_cut = (inputs.twiddles.at[i] for i in range(4))
    forward, backward, mirror = inputs.forward, inputs.backward, inputs.mirror
    kept_out, kept_in, kept = inputs.kept_out, inputs.kept_in, inputs.kept
    lines_in, cut_in = box.lines_in, box.cut_in

    def permute_rows(groups, result):
        tall, blocks = rows // groups, inner // rows
        for p in range(2):
            for part in range(2):
                for group in range(groups):
                    for s in range(blocks):
                        at = part * inner + group * (inner // groups) + s * tall
                        source = part * inner + s * rows + group * tall
                        result[p, pl.ds(at, tall), :] = forward[p, pl.ds(source, tall), :]

    def slope_first(source, out, lines):
        piece.turn_cut(source, lines, outer)
        piece.incoming(lines, -1.0, tw_cut, cut_in)

        def body(r0):
            at = pl.ds(r0, step)
            for k in range(outer):
                re, im = piece.get(k, at, 0), piece.get(k, at, 1)
                scale = first_waves(piece, k)[1]
                piece.put(k, at, 0, -scale * im)
                piece.put(k, at, 1, scale * re)

        piece.chunks(lines, body)
        piece.outgoing(lines, 1.0, tw_natural, backward, False, piece.write_full(out, False))

    def slope_second(source, out):
        slope_second_kernel(length, rows, source, tw_kept, kept_out, kept_in, kept, out, *work)

    def send_columns(source, target):
        return [send(at_all(source.at[q]), at_all(target.at[q])) for q in range(cuts)]

    def turn_slopes(moves, source, back, target):
        count, result = half // cuts, []
        for q, move in enumerate(moves):
            receive(move)
            slope_first(source.at[q], back.at[q], count)
            result.append(send(at_all(back.at[q]), at_lines(target, q * count, count)))
        return result

    def lines_of(side, r0):
        line = row_index(step, 1) + r0 + side * half
        alone = (row_index(step, inner) + r0 + side * half + lax.rem(device, part_devices)) == 0
        return second_wave(piece, device * rows + line), jnp.where(alone, jnp.float32(1.0), jnp.float32(2.0))

    def edges(k):
        wave = first_waves(piece, k)[0]
        middle = jnp.full((1, 1), length // 2, jnp.int32)
        mine, theirs = jnp.where(late, middle, 0), jnp.where(late, 0, middle)
        return [inverse_denominator(wave, signed_waves(p, length)[0]) for p in (mine, theirs)]

    load(2)
    for copy in loads[2:]:
        copy.start()
    piece.spread(inputs.field, inputs.target, strided, both_p)
    piece.pack_cut(lambda k: both_p[k, pl.ds(0, rows), :], [box.s_field.at[q] for q in range(cuts)])
    m_field = send_columns(box.s_field, box.r_field)

    load(len(loads) - 2)
    permute_rows(TILE // rows, lines_in)
    permute_rows(TILE * cuts // rows, cut_in)
    slope_second(both_p, second)
    m_slope = turn_slopes(m_field, box.r_field, box.s_slope, box.r_slope)
    piece.spread(inputs.forcing.at[0], inputs.forcing.at[1], strided, forcing_p)

    receive(*m_slope)
    piece.turn_columns(box.r_slope, first)

    def nonlinear(r0):
        at = pl.ds(r0, step)
        for k in range(outer):
            one, other = first[k, at, :], second[k, at, :]
            piece.put(k, at, 0, both_p[k, at, :] - (0.5 * time_step) * (one * one + other * other))

    piece.chunks(rows, nonlinear)
    piece.outgoing_sides(tw_natural, forward, [box.s_sum.at[side] for side in sides], late)
    m_sum = [send(at_all(box.s_sum.at[side]), at_all(box.r_sum.at[side]), part_devices) for side in sides]

    def divide(side):
        def body(r0):
            at = pl.ds(r0, step)
            wave, weight = lines_of(side, r0)
            for k in range(outer):
                scale = inverse_denominator(first_waves(piece, k)[0], wave)
                for part in range(2):
                    forced = time_step * forcing_p[k, pl.ds(part * rows + side * half + r0, step), :]
                    piece.put(k, at, part, (weight * piece.get(k, at, part) + forced) * scale)

        piece.chunks(half, body)
        if side:
            return

        @pl.when(lax.rem(device, part_devices) == 0)
        def _():
            at = pl.ds(0, 8)
            blocks = []
            for k in range(outer):
                own = tuple(piece.get(k, at, part) for part in range(2))
                joined = tuple(own[part] + time_step * forcing_p[k, pl.ds(part * rows, 8), :] for part in range(2))
                blocks.append([own, joined])
            flipped = piece.mirrored(blocks, mirror)
            for k in range(outer):
                mine, theirs = edges(k)
                for part in range(2):
                    own, joined = blocks[k][0][part], blocks[k][1][part]
                    own_c, joined_c = flipped[k][0][part], flipped[k][1][part]
                    replace(piece, k, part, 0.5 * ((joined + joined_c) * mine + (own - own_c) * theirs))

    m_next = []
    for side in sides:
        receive(m_sum[side])
        piece.turn_cut(box.r_sum.at[side], half, outer // 2)
        piece.incoming_half(half, -1.0, tw_lines, lines_in, flip)
        divide(side)
        sent = box.s_next.at[side]
        piece.outgoing(half, 1.0, tw_natural, backward, False, piece.write_full(sent, False))
        m_next.append(send(at_all(sent), at_lines(box.r_next, side * half, half)))

    receive(*m_next)
    piece.turn_whole(box.r_next, length // TILE)
    low, high = piece.first_imaginary(0), piece.first_imaginary(length // 2)
    piece.turned[:rows, pl.ds(0, TILE)] += high
    piece.turned[:rows, pl.ds(length // 2, TILE)] += low
    piece.incoming(rows, 1.0, tw_natural, backward, real_out=True)
    total[...] = jnp.zeros_like(total)

    def misfit(r0):
        at = pl.ds(r0, step)
        for k in range(outer):
            now = piece.get(k, at, 0)
            value[k, at, :] = now
            residual = now - both_p[k, pl.ds(rows + r0, step), :]
            total[...] += residual * residual
            piece.put(k, at, 0, residual)

    piece.chunks(rows, misfit)
    piece.outgoing_sides(tw_natural, forward, [box.s_kept.at[side] for side in sides])
    m_kept = [send(at_all(box.s_kept.at[side]), at_all(box.r_kept.at[side])) for side in sides]
    box.s_total[...] = jnp.full(box.s_total.shape, 0.5 * jnp.sum(total[...]), jnp.float32)
    m_total = send(at_all(box.s_total), at_all(box.r_total))
    piece.collect(lambda k: value[k], strided, [outs.next])

    def adjoint(side):
        def body(r0):
            at = pl.ds(r0, step)
            wave, weight = lines_of(side, r0)
            for k in range(outer):
                scale = time_step * inverse_denominator(first_waves(piece, k)[0], wave)
                for part in range(2):
                    own = piece.get(k, at, part) * scale
                    full[k, pl.ds(part * rows + side * half + r0, step), :] = own
                    piece.put(k, at, part, weight * own)

        piece.chunks(half, body)
        if side:
            return

        @pl.when(lax.rem(device, part_devices) == 0)
        def _():
            at = pl.ds(0, 8)
            blocks = [[(piece.get(k, at, 0), piece.get(k, at, 1))] for k in range(outer)]
            flipped = piece.mirrored(blocks, mirror)
            row0 = row_index(8, inner) == 0
            for k in range(outer):
                mine, theirs = edges(k)
                for part in range(2):
                    own, own_c = blocks[k][0][part], flipped[k][0][part]
                    line = (0.5 * time_step) * (own + own_c) * mine
                    at_full = pl.ds(part * rows, 8)
                    full[k, at_full, :] = jnp.where(row0, line, full[k, at_full, :])
                    replace(piece, k, part, line + (0.5 * time_step) * (own - own_c) * theirs)

    m_back = []
    for side in sides:
        receive(m_kept[side])
        piece.turn_cut(box.r_kept.at[side], half, outer)
        piece.incoming(half, -1.0, tw_lines, lines_in)
        adjoint(side)
        sent = box.s_back.at[side]
        piece.outgoing_half(half, 1.0, tw_natural, backward, flip, piece.write_full(sent, False))
        m_back.append(send(at_all(sent), at_lines(box.r_back, side * half, half), part_devices))

    receive(*m_back)
    piece.turn_whole(box.r_back, length // (2 * TILE))
    box.extra[:, pl.ds(0, TILE)] = piece.first_imaginary(0)
    box.extra[:, pl.ds(TILE, inner - TILE)] = jnp.zeros((rows, inner - TILE), jnp.float32)
    piece.incoming_half(rows, 1.0, tw_natural, backward, flip, box.extra, real_out=True)

    def products(r0):
        at = pl.ds(r0, step)
        for k in range(outer):
            now = piece.get(k, at, 0)
            value[k, at, :] = (1.0 / time_step) * now
            box.product[k, at, :] = now * second[k, at, :]
            piece.z[k, at, lanes] = now * first[k, at, :]

    piece.chunks(rows, products)
    piece.pack_cut(lambda k: piece.z[k, pl.ds(0, rows), lanes], [box.s_product.at[q] for q in range(cuts)])
    m_product = send_columns(box.s_product, box.r_product)
    slope_second(box.product, second)
    for k in range(outer):
        value[k] = value[k] + second[k]
    m_last = turn_slopes(m_product, box.r_product, box.s_last, box.r_last)

    piece.collect(lambda k: full[k], strided, [outs.forcing.at[i] for i in range(2)])
    receive(m_total)
    outs.total[...] = jnp.sum(box.r_total[...], axis=0) / (length * length)

    receive(*m_last)
    piece.turn_columns(box.r_last, first)
    for k in range(outer):
        outs.field[k] = first[k] + value[k]
    for move in order:
        links.sent(*move)


def joined_step(field, target, forcing, devices, fast, rows, length):
    outer, inner = split_length(length)
    half, step, cuts = rows // 2, math.gcd(rows // 2, 16), 2
    natural, kept, lines = orders(length, rows)
    cut = line_order(inner, rows, TILE * cuts // rows)
    matrix = lambda *args: matrix_table(length, *args)
    tables = dict(
        field=field, target=target,
        twiddles=np.stack([twiddle_table(length, o) for o in (natural, kept, lines, cut)]),
        kept=kept[None, :].astype(np.int32),
        kept_out=matrix(-1.0, natural, kept)[:, :inner],
        kept_in=matrix(1.0, kept, natural)[:, :, :inner],
        forcing=forcing,
        backward=matrix(1.0, natural, natural),
        forward=matrix(-1.0, natural, natural),
        mirror=mirror_table(length),
    )
    operands = [jnp.asarray(table) for table in tables.values()]
    float32 = jnp.float32
    held = lambda *dims: pltpu.VMEM(dims, float32)
    packed, lined = held(2, devices, rows * rows // TILE, TILE), held(2, devices, half, 2 * rows)
    packed_half, lined_half = (held(2, devices // 2, *dims.shape[2:]) for dims in (packed, lined))
    columns, slopes = held(cuts, devices, rows * rows // (TILE * cuts), TILE), held(cuts, devices, half // cuts, 2 * rows)
    returned = held(devices, half, 2 * rows)
    table = pltpu.VMEM((2, 2 * inner, 2 * inner), jnp.bfloat16)
    pair, one = held(outer, 2 * rows, inner), held(outer, rows, inner)
    small = held(devices, 8, TILE)
    halved = pltpu.VMEM((outer, rows, 2 * inner), jnp.bfloat16)
    shapes = dict(
        turned=held(2 * rows, length), top=halved, low=halved, z=held(outer, rows, 2 * inner),
        strided=held(length, TILE), total=held(step, inner),
        both_p=pair, forcing_p=pair, full=pair, first=one, second=one, value=one, product=one,
        lines_in=table, cut_in=table, extra=held(rows, inner),
        s_field=columns, r_field=columns, s_slope=slopes, r_slope=returned,
        s_sum=packed_half, r_sum=packed_half, s_next=lined, r_next=held(devices, rows, 2 * rows),
        s_kept=packed, r_kept=packed, s_total=small, r_total=small,
        s_back=lined_half, r_back=held(devices // 2, rows, 2 * rows),
        s_product=columns, r_product=columns, s_last=slopes, r_last=returned,
        copies=pltpu.SemaphoreType.DMA((len(operands),)),
        sems=pltpu.SemaphoreType.DMA((9 + 4 * cuts, 3)),
    )
    inputs = [pltpu.VMEM(operand.shape, operand.dtype) for operand in operands]

    def body(*refs):
        a, b = len(operands), len(operands) + 4
        c = b + len(operands)
        given = SimpleNamespace(refs=refs[:a], held=refs[b:c], **dict(zip(tables, refs[b:c])))
        outs = SimpleNamespace(next=refs[a], field=refs[a + 1], forcing=refs[a + 2], total=refs[a + 3])
        step_kernel(length, rows, devices, fast, cuts, given, outs, SimpleNamespace(**dict(zip(shapes, refs[c:]))))

    anywhere = pl.BlockSpec(memory_space=pl.ANY)
    vmem, smem = pl.BlockSpec(memory_space=pltpu.VMEM), pl.BlockSpec(memory_space=pltpu.SMEM)
    shape = lambda *dims: jax.ShapeDtypeStruct(dims, float32)
    next_field, slabs, forcing_grad, total = pl.pallas_call(
        body,
        out_shape=(shape(rows, length), shape(outer, rows, inner), shape(2, rows, length), shape(8, TILE)),
        in_specs=[pl.BlockSpec(memory_space=pltpu.HBM)] * len(operands),
        out_specs=(vmem, vmem, vmem, vmem),
        scratch_shapes=inputs + list(shapes.values()),
        compiler_params=pltpu.CompilerParams(vmem_limit_bytes=34 * 2**20, has_side_effects=True),
        cost_estimate=pl.CostEstimate(flops=6 * 10**10, bytes_accessed=4 * 2**20, transcendentals=0),
    )(*[pltpu.with_memory_space_constraint(one, pltpu.HBM) for one in operands])
    return pl.pallas_call(
        functools.partial(tail_kernel, length, rows),
        out_shape=(shape(rows, length), shape(rows, length), shape(2, rows, length), shape(1, 1)),
        in_specs=[vmem] * 4,
        out_specs=(anywhere, anywhere, anywhere, smem),
        scratch_shapes=[held(length, TILE), held(rows, length), pltpu.SemaphoreType.DMA((3,))],
        compiler_params=pltpu.CompilerParams(vmem_limit_bytes=8 * 2**20),
        cost_estimate=pl.CostEstimate(flops=10**9, bytes_accessed=4 * 2**20, transcendentals=0),
    )(next_field, slabs, forcing_grad, total)


def tail_kernel(length, rows, next_field, slabs, forcing_grad, total, next_out, field_out, forcing_out, total_out, strided, held, sems):
    piece = Pieces(length, rows)
    copies = [
        pltpu.make_async_copy(next_field, next_out, sems.at[0]),
        pltpu.make_async_copy(forcing_grad, forcing_out, sems.at[1]),
        pltpu.make_async_copy(held, field_out, sems.at[2]),
    ]
    copies[0].start()
    copies[1].start()
    total_out[0, 0] = jnp.sum(total[0:1, 0:1])
    piece.collect(lambda k: slabs[k], strided, [held])
    copies[2].start()
    for copy in copies:
        copy.wait()


def member_step(device, field, target, forcing_p, devices, rows, length):
    outer, inner = split_length(length)
    half = rows // 2
    float32 = jnp.float32
    shape = lambda *dims: jax.ShapeDtypeStruct(dims, float32)
    kept_blocks = shape(devices, rows * rows // TILE, TILE)
    half_blocks = shape(devices, half, 2 * rows)
    blocks = shape(devices, rows, 2 * rows)
    longer = shape(devices, rows + 8, 2 * rows)
    pair, one = shape(outer, 2 * rows, inner), shape(outer, rows, inner)
    plain = shape(rows, length)
    step = math.gcd(half, 16)
    base = [
        pltpu.VMEM((2 * rows, length), float32),
        pltpu.VMEM((outer, rows, 2 * inner), jnp.bfloat16),
        pltpu.VMEM((outer, rows, 2 * inner), jnp.bfloat16),
        pltpu.VMEM((outer, rows, 2 * inner), float32),
    ]
    strided = pltpu.VMEM((length, TILE), float32)
    total = pltpu.VMEM((step, inner), float32)
    vmem = pl.BlockSpec(memory_space=pltpu.VMEM)
    smem = pl.BlockSpec(memory_space=pltpu.SMEM)

    natural, kept, lines = orders(length, rows)
    tw_natural, tw_kept, tw_lines = [jnp.asarray(twiddle_table(length, o)) for o in (natural, kept, lines)]
    matrix = lambda *args: matrix_table(length, *args)
    forward, backward = matrix(-1.0, natural, natural), matrix(1.0, natural, natural)
    kept_out, kept_in = matrix(-1.0, natural, kept)[:, :inner], matrix(1.0, kept, natural)[:, :, :inner]
    lines_in = matrix(-1.0, lines, natural)
    mirror = jnp.asarray(mirror_table(length))
    kept_lane = jnp.asarray(kept[None, :].astype(np.int32))

    def call(body, outs, scratch, *operands):
        return pl.pallas_call(
            functools.partial(body, length, rows),
            out_shape=outs,
            in_specs=[smem if operand is device else vmem for operand in operands],
            out_specs=jax.tree.map(lambda leaf: vmem, outs),
            scratch_shapes=scratch,
            compiler_params=pltpu.CompilerParams(vmem_limit_bytes=20 * 2**20),
            cost_estimate=pl.CostEstimate(flops=6 * 10**9, bytes_accessed=4 * 2**20, transcendentals=0),
        )(*operands)

    def move(value):
        return lax.all_to_all(value, axes, split_axis=0, concat_axis=0, tiled=True)

    spectral_tables = (tw_lines, lines_in, tw_natural, backward)
    slope_tables = (tw_kept, kept_out, kept_in, kept_lane)
    sent, both_p = call(start_kernel, (kept_blocks, pair), [strided], field, target)
    second = call(slope_second_kernel, one, base, both_p, *slope_tables)
    sent = call(slope_first_kernel, half_blocks, base, move(sent), *spectral_tables)
    sent, first = call(nonlinear_kernel, (kept_blocks, one), base, move(sent), both_p, second, tw_kept, kept_out)
    sent = call(next_kernel, blocks, base, device, move(sent), forcing_p, *spectral_tables, mirror)
    sent, next_field = call(
        residual_kernel, (longer, plain), base + [strided, total],
        move(sent), both_p, tw_natural, backward, forward,
    )
    sent, full, sums = call(
        misfit_kernel, (half_blocks, pair, shape(8, 2 * rows)), base,
        device, move(sent), tw_natural, forward, tw_natural, backward, mirror,
    )
    sent, value, product = call(
        joint_kernel, (kept_blocks, one, one), base, move(sent), first, second, tw_kept, kept_in
    )
    second_part = call(slope_second_kernel, one, base, product, *slope_tables)
    sent = call(slope_first_kernel, half_blocks, base, move(sent), *spectral_tables)
    field_grad = call(
        last_kernel, plain, [strided, pltpu.VMEM((outer, rows, inner), float32)], move(sent), value, second_part
    )
    return next_field, sums[0, 0], field_grad, full


def per_device(devices, fast, initial_field, target_field, forcing):
    members, rows, length = initial_field.shape
    device = lax.axis_index(axes).astype(jnp.int32).reshape(1)
    outer, inner = split_length(length)
    vmem = pl.BlockSpec(memory_space=pltpu.VMEM)
    strided = pltpu.VMEM((length, TILE), jnp.float32)

    def reorder(body, shape, operand):
        return pl.pallas_call(
            functools.partial(body, length, rows),
            out_shape=jax.ShapeDtypeStruct(shape, jnp.float32),
            in_specs=[vmem],
            out_specs=vmem,
            scratch_shapes=[strided],
        )(operand)

    if rows * rows % (TILE * 32) == 0 and TILE % rows == 0:
        results = [
            joined_step(initial_field[m], target_field[m], forcing, devices, fast, rows, length)
            for m in range(members)
        ]
        next_field = jnp.stack([one[0] for one in results])
        field_grad = jnp.stack([one[1] for one in results])
        forcing_grad = sum(one[2] for one in results)
        objective = sum(one[3].reshape(()) for one in results) / members
        return (next_field, objective, field_grad, forcing_grad)
    forcing_p = reorder(spread_kernel, (outer, 2 * rows, inner), forcing)
    results = [
        member_step(device, initial_field[m], target_field[m], forcing_p, devices, rows, length)
        for m in range(members)
    ]
    next_field = jnp.stack([one[0] for one in results])
    objective = sum(one[1] for one in results) / (members * length * length)
    field_grad = jnp.stack([one[2] for one in results])
    forcing_grad = reorder(collect_kernel, (2, rows, length), sum(one[3] for one in results))
    return (next_field, objective, field_grad, forcing_grad)


def solution(mesh):
    devices = mesh.shape["px"] * mesh.shape["py"]
    spec = P(None, axes, None)
    return jax.shard_map(
        functools.partial(per_device, devices, mesh.shape["py"]),
        mesh=mesh,
        in_specs=(spec, spec, spec),
        out_specs=(spec, P(), spec, spec),
        check_vma=False,
    )
```

```python
import functools
import math
from types import SimpleNamespace

import jax
import jax.numpy as jnp
import numpy as np
from jax import lax
from jax.experimental import pallas as pl
from jax.experimental.pallas import tpu as pltpu
from jax.sharding import PartitionSpec as P

time_step = 0.25
axes = ("px", "py")
TILE = 128


def split_length(length):
    inner = 256 if length % 256 == 0 else TILE
    return (length // inner, inner)


def small_dft(items, sign):
    count = len(items)
    if count == 1:
        return items
    evens = small_dft(items[0::2], sign)
    odds = small_dft(items[1::2], sign)
    low, high = [], []
    for k in range(count // 2):
        odd_re, odd_im = odds[k]
        if 4 * k == count:
            odd_re, odd_im = (-odd_im, odd_re) if sign > 0 else (odd_im, -odd_re)
        elif k:
            c = math.cos(2.0 * math.pi * k / count)
            s = sign * math.sin(2.0 * math.pi * k / count)
            if abs(abs(c) - abs(s)) < 1e-12:
                sc, ss = math.copysign(1.0, c), math.copysign(1.0, s)
                odd_re, odd_im = (
                    c * (odd_re - sc * ss * odd_im),
                    c * (odd_im + sc * ss * odd_re),
                )
            else:
                odd_re, odd_im = (c * odd_re - s * odd_im, c * odd_im + s * odd_re)
        even_re, even_im = evens[k]
        low.append((even_re + odd_re, even_im + odd_im))
        high.append((even_re - odd_re, even_im - odd_im))
    return low + high


def half_dft(items, sign):
    count = 2 * len(items)
    turned = []
    for j, (re, im) in enumerate(items):
        c = math.cos(2.0 * math.pi * j / count)
        s = sign * math.sin(2.0 * math.pi * j / count)
        turned.append((re, im) if j == 0 else (c * re - s * im, c * im + s * re))
    pairs = zip(small_dft(items, sign), small_dft(turned, sign))
    return [one for pair in pairs for one in pair]


def halves(value):
    top = value.astype(jnp.bfloat16)
    return top, (value - top.astype(jnp.float32)).astype(jnp.bfloat16)


def orders(length, rows):
    inner = split_length(length)[1]
    half = rows // 2
    lane = np.arange(inner)
    natural = lane
    local = lane % (inner // 2)
    line = local % half
    kept = rows * (local // half) + np.where((lane >= inner // 2) & (line == 0), half, line)
    return natural, kept, line_order(inner, rows, TILE // rows)


def line_order(inner, rows, groups):
    lane = np.arange(inner)
    tall, wide = rows // groups, inner // groups
    within = lane % wide
    return rows * (within // tall) + tall * (lane // wide) + within % tall


def twiddle_table(length, order):
    outer = split_length(length)[0]
    angle = 2.0 * np.pi * np.outer(np.arange(outer), order) / length
    return (np.stack([np.cos(angle), np.sin(angle)]) / math.sqrt(length)).astype(np.float32)


def matrix_table(length, sign, left, right):
    inner = split_length(length)[1]
    angle = 2.0 * np.pi * (np.outer(left, right) % inner) / inner
    c, s = np.cos(angle), np.sin(angle)
    full = np.block([[c, sign * s], [-sign * s, c]])
    top = full.astype(jnp.bfloat16)
    return np.stack([top, (full - top.astype(np.float64)).astype(jnp.bfloat16)])


def mirror_table(length):
    inner = split_length(length)[1]
    lane = np.arange(inner)
    both = np.zeros((2, inner, inner))
    both[0, (inner - lane) % inner, lane] = 1.0
    both[1, inner - 1 - lane, lane] = 1.0
    return both.astype(jnp.bfloat16)


class Pieces:
    def __init__(self, length, rows, turned=None, top=None, low=None, grid_out=None):
        self.length, self.rows, self.half = length, rows, rows // 2
        self.outer, self.inner = split_length(length)
        self.turned, self.top, self.low, self.z = turned, top, low, grid_out
        self.step = math.gcd(rows // 2, 16)

    def chunks(self, lines, body):
        def run(i, carry):
            body(pl.multiple_of(i * self.step, self.step))
            return carry

        lax.fori_loop(0, lines // self.step, run, 0)

    def put(self, k, at, part, value):
        lanes = pl.ds(part * self.inner, self.inner)
        top, low = halves(value)
        self.top[k, at, lanes] = top
        self.low[k, at, lanes] = low

    def get(self, k, at, part):
        return self.z[k, at, pl.ds(part * self.inner, self.inner)]

    def multiply(self, lines, matrix, real_in=False, real_out=False):
        deep = self.inner if real_in else 2 * self.inner
        wide = self.inner if real_out else 2 * self.inner
        count = self.outer * lines
        top = self.top[:, :lines, :deep].reshape(count, deep)
        low = self.low[:, :lines, :deep].reshape(count, deep)
        right_top = matrix[0, :deep, :wide]
        right_low = matrix[1, :deep, :wide]
        dot = functools.partial(jnp.dot, preferred_element_type=jnp.float32)
        total = dot(top, right_top) + dot(low, right_top) + dot(top, right_low)
        self.z[:, :lines, :wide] = total.reshape(self.outer, lines, wide)

    def twist(self, k, pair, sign, twiddle, flip=None):
        c = twiddle[0, pl.ds(k, 1), :]
        s = twiddle[1, pl.ds(k, 1), :]
        if flip is not None and k % 2:
            c, s = flip * c, flip * s
        s = s if sign > 0 else -s
        re, im = pair
        return (re * c - im * s, re * s + im * c)

    def turn_full(self, source):
        rows, blocks = self.rows, TILE // self.rows
        for t in range(self.length // TILE):
            tile = source[pl.ds(t * blocks, blocks), :rows, :].reshape(TILE, 2 * rows)
            self.turned[: 2 * rows, pl.ds(t * TILE, TILE)] = tile.T

    def turn_lines(self, source):
        rows = self.rows
        groups = TILE // rows
        blocks, wide = self.inner // rows, self.inner // groups
        for t in range(self.outer):
            tile = source[pl.ds(t * blocks, blocks), :, :].reshape(wide, TILE).T
            for h in range(groups):
                self.turned[:rows, pl.ds(t * self.inner + h * wide, wide)] = tile[h * rows : (h + 1) * rows]

    def kept_lanes(self, j):
        wide = self.inner // 2
        return j * self.inner + (wide if 2 * j >= self.outer else 0), wide

    def clear_other(self, j):
        at, wide = self.kept_lanes(j)
        other = j * self.inner + (0 if 2 * j >= self.outer else wide)
        self.turned[: 2 * self.rows, pl.ds(other, wide)] = jnp.zeros((2 * self.rows, wide), jnp.float32)

    def turn_kept(self, source):
        rows, half, blocks = self.rows, self.half, self.inner // self.rows
        for j in range(self.outer):
            at, wide = self.kept_lanes(j)
            tile = source[pl.ds(j * blocks, blocks), :, :].reshape(wide, 2 * rows)
            self.turned[: 2 * rows, pl.ds(at, wide)] = tile.T
            self.clear_other(j)

    def unpack_middle(self):
        rows, middle = self.rows, (self.outer // 2) * self.inner
        first = self.turned[rows : 2 * rows, :TILE]
        lane0 = lax.broadcasted_iota(jnp.int32, first.shape, 1) == 0
        zero = jnp.zeros_like(first)
        self.turned[:rows, pl.ds(middle, TILE)] += jnp.where(lane0, first, zero)
        self.turned[rows : 2 * rows, :TILE] = jnp.where(lane0, zero, first)

    def incoming(self, lines, sign, twiddle, matrix, real_out=False):
        def body(r0):
            items = []
            for j in range(self.outer):
                lanes = pl.ds(j * self.inner, self.inner)
                items.append((
                    self.turned[pl.ds(r0, self.step), lanes],
                    self.turned[pl.ds(lines + r0, self.step), lanes],
                ))
            for k, pair in enumerate(small_dft(items, sign)):
                re, im = self.twist(k, pair, sign, twiddle)
                self.put(k, pl.ds(r0, self.step), 0, re)
                self.put(k, pl.ds(r0, self.step), 1, im)

        self.chunks(lines, body)
        self.multiply(lines, matrix, real_out=real_out)

    def outgoing(self, lines, sign, twiddle, matrix, real_in, write):
        self.multiply(lines, matrix, real_in=real_in)

        def body(r0):
            at = pl.ds(r0, self.step)
            write(r0, small_dft([
                self.twist(k, (self.get(k, at, 0), self.get(k, at, 1)), sign, twiddle)
                for k in range(self.outer)
            ], sign))

        self.chunks(lines, body)

    def pack_middle(self, items):
        re, im = items[0]
        lane0 = lax.broadcasted_iota(jnp.int32, im.shape, 1) == 0
        return [(re, jnp.where(lane0, items[self.outer // 2][0], im))] + items[1:]

    def write_full(self, result, pack):
        rows = self.rows

        def write(r0, items):
            at = pl.ds(r0, self.step)
            for j, (re, im) in enumerate(self.pack_middle(items) if pack else items):
                for piece in range(self.inner // rows):
                    to = j * (self.inner // rows) + piece
                    lanes = slice(piece * rows, (piece + 1) * rows)
                    result[to, at, pl.ds(0, rows)] = re[:, lanes]
                    result[to, at, pl.ds(rows, rows)] = im[:, lanes]

        return write

    def pack_cut(self, slabs, results):
        rows, half, wide = self.rows, self.half, self.inner // 2
        cuts, count = len(results), half // len(results)
        groups = TILE // (2 * count)
        tall = rows // groups
        for k in range(self.outer):
            slab = slabs(k)
            for s in range(self.inner // rows):
                for q, result in enumerate(results):
                    parts = []
                    for group in range(groups):
                        for part in range(2):
                            at = part * wide + s * half + q * count
                            parts.append(slab[group * tall : (group + 1) * tall, at : at + count])
                    result[k * (self.inner // rows) + s] = jnp.concatenate(parts, axis=1)

    def turn_cut(self, source, lines, spans):
        blocks = self.inner // self.rows
        groups = TILE // (2 * lines)
        wide = self.inner // groups
        for t in range(spans):
            tile = source[pl.ds(t * blocks, blocks), :, :].reshape(wide, TILE).T
            for h in range(groups):
                held = tile[h * 2 * lines : (h + 1) * 2 * lines]
                self.turned[: 2 * lines, pl.ds(t * self.inner + h * wide, wide)] = held

    def turn_whole(self, source, tiles):
        rows, blocks = self.rows, TILE // self.rows
        for t in range(tiles):
            tile = source[pl.ds(t * blocks, blocks), :rows, :].reshape(TILE, 2 * rows)
            self.turned[: 2 * rows, pl.ds(t * TILE, TILE)] = tile.T

    def first_imaginary(self, at):
        rows = self.rows
        part = self.turned[rows : 2 * rows, pl.ds(at, TILE)]
        lane0 = lax.broadcasted_iota(jnp.int32, part.shape, 1) == 0
        self.turned[rows : 2 * rows, pl.ds(at, TILE)] = jnp.where(lane0, 0.0, part)
        return jnp.where(lane0, part, 0.0)

    def incoming_half(self, lines, sign, twiddle, matrix, flip, extra=None, real_out=False):
        def body(r0):
            at = pl.ds(r0, self.step)
            items = []
            for j in range(self.outer // 2):
                lanes = pl.ds(j * self.inner, self.inner)
                items.append((self.turned[at, lanes], self.turned[pl.ds(lines + r0, self.step), lanes]))
            for k, (re, im) in enumerate(half_dft(items, sign)):
                if extra is not None:
                    re = re - extra[at, :] if k % 2 else re + extra[at, :]
                re, im = self.twist(k, (re, im), sign, twiddle, flip)
                self.put(k, at, 0, re)
                self.put(k, at, 1, im)

        self.chunks(lines, body)
        self.multiply(lines, matrix, real_out=real_out)

    def outgoing_half(self, lines, sign, twiddle, matrix, flip, write):
        self.multiply(lines, matrix)

        def body(r0):
            at = pl.ds(r0, self.step)
            write(r0, small_dft([
                self.twist(k, (self.get(k, at, 0), self.get(k, at, 1)), sign, twiddle, flip)
                for k in range(self.outer)
            ], sign)[: self.outer // 2])

        self.chunks(lines, body)

    def outgoing_sides(self, twiddle, matrix, sides, late=None):
        self.multiply(self.rows, matrix, real_in=True)
        rows, half, blocks, middle = self.rows, self.half, self.inner // self.rows, self.outer // 2
        tall, step = rows * rows // TILE, self.step
        for h in range(rows // tall):

            def body(i, carry, h=h):
                r0 = pl.multiple_of(i * step, step)
                at = pl.ds(h * tall + r0, step)
                items = small_dft([
                    self.twist(k, (self.get(k, at, 0), self.get(k, at, 1)), -1.0, twiddle)
                    for k in range(self.outer)
                ], -1.0)
                (low, low_im), (high, high_im) = items[0], items[middle]
                lane0 = lax.broadcasted_iota(jnp.int32, low.shape, 1) == 0
                items[0] = (low, jnp.where(lane0, high, low_im))
                items[middle] = (high, jnp.where(lane0, low, high_im))
                if late is not None:
                    items = [
                        tuple(jnp.where(late, one, other) for one, other in zip(items[middle + j], items[j]))
                        for j in range(middle)
                    ]
                for j, pair in enumerate(items):
                    for part, value in enumerate(pair):
                        to = pl.ds(h * rows + part * half, half)
                        for piece in range(blocks):
                            for side, result in enumerate(sides):
                                base = piece * rows + side * half
                                result[j * blocks + piece, pl.ds(r0, step), to] = value[:, base : base + half]
                return carry

            lax.fori_loop(0, tall // step, body, 0)

    def outgoing_kept(self, twiddle, matrix, result):
        self.multiply(self.rows, matrix, real_in=True)
        rows, half, blocks = self.rows, self.half, self.inner // self.rows
        tall = rows * rows // TILE
        step = math.gcd(rows, 16)
        span = min(tall, step)
        for h in range(rows // max(tall, step)):

            def body(i, carry, h=h):
                r0 = i * step if isinstance(i, int) else pl.multiple_of(i * step, step)
                at = pl.ds(h * max(tall, step) + r0, step)
                items = self.pack_middle(small_dft([
                    self.twist(k, (self.get(k, at, 0), self.get(k, at, 1)), -1.0, twiddle)
                    for k in range(self.outer)
                ], -1.0))
                for j, pair in enumerate(items):
                    base = self.inner // 2 if 2 * j >= self.outer else 0
                    for piece in range(blocks):
                        lanes = slice(base + piece * half, base + (piece + 1) * half)
                        for part, value in enumerate(pair):
                            for sub in range(step // span):
                                group = h * (step // span) + sub
                                to = pl.ds(group * rows + part * half, half)
                                held = value[sub * span : (sub + 1) * span, lanes]
                                result[j * blocks + piece, pl.ds(r0, span), to] = held
                return carry

            if tall > step:
                lax.fori_loop(0, tall // step, body, 0)
            else:
                body(0, 0)

    def mirrored(self, blocks, mirror):
        dot = functools.partial(jnp.dot, preferred_element_type=jnp.float32)

        def flip(values, which):
            top, low = halves(jnp.concatenate(values, axis=0))
            return dot(top, mirror[which]) + dot(low, mirror[which])

        flat = [part for k in range(self.outer) for pair in blocks[k] for part in pair]
        per = 2 * len(blocks[0])
        low = flip(flat[:per], 0)
        high = flip(flat[per:], 1)
        out = []
        for k in range(self.outer):
            part, base = (low, 0) if k == 0 else (high, (self.outer - k - 1) * per)
            take = lambda i: part[(base + i) * 8 : (base + i + 1) * 8]
            out.append([(take(2 * i), -take(2 * i + 1)) for i in range(per // 2)])
        return out

    def pack_columns(self, slabs, result):
        rows, half, wide = self.rows, self.half, self.inner // 2
        blocks, groups = self.inner // rows, TILE // rows
        tall = rows // groups
        for k in range(self.outer):
            slab = slabs(k)
            for s in range(blocks):
                parts = []
                for group in range(groups):
                    for part in range(2):
                        at = part * wide + s * half
                        parts.append(slab[group * tall : (group + 1) * tall, at : at + half])
                result[k * blocks + s] = jnp.concatenate(parts, axis=1)

    def turn_columns(self, source, result):
        rows, wide, blocks = self.rows, self.inner // 2, self.inner // self.rows
        for j in range(self.outer):
            tile = source[pl.ds(j * blocks, blocks), :, :].reshape(wide, 2 * rows).T
            result[j, :, pl.ds(0, wide)] = tile[:rows]
            result[j, :, pl.ds(wide, wide)] = tile[rows:]

    def spread(self, first, second, strided, result):
        rows, fill = self.rows, TILE - 2 * self.rows
        for t in range(self.length // TILE):
            lanes = pl.ds(t * TILE, TILE)
            parts = [first[:, lanes], second[:, lanes]]
            if fill:
                parts.append(jnp.zeros((fill, TILE), jnp.float32))
            strided[pl.ds(t * TILE, TILE), :] = jnp.concatenate(parts, axis=0).T
        for k in range(self.outer):
            slab = strided[pl.ds(k, self.inner, stride=self.outer), :].T
            result[k] = slab[: 2 * rows, :]

    def collect(self, slabs, strided, results):
        rows = self.rows
        for k in range(self.outer):
            slab = slabs(k)
            fill = TILE - slab.shape[0]
            if fill:
                slab = jnp.concatenate([slab, jnp.zeros((fill, self.inner), jnp.float32)], axis=0)
            strided[pl.ds(k, self.inner, stride=self.outer), :] = slab.T
        for t in range(self.length // TILE):
            block = strided[pl.ds(t * TILE, TILE), :].T
            for i, result in enumerate(results):
                result[:, pl.ds(t * TILE, TILE)] = block[i * rows : (i + 1) * rows, :]


def signed_waves(position, count):
    signed = jnp.where(position < count // 2, position, position - count)
    waves = 4.0 * signed.astype(jnp.float32) / count
    return waves, jnp.where(position == count // 2, jnp.float32(0.0), waves)


def first_waves(piece, k):
    lanes = lax.broadcasted_iota(jnp.int32, (1, piece.inner), 1)
    return signed_waves(piece.outer * lanes + k, piece.length)


def inverse_denominator(wave_first, wave_second):
    square = wave_first * wave_first + wave_second * wave_second
    return 1.0 / (1.0 + time_step * (square * square - square))


def second_wave(piece, position):
    shape = (position.shape[0], piece.inner)
    return jnp.broadcast_to(signed_waves(position, piece.length)[0], shape)


def row_index(count, width):
    return lax.broadcasted_iota(jnp.int32, (count, width), 0)


class Links:
    def __init__(self, devices, fast):
        self.devices, self.fast = devices, fast
        self.device = lax.axis_index(axes[0]) * fast + lax.axis_index(axes[1])

    def partner(self, i):
        total, bit = 0, 1
        while bit < self.devices:
            total += bit * lax.rem(lax.div(self.device, bit) + lax.div(i, bit), 2)
            bit *= 2
        return total

    def place(self, peer):
        return (lax.div(peer, self.fast), lax.rem(peer, self.fast))

    def greet(self):
        barrier = pltpu.get_barrier_semaphore()

        def go(i, carry):
            at = self.place(self.partner(self.devices - i))
            pl.semaphore_signal(barrier, inc=1, device_id=at, device_id_type=pl.DeviceIdType.MESH)
            return carry

        lax.fori_loop(1, self.devices, go, 0)

    def meet(self):
        pl.semaphore_wait(pltpu.get_barrier_semaphore(), self.devices - 1)

    def send(self, source, target, sems, count):
        send_sem, recv_sem, own_sem = sems
        own = lax.rem(self.device, count)

        def go(i, carry):
            peer = self.partner(count - i)
            pltpu.make_async_remote_copy(
                src_ref=source(lax.rem(peer, count)),
                dst_ref=target(own),
                send_sem=send_sem,
                recv_sem=recv_sem,
                device_id=self.place(peer),
                device_id_type=pl.DeviceIdType.MESH,
            ).start()
            return carry

        lax.fori_loop(1, count, go, 0)
        pltpu.make_async_copy(source(own), target(own), own_sem).start()

    def whole(self, source, target, sems, count):
        others = pl.ds(0, count - 1)
        return pltpu.make_async_remote_copy(
            src_ref=source(others),
            dst_ref=target(others),
            send_sem=sems[0],
            recv_sem=sems[1],
            device_id=(0, 0),
            device_id_type=pl.DeviceIdType.MESH,
        )

    def receive(self, source, target, sems, count):
        own = lax.rem(self.device, count)
        pltpu.make_async_copy(source(own), target(own), sems[2]).wait()
        self.whole(source, target, sems, count).wait_recv()

    def sent(self, source, target, sems, count):
        self.whole(source, target, sems, count).wait_send()


def start_kernel(length, rows, field, target, out, both_p, *scratch):
    piece = Pieces(length, rows)
    piece.spread(field, target, scratch[0], both_p)
    piece.pack_columns(lambda k: both_p[k, pl.ds(0, rows), :], out)


def slope_second_kernel(length, rows, field_p, twiddle, out_matrix, in_matrix, kept, result, *scratch):
    piece = Pieces(length, rows, *scratch)

    def body(r0):
        at = pl.ds(r0, piece.step)
        for k in range(piece.outer):
            piece.put(k, at, 0, field_p[k, at, :])

    piece.chunks(rows, body)
    for j in range(piece.outer):
        piece.clear_other(j)

    def write(r0, items):
        for j, (re, im) in enumerate(items):
            at, wide = piece.kept_lanes(j)
            base = at - j * piece.inner
            position = j * piece.inner + kept[:, base : base + wide]
            slope = 2.0 * signed_waves(position, length)[1]
            piece.turned[pl.ds(r0, piece.step), pl.ds(at, wide)] = -slope * im[:, base : base + wide]
            piece.turned[pl.ds(rows + r0, piece.step), pl.ds(at, wide)] = slope * re[:, base : base + wide]

    piece.outgoing(rows, -1.0, twiddle, out_matrix, True, write)
    piece.incoming(rows, 1.0, twiddle, in_matrix, real_out=True)
    result[...] = piece.z[:, :, : piece.inner]


def spread_kernel(length, rows, forcing, result, strided):
    Pieces(length, rows).spread(forcing.at[0], forcing.at[1], strided, result)


def collect_kernel(length, rows, slabs, result, strided):
    piece = Pieces(length, rows)
    piece.collect(lambda k: slabs[k], strided, [result.at[i] for i in range(result.shape[0])])


def weight_of(device, r0, step, inner):
    alone = (row_index(step, inner) + r0 + device) == 0
    return jnp.where(alone, jnp.float32(1.0), jnp.float32(2.0))


def slope_first_kernel(length, rows, source, in_twiddle, in_matrix, out_twiddle, out_matrix, out, *scratch):
    piece = Pieces(length, rows, *scratch)
    half = piece.half
    piece.turn_lines(source)
    piece.incoming(half, -1.0, in_twiddle, in_matrix)

    def body(r0):
        at = pl.ds(r0, piece.step)
        for k in range(piece.outer):
            re, im = piece.get(k, at, 0), piece.get(k, at, 1)
            scale = first_waves(piece, k)[1]
            piece.put(k, at, 0, -scale * im)
            piece.put(k, at, 1, scale * re)

    piece.chunks(half, body)
    piece.outgoing(half, 1.0, out_twiddle, out_matrix, False, piece.write_full(out, False))


def edge_inverses(piece, k):
    wave_first = first_waves(piece, k)[0]
    middle = jnp.full((1, 1), piece.length // 2, jnp.int32)
    zero = jnp.zeros((1, 1), jnp.int32)
    return [inverse_denominator(wave_first, signed_waves(p, piece.length)[0]) for p in (zero, middle)]


def next_kernel(length, rows, device_ref, source, forcing, in_twiddle, in_matrix, out_twiddle, out_matrix, mirror, out, *scratch):
    device = device_ref[0]
    piece = Pieces(length, rows, *scratch)
    half, step, inner = piece.half, piece.step, piece.inner
    late = device >= (length // rows) // 2
    piece.turn_lines(source)
    piece.incoming(half, -1.0, in_twiddle, in_matrix)

    def body(r0):
        at, also = pl.ds(r0, step), pl.ds(half + r0, step)
        index = row_index(step, 1) + r0
        low_wave = second_wave(piece, device * rows + index)
        high_wave = second_wave(piece, device * rows + half + index)
        moved = jnp.logical_and(row_index(step, inner) + r0 == 0, late)
        weight = weight_of(device, r0, step, inner)
        for k in range(piece.outer):
            wave_first = first_waves(piece, k)[0]
            low = inverse_denominator(wave_first, low_wave)
            high = inverse_denominator(wave_first, high_wave)
            for part in range(2):
                own = weight * piece.get(k, at, part)
                f_low = time_step * forcing[k, pl.ds(part * rows + r0, step), :]
                f_high = time_step * forcing[k, pl.ds(part * rows + half + r0, step), :]
                piece.put(k, at, part, (f_low + jnp.where(moved, 0.0, own)) * low)
                piece.put(k, also, part, (f_high + jnp.where(moved, own, 0.0)) * high)

    piece.chunks(half, body)

    @pl.when(device == 0)
    def _():
        at = pl.ds(0, 8)
        blocks = []
        for k in range(piece.outer):
            own = tuple(piece.get(k, at, part) for part in range(2))
            full = tuple(
                own[part] + time_step * forcing[k, pl.ds(part * rows, 8), :] for part in range(2)
            )
            blocks.append([own, full])
        flipped = piece.mirrored(blocks, mirror)
        rest = pl.ds(0, 16)
        row0 = row_index(16, inner) == 0
        for k in range(piece.outer):
            zero, middle = edge_inverses(piece, k)
            for part in range(2):
                own, full = blocks[k][0][part], blocks[k][1][part]
                own_c, full_c = flipped[k][0][part], flipped[k][1][part]
                value = 0.5 * ((full + full_c) * zero + (own - own_c) * middle)
                replace(piece, k, part, value)

    piece.outgoing(rows, 1.0, out_twiddle, out_matrix, False, piece.write_full(out, False))


def replace(piece, k, part, value):
    lanes = pl.ds(part * piece.inner, piece.inner)
    row0 = row_index(16, piece.inner) == 0
    value = jnp.concatenate([value, value], axis=0)
    for held, new in zip((piece.top, piece.low), halves(value)):
        old = held[k, pl.ds(0, 16), lanes].astype(jnp.float32)
        held[k, pl.ds(0, 16), lanes] = jnp.where(row0, new.astype(jnp.float32), old).astype(jnp.bfloat16)


def misfit_kernel(length, rows, device_ref, source, in_twiddle, in_matrix, out_twiddle, out_matrix, mirror, out, full, total_out, *scratch):
    device = device_ref[0]
    piece = Pieces(length, rows, *scratch)
    half, step, inner = piece.half, piece.step, piece.inner
    late = device >= (length // rows) // 2
    piece.turn_full(source)
    piece.incoming(rows, -1.0, in_twiddle, in_matrix)

    def body(r0):
        at, also = pl.ds(r0, step), pl.ds(half + r0, step)
        index = row_index(step, 1) + r0
        low_wave = second_wave(piece, device * rows + index)
        high_wave = second_wave(piece, device * rows + half + index)
        moved = jnp.logical_and(row_index(step, inner) + r0 == 0, late)
        weight = weight_of(device, r0, step, inner)
        for k in range(piece.outer):
            wave_first = first_waves(piece, k)[0]
            low = time_step * inverse_denominator(wave_first, low_wave)
            high = time_step * inverse_denominator(wave_first, high_wave)
            for part in range(2):
                low_value = piece.get(k, at, part) * low
                high_value = piece.get(k, also, part) * high
                full[k, pl.ds(part * rows + r0, step), :] = low_value
                full[k, pl.ds(part * rows + half + r0, step), :] = high_value
                own = jnp.where(moved, high_value, low_value)
                piece.put(k, at, part, weight * own)

    piece.chunks(half, body)

    @pl.when(device == 0)
    def _():
        at = pl.ds(0, 8)
        blocks = [[(piece.get(k, at, 0), piece.get(k, at, 1))] for k in range(piece.outer)]
        flipped = piece.mirrored(blocks, mirror)
        row0 = row_index(8, inner) == 0
        for k in range(piece.outer):
            zero, middle = edge_inverses(piece, k)
            for part in range(2):
                own, own_c = blocks[k][0][part], flipped[k][0][part]
                first = (0.5 * time_step) * (own + own_c) * zero
                value = first + (0.5 * time_step) * (own - own_c) * middle
                at_full = pl.ds(part * rows, 8)
                full[k, at_full, :] = jnp.where(row0, first, full[k, at_full, :])
                replace(piece, k, part, value)

    piece.outgoing(half, 1.0, out_twiddle, out_matrix, False, piece.write_full(out, False))
    total_out[...] = jnp.sum(source[:, pl.ds(rows, 8), :], axis=0)


def nonlinear_kernel(length, rows, source, both_p, second, twiddle, out_matrix, out, first, *scratch):
    piece = Pieces(length, rows, *scratch)
    piece.turn_columns(source, first)

    def body(r0):
        at = pl.ds(r0, piece.step)
        for k in range(piece.outer):
            one, other = first[k, at, :], second[k, at, :]
            piece.put(k, at, 0, both_p[k, at, :] - (0.5 * time_step) * (one * one + other * other))

    piece.chunks(rows, body)
    piece.outgoing_kept(twiddle, out_matrix, out)


def joint_kernel(length, rows, source, first, second, twiddle, in_matrix, out, value_out, second_out, *scratch):
    piece = Pieces(length, rows, *scratch)
    piece.turn_kept(source)
    piece.unpack_middle()
    piece.incoming(rows, 1.0, twiddle, in_matrix, real_out=True)
    lanes = pl.ds(0, piece.inner)

    def body(r0):
        at = pl.ds(r0, piece.step)
        for k in range(piece.outer):
            value = piece.get(k, at, 0)
            value_out[k, at, :] = (1.0 / time_step) * value
            second_out[k, at, :] = value * second[k, at, :]
            piece.z[k, at, lanes] = value * first[k, at, :]

    piece.chunks(rows, body)
    piece.pack_columns(lambda k: piece.z[k, pl.ds(0, rows), lanes], out)


def residual_kernel(length, rows, source, both_p, twiddle, in_matrix, out_matrix, out, field_out, *scratch):
    piece = Pieces(length, rows, *scratch[:4])
    strided, total = scratch[4:]
    piece.turn_full(source)
    piece.unpack_middle()
    piece.incoming(rows, 1.0, twiddle, in_matrix, real_out=True)
    piece.collect(lambda k: piece.get(k, pl.ds(0, rows), 0), strided, [field_out])
    total[...] = jnp.zeros_like(total)

    def body(r0):
        at = pl.ds(r0, piece.step)
        for k in range(piece.outer):
            residual = piece.get(k, at, 0) - both_p[k, pl.ds(rows + r0, piece.step), :]
            total[...] += residual * residual
            piece.put(k, at, 0, residual)

    piece.chunks(rows, body)
    piece.outgoing(rows, -1.0, twiddle, out_matrix, True, piece.write_full(out, True))
    value = 0.5 * jnp.sum(total[...])
    out[:, pl.ds(rows, 8), :] = jnp.full((out.shape[0], 8, 2 * rows), value, jnp.float32)


def last_kernel(length, rows, source, value, second, field_out, strided, first):
    piece = Pieces(length, rows)
    piece.turn_columns(source, first)
    piece.collect(lambda k: first[k] + value[k] + second[k], strided, [field_out])


def step_kernel(length, rows, devices, fast, cuts, inputs, outs, box):
    links = Links(devices, fast)
    device, half, part_devices = links.device, rows // 2, devices // 2
    late = device >= part_devices
    flip = jnp.where(late, -1.0, 1.0).astype(jnp.float32)
    sides = range(2)
    copies, sems = box.copies, box.sems
    work = (box.turned, box.top, box.low, box.z)
    piece = Pieces(length, rows, *work)
    step, inner, outer = piece.step, piece.inner, piece.outer
    both_p, forcing_p, full = box.both_p, box.forcing_p, box.full
    first, second, value = box.first, box.second, box.value
    strided, total = box.strided, box.total
    lanes = pl.ds(0, inner)

    loads = [
        pltpu.make_async_copy(ref, held, copies.at[i])
        for i, (ref, held) in enumerate(zip(inputs.refs, inputs.held))
    ]
    for copy in loads[:2]:
        copy.start()
    links.greet()
    waiting = iter(loads)

    def load(count):
        for i in range(count):
            next(waiting).wait()

    at_all = lambda ref: lambda e: ref.at[e]
    at_lines = lambda ref, base, count: lambda e: ref.at[e, pl.ds(base, count)]
    order = []

    def send(source, target, count=devices):
        i = len(order)
        order.append((source, target, (sems.at[i, 0], sems.at[i, 1], sems.at[i, 2]), count))
        links.send(*order[-1])
        return order[-1]

    def receive(*moves):
        for move in moves:
            links.receive(*move)

    tw_natural, tw_kept, tw_lines, tw_cut = (inputs.twiddles.at[i] for i in range(4))
    forward, backward, mirror = inputs.forward, inputs.backward, inputs.mirror
    kept_out, kept_in, kept = inputs.kept_out, inputs.kept_in, inputs.kept
    lines_in, cut_in = box.lines_in, box.cut_in

    def permute_rows(groups, result):
        tall, blocks = rows // groups, inner // rows
        for p in range(2):
            for part in range(2):
                for group in range(groups):
                    for s in range(blocks):
                        at = part * inner + group * (inner // groups) + s * tall
                        source = part * inner + s * rows + group * tall
                        result[p, pl.ds(at, tall), :] = forward[p, pl.ds(source, tall), :]

    def slope_first(source, out, lines):
        piece.turn_cut(source, lines, outer)
        piece.incoming(lines, -1.0, tw_cut, cut_in)

        def body(r0):
            at = pl.ds(r0, step)
            for k in range(outer):
                re, im = piece.get(k, at, 0), piece.get(k, at, 1)
                scale = first_waves(piece, k)[1]
                piece.put(k, at, 0, -scale * im)
                piece.put(k, at, 1, scale * re)

        piece.chunks(lines, body)
        piece.outgoing(lines, 1.0, tw_natural, backward, False, piece.write_full(out, False))

    def slope_second(source, out):
        slope_second_kernel(length, rows, source, tw_kept, kept_out, kept_in, kept, out, *work)

    def send_columns(source, target):
        return [send(at_all(source.at[q]), at_all(target.at[q])) for q in range(cuts)]

    def turn_slopes(moves, source, back, target):
        count, result = half // cuts, []
        for q, move in enumerate(moves):
            receive(move)
            slope_first(source.at[q], back.at[q], count)
            result.append(send(at_all(back.at[q]), at_lines(target, q * count, count)))
        return result

    def lines_of(side, r0):
        line = row_index(step, 1) + r0 + side * half
        alone = (row_index(step, inner) + r0 + side * half + lax.rem(device, part_devices)) == 0
        return second_wave(piece, device * rows + line), jnp.where(alone, jnp.float32(1.0), jnp.float32(2.0))

    def edges(k):
        wave = first_waves(piece, k)[0]
        middle = jnp.full((1, 1), length // 2, jnp.int32)
        mine, theirs = jnp.where(late, middle, 0), jnp.where(late, 0, middle)
        return [inverse_denominator(wave, signed_waves(p, length)[0]) for p in (mine, theirs)]

    load(2)
    for copy in loads[2:]:
        copy.start()
    piece.spread(inputs.field, inputs.target, strided, both_p)
    piece.pack_cut(lambda k: both_p[k, pl.ds(0, rows), :], [box.s_field.at[q] for q in range(cuts)])
    links.meet()
    m_field = send_columns(box.s_field, box.r_field)

    load(len(loads) - 2)
    permute_rows(TILE // rows, lines_in)
    permute_rows(TILE * cuts // rows, cut_in)
    slope_second(both_p, second)
    m_slope = turn_slopes(m_field, box.r_field, box.s_slope, box.r_slope)
    piece.spread(inputs.forcing.at[0], inputs.forcing.at[1], strided, forcing_p)

    receive(*m_slope)
    piece.turn_columns(box.r_slope, first)

    def nonlinear(r0):
        at = pl.ds(r0, step)
        for k in range(outer):
            one, other = first[k, at, :], second[k, at, :]
            piece.put(k, at, 0, both_p[k, at, :] - (0.5 * time_step) * (one * one + other * other))

    piece.chunks(rows, nonlinear)
    piece.outgoing_sides(tw_natural, forward, [box.s_sum.at[side] for side in sides], late)
    m_sum = [send(at_all(box.s_sum.at[side]), at_all(box.r_sum.at[side]), part_devices) for side in sides]

    def divide(side):
        def body(r0):
            at = pl.ds(r0, step)
            wave, weight = lines_of(side, r0)
            for k in range(outer):
                scale = inverse_denominator(first_waves(piece, k)[0], wave)
                for part in range(2):
                    forced = time_step * forcing_p[k, pl.ds(part * rows + side * half + r0, step), :]
                    piece.put(k, at, part, (weight * piece.get(k, at, part) + forced) * scale)

        piece.chunks(half, body)
        if side:
            return

        @pl.when(lax.rem(device, part_devices) == 0)
        def _():
            at = pl.ds(0, 8)
            blocks = []
            for k in range(outer):
                own = tuple(piece.get(k, at, part) for part in range(2))
                joined = tuple(own[part] + time_step * forcing_p[k, pl.ds(part * rows, 8), :] for part in range(2))
                blocks.append([own, joined])
            flipped = piece.mirrored(blocks, mirror)
            for k in range(outer):
                mine, theirs = edges(k)
                for part in range(2):
                    own, joined = blocks[k][0][part], blocks[k][1][part]
                    own_c, joined_c = flipped[k][0][part], flipped[k][1][part]
                    replace(piece, k, part, 0.5 * ((joined + joined_c) * mine + (own - own_c) * theirs))

    m_next = []
    for side in sides:
        receive(m_sum[side])
        piece.turn_cut(box.r_sum.at[side], half, outer // 2)
        piece.incoming_half(half, -1.0, tw_lines, lines_in, flip)
        divide(side)
        sent = box.s_next.at[side]
        piece.outgoing(half, 1.0, tw_natural, backward, False, piece.write_full(sent, False))
        m_next.append(send(at_all(sent), at_lines(box.r_next, side * half, half)))

    receive(*m_next)
    piece.turn_whole(box.r_next, length // TILE)
    low, high = piece.first_imaginary(0), piece.first_imaginary(length // 2)
    piece.turned[:rows, pl.ds(0, TILE)] += high
    piece.turned[:rows, pl.ds(length // 2, TILE)] += low
    piece.incoming(rows, 1.0, tw_natural, backward, real_out=True)
    total[...] = jnp.zeros_like(total)

    def misfit(r0):
        at = pl.ds(r0, step)
        for k in range(outer):
            now = piece.get(k, at, 0)
            value[k, at, :] = now
            residual = now - both_p[k, pl.ds(rows + r0, step), :]
            total[...] += residual * residual
            piece.put(k, at, 0, residual)

    piece.chunks(rows, misfit)
    piece.outgoing_sides(tw_natural, forward, [box.s_kept.at[side] for side in sides])
    m_kept = [send(at_all(box.s_kept.at[side]), at_all(box.r_kept.at[side])) for side in sides]
    box.s_total[...] = jnp.full(box.s_total.shape, 0.5 * jnp.sum(total[...]), jnp.float32)
    m_total = send(at_all(box.s_total), at_all(box.r_total))
    piece.collect(lambda k: value[k], strided, [outs.next])

    def adjoint(side):
        def body(r0):
            at = pl.ds(r0, step)
            wave, weight = lines_of(side, r0)
            for k in range(outer):
                scale = time_step * inverse_denominator(first_waves(piece, k)[0], wave)
                for part in range(2):
                    own = piece.get(k, at, part) * scale
                    full[k, pl.ds(part * rows + side * half + r0, step), :] = own
                    piece.put(k, at, part, weight * own)

        piece.chunks(half, body)
        if side:
            return

        @pl.when(lax.rem(device, part_devices) == 0)
        def _():
            at = pl.ds(0, 8)
            blocks = [[(piece.get(k, at, 0), piece.get(k, at, 1))] for k in range(outer)]
            flipped = piece.mirrored(blocks, mirror)
            row0 = row_index(8, inner) == 0
            for k in range(outer):
                mine, theirs = edges(k)
                for part in range(2):
                    own, own_c = blocks[k][0][part], flipped[k][0][part]
                    line = (0.5 * time_step) * (own + own_c) * mine
                    at_full = pl.ds(part * rows, 8)
                    full[k, at_full, :] = jnp.where(row0, line, full[k, at_full, :])
                    replace(piece, k, part, line + (0.5 * time_step) * (own - own_c) * theirs)

    m_back = []
    for side in sides:
        receive(m_kept[side])
        piece.turn_cut(box.r_kept.at[side], half, outer)
        piece.incoming(half, -1.0, tw_lines, lines_in)
        adjoint(side)
        sent = box.s_back.at[side]
        piece.outgoing_half(half, 1.0, tw_natural, backward, flip, piece.write_full(sent, False))
        m_back.append(send(at_all(sent), at_lines(box.r_back, side * half, half), part_devices))

    receive(*m_back)
    piece.turn_whole(box.r_back, length // (2 * TILE))
    box.extra[:, pl.ds(0, TILE)] = piece.first_imaginary(0)
    box.extra[:, pl.ds(TILE, inner - TILE)] = jnp.zeros((rows, inner - TILE), jnp.float32)
    piece.incoming_half(rows, 1.0, tw_natural, backward, flip, box.extra, real_out=True)

    def products(r0):
        at = pl.ds(r0, step)
        for k in range(outer):
            now = piece.get(k, at, 0)
            value[k, at, :] = (1.0 / time_step) * now
            box.product[k, at, :] = now * second[k, at, :]
            piece.z[k, at, lanes] = now * first[k, at, :]

    piece.chunks(rows, products)
    piece.pack_cut(lambda k: piece.z[k, pl.ds(0, rows), lanes], [box.s_product.at[q] for q in range(cuts)])
    m_product = send_columns(box.s_product, box.r_product)
    slope_second(box.product, second)
    for k in range(outer):
        value[k] = value[k] + second[k]
    m_last = turn_slopes(m_product, box.r_product, box.s_last, box.r_last)

    piece.collect(lambda k: full[k], strided, [outs.forcing.at[i] for i in range(2)])
    receive(m_total)
    outs.total[...] = jnp.sum(box.r_total[...], axis=0) / (length * length)

    receive(*m_last)
    piece.turn_columns(box.r_last, first)
    for k in range(outer):
        outs.field[k] = first[k] + value[k]
    for move in order:
        links.sent(*move)


def joined_step(field, target, forcing, devices, fast, rows, length):
    outer, inner = split_length(length)
    half, step, cuts = rows // 2, math.gcd(rows // 2, 16), 2
    natural, kept, lines = orders(length, rows)
    cut = line_order(inner, rows, TILE * cuts // rows)
    matrix = lambda *args: matrix_table(length, *args)
    tables = dict(
        field=field, target=target,
        twiddles=np.stack([twiddle_table(length, o) for o in (natural, kept, lines, cut)]),
        kept=kept[None, :].astype(np.int32),
        kept_out=matrix(-1.0, natural, kept)[:, :inner],
        kept_in=matrix(1.0, kept, natural)[:, :, :inner],
        forcing=forcing,
        backward=matrix(1.0, natural, natural),
        forward=matrix(-1.0, natural, natural),
        mirror=mirror_table(length),
    )
    operands = [jnp.asarray(table) for table in tables.values()]
    float32 = jnp.float32
    held = lambda *dims: pltpu.VMEM(dims, float32)
    packed, lined = held(2, devices, rows * rows // TILE, TILE), held(2, devices, half, 2 * rows)
    packed_half, lined_half = (held(2, devices // 2, *dims.shape[2:]) for dims in (packed, lined))
    columns, slopes = held(cuts, devices, rows * rows // (TILE * cuts), TILE), held(cuts, devices, half // cuts, 2 * rows)
    returned = held(devices, half, 2 * rows)
    table = pltpu.VMEM((2, 2 * inner, 2 * inner), jnp.bfloat16)
    pair, one = held(outer, 2 * rows, inner), held(outer, rows, inner)
    small = held(devices, 8, TILE)
    halved = pltpu.VMEM((outer, rows, 2 * inner), jnp.bfloat16)
    shapes = dict(
        turned=held(2 * rows, length), top=halved, low=halved, z=held(outer, rows, 2 * inner),
        strided=held(length, TILE), total=held(step, inner),
        both_p=pair, forcing_p=pair, full=pair, first=one, second=one, value=one, product=one,
        lines_in=table, cut_in=table, extra=held(rows, inner),
        s_field=columns, r_field=columns, s_slope=slopes, r_slope=returned,
        s_sum=packed_half, r_sum=packed_half, s_next=lined, r_next=held(devices, rows, 2 * rows),
        s_kept=packed, r_kept=packed, s_total=small, r_total=small,
        s_back=lined_half, r_back=held(devices // 2, rows, 2 * rows),
        s_product=columns, r_product=columns, s_last=slopes, r_last=returned,
        copies=pltpu.SemaphoreType.DMA((len(operands),)),
        sems=pltpu.SemaphoreType.DMA((9 + 4 * cuts, 3)),
    )
    inputs = [pltpu.VMEM(operand.shape, operand.dtype) for operand in operands]

    def body(*refs):
        a, b = len(operands), len(operands) + 4
        c = b + len(operands)
        given = SimpleNamespace(refs=refs[:a], held=refs[b:c], **dict(zip(tables, refs[b:c])))
        outs = SimpleNamespace(next=refs[a], field=refs[a + 1], forcing=refs[a + 2], total=refs[a + 3])
        step_kernel(length, rows, devices, fast, cuts, given, outs, SimpleNamespace(**dict(zip(shapes, refs[c:]))))

    anywhere = pl.BlockSpec(memory_space=pl.ANY)
    vmem, smem = pl.BlockSpec(memory_space=pltpu.VMEM), pl.BlockSpec(memory_space=pltpu.SMEM)
    shape = lambda *dims: jax.ShapeDtypeStruct(dims, float32)
    next_field, slabs, forcing_grad, total = pl.pallas_call(
        body,
        out_shape=(shape(rows, length), shape(outer, rows, inner), shape(2, rows, length), shape(8, TILE)),
        in_specs=[pl.BlockSpec(memory_space=pltpu.HBM)] * len(operands),
        out_specs=(vmem, vmem, vmem, vmem),
        scratch_shapes=inputs + list(shapes.values()),
        compiler_params=pltpu.CompilerParams(vmem_limit_bytes=34 * 2**20, has_side_effects=True, collective_id=0),
        cost_estimate=pl.CostEstimate(flops=6 * 10**10, bytes_accessed=4 * 2**20, transcendentals=0),
    )(*[pltpu.with_memory_space_constraint(one, pltpu.HBM) for one in operands])
    return pl.pallas_call(
        functools.partial(tail_kernel, length, rows),
        out_shape=(shape(rows, length), shape(rows, length), shape(2, rows, length), shape(1, 1)),
        in_specs=[vmem] * 4,
        out_specs=(anywhere, anywhere, anywhere, smem),
        scratch_shapes=[held(length, TILE), held(rows, length), pltpu.SemaphoreType.DMA((3,))],
        compiler_params=pltpu.CompilerParams(vmem_limit_bytes=8 * 2**20),
        cost_estimate=pl.CostEstimate(flops=10**9, bytes_accessed=4 * 2**20, transcendentals=0),
    )(next_field, slabs, forcing_grad, total)


def tail_kernel(length, rows, next_field, slabs, forcing_grad, total, next_out, field_out, forcing_out, total_out, strided, held, sems):
    piece = Pieces(length, rows)
    copies = [
        pltpu.make_async_copy(next_field, next_out, sems.at[0]),
        pltpu.make_async_copy(forcing_grad, forcing_out, sems.at[1]),
        pltpu.make_async_copy(held, field_out, sems.at[2]),
    ]
    copies[0].start()
    copies[1].start()
    total_out[0, 0] = jnp.sum(total[0:1, 0:1])
    piece.collect(lambda k: slabs[k], strided, [held])
    copies[2].start()
    for copy in copies:
        copy.wait()


def member_step(device, field, target, forcing_p, devices, rows, length):
    outer, inner = split_length(length)
    half = rows // 2
    float32 = jnp.float32
    shape = lambda *dims: jax.ShapeDtypeStruct(dims, float32)
    kept_blocks = shape(devices, rows * rows // TILE, TILE)
    half_blocks = shape(devices, half, 2 * rows)
    blocks = shape(devices, rows, 2 * rows)
    longer = shape(devices, rows + 8, 2 * rows)
    pair, one = shape(outer, 2 * rows, inner), shape(outer, rows, inner)
    plain = shape(rows, length)
    step = math.gcd(half, 16)
    base = [
        pltpu.VMEM((2 * rows, length), float32),
        pltpu.VMEM((outer, rows, 2 * inner), jnp.bfloat16),
        pltpu.VMEM((outer, rows, 2 * inner), jnp.bfloat16),
        pltpu.VMEM((outer, rows, 2 * inner), float32),
    ]
    strided = pltpu.VMEM((length, TILE), float32)
    total = pltpu.VMEM((step, inner), float32)
    vmem = pl.BlockSpec(memory_space=pltpu.VMEM)
    smem = pl.BlockSpec(memory_space=pltpu.SMEM)

    natural, kept, lines = orders(length, rows)
    tw_natural, tw_kept, tw_lines = [jnp.asarray(twiddle_table(length, o)) for o in (natural, kept, lines)]
    matrix = lambda *args: matrix_table(length, *args)
    forward, backward = matrix(-1.0, natural, natural), matrix(1.0, natural, natural)
    kept_out, kept_in = matrix(-1.0, natural, kept)[:, :inner], matrix(1.0, kept, natural)[:, :, :inner]
    lines_in = matrix(-1.0, lines, natural)
    mirror = jnp.asarray(mirror_table(length))
    kept_lane = jnp.asarray(kept[None, :].astype(np.int32))

    def call(body, outs, scratch, *operands):
        return pl.pallas_call(
            functools.partial(body, length, rows),
            out_shape=outs,
            in_specs=[smem if operand is device else vmem for operand in operands],
            out_specs=jax.tree.map(lambda leaf: vmem, outs),
            scratch_shapes=scratch,
            compiler_params=pltpu.CompilerParams(vmem_limit_bytes=20 * 2**20),
            cost_estimate=pl.CostEstimate(flops=6 * 10**9, bytes_accessed=4 * 2**20, transcendentals=0),
        )(*operands)

    def move(value):
        return lax.all_to_all(value, axes, split_axis=0, concat_axis=0, tiled=True)

    spectral_tables = (tw_lines, lines_in, tw_natural, backward)
    slope_tables = (tw_kept, kept_out, kept_in, kept_lane)
    sent, both_p = call(start_kernel, (kept_blocks, pair), [strided], field, target)
    second = call(slope_second_kernel, one, base, both_p, *slope_tables)
    sent = call(slope_first_kernel, half_blocks, base, move(sent), *spectral_tables)
    sent, first = call(nonlinear_kernel, (kept_blocks, one), base, move(sent), both_p, second, tw_kept, kept_out)
    sent = call(next_kernel, blocks, base, device, move(sent), forcing_p, *spectral_tables, mirror)
    sent, next_field = call(
        residual_kernel, (longer, plain), base + [strided, total],
        move(sent), both_p, tw_natural, backward, forward,
    )
    sent, full, sums = call(
        misfit_kernel, (half_blocks, pair, shape(8, 2 * rows)), base,
        device, move(sent), tw_natural, forward, tw_natural, backward, mirror,
    )
    sent, value, product = call(
        joint_kernel, (kept_blocks, one, one), base, move(sent), first, second, tw_kept, kept_in
    )
    second_part = call(slope_second_kernel, one, base, product, *slope_tables)
    sent = call(slope_first_kernel, half_blocks, base, move(sent), *spectral_tables)
    field_grad = call(
        last_kernel, plain, [strided, pltpu.VMEM((outer, rows, inner), float32)], move(sent), value, second_part
    )
    return next_field, sums[0, 0], field_grad, full


def per_device(devices, fast, initial_field, target_field, forcing):
    members, rows, length = initial_field.shape
    device = lax.axis_index(axes).astype(jnp.int32).reshape(1)
    outer, inner = split_length(length)
    vmem = pl.BlockSpec(memory_space=pltpu.VMEM)
    strided = pltpu.VMEM((length, TILE), jnp.float32)

    def reorder(body, shape, operand):
        return pl.pallas_call(
            functools.partial(body, length, rows),
            out_shape=jax.ShapeDtypeStruct(shape, jnp.float32),
            in_specs=[vmem],
            out_specs=vmem,
            scratch_shapes=[strided],
        )(operand)

    if rows * rows % (TILE * 32) == 0 and TILE % rows == 0:
        results = [
            joined_step(initial_field[m], target_field[m], forcing, devices, fast, rows, length)
            for m in range(members)
        ]
        next_field = jnp.stack([one[0] for one in results])
        field_grad = jnp.stack([one[1] for one in results])
        forcing_grad = sum(one[2] for one in results)
        objective = sum(one[3].reshape(()) for one in results) / members
        return (next_field, objective, field_grad, forcing_grad)
    forcing_p = reorder(spread_kernel, (outer, 2 * rows, inner), forcing)
    results = [
        member_step(device, initial_field[m], target_field[m], forcing_p, devices, rows, length)
        for m in range(members)
    ]
    next_field = jnp.stack([one[0] for one in results])
    objective = sum(one[1] for one in results) / (members * length * length)
    field_grad = jnp.stack([one[2] for one in results])
    forcing_grad = reorder(collect_kernel, (2, rows, length), sum(one[3] for one in results))
    return (next_field, objective, field_grad, forcing_grad)


def solution(mesh):
    devices = mesh.shape["px"] * mesh.shape["py"]
    spec = P(None, axes, None)
    return jax.shard_map(
        functools.partial(per_device, devices, mesh.shape["py"]),
        mesh=mesh,
        in_specs=(spec, spec, spec),
        out_specs=(spec, P(), spec, spec),
        check_vma=False,
    )
```

```python
import functools
import math
from types import SimpleNamespace

import jax
import jax.numpy as jnp
import numpy as np
from jax import lax
from jax.experimental import pallas as pl
from jax.experimental.pallas import tpu as pltpu
from jax.sharding import PartitionSpec as P

time_step = 0.25
axes = ("px", "py")
TILE = 128


def split_length(length):
    inner = 256 if length % 256 == 0 else TILE
    return (length // inner, inner)


def small_dft(items, sign):
    count = len(items)
    if count == 1:
        return items
    evens = small_dft(items[0::2], sign)
    odds = small_dft(items[1::2], sign)
    low, high = [], []
    for k in range(count // 2):
        odd_re, odd_im = odds[k]
        if 4 * k == count:
            odd_re, odd_im = (-odd_im, odd_re) if sign > 0 else (odd_im, -odd_re)
        elif k:
            c = math.cos(2.0 * math.pi * k / count)
            s = sign * math.sin(2.0 * math.pi * k / count)
            if abs(abs(c) - abs(s)) < 1e-12:
                sc, ss = math.copysign(1.0, c), math.copysign(1.0, s)
                odd_re, odd_im = (
                    c * (odd_re - sc * ss * odd_im),
                    c * (odd_im + sc * ss * odd_re),
                )
            else:
                odd_re, odd_im = (c * odd_re - s * odd_im, c * odd_im + s * odd_re)
        even_re, even_im = evens[k]
        low.append((even_re + odd_re, even_im + odd_im))
        high.append((even_re - odd_re, even_im - odd_im))
    return low + high


def half_dft(items, sign):
    count = 2 * len(items)
    turned = []
    for j, (re, im) in enumerate(items):
        c = math.cos(2.0 * math.pi * j / count)
        s = sign * math.sin(2.0 * math.pi * j / count)
        turned.append((re, im) if j == 0 else (c * re - s * im, c * im + s * re))
    pairs = zip(small_dft(items, sign), small_dft(turned, sign))
    return [one for pair in pairs for one in pair]


def halves(value):
    top = value.astype(jnp.bfloat16)
    return top, (value - top.astype(jnp.float32)).astype(jnp.bfloat16)


def orders(length, rows):
    inner = split_length(length)[1]
    half = rows // 2
    lane = np.arange(inner)
    natural = lane
    local = lane % (inner // 2)
    line = local % half
    kept = rows * (local // half) + np.where((lane >= inner // 2) & (line == 0), half, line)
    return natural, kept, line_order(inner, rows, TILE // rows)


def line_order(inner, rows, groups):
    lane = np.arange(inner)
    tall, wide = rows // groups, inner // groups
    within = lane % wide
    return rows * (within // tall) + tall * (lane // wide) + within % tall


def twiddle_table(length, order):
    outer = split_length(length)[0]
    angle = 2.0 * np.pi * np.outer(np.arange(outer), order) / length
    return (np.stack([np.cos(angle), np.sin(angle)]) / math.sqrt(length)).astype(np.float32)


def matrix_table(length, sign, left, right):
    inner = split_length(length)[1]
    angle = 2.0 * np.pi * (np.outer(left, right) % inner) / inner
    c, s = np.cos(angle), np.sin(angle)
    full = np.block([[c, sign * s], [-sign * s, c]])
    top = full.astype(jnp.bfloat16)
    return np.stack([top, (full - top.astype(np.float64)).astype(jnp.bfloat16)])


def mirror_table(length):
    inner = split_length(length)[1]
    lane = np.arange(inner)
    both = np.zeros((2, inner, inner))
    both[0, (inner - lane) % inner, lane] = 1.0
    both[1, inner - 1 - lane, lane] = 1.0
    return both.astype(jnp.bfloat16)


class Pieces:
    def __init__(self, length, rows, turned=None, top=None, low=None, grid_out=None):
        self.length, self.rows, self.half = length, rows, rows // 2
        self.outer, self.inner = split_length(length)
        self.turned, self.top, self.low, self.z = turned, top, low, grid_out
        self.step = math.gcd(rows // 2, 16)

    def chunks(self, lines, body):
        def run(i, carry):
            body(pl.multiple_of(i * self.step, self.step))
            return carry

        lax.fori_loop(0, lines // self.step, run, 0)

    def put(self, k, at, part, value):
        lanes = pl.ds(part * self.inner, self.inner)
        top, low = halves(value)
        self.top[k, at, lanes] = top
        self.low[k, at, lanes] = low

    def get(self, k, at, part):
        return self.z[k, at, pl.ds(part * self.inner, self.inner)]

    def multiply(self, lines, matrix, real_in=False, real_out=False):
        deep = self.inner if real_in else 2 * self.inner
        wide = self.inner if real_out else 2 * self.inner
        count = self.outer * lines
        top = self.top[:, :lines, :deep].reshape(count, deep)
        low = self.low[:, :lines, :deep].reshape(count, deep)
        right_top = matrix[0, :deep, :wide]
        right_low = matrix[1, :deep, :wide]
        dot = functools.partial(jnp.dot, preferred_element_type=jnp.float32)
        total = dot(top, right_top) + dot(low, right_top) + dot(top, right_low)
        self.z[:, :lines, :wide] = total.reshape(self.outer, lines, wide)

    def twist(self, k, pair, sign, twiddle, flip=None):
        c = twiddle[0, pl.ds(k, 1), :]
        s = twiddle[1, pl.ds(k, 1), :]
        if flip is not None and k % 2:
            c, s = flip * c, flip * s
        s = s if sign > 0 else -s
        re, im = pair
        return (re * c - im * s, re * s + im * c)

    def turn_full(self, source):
        rows, blocks = self.rows, TILE // self.rows
        for t in range(self.length // TILE):
            tile = source[pl.ds(t * blocks, blocks), :rows, :].reshape(TILE, 2 * rows)
            self.turned[: 2 * rows, pl.ds(t * TILE, TILE)] = tile.T

    def turn_lines(self, source):
        rows = self.rows
        groups = TILE // rows
        blocks, wide = self.inner // rows, self.inner // groups
        for t in range(self.outer):
            tile = source[pl.ds(t * blocks, blocks), :, :].reshape(wide, TILE).T
            for h in range(groups):
                self.turned[:rows, pl.ds(t * self.inner + h * wide, wide)] = tile[h * rows : (h + 1) * rows]

    def kept_lanes(self, j):
        wide = self.inner // 2
        return j * self.inner + (wide if 2 * j >= self.outer else 0), wide

    def clear_other(self, j):
        at, wide = self.kept_lanes(j)
        other = j * self.inner + (0 if 2 * j >= self.outer else wide)
        self.turned[: 2 * self.rows, pl.ds(other, wide)] = jnp.zeros((2 * self.rows, wide), jnp.float32)

    def turn_kept(self, source):
        rows, half, blocks = self.rows, self.half, self.inner // self.rows
        for j in range(self.outer):
            at, wide = self.kept_lanes(j)
            tile = source[pl.ds(j * blocks, blocks), :, :].reshape(wide, 2 * rows)
            self.turned[: 2 * rows, pl.ds(at, wide)] = tile.T
            self.clear_other(j)

    def unpack_middle(self):
        rows, middle = self.rows, (self.outer // 2) * self.inner
        first = self.turned[rows : 2 * rows, :TILE]
        lane0 = lax.broadcasted_iota(jnp.int32, first.shape, 1) == 0
        zero = jnp.zeros_like(first)
        self.turned[:rows, pl.ds(middle, TILE)] += jnp.where(lane0, first, zero)
        self.turned[rows : 2 * rows, :TILE] = jnp.where(lane0, zero, first)

    def incoming(self, lines, sign, twiddle, matrix, real_out=False):
        def body(r0):
            items = []
            for j in range(self.outer):
                lanes = pl.ds(j * self.inner, self.inner)
                items.append((
                    self.turned[pl.ds(r0, self.step), lanes],
                    self.turned[pl.ds(lines + r0, self.step), lanes],
                ))
            for k, pair in enumerate(small_dft(items, sign)):
                re, im = self.twist(k, pair, sign, twiddle)
                self.put(k, pl.ds(r0, self.step), 0, re)
                self.put(k, pl.ds(r0, self.step), 1, im)

        self.chunks(lines, body)
        self.multiply(lines, matrix, real_out=real_out)

    def outgoing(self, lines, sign, twiddle, matrix, real_in, write):
        self.multiply(lines, matrix, real_in=real_in)

        def body(r0):
            at = pl.ds(r0, self.step)
            write(r0, small_dft([
                self.twist(k, (self.get(k, at, 0), self.get(k, at, 1)), sign, twiddle)
                for k in range(self.outer)
            ], sign))

        self.chunks(lines, body)

    def pack_middle(self, items):
        re, im = items[0]
        lane0 = lax.broadcasted_iota(jnp.int32, im.shape, 1) == 0
        return [(re, jnp.where(lane0, items[self.outer // 2][0], im))] + items[1:]

    def write_full(self, result, pack):
        rows = self.rows

        def write(r0, items):
            at = pl.ds(r0, self.step)
            for j, (re, im) in enumerate(self.pack_middle(items) if pack else items):
                for piece in range(self.inner // rows):
                    to = j * (self.inner // rows) + piece
                    lanes = slice(piece * rows, (piece + 1) * rows)
                    result[to, at, pl.ds(0, rows)] = re[:, lanes]
                    result[to, at, pl.ds(rows, rows)] = im[:, lanes]

        return write

    def pack_cut(self, slabs, results):
        rows, half, wide = self.rows, self.half, self.inner // 2
        cuts, count = len(results), half // len(results)
        groups = TILE // (2 * count)
        tall = rows // groups
        for k in range(self.outer):
            slab = slabs(k)
            for s in range(self.inner // rows):
                for q, result in enumerate(results):
                    parts = []
                    for group in range(groups):
                        for part in range(2):
                            at = part * wide + s * half + q * count
                            parts.append(slab[group * tall : (group + 1) * tall, at : at + count])
                    result[k * (self.inner // rows) + s] = jnp.concatenate(parts, axis=1)

    def turn_cut(self, source, lines, spans):
        blocks = self.inner // self.rows
        groups = TILE // (2 * lines)
        wide = self.inner // groups
        for t in range(spans):
            tile = source[pl.ds(t * blocks, blocks), :, :].reshape(wide, TILE).T
            for h in range(groups):
                held = tile[h * 2 * lines : (h + 1) * 2 * lines]
                self.turned[: 2 * lines, pl.ds(t * self.inner + h * wide, wide)] = held

    def turn_whole(self, source, tiles):
        rows, blocks = self.rows, TILE // self.rows
        for t in range(tiles):
            tile = source[pl.ds(t * blocks, blocks), :rows, :].reshape(TILE, 2 * rows)
            self.turned[: 2 * rows, pl.ds(t * TILE, TILE)] = tile.T

    def first_imaginary(self, at):
        rows = self.rows
        part = self.turned[rows : 2 * rows, pl.ds(at, TILE)]
        lane0 = lax.broadcasted_iota(jnp.int32, part.shape, 1) == 0
        self.turned[rows : 2 * rows, pl.ds(at, TILE)] = jnp.where(lane0, 0.0, part)
        return jnp.where(lane0, part, 0.0)

    def incoming_half(self, lines, sign, twiddle, matrix, flip, extra=None, real_out=False):
        def body(r0):
            at = pl.ds(r0, self.step)
            items = []
            for j in range(self.outer // 2):
                lanes = pl.ds(j * self.inner, self.inner)
                items.append((self.turned[at, lanes], self.turned[pl.ds(lines + r0, self.step), lanes]))
            for k, (re, im) in enumerate(half_dft(items, sign)):
                if extra is not None:
                    re = re - extra[at, :] if k % 2 else re + extra[at, :]
                re, im = self.twist(k, (re, im), sign, twiddle, flip)
                self.put(k, at, 0, re)
                self.put(k, at, 1, im)

        self.chunks(lines, body)
        self.multiply(lines, matrix, real_out=real_out)

    def outgoing_half(self, lines, sign, twiddle, matrix, flip, write):
        self.multiply(lines, matrix)

        def body(r0):
            at = pl.ds(r0, self.step)
            write(r0, small_dft([
                self.twist(k, (self.get(k, at, 0), self.get(k, at, 1)), sign, twiddle, flip)
                for k in range(self.outer)
            ], sign)[: self.outer // 2])

        self.chunks(lines, body)

    def outgoing_sides(self, twiddle, matrix, sides, late=None):
        self.multiply(self.rows, matrix, real_in=True)
        rows, blocks, middle = self.rows, self.inner // self.rows, self.outer // 2
        lines, step = rows // len(sides), self.step
        tall = 2 * lines * rows // TILE
        for h in range(rows // tall):

            def body(i, carry, h=h):
                r0 = pl.multiple_of(i * step, step)
                at = pl.ds(h * tall + r0, step)
                items = small_dft([
                    self.twist(k, (self.get(k, at, 0), self.get(k, at, 1)), -1.0, twiddle)
                    for k in range(self.outer)
                ], -1.0)
                (low, low_im), (high, high_im) = items[0], items[middle]
                lane0 = lax.broadcasted_iota(jnp.int32, low.shape, 1) == 0
                items[0] = (low, jnp.where(lane0, high, low_im))
                items[middle] = (high, jnp.where(lane0, low, high_im))
                if late is not None:
                    items = [
                        tuple(jnp.where(late, one, other) for one, other in zip(items[middle + j], items[j]))
                        for j in range(middle)
                    ]
                for j, pair in enumerate(items):
                    for part, value in enumerate(pair):
                        to = pl.ds((2 * h + part) * lines, lines)
                        for piece in range(blocks):
                            for side, result in enumerate(sides):
                                base = piece * rows + side * lines
                                result[j * blocks + piece, pl.ds(r0, step), to] = value[:, base : base + lines]
                return carry

            lax.fori_loop(0, tall // step, body, 0)

    def outgoing_kept(self, twiddle, matrix, result):
        self.multiply(self.rows, matrix, real_in=True)
        rows, half, blocks = self.rows, self.half, self.inner // self.rows
        tall = rows * rows // TILE
        step = math.gcd(rows, 16)
        span = min(tall, step)
        for h in range(rows // max(tall, step)):

            def body(i, carry, h=h):
                r0 = i * step if isinstance(i, int) else pl.multiple_of(i * step, step)
                at = pl.ds(h * max(tall, step) + r0, step)
                items = self.pack_middle(small_dft([
                    self.twist(k, (self.get(k, at, 0), self.get(k, at, 1)), -1.0, twiddle)
                    for k in range(self.outer)
                ], -1.0))
                for j, pair in enumerate(items):
                    base = self.inner // 2 if 2 * j >= self.outer else 0
                    for piece in range(blocks):
                        lanes = slice(base + piece * half, base + (piece + 1) * half)
                        for part, value in enumerate(pair):
                            for sub in range(step // span):
                                group = h * (step // span) + sub
                                to = pl.ds(group * rows + part * half, half)
                                held = value[sub * span : (sub + 1) * span, lanes]
                                result[j * blocks + piece, pl.ds(r0, span), to] = held
                return carry

            if tall > step:
                lax.fori_loop(0, tall // step, body, 0)
            else:
                body(0, 0)

    def mirrored(self, blocks, mirror):
        dot = functools.partial(jnp.dot, preferred_element_type=jnp.float32)

        def flip(values, which):
            top, low = halves(jnp.concatenate(values, axis=0))
            return dot(top, mirror[which]) + dot(low, mirror[which])

        flat = [part for k in range(self.outer) for pair in blocks[k] for part in pair]
        per = 2 * len(blocks[0])
        low = flip(flat[:per], 0)
        high = flip(flat[per:], 1)
        out = []
        for k in range(self.outer):
            part, base = (low, 0) if k == 0 else (high, (self.outer - k - 1) * per)
            take = lambda i: part[(base + i) * 8 : (base + i + 1) * 8]
            out.append([(take(2 * i), -take(2 * i + 1)) for i in range(per // 2)])
        return out

    def pack_columns(self, slabs, result):
        rows, half, wide = self.rows, self.half, self.inner // 2
        blocks, groups = self.inner // rows, TILE // rows
        tall = rows // groups
        for k in range(self.outer):
            slab = slabs(k)
            for s in range(blocks):
                parts = []
                for group in range(groups):
                    for part in range(2):
                        at = part * wide + s * half
                        parts.append(slab[group * tall : (group + 1) * tall, at : at + half])
                result[k * blocks + s] = jnp.concatenate(parts, axis=1)

    def turn_columns(self, source, result):
        rows, wide, blocks = self.rows, self.inner // 2, self.inner // self.rows
        for j in range(self.outer):
            tile = source[pl.ds(j * blocks, blocks), :, :].reshape(wide, 2 * rows).T
            result[j, :, pl.ds(0, wide)] = tile[:rows]
            result[j, :, pl.ds(wide, wide)] = tile[rows:]

    def spread(self, first, second, strided, result):
        rows, fill = self.rows, TILE - 2 * self.rows
        for t in range(self.length // TILE):
            lanes = pl.ds(t * TILE, TILE)
            parts = [first[:, lanes], second[:, lanes]]
            if fill:
                parts.append(jnp.zeros((fill, TILE), jnp.float32))
            strided[pl.ds(t * TILE, TILE), :] = jnp.concatenate(parts, axis=0).T
        for k in range(self.outer):
            slab = strided[pl.ds(k, self.inner, stride=self.outer), :].T
            result[k] = slab[: 2 * rows, :]

    def collect(self, slabs, strided, results):
        rows = self.rows
        for k in range(self.outer):
            slab = slabs(k)
            fill = TILE - slab.shape[0]
            if fill:
                slab = jnp.concatenate([slab, jnp.zeros((fill, self.inner), jnp.float32)], axis=0)
            strided[pl.ds(k, self.inner, stride=self.outer), :] = slab.T
        for t in range(self.length // TILE):
            block = strided[pl.ds(t * TILE, TILE), :].T
            for i, result in enumerate(results):
                result[:, pl.ds(t * TILE, TILE)] = block[i * rows : (i + 1) * rows, :]


def signed_waves(position, count):
    signed = jnp.where(position < count // 2, position, position - count)
    waves = 4.0 * signed.astype(jnp.float32) / count
    return waves, jnp.where(position == count // 2, jnp.float32(0.0), waves)


def first_waves(piece, k):
    lanes = lax.broadcasted_iota(jnp.int32, (1, piece.inner), 1)
    return signed_waves(piece.outer * lanes + k, piece.length)


def inverse_denominator(wave_first, wave_second):
    square = wave_first * wave_first + wave_second * wave_second
    return 1.0 / (1.0 + time_step * (square * square - square))


def second_wave(piece, position):
    shape = (position.shape[0], piece.inner)
    return jnp.broadcast_to(signed_waves(position, piece.length)[0], shape)


def row_index(count, width):
    return lax.broadcasted_iota(jnp.int32, (count, width), 0)


class Links:
    def __init__(self, devices, fast):
        self.devices, self.fast = devices, fast
        self.device = lax.axis_index(axes[0]) * fast + lax.axis_index(axes[1])
        self.near = min(8, devices // 2)
        self.steps = []
        for low in range(self.near):
            step, bit = 0, 1
            while bit < self.near:
                if low // bit % 2:
                    step += bit * (1 - 2 * lax.rem(lax.div(self.device, bit), 2))
                bit *= 2
            self.steps.append(step)

    def visit(self, count, body):
        near = self.near

        def far(i, carry):
            base = self.partner(count - near * i)
            for low in reversed(range(near)):
                body(base + self.steps[low])
            return carry

        lax.fori_loop(1, count // near, far, 0)
        for low in reversed(range(1, near)):
            body(self.device + self.steps[low])

    def partner(self, i):
        total, bit = 0, 1
        while bit < self.devices:
            total += bit * lax.rem(lax.div(self.device, bit) + lax.div(i, bit), 2)
            bit *= 2
        return total

    def place(self, peer):
        return (lax.div(peer, self.fast), lax.rem(peer, self.fast))

    def greet(self):
        barrier = pltpu.get_barrier_semaphore()

        def go(peer):
            at = self.place(peer)
            pl.semaphore_signal(barrier, inc=1, device_id=at, device_id_type=pl.DeviceIdType.MESH)

        self.visit(self.devices, go)

    def meet(self):
        pl.semaphore_wait(pltpu.get_barrier_semaphore(), self.devices - 1)

    def send(self, source, target, sems, count):
        send_sem, recv_sem, own_sem = sems
        own = lax.rem(self.device, count)

        def go(peer):
            pltpu.make_async_remote_copy(
                src_ref=source(peer if count == self.devices else lax.rem(peer, count)),
                dst_ref=target(own),
                send_sem=send_sem,
                recv_sem=recv_sem,
                device_id=self.place(peer),
                device_id_type=pl.DeviceIdType.MESH,
            ).start()

        self.visit(count, go)
        pltpu.make_async_copy(source(own), target(own), own_sem).start()

    def whole(self, source, target, sems, count):
        others = pl.ds(0, count - 1)
        return pltpu.make_async_remote_copy(
            src_ref=source(others),
            dst_ref=target(others),
            send_sem=sems[0],
            recv_sem=sems[1],
            device_id=(0, 0),
            device_id_type=pl.DeviceIdType.MESH,
        )

    def receive(self, source, target, sems, count):
        own = lax.rem(self.device, count)
        pltpu.make_async_copy(source(own), target(own), sems[2]).wait()
        self.whole(source, target, sems, count).wait_recv()

    def sent(self, source, target, sems, count):
        self.whole(source, target, sems, count).wait_send()


def start_kernel(length, rows, field, target, out, both_p, *scratch):
    piece = Pieces(length, rows)
    piece.spread(field, target, scratch[0], both_p)
    piece.pack_columns(lambda k: both_p[k, pl.ds(0, rows), :], out)


def slope_second_kernel(length, rows, field_p, twiddle, out_matrix, in_matrix, kept, result, *scratch):
    piece = Pieces(length, rows, *scratch)

    def body(r0):
        at = pl.ds(r0, piece.step)
        for k in range(piece.outer):
            piece.put(k, at, 0, field_p[k, at, :])

    piece.chunks(rows, body)
    for j in range(piece.outer):
        piece.clear_other(j)

    def write(r0, items):
        for j, (re, im) in enumerate(items):
            at, wide = piece.kept_lanes(j)
            base = at - j * piece.inner
            position = j * piece.inner + kept[:, base : base + wide]
            slope = 2.0 * signed_waves(position, length)[1]
            piece.turned[pl.ds(r0, piece.step), pl.ds(at, wide)] = -slope * im[:, base : base + wide]
            piece.turned[pl.ds(rows + r0, piece.step), pl.ds(at, wide)] = slope * re[:, base : base + wide]

    piece.outgoing(rows, -1.0, twiddle, out_matrix, True, write)
    piece.incoming(rows, 1.0, twiddle, in_matrix, real_out=True)
    result[...] = piece.z[:, :, : piece.inner]


def spread_kernel(length, rows, forcing, result, strided):
    Pieces(length, rows).spread(forcing.at[0], forcing.at[1], strided, result)


def collect_kernel(length, rows, slabs, result, strided):
    piece = Pieces(length, rows)
    piece.collect(lambda k: slabs[k], strided, [result.at[i] for i in range(result.shape[0])])


def weight_of(device, r0, step, inner):
    alone = (row_index(step, inner) + r0 + device) == 0
    return jnp.where(alone, jnp.float32(1.0), jnp.float32(2.0))


def slope_first_kernel(length, rows, source, in_twiddle, in_matrix, out_twiddle, out_matrix, out, *scratch):
    piece = Pieces(length, rows, *scratch)
    half = piece.half
    piece.turn_lines(source)
    piece.incoming(half, -1.0, in_twiddle, in_matrix)

    def body(r0):
        at = pl.ds(r0, piece.step)
        for k in range(piece.outer):
            re, im = piece.get(k, at, 0), piece.get(k, at, 1)
            scale = first_waves(piece, k)[1]
            piece.put(k, at, 0, -scale * im)
            piece.put(k, at, 1, scale * re)

    piece.chunks(half, body)
    piece.outgoing(half, 1.0, out_twiddle, out_matrix, False, piece.write_full(out, False))


def edge_inverses(piece, k):
    wave_first = first_waves(piece, k)[0]
    middle = jnp.full((1, 1), piece.length // 2, jnp.int32)
    zero = jnp.zeros((1, 1), jnp.int32)
    return [inverse_denominator(wave_first, signed_waves(p, piece.length)[0]) for p in (zero, middle)]


def next_kernel(length, rows, device_ref, source, forcing, in_twiddle, in_matrix, out_twiddle, out_matrix, mirror, out, *scratch):
    device = device_ref[0]
    piece = Pieces(length, rows, *scratch)
    half, step, inner = piece.half, piece.step, piece.inner
    late = device >= (length // rows) // 2
    piece.turn_lines(source)
    piece.incoming(half, -1.0, in_twiddle, in_matrix)

    def body(r0):
        at, also = pl.ds(r0, step), pl.ds(half + r0, step)
        index = row_index(step, 1) + r0
        low_wave = second_wave(piece, device * rows + index)
        high_wave = second_wave(piece, device * rows + half + index)
        moved = jnp.logical_and(row_index(step, inner) + r0 == 0, late)
        weight = weight_of(device, r0, step, inner)
        for k in range(piece.outer):
            wave_first = first_waves(piece, k)[0]
            low = inverse_denominator(wave_first, low_wave)
            high = inverse_denominator(wave_first, high_wave)
            for part in range(2):
                own = weight * piece.get(k, at, part)
                f_low = time_step * forcing[k, pl.ds(part * rows + r0, step), :]
                f_high = time_step * forcing[k, pl.ds(part * rows + half + r0, step), :]
                piece.put(k, at, part, (f_low + jnp.where(moved, 0.0, own)) * low)
                piece.put(k, also, part, (f_high + jnp.where(moved, own, 0.0)) * high)

    piece.chunks(half, body)

    @pl.when(device == 0)
    def _():
        at = pl.ds(0, 8)
        blocks = []
        for k in range(piece.outer):
            own = tuple(piece.get(k, at, part) for part in range(2))
            full = tuple(
                own[part] + time_step * forcing[k, pl.ds(part * rows, 8), :] for part in range(2)
            )
            blocks.append([own, full])
        flipped = piece.mirrored(blocks, mirror)
        rest = pl.ds(0, 16)
        row0 = row_index(16, inner) == 0
        for k in range(piece.outer):
            zero, middle = edge_inverses(piece, k)
            for part in range(2):
                own, full = blocks[k][0][part], blocks[k][1][part]
                own_c, full_c = flipped[k][0][part], flipped[k][1][part]
                value = 0.5 * ((full + full_c) * zero + (own - own_c) * middle)
                replace(piece, k, part, value)

    piece.outgoing(rows, 1.0, out_twiddle, out_matrix, False, piece.write_full(out, False))


def replace(piece, k, part, value):
    lanes = pl.ds(part * piece.inner, piece.inner)
    row0 = row_index(16, piece.inner) == 0
    value = jnp.concatenate([value, value], axis=0)
    for held, new in zip((piece.top, piece.low), halves(value)):
        old = held[k, pl.ds(0, 16), lanes].astype(jnp.float32)
        held[k, pl.ds(0, 16), lanes] = jnp.where(row0, new.astype(jnp.float32), old).astype(jnp.bfloat16)


def misfit_kernel(length, rows, device_ref, source, in_twiddle, in_matrix, out_twiddle, out_matrix, mirror, out, full, total_out, *scratch):
    device = device_ref[0]
    piece = Pieces(length, rows, *scratch)
    half, step, inner = piece.half, piece.step, piece.inner
    late = device >= (length // rows) // 2
    piece.turn_full(source)
    piece.incoming(rows, -1.0, in_twiddle, in_matrix)

    def body(r0):
        at, also = pl.ds(r0, step), pl.ds(half + r0, step)
        index = row_index(step, 1) + r0
        low_wave = second_wave(piece, device * rows + index)
        high_wave = second_wave(piece, device * rows + half + index)
        moved = jnp.logical_and(row_index(step, inner) + r0 == 0, late)
        weight = weight_of(device, r0, step, inner)
        for k in range(piece.outer):
            wave_first = first_waves(piece, k)[0]
            low = time_step * inverse_denominator(wave_first, low_wave)
            high = time_step * inverse_denominator(wave_first, high_wave)
            for part in range(2):
                low_value = piece.get(k, at, part) * low
                high_value = piece.get(k, also, part) * high
                full[k, pl.ds(part * rows + r0, step), :] = low_value
                full[k, pl.ds(part * rows + half + r0, step), :] = high_value
                own = jnp.where(moved, high_value, low_value)
                piece.put(k, at, part, weight * own)

    piece.chunks(half, body)

    @pl.when(device == 0)
    def _():
        at = pl.ds(0, 8)
        blocks = [[(piece.get(k, at, 0), piece.get(k, at, 1))] for k in range(piece.outer)]
        flipped = piece.mirrored(blocks, mirror)
        row0 = row_index(8, inner) == 0
        for k in range(piece.outer):
            zero, middle = edge_inverses(piece, k)
            for part in range(2):
                own, own_c = blocks[k][0][part], flipped[k][0][part]
                first = (0.5 * time_step) * (own + own_c) * zero
                value = first + (0.5 * time_step) * (own - own_c) * middle
                at_full = pl.ds(part * rows, 8)
                full[k, at_full, :] = jnp.where(row0, first, full[k, at_full, :])
                replace(piece, k, part, value)

    piece.outgoing(half, 1.0, out_twiddle, out_matrix, False, piece.write_full(out, False))
    total_out[...] = jnp.sum(source[:, pl.ds(rows, 8), :], axis=0)


def nonlinear_kernel(length, rows, source, both_p, second, twiddle, out_matrix, out, first, *scratch):
    piece = Pieces(length, rows, *scratch)
    piece.turn_columns(source, first)

    def body(r0):
        at = pl.ds(r0, piece.step)
        for k in range(piece.outer):
            one, other = first[k, at, :], second[k, at, :]
            piece.put(k, at, 0, both_p[k, at, :] - (0.5 * time_step) * (one * one + other * other))

    piece.chunks(rows, body)
    piece.outgoing_kept(twiddle, out_matrix, out)


def joint_kernel(length, rows, source, first, second, twiddle, in_matrix, out, value_out, second_out, *scratch):
    piece = Pieces(length, rows, *scratch)
    piece.turn_kept(source)
    piece.unpack_middle()
    piece.incoming(rows, 1.0, twiddle, in_matrix, real_out=True)
    lanes = pl.ds(0, piece.inner)

    def body(r0):
        at = pl.ds(r0, piece.step)
        for k in range(piece.outer):
            value = piece.get(k, at, 0)
            value_out[k, at, :] = (1.0 / time_step) * value
            second_out[k, at, :] = value * second[k, at, :]
            piece.z[k, at, lanes] = value * first[k, at, :]

    piece.chunks(rows, body)
    piece.pack_columns(lambda k: piece.z[k, pl.ds(0, rows), lanes], out)


def residual_kernel(length, rows, source, both_p, twiddle, in_matrix, out_matrix, out, field_out, *scratch):
    piece = Pieces(length, rows, *scratch[:4])
    strided, total = scratch[4:]
    piece.turn_full(source)
    piece.unpack_middle()
    piece.incoming(rows, 1.0, twiddle, in_matrix, real_out=True)
    piece.collect(lambda k: piece.get(k, pl.ds(0, rows), 0), strided, [field_out])
    total[...] = jnp.zeros_like(total)

    def body(r0):
        at = pl.ds(r0, piece.step)
        for k in range(piece.outer):
            residual = piece.get(k, at, 0) - both_p[k, pl.ds(rows + r0, piece.step), :]
            total[...] += residual * residual
            piece.put(k, at, 0, residual)

    piece.chunks(rows, body)
    piece.outgoing(rows, -1.0, twiddle, out_matrix, True, piece.write_full(out, True))
    value = 0.5 * jnp.sum(total[...])
    out[:, pl.ds(rows, 8), :] = jnp.full((out.shape[0], 8, 2 * rows), value, jnp.float32)


def last_kernel(length, rows, source, value, second, field_out, strided, first):
    piece = Pieces(length, rows)
    piece.turn_columns(source, first)
    piece.collect(lambda k: first[k] + value[k] + second[k], strided, [field_out])


def step_kernel(length, rows, devices, fast, cuts, parts, inputs, outs, box):
    links = Links(devices, fast)
    device, half, part_devices = links.device, rows // 2, devices // 2
    late = device >= part_devices
    flip = jnp.where(late, -1.0, 1.0).astype(jnp.float32)
    sides, count = range(parts), rows // parts
    copies, sems = box.copies, box.sems
    work = (box.turned, box.top, box.low, box.z)
    piece = Pieces(length, rows, *work)
    step, inner, outer = piece.step, piece.inner, piece.outer
    both_p, forcing_p, full = box.both_p, box.forcing_p, box.full
    first, second, value = box.first, box.second, box.value
    strided, total = box.strided, box.total
    lanes = pl.ds(0, inner)

    loads = [
        pltpu.make_async_copy(ref, held, copies.at[i])
        for i, (ref, held) in enumerate(zip(inputs.refs, inputs.held))
    ]
    for copy in loads[:2]:
        copy.start()
    links.greet()
    waiting = iter(loads)

    def load(count):
        for i in range(count):
            next(waiting).wait()

    at_all = lambda ref: lambda e: ref.at[e]
    at_lines = lambda ref, base, count: lambda e: ref.at[e, pl.ds(base, count)]
    order = []

    def send(source, target, count=devices):
        i = len(order)
        order.append((source, target, (sems.at[i, 0], sems.at[i, 1], sems.at[i, 2]), count))
        links.send(*order[-1])
        return order[-1]

    def receive(*moves):
        for move in moves:
            links.receive(*move)

    tw_natural, tw_kept, tw_lines, tw_cut = (inputs.twiddles.at[i] for i in range(4))
    forward, backward, mirror = inputs.forward, inputs.backward, inputs.mirror
    kept_out, kept_in, kept = inputs.kept_out, inputs.kept_in, inputs.kept
    lines_in, cut_in = box.lines_in, box.cut_in
    if parts == 2 * cuts:
        tw_lines, lines_in = tw_cut, cut_in

    def permute_rows(groups, result):
        tall, blocks = rows // groups, inner // rows
        for p in range(2):
            for part in range(2):
                for group in range(groups):
                    for s in range(blocks):
                        at = part * inner + group * (inner // groups) + s * tall
                        source = part * inner + s * rows + group * tall
                        result[p, pl.ds(at, tall), :] = forward[p, pl.ds(source, tall), :]

    def slope_first(source, out, lines):
        piece.turn_cut(source, lines, outer)
        piece.incoming(lines, -1.0, tw_cut, cut_in)

        def body(r0):
            at = pl.ds(r0, step)
            for k in range(outer):
                re, im = piece.get(k, at, 0), piece.get(k, at, 1)
                scale = first_waves(piece, k)[1]
                piece.put(k, at, 0, -scale * im)
                piece.put(k, at, 1, scale * re)

        piece.chunks(lines, body)
        piece.outgoing(lines, 1.0, tw_natural, backward, False, piece.write_full(out, False))

    def slope_second(source, out):
        slope_second_kernel(length, rows, source, tw_kept, kept_out, kept_in, kept, out, *work)

    def send_columns(source, target):
        return [send(at_all(source.at[q]), at_all(target.at[q])) for q in range(cuts)]

    def turn_slopes(moves, source, back, target):
        size, result = half // cuts, []
        for q, move in enumerate(moves):
            receive(move)
            slope_first(source.at[q], back.at[q], size)
            result.append(send(at_all(back.at[q]), at_lines(target, q * size, size)))
        return result

    def lines_of(side, r0):
        line = row_index(step, 1) + r0 + side * count
        alone = (row_index(step, inner) + r0 + side * count + lax.rem(device, part_devices)) == 0
        return second_wave(piece, device * rows + line), jnp.where(alone, jnp.float32(1.0), jnp.float32(2.0))

    def edges(k):
        wave = first_waves(piece, k)[0]
        middle = jnp.full((1, 1), length // 2, jnp.int32)
        mine, theirs = jnp.where(late, middle, 0), jnp.where(late, 0, middle)
        return [inverse_denominator(wave, signed_waves(p, length)[0]) for p in (mine, theirs)]

    load(2)
    for copy in loads[2:]:
        copy.start()
    piece.spread(inputs.field, inputs.target, strided, both_p)
    piece.pack_cut(lambda k: both_p[k, pl.ds(0, rows), :], [box.s_field.at[q] for q in range(cuts)])
    links.meet()
    m_field = send_columns(box.s_field, box.r_field)

    load(len(loads) - 2)
    if parts != 2 * cuts:
        permute_rows(TILE * parts // (2 * rows), lines_in)
    permute_rows(TILE * cuts // rows, cut_in)
    slope_second(both_p, second)
    m_slope = turn_slopes(m_field, box.r_field, box.s_slope, box.r_slope)
    piece.spread(inputs.forcing.at[0], inputs.forcing.at[1], strided, forcing_p)

    receive(*m_slope)
    piece.turn_columns(box.r_slope, first)

    def nonlinear(r0):
        at = pl.ds(r0, step)
        for k in range(outer):
            one, other = first[k, at, :], second[k, at, :]
            piece.put(k, at, 0, both_p[k, at, :] - (0.5 * time_step) * (one * one + other * other))

    piece.chunks(rows, nonlinear)
    piece.outgoing_sides(tw_natural, forward, [box.s_sum.at[side] for side in sides], late)
    m_sum = [send(at_all(box.s_sum.at[side]), at_all(box.r_sum.at[side]), part_devices) for side in sides]

    def divide(side):
        def body(r0):
            at = pl.ds(r0, step)
            wave, weight = lines_of(side, r0)
            for k in range(outer):
                scale = inverse_denominator(first_waves(piece, k)[0], wave)
                for part in range(2):
                    forced = time_step * forcing_p[k, pl.ds(part * rows + side * count + r0, step), :]
                    piece.put(k, at, part, (weight * piece.get(k, at, part) + forced) * scale)

        piece.chunks(count, body)
        if side:
            return

        @pl.when(lax.rem(device, part_devices) == 0)
        def _():
            at = pl.ds(0, 8)
            blocks = []
            for k in range(outer):
                own = tuple(piece.get(k, at, part) for part in range(2))
                joined = tuple(own[part] + time_step * forcing_p[k, pl.ds(part * rows, 8), :] for part in range(2))
                blocks.append([own, joined])
            flipped = piece.mirrored(blocks, mirror)
            for k in range(outer):
                mine, theirs = edges(k)
                for part in range(2):
                    own, joined = blocks[k][0][part], blocks[k][1][part]
                    own_c, joined_c = flipped[k][0][part], flipped[k][1][part]
                    replace(piece, k, part, 0.5 * ((joined + joined_c) * mine + (own - own_c) * theirs))

    m_next = []
    for side in sides:
        receive(m_sum[side])
        piece.turn_cut(box.r_sum.at[side], count, outer // 2)
        piece.incoming_half(count, -1.0, tw_lines, lines_in, flip)
        divide(side)
        sent = box.s_next.at[side]
        piece.outgoing(count, 1.0, tw_natural, backward, False, piece.write_full(sent, False))
        m_next.append(send(at_all(sent), at_lines(box.r_next, side * count, count)))

    receive(*m_next)
    piece.turn_whole(box.r_next, length // TILE)
    low, high = piece.first_imaginary(0), piece.first_imaginary(length // 2)
    piece.turned[:rows, pl.ds(0, TILE)] += high
    piece.turned[:rows, pl.ds(length // 2, TILE)] += low
    piece.incoming(rows, 1.0, tw_natural, backward, real_out=True)
    total[...] = jnp.zeros_like(total)

    def misfit(r0):
        at = pl.ds(r0, step)
        for k in range(outer):
            now = piece.get(k, at, 0)
            value[k, at, :] = now
            residual = now - both_p[k, pl.ds(rows + r0, step), :]
            total[...] += residual * residual
            piece.put(k, at, 0, residual)

    piece.chunks(rows, misfit)
    piece.outgoing_sides(tw_natural, forward, [box.s_kept.at[side] for side in sides])
    m_kept = [send(at_all(box.s_kept.at[side]), at_all(box.r_kept.at[side])) for side in sides]
    box.s_total[...] = jnp.full(box.s_total.shape, 0.5 * jnp.sum(total[...]), jnp.float32)
    m_total = send(at_all(box.s_total), at_all(box.r_total))
    piece.collect(lambda k: value[k], strided, [outs.next])

    def adjoint(side):
        def body(r0):
            at = pl.ds(r0, step)
            wave, weight = lines_of(side, r0)
            for k in range(outer):
                scale = time_step * inverse_denominator(first_waves(piece, k)[0], wave)
                for part in range(2):
                    own = piece.get(k, at, part) * scale
                    full[k, pl.ds(part * rows + side * count + r0, step), :] = own
                    piece.put(k, at, part, weight * own)

        piece.chunks(count, body)
        if side:
            return

        @pl.when(lax.rem(device, part_devices) == 0)
        def _():
            at = pl.ds(0, 8)
            blocks = [[(piece.get(k, at, 0), piece.get(k, at, 1))] for k in range(outer)]
            flipped = piece.mirrored(blocks, mirror)
            row0 = row_index(8, inner) == 0
            for k in range(outer):
                mine, theirs = edges(k)
                for part in range(2):
                    own, own_c = blocks[k][0][part], flipped[k][0][part]
                    line = (0.5 * time_step) * (own + own_c) * mine
                    at_full = pl.ds(part * rows, 8)
                    full[k, at_full, :] = jnp.where(row0, line, full[k, at_full, :])
                    replace(piece, k, part, line + (0.5 * time_step) * (own - own_c) * theirs)

    m_back = []
    for side in sides:
        receive(m_kept[side])
        piece.turn_cut(box.r_kept.at[side], count, outer)
        piece.incoming(count, -1.0, tw_lines, lines_in)
        adjoint(side)
        sent = box.s_back.at[side]
        piece.outgoing_half(count, 1.0, tw_natural, backward, flip, piece.write_full(sent, False))
        m_back.append(send(at_all(sent), at_lines(box.r_back, side * count, count), part_devices))

    receive(*m_back)
    piece.turn_whole(box.r_back, length // (2 * TILE))
    box.extra[:, pl.ds(0, TILE)] = piece.first_imaginary(0)
    box.extra[:, pl.ds(TILE, inner - TILE)] = jnp.zeros((rows, inner - TILE), jnp.float32)
    piece.incoming_half(rows, 1.0, tw_natural, backward, flip, box.extra, real_out=True)

    def products(r0):
        at = pl.ds(r0, step)
        for k in range(outer):
            now = piece.get(k, at, 0)
            value[k, at, :] = (1.0 / time_step) * now
            box.product[k, at, :] = now * second[k, at, :]
            piece.z[k, at, lanes] = now * first[k, at, :]

    piece.chunks(rows, products)
    piece.pack_cut(lambda k: piece.z[k, pl.ds(0, rows), lanes], [box.s_product.at[q] for q in range(cuts)])
    m_product = send_columns(box.s_product, box.r_product)
    slope_second(box.product, second)
    for k in range(outer):
        value[k] = value[k] + second[k]
    m_last = turn_slopes(m_product, box.r_product, box.s_last, box.r_last)

    piece.collect(lambda k: full[k], strided, [outs.forcing.at[i] for i in range(2)])
    receive(m_total)
    outs.total[...] = jnp.sum(box.r_total[...], axis=0) / (length * length)

    receive(*m_last)
    piece.turn_columns(box.r_last, first)
    for k in range(outer):
        outs.field[k] = first[k] + value[k]
    for move in order:
        links.sent(*move)


def joined_step(field, target, forcing, devices, fast, rows, length):
    outer, inner = split_length(length)
    half, step, cuts = rows // 2, math.gcd(rows // 2, 16), 2
    parts = 2
    natural, kept = orders(length, rows)[:2]
    lines = line_order(inner, rows, TILE * parts // (2 * rows))
    cut = line_order(inner, rows, TILE * cuts // rows)
    matrix = lambda *args: matrix_table(length, *args)
    tables = dict(
        field=field, target=target,
        twiddles=np.stack([twiddle_table(length, o) for o in (natural, kept, lines, cut)]),
        kept=kept[None, :].astype(np.int32),
        kept_out=matrix(-1.0, natural, kept)[:, :inner],
        kept_in=matrix(1.0, kept, natural)[:, :, :inner],
        forcing=forcing,
        backward=matrix(1.0, natural, natural),
        forward=matrix(-1.0, natural, natural),
        mirror=mirror_table(length),
    )
    operands = [jnp.asarray(table) for table in tables.values()]
    float32 = jnp.float32
    held = lambda *dims: pltpu.VMEM(dims, float32)
    packed = held(parts, devices, 2 * rows * rows // (parts * TILE), TILE)
    lined = held(parts, devices, rows // parts, 2 * rows)
    packed_half, lined_half = (held(parts, devices // 2, *dims.shape[2:]) for dims in (packed, lined))
    columns, slopes = held(cuts, devices, rows * rows // (TILE * cuts), TILE), held(cuts, devices, half // cuts, 2 * rows)
    returned = held(devices, half, 2 * rows)
    table = pltpu.VMEM((2, 2 * inner, 2 * inner), jnp.bfloat16)
    pair, one = held(outer, 2 * rows, inner), held(outer, rows, inner)
    small = held(devices, 1, TILE)
    halved = pltpu.VMEM((outer, rows, 2 * inner), jnp.bfloat16)
    shapes = dict(
        turned=held(2 * rows, length), top=halved, low=halved, z=held(outer, rows, 2 * inner),
        strided=held(length, TILE), total=held(step, inner),
        both_p=pair, forcing_p=pair, full=pair, first=one, second=one, value=one, product=one,
        lines_in=table, cut_in=table, extra=held(rows, inner),
        s_field=columns, r_field=columns, s_slope=slopes, r_slope=returned,
        s_sum=packed_half, r_sum=packed_half, s_next=lined, r_next=held(devices, rows, 2 * rows),
        s_kept=packed, r_kept=packed, s_total=small, r_total=small,
        s_back=lined_half, r_back=held(devices // 2, rows, 2 * rows),
        s_product=columns, r_product=columns, s_last=slopes, r_last=returned,
        copies=pltpu.SemaphoreType.DMA((len(operands),)),
        sems=pltpu.SemaphoreType.DMA((1 + 4 * parts + 4 * cuts, 3)),
    )
    inputs = [pltpu.VMEM(operand.shape, operand.dtype) for operand in operands]

    def body(*refs):
        a, b = len(operands), len(operands) + 4
        c = b + len(operands)
        given = SimpleNamespace(refs=refs[:a], held=refs[b:c], **dict(zip(tables, refs[b:c])))
        outs = SimpleNamespace(next=refs[a], field=refs[a + 1], forcing=refs[a + 2], total=refs[a + 3])
        step_kernel(length, rows, devices, fast, cuts, parts, given, outs, SimpleNamespace(**dict(zip(shapes, refs[c:]))))

    anywhere = pl.BlockSpec(memory_space=pl.ANY)
    vmem, smem = pl.BlockSpec(memory_space=pltpu.VMEM), pl.BlockSpec(memory_space=pltpu.SMEM)
    shape = lambda *dims: jax.ShapeDtypeStruct(dims, float32)
    next_field, slabs, forcing_grad, total = pl.pallas_call(
        body,
        out_shape=(shape(rows, length), shape(outer, rows, inner), shape(2, rows, length), shape(1, TILE)),
        in_specs=[pl.BlockSpec(memory_space=pltpu.HBM)] * len(operands),
        out_specs=(vmem, vmem, vmem, vmem),
        scratch_shapes=inputs + list(shapes.values()),
        compiler_params=pltpu.CompilerParams(vmem_limit_bytes=34 * 2**20, has_side_effects=True, collective_id=0),
        cost_estimate=pl.CostEstimate(flops=6 * 10**10, bytes_accessed=4 * 2**20, transcendentals=0),
    )(*[pltpu.with_memory_space_constraint(one, pltpu.HBM) for one in operands])
    return pl.pallas_call(
        functools.partial(tail_kernel, length, rows),
        out_shape=(shape(rows, length), shape(rows, length), shape(2, rows, length), shape(1, 1)),
        in_specs=[vmem] * 4,
        out_specs=(anywhere, anywhere, anywhere, smem),
        scratch_shapes=[held(length, TILE), held(rows, length), pltpu.SemaphoreType.DMA((3,))],
        compiler_params=pltpu.CompilerParams(vmem_limit_bytes=8 * 2**20),
        cost_estimate=pl.CostEstimate(flops=10**9, bytes_accessed=4 * 2**20, transcendentals=0),
    )(next_field, slabs, forcing_grad, total)


def tail_kernel(length, rows, next_field, slabs, forcing_grad, total, next_out, field_out, forcing_out, total_out, strided, held, sems):
    piece = Pieces(length, rows)
    copies = [
        pltpu.make_async_copy(next_field, next_out, sems.at[0]),
        pltpu.make_async_copy(forcing_grad, forcing_out, sems.at[1]),
        pltpu.make_async_copy(held, field_out, sems.at[2]),
    ]
    copies[0].start()
    copies[1].start()
    total_out[0, 0] = jnp.sum(total[0:1, 0:1])
    piece.collect(lambda k: slabs[k], strided, [held])
    copies[2].start()
    for copy in copies:
        copy.wait()


def member_step(device, field, target, forcing_p, devices, rows, length):
    outer, inner = split_length(length)
    half = rows // 2
    float32 = jnp.float32
    shape = lambda *dims: jax.ShapeDtypeStruct(dims, float32)
    kept_blocks = shape(devices, rows * rows // TILE, TILE)
    half_blocks = shape(devices, half, 2 * rows)
    blocks = shape(devices, rows, 2 * rows)
    longer = shape(devices, rows + 8, 2 * rows)
    pair, one = shape(outer, 2 * rows, inner), shape(outer, rows, inner)
    plain = shape(rows, length)
    step = math.gcd(half, 16)
    base = [
        pltpu.VMEM((2 * rows, length), float32),
        pltpu.VMEM((outer, rows, 2 * inner), jnp.bfloat16),
        pltpu.VMEM((outer, rows, 2 * inner), jnp.bfloat16),
        pltpu.VMEM((outer, rows, 2 * inner), float32),
    ]
    strided = pltpu.VMEM((length, TILE), float32)
    total = pltpu.VMEM((step, inner), float32)
    vmem = pl.BlockSpec(memory_space=pltpu.VMEM)
    smem = pl.BlockSpec(memory_space=pltpu.SMEM)

    natural, kept, lines = orders(length, rows)
    tw_natural, tw_kept, tw_lines = [jnp.asarray(twiddle_table(length, o)) for o in (natural, kept, lines)]
    matrix = lambda *args: matrix_table(length, *args)
    forward, backward = matrix(-1.0, natural, natural), matrix(1.0, natural, natural)
    kept_out, kept_in = matrix(-1.0, natural, kept)[:, :inner], matrix(1.0, kept, natural)[:, :, :inner]
    lines_in = matrix(-1.0, lines, natural)
    mirror = jnp.asarray(mirror_table(length))
    kept_lane = jnp.asarray(kept[None, :].astype(np.int32))

    def call(body, outs, scratch, *operands):
        return pl.pallas_call(
            functools.partial(body, length, rows),
            out_shape=outs,
            in_specs=[smem if operand is device else vmem for operand in operands],
            out_specs=jax.tree.map(lambda leaf: vmem, outs),
            scratch_shapes=scratch,
            compiler_params=pltpu.CompilerParams(vmem_limit_bytes=20 * 2**20),
            cost_estimate=pl.CostEstimate(flops=6 * 10**9, bytes_accessed=4 * 2**20, transcendentals=0),
        )(*operands)

    def move(value):
        return lax.all_to_all(value, axes, split_axis=0, concat_axis=0, tiled=True)

    spectral_tables = (tw_lines, lines_in, tw_natural, backward)
    slope_tables = (tw_kept, kept_out, kept_in, kept_lane)
    sent, both_p = call(start_kernel, (kept_blocks, pair), [strided], field, target)
    second = call(slope_second_kernel, one, base, both_p, *slope_tables)
    sent = call(slope_first_kernel, half_blocks, base, move(sent), *spectral_tables)
    sent, first = call(nonlinear_kernel, (kept_blocks, one), base, move(sent), both_p, second, tw_kept, kept_out)
    sent = call(next_kernel, blocks, base, device, move(sent), forcing_p, *spectral_tables, mirror)
    sent, next_field = call(
        residual_kernel, (longer, plain), base + [strided, total],
        move(sent), both_p, tw_natural, backward, forward,
    )
    sent, full, sums = call(
        misfit_kernel, (half_blocks, pair, shape(8, 2 * rows)), base,
        device, move(sent), tw_natural, forward, tw_natural, backward, mirror,
    )
    sent, value, product = call(
        joint_kernel, (kept_blocks, one, one), base, move(sent), first, second, tw_kept, kept_in
    )
    second_part = call(slope_second_kernel, one, base, product, *slope_tables)
    sent = call(slope_first_kernel, half_blocks, base, move(sent), *spectral_tables)
    field_grad = call(
        last_kernel, plain, [strided, pltpu.VMEM((outer, rows, inner), float32)], move(sent), value, second_part
    )
    return next_field, sums[0, 0], field_grad, full


def per_device(devices, fast, initial_field, target_field, forcing):
    members, rows, length = initial_field.shape
    device = lax.axis_index(axes).astype(jnp.int32).reshape(1)
    outer, inner = split_length(length)
    vmem = pl.BlockSpec(memory_space=pltpu.VMEM)
    strided = pltpu.VMEM((length, TILE), jnp.float32)

    def reorder(body, shape, operand):
        return pl.pallas_call(
            functools.partial(body, length, rows),
            out_shape=jax.ShapeDtypeStruct(shape, jnp.float32),
            in_specs=[vmem],
            out_specs=vmem,
            scratch_shapes=[strided],
        )(operand)

    if rows * rows % (TILE * 32) == 0 and TILE % rows == 0:
        results = [
            joined_step(initial_field[m], target_field[m], forcing, devices, fast, rows, length)
            for m in range(members)
        ]
        next_field = jnp.stack([one[0] for one in results])
        field_grad = jnp.stack([one[1] for one in results])
        forcing_grad = sum(one[2] for one in results)
        objective = sum(one[3].reshape(()) for one in results) / members
        return (next_field, objective, field_grad, forcing_grad)
    forcing_p = reorder(spread_kernel, (outer, 2 * rows, inner), forcing)
    results = [
        member_step(device, initial_field[m], target_field[m], forcing_p, devices, rows, length)
        for m in range(members)
    ]
    next_field = jnp.stack([one[0] for one in results])
    objective = sum(one[1] for one in results) / (members * length * length)
    field_grad = jnp.stack([one[2] for one in results])
    forcing_grad = reorder(collect_kernel, (2, rows, length), sum(one[3] for one in results))
    return (next_field, objective, field_grad, forcing_grad)


def solution(mesh):
    devices = mesh.shape["px"] * mesh.shape["py"]
    spec = P(None, axes, None)
    return jax.shard_map(
        functools.partial(per_device, devices, mesh.shape["py"]),
        mesh=mesh,
        in_specs=(spec, spec, spec),
        out_specs=(spec, P(), spec, spec),
        check_vma=False,
    )
```

```python
import functools
import math
from types import SimpleNamespace

import jax
import jax.numpy as jnp
import numpy as np
from jax import lax
from jax.experimental import pallas as pl
from jax.experimental.pallas import tpu as pltpu
from jax.sharding import PartitionSpec as P

time_step = 0.25
axes = ("px", "py")
TILE = 128


def split_length(length):
    inner = 256 if length % 256 == 0 else TILE
    return (length // inner, inner)


def small_dft(items, sign):
    count = len(items)
    if count == 1:
        return items
    evens = small_dft(items[0::2], sign)
    odds = small_dft(items[1::2], sign)
    low, high = [], []
    for k in range(count // 2):
        odd_re, odd_im = odds[k]
        if 4 * k == count:
            odd_re, odd_im = (-odd_im, odd_re) if sign > 0 else (odd_im, -odd_re)
        elif k:
            c = math.cos(2.0 * math.pi * k / count)
            s = sign * math.sin(2.0 * math.pi * k / count)
            if abs(abs(c) - abs(s)) < 1e-12:
                sc, ss = math.copysign(1.0, c), math.copysign(1.0, s)
                odd_re, odd_im = (
                    c * (odd_re - sc * ss * odd_im),
                    c * (odd_im + sc * ss * odd_re),
                )
            else:
                odd_re, odd_im = (c * odd_re - s * odd_im, c * odd_im + s * odd_re)
        even_re, even_im = evens[k]
        low.append((even_re + odd_re, even_im + odd_im))
        high.append((even_re - odd_re, even_im - odd_im))
    return low + high


def half_dft(items, sign):
    count = 2 * len(items)
    turned = []
    for j, (re, im) in enumerate(items):
        c = math.cos(2.0 * math.pi * j / count)
        s = sign * math.sin(2.0 * math.pi * j / count)
        turned.append((re, im) if j == 0 else (c * re - s * im, c * im + s * re))
    pairs = zip(small_dft(items, sign), small_dft(turned, sign))
    return [one for pair in pairs for one in pair]


def halves(value):
    top = value.astype(jnp.bfloat16)
    return top, (value - top.astype(jnp.float32)).astype(jnp.bfloat16)


def orders(length, rows):
    inner = split_length(length)[1]
    half = rows // 2
    lane = np.arange(inner)
    natural = lane
    local = lane % (inner // 2)
    line = local % half
    kept = rows * (local // half) + np.where((lane >= inner // 2) & (line == 0), half, line)
    return natural, kept, line_order(inner, rows, TILE // rows)


def line_order(inner, rows, groups):
    lane = np.arange(inner)
    tall, wide = rows // groups, inner // groups
    within = lane % wide
    return rows * (within // tall) + tall * (lane // wide) + within % tall


def twiddle_table(length, order):
    outer = split_length(length)[0]
    angle = 2.0 * np.pi * np.outer(np.arange(outer), order) / length
    return (np.stack([np.cos(angle), np.sin(angle)]) / math.sqrt(length)).astype(np.float32)


def matrix_table(length, sign, left, right):
    inner = split_length(length)[1]
    angle = 2.0 * np.pi * (np.outer(left, right) % inner) / inner
    c, s = np.cos(angle), np.sin(angle)
    full = np.block([[c, sign * s], [-sign * s, c]])
    top = full.astype(jnp.bfloat16)
    return np.stack([top, (full - top.astype(np.float64)).astype(jnp.bfloat16)])


def mirror_table(length):
    inner = split_length(length)[1]
    lane = np.arange(inner)
    both = np.zeros((2, inner, inner))
    both[0, (inner - lane) % inner, lane] = 1.0
    both[1, inner - 1 - lane, lane] = 1.0
    return both.astype(jnp.bfloat16)


class Pieces:
    def __init__(self, length, rows, turned=None, top=None, low=None, grid_out=None):
        self.length, self.rows, self.half = length, rows, rows // 2
        self.outer, self.inner = split_length(length)
        self.turned, self.top, self.low, self.z = turned, top, low, grid_out
        self.step = math.gcd(rows // 2, 16)

    def chunks(self, lines, body):
        def run(i, carry):
            body(pl.multiple_of(i * self.step, self.step))
            return carry

        lax.fori_loop(0, lines // self.step, run, 0)

    def put(self, k, at, part, value):
        lanes = pl.ds(part * self.inner, self.inner)
        top, low = halves(value)
        self.top[k, at, lanes] = top
        self.low[k, at, lanes] = low

    def get(self, k, at, part):
        return self.z[k, at, pl.ds(part * self.inner, self.inner)]

    def multiply(self, lines, matrix, real_in=False, real_out=False):
        deep = self.inner if real_in else 2 * self.inner
        wide = self.inner if real_out else 2 * self.inner
        count = self.outer * lines
        top = self.top[:, :lines, :deep].reshape(count, deep)
        low = self.low[:, :lines, :deep].reshape(count, deep)
        right_top = matrix[0, :deep, :wide]
        right_low = matrix[1, :deep, :wide]
        dot = functools.partial(jnp.dot, preferred_element_type=jnp.float32)
        total = dot(top, right_top) + dot(low, right_top) + dot(top, right_low)
        self.z[:, :lines, :wide] = total.reshape(self.outer, lines, wide)

    def twist(self, k, pair, sign, twiddle, flip=None):
        c = twiddle[0, pl.ds(k, 1), :]
        s = twiddle[1, pl.ds(k, 1), :]
        if flip is not None and k % 2:
            c, s = flip * c, flip * s
        s = s if sign > 0 else -s
        re, im = pair
        return (re * c - im * s, re * s + im * c)

    def turn_full(self, source):
        rows, blocks = self.rows, TILE // self.rows
        for t in range(self.length // TILE):
            tile = source[pl.ds(t * blocks, blocks), :rows, :].reshape(TILE, 2 * rows)
            self.turned[: 2 * rows, pl.ds(t * TILE, TILE)] = tile.T

    def turn_lines(self, source):
        rows = self.rows
        groups = TILE // rows
        blocks, wide = self.inner // rows, self.inner // groups
        for t in range(self.outer):
            tile = source[pl.ds(t * blocks, blocks), :, :].reshape(wide, TILE).T
            for h in range(groups):
                self.turned[:rows, pl.ds(t * self.inner + h * wide, wide)] = tile[h * rows : (h + 1) * rows]

    def kept_lanes(self, j):
        wide = self.inner // 2
        return j * self.inner + (wide if 2 * j >= self.outer else 0), wide

    def clear_other(self, j):
        at, wide = self.kept_lanes(j)
        other = j * self.inner + (0 if 2 * j >= self.outer else wide)
        self.turned[: 2 * self.rows, pl.ds(other, wide)] = jnp.zeros((2 * self.rows, wide), jnp.float32)

    def turn_kept(self, source):
        rows, half, blocks = self.rows, self.half, self.inner // self.rows
        for j in range(self.outer):
            at, wide = self.kept_lanes(j)
            tile = source[pl.ds(j * blocks, blocks), :, :].reshape(wide, 2 * rows)
            self.turned[: 2 * rows, pl.ds(at, wide)] = tile.T
            self.clear_other(j)

    def unpack_middle(self):
        rows, middle = self.rows, (self.outer // 2) * self.inner
        first = self.turned[rows : 2 * rows, :TILE]
        lane0 = lax.broadcasted_iota(jnp.int32, first.shape, 1) == 0
        zero = jnp.zeros_like(first)
        self.turned[:rows, pl.ds(middle, TILE)] += jnp.where(lane0, first, zero)
        self.turned[rows : 2 * rows, :TILE] = jnp.where(lane0, zero, first)

    def incoming(self, lines, sign, twiddle, matrix, real_out=False):
        def body(r0):
            items = []
            for j in range(self.outer):
                lanes = pl.ds(j * self.inner, self.inner)
                items.append((
                    self.turned[pl.ds(r0, self.step), lanes],
                    self.turned[pl.ds(lines + r0, self.step), lanes],
                ))
            for k, pair in enumerate(small_dft(items, sign)):
                re, im = self.twist(k, pair, sign, twiddle)
                self.put(k, pl.ds(r0, self.step), 0, re)
                self.put(k, pl.ds(r0, self.step), 1, im)

        self.chunks(lines, body)
        self.multiply(lines, matrix, real_out=real_out)

    def outgoing(self, lines, sign, twiddle, matrix, real_in, write):
        self.multiply(lines, matrix, real_in=real_in)

        def body(r0):
            at = pl.ds(r0, self.step)
            write(r0, small_dft([
                self.twist(k, (self.get(k, at, 0), self.get(k, at, 1)), sign, twiddle)
                for k in range(self.outer)
            ], sign))

        self.chunks(lines, body)

    def pack_middle(self, items):
        re, im = items[0]
        lane0 = lax.broadcasted_iota(jnp.int32, im.shape, 1) == 0
        return [(re, jnp.where(lane0, items[self.outer // 2][0], im))] + items[1:]

    def write_full(self, result, pack):
        rows = self.rows

        def write(r0, items):
            at = pl.ds(r0, self.step)
            for j, (re, im) in enumerate(self.pack_middle(items) if pack else items):
                for piece in range(self.inner // rows):
                    to = j * (self.inner // rows) + piece
                    lanes = slice(piece * rows, (piece + 1) * rows)
                    result[to, at, pl.ds(0, rows)] = re[:, lanes]
                    result[to, at, pl.ds(rows, rows)] = im[:, lanes]

        return write

    def pack_cut(self, slabs, results):
        rows, half, wide = self.rows, self.half, self.inner // 2
        cuts, count = len(results), half // len(results)
        groups = TILE // (2 * count)
        tall = rows // groups
        for k in range(self.outer):
            slab = slabs(k)
            for s in range(self.inner // rows):
                for q, result in enumerate(results):
                    parts = []
                    for group in range(groups):
                        for part in range(2):
                            at = part * wide + (q * (self.inner // rows) + s) * count
                            parts.append(slab[group * tall : (group + 1) * tall, at : at + count])
                    result[k * (self.inner // rows) + s] = jnp.concatenate(parts, axis=1)

    def turn_cut(self, source, lines, spans):
        blocks = self.inner // self.rows
        groups = TILE // (2 * lines)
        wide = self.inner // groups
        for t in range(spans):
            tile = source[pl.ds(t * blocks, blocks), :, :].reshape(wide, TILE).T
            for h in range(groups):
                held = tile[h * 2 * lines : (h + 1) * 2 * lines]
                self.turned[: 2 * lines, pl.ds(t * self.inner + h * wide, wide)] = held

    def turn_whole(self, source, tiles):
        rows, blocks = self.rows, TILE // self.rows
        for t in range(tiles):
            tile = source[pl.ds(t * blocks, blocks), :rows, :].reshape(TILE, 2 * rows)
            self.turned[: 2 * rows, pl.ds(t * TILE, TILE)] = tile.T

    def turn_side(self, source, base, lines, spans):
        blocks = self.inner // self.rows
        for j in range(spans):
            tile = source[pl.ds(j * blocks, blocks), pl.ds(base, lines), :].reshape(blocks * lines, 2 * self.rows)
            self.turned[: 2 * self.rows, pl.ds(j * self.inner, blocks * lines)] = tile.T

    def turn_part(self, source, base, lines, result):
        rows, wide, blocks = self.rows, self.inner // 2, self.inner // self.rows
        count = blocks * lines
        for j in range(self.outer):
            tile = source[pl.ds(j * blocks, blocks), pl.ds(base, lines), :].reshape(count, 2 * rows).T
            result[j, :, pl.ds(base * blocks, count)] = tile[:rows]
            result[j, :, pl.ds(wide + base * blocks, count)] = tile[rows:]

    def incoming_side(self, side, spans, twiddle, matrix, flip=None, extra=None):
        rows, inner = self.rows, self.inner
        wide = matrix.shape[2] // 2
        held = twiddle.at[:, :, pl.ds(side * wide, wide)]
        transform = small_dft if spans == self.outer else half_dft

        def body(r0):
            at = pl.ds(r0, self.step)
            items = []
            for j in range(spans):
                lanes = pl.ds(j * inner, wide)
                items.append((self.turned[at, lanes], self.turned[pl.ds(rows + r0, self.step), lanes]))
            for k, (re, im) in enumerate(transform(items, 1.0)):
                if extra is not None:
                    re = re - extra[at, :wide] if k % 2 else re + extra[at, :wide]
                for part, value in enumerate(self.twist(k, (re, im), 1.0, held, flip)):
                    top, low = halves(value)
                    self.top[k, at, pl.ds(part * wide, wide)] = top
                    self.low[k, at, pl.ds(part * wide, wide)] = low

        self.chunks(rows, body)
        deep, count = 2 * wide, self.outer * rows
        top = self.top[:, :rows, :deep].reshape(count, deep)
        low = self.low[:, :rows, :deep].reshape(count, deep)
        right_top, right_low = matrix[0, side], matrix[1, side]
        dot = functools.partial(jnp.dot, preferred_element_type=jnp.float32)
        total = dot(top, right_top) + dot(low, right_top) + dot(top, right_low)
        total = total.reshape(self.outer, rows, inner)
        if side:
            total = self.z[:, :rows, :inner] + total
        self.z[:, :rows, :inner] = total

    def first_imaginary(self, at):
        rows = self.rows
        part = self.turned[rows : 2 * rows, pl.ds(at, TILE)]
        lane0 = lax.broadcasted_iota(jnp.int32, part.shape, 1) == 0
        self.turned[rows : 2 * rows, pl.ds(at, TILE)] = jnp.where(lane0, 0.0, part)
        return jnp.where(lane0, part, 0.0)

    def incoming_half(self, lines, sign, twiddle, matrix, flip, extra=None, real_out=False):
        def body(r0):
            at = pl.ds(r0, self.step)
            items = []
            for j in range(self.outer // 2):
                lanes = pl.ds(j * self.inner, self.inner)
                items.append((self.turned[at, lanes], self.turned[pl.ds(lines + r0, self.step), lanes]))
            for k, (re, im) in enumerate(half_dft(items, sign)):
                if extra is not None:
                    re = re - extra[at, :] if k % 2 else re + extra[at, :]
                re, im = self.twist(k, (re, im), sign, twiddle, flip)
                self.put(k, at, 0, re)
                self.put(k, at, 1, im)

        self.chunks(lines, body)
        self.multiply(lines, matrix, real_out=real_out)

    def outgoing_half(self, lines, sign, twiddle, matrix, flip, write):
        self.multiply(lines, matrix)

        def body(r0):
            at = pl.ds(r0, self.step)
            write(r0, small_dft([
                self.twist(k, (self.get(k, at, 0), self.get(k, at, 1)), sign, twiddle, flip)
                for k in range(self.outer)
            ], sign)[: self.outer // 2])

        self.chunks(lines, body)

    def outgoing_sides(self, twiddle, matrix, sides, late=None):
        self.multiply(self.rows, matrix, real_in=True)
        rows, blocks, middle = self.rows, self.inner // self.rows, self.outer // 2
        lines, step = rows // len(sides), self.step
        tall = 2 * lines * rows // TILE
        for h in range(rows // tall):

            def body(i, carry, h=h):
                r0 = pl.multiple_of(i * step, step)
                at = pl.ds(h * tall + r0, step)
                items = small_dft([
                    self.twist(k, (self.get(k, at, 0), self.get(k, at, 1)), -1.0, twiddle)
                    for k in range(self.outer)
                ], -1.0)
                (low, low_im), (high, high_im) = items[0], items[middle]
                lane0 = lax.broadcasted_iota(jnp.int32, low.shape, 1) == 0
                items[0] = (low, jnp.where(lane0, high, low_im))
                items[middle] = (high, jnp.where(lane0, low, high_im))
                if late is not None:
                    items = [
                        tuple(jnp.where(late, one, other) for one, other in zip(items[middle + j], items[j]))
                        for j in range(middle)
                    ]
                for j, pair in enumerate(items):
                    for part, value in enumerate(pair):
                        to = pl.ds((2 * h + part) * lines, lines)
                        for piece in range(blocks):
                            for side, result in enumerate(sides):
                                base = piece * rows + side * lines
                                result[j * blocks + piece, pl.ds(r0, step), to] = value[:, base : base + lines]
                return carry

            lax.fori_loop(0, tall // step, body, 0)

    def outgoing_kept(self, twiddle, matrix, result):
        self.multiply(self.rows, matrix, real_in=True)
        rows, half, blocks = self.rows, self.half, self.inner // self.rows
        tall = rows * rows // TILE
        step = math.gcd(rows, 16)
        span = min(tall, step)
        for h in range(rows // max(tall, step)):

            def body(i, carry, h=h):
                r0 = i * step if isinstance(i, int) else pl.multiple_of(i * step, step)
                at = pl.ds(h * max(tall, step) + r0, step)
                items = self.pack_middle(small_dft([
                    self.twist(k, (self.get(k, at, 0), self.get(k, at, 1)), -1.0, twiddle)
                    for k in range(self.outer)
                ], -1.0))
                for j, pair in enumerate(items):
                    base = self.inner // 2 if 2 * j >= self.outer else 0
                    for piece in range(blocks):
                        lanes = slice(base + piece * half, base + (piece + 1) * half)
                        for part, value in enumerate(pair):
                            for sub in range(step // span):
                                group = h * (step // span) + sub
                                to = pl.ds(group * rows + part * half, half)
                                held = value[sub * span : (sub + 1) * span, lanes]
                                result[j * blocks + piece, pl.ds(r0, span), to] = held
                return carry

            if tall > step:
                lax.fori_loop(0, tall // step, body, 0)
            else:
                body(0, 0)

    def mirrored(self, blocks, mirror):
        dot = functools.partial(jnp.dot, preferred_element_type=jnp.float32)

        def flip(values, which):
            top, low = halves(jnp.concatenate(values, axis=0))
            return dot(top, mirror[which]) + dot(low, mirror[which])

        flat = [part for k in range(self.outer) for pair in blocks[k] for part in pair]
        per = 2 * len(blocks[0])
        low = flip(flat[:per], 0)
        high = flip(flat[per:], 1)
        out = []
        for k in range(self.outer):
            part, base = (low, 0) if k == 0 else (high, (self.outer - k - 1) * per)
            take = lambda i: part[(base + i) * 8 : (base + i + 1) * 8]
            out.append([(take(2 * i), -take(2 * i + 1)) for i in range(per // 2)])
        return out

    def pack_columns(self, slabs, result):
        rows, half, wide = self.rows, self.half, self.inner // 2
        blocks, groups = self.inner // rows, TILE // rows
        tall = rows // groups
        for k in range(self.outer):
            slab = slabs(k)
            for s in range(blocks):
                parts = []
                for group in range(groups):
                    for part in range(2):
                        at = part * wide + s * half
                        parts.append(slab[group * tall : (group + 1) * tall, at : at + half])
                result[k * blocks + s] = jnp.concatenate(parts, axis=1)

    def turn_columns(self, source, result):
        rows, wide, blocks = self.rows, self.inner // 2, self.inner // self.rows
        for j in range(self.outer):
            tile = source[pl.ds(j * blocks, blocks), :, :].reshape(wide, 2 * rows).T
            result[j, :, pl.ds(0, wide)] = tile[:rows]
            result[j, :, pl.ds(wide, wide)] = tile[rows:]

    def spread(self, first, second, strided, result):
        rows, fill = self.rows, TILE - 2 * self.rows
        for t in range(self.length // TILE):
            lanes = pl.ds(t * TILE, TILE)
            parts = [first[:, lanes], second[:, lanes]]
            if fill:
                parts.append(jnp.zeros((fill, TILE), jnp.float32))
            strided[pl.ds(t * TILE, TILE), :] = jnp.concatenate(parts, axis=0).T
        for k in range(self.outer):
            slab = strided[pl.ds(k, self.inner, stride=self.outer), :].T
            result[k] = slab[: 2 * rows, :]

    def collect(self, slabs, strided, results):
        rows = self.rows
        for k in range(self.outer):
            slab = slabs(k)
            fill = TILE - slab.shape[0]
            if fill:
                slab = jnp.concatenate([slab, jnp.zeros((fill, self.inner), jnp.float32)], axis=0)
            strided[pl.ds(k, self.inner, stride=self.outer), :] = slab.T
        for t in range(self.length // TILE):
            block = strided[pl.ds(t * TILE, TILE), :].T
            for i, result in enumerate(results):
                result[:, pl.ds(t * TILE, TILE)] = block[i * rows : (i + 1) * rows, :]


def signed_waves(position, count):
    signed = jnp.where(position < count // 2, position, position - count)
    waves = 4.0 * signed.astype(jnp.float32) / count
    return waves, jnp.where(position == count // 2, jnp.float32(0.0), waves)


def first_waves(piece, k):
    lanes = lax.broadcasted_iota(jnp.int32, (1, piece.inner), 1)
    return signed_waves(piece.outer * lanes + k, piece.length)


def inverse_denominator(wave_first, wave_second):
    square = wave_first * wave_first + wave_second * wave_second
    return 1.0 / (1.0 + time_step * (square * square - square))


def second_wave(piece, position):
    shape = (position.shape[0], piece.inner)
    return jnp.broadcast_to(signed_waves(position, piece.length)[0], shape)


def row_index(count, width):
    return lax.broadcasted_iota(jnp.int32, (count, width), 0)


class Links:
    def __init__(self, devices, fast):
        self.devices, self.fast = devices, fast
        self.device = lax.axis_index(axes[0]) * fast + lax.axis_index(axes[1])
        self.near = min(8, devices // 2)
        self.steps = []
        for low in range(self.near):
            step, bit = 0, 1
            while bit < self.near:
                if low // bit % 2:
                    step += bit * (1 - 2 * lax.rem(lax.div(self.device, bit), 2))
                bit *= 2
            self.steps.append(step)

    def visit(self, count, body):
        near = self.near

        def far(i, carry):
            base = self.partner(count - near * i)
            for low in reversed(range(near)):
                body(base + self.steps[low])
            return carry

        lax.fori_loop(1, count // near, far, 0)
        for low in reversed(range(1, near)):
            body(self.device + self.steps[low])

    def partner(self, i):
        total, bit = 0, 1
        while bit < self.devices:
            total += bit * lax.rem(lax.div(self.device, bit) + lax.div(i, bit), 2)
            bit *= 2
        return total

    def place(self, peer):
        return (lax.div(peer, self.fast), lax.rem(peer, self.fast))

    def greet(self):
        barrier = pltpu.get_barrier_semaphore()

        def go(peer):
            at = self.place(peer)
            pl.semaphore_signal(barrier, inc=1, device_id=at, device_id_type=pl.DeviceIdType.MESH)

        self.visit(self.devices, go)

    def meet(self):
        pl.semaphore_wait(pltpu.get_barrier_semaphore(), self.devices - 1)

    def send(self, source, target, sems, count):
        send_sem, recv_sem, own_sem = sems
        own = lax.rem(self.device, count)

        def go(peer):
            pltpu.make_async_remote_copy(
                src_ref=source(peer if count == self.devices else lax.rem(peer, count)),
                dst_ref=target(own),
                send_sem=send_sem,
                recv_sem=recv_sem,
                device_id=self.place(peer),
                device_id_type=pl.DeviceIdType.MESH,
            ).start()

        self.visit(count, go)
        pltpu.make_async_copy(source(own), target(own), own_sem).start()

    def whole(self, source, target, sems, count):
        others = pl.ds(0, count - 1)
        return pltpu.make_async_remote_copy(
            src_ref=source(others),
            dst_ref=target(others),
            send_sem=sems[0],
            recv_sem=sems[1],
            device_id=(0, 0),
            device_id_type=pl.DeviceIdType.MESH,
        )

    def receive(self, source, target, sems, count):
        own = lax.rem(self.device, count)
        pltpu.make_async_copy(source(own), target(own), sems[2]).wait()
        self.whole(source, target, sems, count).wait_recv()

    def sent(self, source, target, sems, count):
        self.whole(source, target, sems, count).wait_send()


def start_kernel(length, rows, field, target, out, both_p, *scratch):
    piece = Pieces(length, rows)
    piece.spread(field, target, scratch[0], both_p)
    piece.pack_columns(lambda k: both_p[k, pl.ds(0, rows), :], out)


def slope_second_kernel(length, rows, field_p, twiddle, out_matrix, in_matrix, kept, result, *scratch):
    piece = Pieces(length, rows, *scratch)

    def body(r0):
        at = pl.ds(r0, piece.step)
        for k in range(piece.outer):
            piece.put(k, at, 0, field_p[k, at, :])

    piece.chunks(rows, body)
    for j in range(piece.outer):
        piece.clear_other(j)

    def write(r0, items):
        for j, (re, im) in enumerate(items):
            at, wide = piece.kept_lanes(j)
            base = at - j * piece.inner
            position = j * piece.inner + kept[:, base : base + wide]
            slope = 2.0 * signed_waves(position, length)[1]
            piece.turned[pl.ds(r0, piece.step), pl.ds(at, wide)] = -slope * im[:, base : base + wide]
            piece.turned[pl.ds(rows + r0, piece.step), pl.ds(at, wide)] = slope * re[:, base : base + wide]

    piece.outgoing(rows, -1.0, twiddle, out_matrix, True, write)
    piece.incoming(rows, 1.0, twiddle, in_matrix, real_out=True)
    result[...] = piece.z[:, :, : piece.inner]


def spread_kernel(length, rows, forcing, result, strided):
    Pieces(length, rows).spread(forcing.at[0], forcing.at[1], strided, result)


def collect_kernel(length, rows, slabs, result, strided):
    piece = Pieces(length, rows)
    piece.collect(lambda k: slabs[k], strided, [result.at[i] for i in range(result.shape[0])])


def weight_of(device, r0, step, inner):
    alone = (row_index(step, inner) + r0 + device) == 0
    return jnp.where(alone, jnp.float32(1.0), jnp.float32(2.0))


def slope_first_kernel(length, rows, source, in_twiddle, in_matrix, out_twiddle, out_matrix, out, *scratch):
    piece = Pieces(length, rows, *scratch)
    half = piece.half
    piece.turn_lines(source)
    piece.incoming(half, -1.0, in_twiddle, in_matrix)

    def body(r0):
        at = pl.ds(r0, piece.step)
        for k in range(piece.outer):
            re, im = piece.get(k, at, 0), piece.get(k, at, 1)
            scale = first_waves(piece, k)[1]
            piece.put(k, at, 0, -scale * im)
            piece.put(k, at, 1, scale * re)

    piece.chunks(half, body)
    piece.outgoing(half, 1.0, out_twiddle, out_matrix, False, piece.write_full(out, False))


def edge_inverses(piece, k):
    wave_first = first_waves(piece, k)[0]
    middle = jnp.full((1, 1), piece.length // 2, jnp.int32)
    zero = jnp.zeros((1, 1), jnp.int32)
    return [inverse_denominator(wave_first, signed_waves(p, piece.length)[0]) for p in (zero, middle)]


def next_kernel(length, rows, device_ref, source, forcing, in_twiddle, in_matrix, out_twiddle, out_matrix, mirror, out, *scratch):
    device = device_ref[0]
    piece = Pieces(length, rows, *scratch)
    half, step, inner = piece.half, piece.step, piece.inner
    late = device >= (length // rows) // 2
    piece.turn_lines(source)
    piece.incoming(half, -1.0, in_twiddle, in_matrix)

    def body(r0):
        at, also = pl.ds(r0, step), pl.ds(half + r0, step)
        index = row_index(step, 1) + r0
        low_wave = second_wave(piece, device * rows + index)
        high_wave = second_wave(piece, device * rows + half + index)
        moved = jnp.logical_and(row_index(step, inner) + r0 == 0, late)
        weight = weight_of(device, r0, step, inner)
        for k in range(piece.outer):
            wave_first = first_waves(piece, k)[0]
            low = inverse_denominator(wave_first, low_wave)
            high = inverse_denominator(wave_first, high_wave)
            for part in range(2):
                own = weight * piece.get(k, at, part)
                f_low = time_step * forcing[k, pl.ds(part * rows + r0, step), :]
                f_high = time_step * forcing[k, pl.ds(part * rows + half + r0, step), :]
                piece.put(k, at, part, (f_low + jnp.where(moved, 0.0, own)) * low)
                piece.put(k, also, part, (f_high + jnp.where(moved, own, 0.0)) * high)

    piece.chunks(half, body)

    @pl.when(device == 0)
    def _():
        at = pl.ds(0, 8)
        blocks = []
        for k in range(piece.outer):
            own = tuple(piece.get(k, at, part) for part in range(2))
            full = tuple(
                own[part] + time_step * forcing[k, pl.ds(part * rows, 8), :] for part in range(2)
            )
            blocks.append([own, full])
        flipped = piece.mirrored(blocks, mirror)
        rest = pl.ds(0, 16)
        row0 = row_index(16, inner) == 0
        for k in range(piece.outer):
            zero, middle = edge_inverses(piece, k)
            for part in range(2):
                own, full = blocks[k][0][part], blocks[k][1][part]
                own_c, full_c = flipped[k][0][part], flipped[k][1][part]
                value = 0.5 * ((full + full_c) * zero + (own - own_c) * middle)
                replace(piece, k, part, value)

    piece.outgoing(rows, 1.0, out_twiddle, out_matrix, False, piece.write_full(out, False))


def replace(piece, k, part, value):
    lanes = pl.ds(part * piece.inner, piece.inner)
    row0 = row_index(16, piece.inner) == 0
    value = jnp.concatenate([value, value], axis=0)
    for held, new in zip((piece.top, piece.low), halves(value)):
        old = held[k, pl.ds(0, 16), lanes].astype(jnp.float32)
        held[k, pl.ds(0, 16), lanes] = jnp.where(row0, new.astype(jnp.float32), old).astype(jnp.bfloat16)


def misfit_kernel(length, rows, device_ref, source, in_twiddle, in_matrix, out_twiddle, out_matrix, mirror, out, full, total_out, *scratch):
    device = device_ref[0]
    piece = Pieces(length, rows, *scratch)
    half, step, inner = piece.half, piece.step, piece.inner
    late = device >= (length // rows) // 2
    piece.turn_full(source)
    piece.incoming(rows, -1.0, in_twiddle, in_matrix)

    def body(r0):
        at, also = pl.ds(r0, step), pl.ds(half + r0, step)
        index = row_index(step, 1) + r0
        low_wave = second_wave(piece, device * rows + index)
        high_wave = second_wave(piece, device * rows + half + index)
        moved = jnp.logical_and(row_index(step, inner) + r0 == 0, late)
        weight = weight_of(device, r0, step, inner)
        for k in range(piece.outer):
            wave_first = first_waves(piece, k)[0]
            low = time_step * inverse_denominator(wave_first, low_wave)
            high = time_step * inverse_denominator(wave_first, high_wave)
            for part in range(2):
                low_value = piece.get(k, at, part) * low
                high_value = piece.get(k, also, part) * high
                full[k, pl.ds(part * rows + r0, step), :] = low_value
                full[k, pl.ds(part * rows + half + r0, step), :] = high_value
                own = jnp.where(moved, high_value, low_value)
                piece.put(k, at, part, weight * own)

    piece.chunks(half, body)

    @pl.when(device == 0)
    def _():
        at = pl.ds(0, 8)
        blocks = [[(piece.get(k, at, 0), piece.get(k, at, 1))] for k in range(piece.outer)]
        flipped = piece.mirrored(blocks, mirror)
        row0 = row_index(8, inner) == 0
        for k in range(piece.outer):
            zero, middle = edge_inverses(piece, k)
            for part in range(2):
                own, own_c = blocks[k][0][part], flipped[k][0][part]
                first = (0.5 * time_step) * (own + own_c) * zero
                value = first + (0.5 * time_step) * (own - own_c) * middle
                at_full = pl.ds(part * rows, 8)
                full[k, at_full, :] = jnp.where(row0, first, full[k, at_full, :])
                replace(piece, k, part, value)

    piece.outgoing(half, 1.0, out_twiddle, out_matrix, False, piece.write_full(out, False))
    total_out[...] = jnp.sum(source[:, pl.ds(rows, 8), :], axis=0)


def nonlinear_kernel(length, rows, source, both_p, second, twiddle, out_matrix, out, first, *scratch):
    piece = Pieces(length, rows, *scratch)
    piece.turn_columns(source, first)

    def body(r0):
        at = pl.ds(r0, piece.step)
        for k in range(piece.outer):
            one, other = first[k, at, :], second[k, at, :]
            piece.put(k, at, 0, both_p[k, at, :] - (0.5 * time_step) * (one * one + other * other))

    piece.chunks(rows, body)
    piece.outgoing_kept(twiddle, out_matrix, out)


def joint_kernel(length, rows, source, first, second, twiddle, in_matrix, out, value_out, second_out, *scratch):
    piece = Pieces(length, rows, *scratch)
    piece.turn_kept(source)
    piece.unpack_middle()
    piece.incoming(rows, 1.0, twiddle, in_matrix, real_out=True)
    lanes = pl.ds(0, piece.inner)

    def body(r0):
        at = pl.ds(r0, piece.step)
        for k in range(piece.outer):
            value = piece.get(k, at, 0)
            value_out[k, at, :] = (1.0 / time_step) * value
            second_out[k, at, :] = value * second[k, at, :]
            piece.z[k, at, lanes] = value * first[k, at, :]

    piece.chunks(rows, body)
    piece.pack_columns(lambda k: piece.z[k, pl.ds(0, rows), lanes], out)


def residual_kernel(length, rows, source, both_p, twiddle, in_matrix, out_matrix, out, field_out, *scratch):
    piece = Pieces(length, rows, *scratch[:4])
    strided, total = scratch[4:]
    piece.turn_full(source)
    piece.unpack_middle()
    piece.incoming(rows, 1.0, twiddle, in_matrix, real_out=True)
    piece.collect(lambda k: piece.get(k, pl.ds(0, rows), 0), strided, [field_out])
    total[...] = jnp.zeros_like(total)

    def body(r0):
        at = pl.ds(r0, piece.step)
        for k in range(piece.outer):
            residual = piece.get(k, at, 0) - both_p[k, pl.ds(rows + r0, piece.step), :]
            total[...] += residual * residual
            piece.put(k, at, 0, residual)

    piece.chunks(rows, body)
    piece.outgoing(rows, -1.0, twiddle, out_matrix, True, piece.write_full(out, True))
    value = 0.5 * jnp.sum(total[...])
    out[:, pl.ds(rows, 8), :] = jnp.full((out.shape[0], 8, 2 * rows), value, jnp.float32)


def last_kernel(length, rows, source, value, second, field_out, strided, first):
    piece = Pieces(length, rows)
    piece.turn_columns(source, first)
    piece.collect(lambda k: first[k] + value[k] + second[k], strided, [field_out])


def step_kernel(length, rows, devices, fast, cuts, parts, inputs, outs, box):
    links = Links(devices, fast)
    device, half, part_devices = links.device, rows // 2, devices // 2
    late = device >= part_devices
    flip = jnp.where(late, -1.0, 1.0).astype(jnp.float32)
    sides, count = range(parts), rows // parts
    copies, sems = box.copies, box.sems
    work = (box.turned, box.top, box.low, box.z)
    piece = Pieces(length, rows, *work)
    step, inner, outer = piece.step, piece.inner, piece.outer
    both_p, forcing_p, full = box.both_p, box.forcing_p, box.full
    first, second, value = box.first, box.second, box.value
    strided, total = box.strided, box.total
    lanes = pl.ds(0, inner)

    loads = [
        pltpu.make_async_copy(ref, held, copies.at[i])
        for i, (ref, held) in enumerate(zip(inputs.refs, inputs.held))
    ]
    for copy in loads[:2]:
        copy.start()
    links.greet()
    waiting = iter(loads)

    def load(count):
        for i in range(count):
            next(waiting).wait()

    at_all = lambda ref: lambda e: ref.at[e]
    at_lines = lambda ref, base, count: lambda e: ref.at[e, pl.ds(base, count)]
    order = []

    def send(source, target, count=devices):
        i = len(order)
        order.append((source, target, (sems.at[i, 0], sems.at[i, 1], sems.at[i, 2]), count))
        links.send(*order[-1])
        return order[-1]

    def receive(*moves):
        for move in moves:
            links.receive(*move)

    tw_natural, tw_kept, tw_lines, tw_cut, tw_sided = (inputs.twiddles.at[i] for i in range(5))
    forward, backward, mirror = inputs.forward, inputs.backward, inputs.mirror
    kept_out, kept_in, kept = inputs.kept_out, inputs.kept_in, inputs.kept
    lines_in, cut_in = box.lines_in, box.cut_in
    if parts == 2 * cuts:
        tw_lines, lines_in = tw_cut, cut_in

    def permute_rows(groups, result):
        tall, blocks = rows // groups, inner // rows
        for p in range(2):
            for part in range(2):
                for group in range(groups):
                    for s in range(blocks):
                        at = part * inner + group * (inner // groups) + s * tall
                        source = part * inner + s * rows + group * tall
                        result[p, pl.ds(at, tall), :] = forward[p, pl.ds(source, tall), :]

    def slope_first(source, out, lines):
        piece.turn_cut(source, lines, outer)
        piece.incoming(lines, -1.0, tw_cut, cut_in)

        def body(r0):
            at = pl.ds(r0, step)
            for k in range(outer):
                re, im = piece.get(k, at, 0), piece.get(k, at, 1)
                scale = first_waves(piece, k)[1]
                piece.put(k, at, 0, -scale * im)
                piece.put(k, at, 1, scale * re)

        piece.chunks(lines, body)
        piece.outgoing(lines, 1.0, tw_natural, backward, False, piece.write_full(out, False))

    def slope_second(source, out):
        slope_second_kernel(length, rows, source, tw_kept, kept_out, kept_in, kept, out, *work)

    def send_columns(source, target):
        return [send(at_all(source.at[q]), at_all(target.at[q])) for q in range(cuts)]

    def turn_slopes(moves, source, back, target):
        size, result = half // cuts, []
        for q, move in enumerate(moves):
            receive(move)
            slope_first(source.at[q], back.at[q], size)
            result.append(send(at_all(back.at[q]), at_lines(target, q * size, size)))
        return result

    def lines_of(side, r0):
        line = row_index(step, 1) + r0 + side * count
        alone = (row_index(step, inner) + r0 + side * count + lax.rem(device, part_devices)) == 0
        return second_wave(piece, device * rows + line), jnp.where(alone, jnp.float32(1.0), jnp.float32(2.0))

    def edges(k):
        wave = first_waves(piece, k)[0]
        middle = jnp.full((1, 1), length // 2, jnp.int32)
        mine, theirs = jnp.where(late, middle, 0), jnp.where(late, 0, middle)
        return [inverse_denominator(wave, signed_waves(p, length)[0]) for p in (mine, theirs)]

    load(2)
    for copy in loads[2:]:
        copy.start()
    piece.spread(inputs.field, inputs.target, strided, both_p)
    piece.pack_cut(lambda k: both_p[k, pl.ds(0, rows), :], [box.s_field.at[q] for q in range(cuts)])
    links.meet()
    m_field = send_columns(box.s_field, box.r_field)

    load(len(loads) - 2)
    if parts != 2 * cuts:
        permute_rows(TILE * parts // (2 * rows), lines_in)
    permute_rows(TILE * cuts // rows, cut_in)
    for side in sides:
        for p in range(2):
            for part in range(2):
                for s in range(inner // rows):
                    at = part * (inner // parts) + s * count
                    source = part * inner + s * rows + side * count
                    box.sided[p, side, pl.ds(at, count), :] = backward[p, pl.ds(source, count), :inner]
    slope_second(both_p, second)
    m_slope = turn_slopes(m_field, box.r_field, box.s_slope, box.r_slope)
    piece.spread(inputs.forcing.at[0], inputs.forcing.at[1], strided, forcing_p)

    for q in range(cuts):
        receive(m_slope[q])
        piece.turn_part(box.r_slope, q * half // cuts, half // cuts, first)

    def nonlinear(r0):
        at = pl.ds(r0, step)
        for k in range(outer):
            one, other = first[k, at, :], second[k, at, :]
            piece.put(k, at, 0, both_p[k, at, :] - (0.5 * time_step) * (one * one + other * other))

    piece.chunks(rows, nonlinear)
    piece.outgoing_sides(tw_natural, forward, [box.s_sum.at[side] for side in sides], late)
    m_sum = [send(at_all(box.s_sum.at[side]), at_all(box.r_sum.at[side]), part_devices) for side in sides]

    def divide(side):
        def body(r0):
            at = pl.ds(r0, step)
            wave, weight = lines_of(side, r0)
            for k in range(outer):
                scale = inverse_denominator(first_waves(piece, k)[0], wave)
                for part in range(2):
                    forced = time_step * forcing_p[k, pl.ds(part * rows + side * count + r0, step), :]
                    piece.put(k, at, part, (weight * piece.get(k, at, part) + forced) * scale)

        piece.chunks(count, body)
        if side:
            return

        @pl.when(lax.rem(device, part_devices) == 0)
        def _():
            at = pl.ds(0, 8)
            blocks = []
            for k in range(outer):
                own = tuple(piece.get(k, at, part) for part in range(2))
                joined = tuple(own[part] + time_step * forcing_p[k, pl.ds(part * rows, 8), :] for part in range(2))
                blocks.append([own, joined])
            flipped = piece.mirrored(blocks, mirror)
            for k in range(outer):
                mine, theirs = edges(k)
                for part in range(2):
                    own, joined = blocks[k][0][part], blocks[k][1][part]
                    own_c, joined_c = flipped[k][0][part], flipped[k][1][part]
                    replace(piece, k, part, 0.5 * ((joined + joined_c) * mine + (own - own_c) * theirs))

    m_next = []
    for side in sides:
        receive(m_sum[side])
        piece.turn_cut(box.r_sum.at[side], count, outer // 2)
        piece.incoming_half(count, -1.0, tw_lines, lines_in, flip)
        divide(side)
        sent = box.s_next.at[side]
        piece.outgoing(count, 1.0, tw_natural, backward, False, piece.write_full(sent, False))
        m_next.append(send(at_all(sent), at_lines(box.r_next, side * count, count)))

    for side in sides:
        receive(m_next[side])
        piece.turn_side(box.r_next, side * count, count, outer)
        if side == 0:
            low, high = piece.first_imaginary(0), piece.first_imaginary(length // 2)
            piece.turned[:rows, pl.ds(0, TILE)] += high
            piece.turned[:rows, pl.ds(length // 2, TILE)] += low
        piece.incoming_side(side, outer, tw_sided, box.sided)
    total[...] = jnp.zeros_like(total)

    def misfit(r0):
        at = pl.ds(r0, step)
        for k in range(outer):
            now = piece.get(k, at, 0)
            value[k, at, :] = now
            residual = now - both_p[k, pl.ds(rows + r0, step), :]
            total[...] += residual * residual
            piece.put(k, at, 0, residual)

    piece.chunks(rows, misfit)
    piece.outgoing_sides(tw_natural, forward, [box.s_kept.at[side] for side in sides])
    m_kept = [send(at_all(box.s_kept.at[side]), at_all(box.r_kept.at[side])) for side in sides]
    box.s_total[...] = jnp.full(box.s_total.shape, 0.5 * jnp.sum(total[...]), jnp.float32)
    m_total = send(at_all(box.s_total), at_all(box.r_total))
    piece.collect(lambda k: value[k], strided, [outs.next])

    def adjoint(side):
        def body(r0):
            at = pl.ds(r0, step)
            wave, weight = lines_of(side, r0)
            for k in range(outer):
                scale = time_step * inverse_denominator(first_waves(piece, k)[0], wave)
                for part in range(2):
                    own = piece.get(k, at, part) * scale
                    full[k, pl.ds(part * rows + side * count + r0, step), :] = own
                    piece.put(k, at, part, weight * own)

        piece.chunks(count, body)
        if side:
            return

        @pl.when(lax.rem(device, part_devices) == 0)
        def _():
            at = pl.ds(0, 8)
            blocks = [[(piece.get(k, at, 0), piece.get(k, at, 1))] for k in range(outer)]
            flipped = piece.mirrored(blocks, mirror)
            row0 = row_index(8, inner) == 0
            for k in range(outer):
                mine, theirs = edges(k)
                for part in range(2):
                    own, own_c = blocks[k][0][part], flipped[k][0][part]
                    line = (0.5 * time_step) * (own + own_c) * mine
                    at_full = pl.ds(part * rows, 8)
                    full[k, at_full, :] = jnp.where(row0, line, full[k, at_full, :])
                    replace(piece, k, part, line + (0.5 * time_step) * (own - own_c) * theirs)

    m_back = []
    for side in sides:
        receive(m_kept[side])
        piece.turn_cut(box.r_kept.at[side], count, outer)
        piece.incoming(count, -1.0, tw_lines, lines_in)
        adjoint(side)
        sent = box.s_back.at[side]
        piece.outgoing_half(count, 1.0, tw_natural, backward, flip, piece.write_full(sent, False))
        m_back.append(send(at_all(sent), at_lines(box.r_back, side * count, count), part_devices))

    for side in sides:
        receive(m_back[side])
        piece.turn_side(box.r_back, side * count, count, outer // 2)
        if side == 0:
            box.extra[...] = piece.first_imaginary(0)
        piece.incoming_side(side, outer // 2, tw_sided, box.sided, flip, None if side else box.extra)

    def products(r0):
        at = pl.ds(r0, step)
        for k in range(outer):
            now = piece.get(k, at, 0)
            value[k, at, :] = (1.0 / time_step) * now
            box.product[k, at, :] = now * second[k, at, :]
            piece.z[k, at, lanes] = now * first[k, at, :]

    piece.chunks(rows, products)
    piece.pack_cut(lambda k: piece.z[k, pl.ds(0, rows), lanes], [box.s_product.at[q] for q in range(cuts)])
    m_product = send_columns(box.s_product, box.r_product)
    slope_second(box.product, second)
    for k in range(outer):
        value[k] = value[k] + second[k]
    m_last = turn_slopes(m_product, box.r_product, box.s_last, box.r_last)

    piece.collect(lambda k: full[k], strided, [outs.forcing.at[i] for i in range(2)])
    receive(m_total)
    outs.total[...] = jnp.sum(box.r_total[...], axis=0) / (length * length)

    for q in range(cuts):
        receive(m_last[q])
        piece.turn_part(box.r_last, q * half // cuts, half // cuts, first)
    for k in range(outer):
        outs.field[k] = first[k] + value[k]
    for move in order:
        links.sent(*move)


def joined_step(field, target, forcing, devices, fast, rows, length):
    outer, inner = split_length(length)
    half, step, cuts = rows // 2, math.gcd(rows // 2, 16), 2
    parts = 2
    natural, kept = orders(length, rows)[:2]
    lines = line_order(inner, rows, TILE * parts // (2 * rows))
    cut = line_order(inner, rows, TILE * cuts // rows)
    sided = natural.reshape(inner // rows, parts, rows // parts).transpose(1, 0, 2).reshape(inner)
    matrix = lambda *args: matrix_table(length, *args)
    tables = dict(
        field=field, target=target,
        twiddles=np.stack([twiddle_table(length, o) for o in (natural, kept, lines, cut, sided)]),
        kept=kept[None, :].astype(np.int32),
        kept_out=matrix(-1.0, natural, kept)[:, :inner],
        kept_in=matrix(1.0, kept, natural)[:, :, :inner],
        forcing=forcing,
        backward=matrix(1.0, natural, natural),
        forward=matrix(-1.0, natural, natural),
        mirror=mirror_table(length),
    )
    operands = [jnp.asarray(table) for table in tables.values()]
    float32 = jnp.float32
    held = lambda *dims: pltpu.VMEM(dims, float32)
    packed = held(parts, devices, 2 * rows * rows // (parts * TILE), TILE)
    lined = held(parts, devices, rows // parts, 2 * rows)
    packed_half, lined_half = (held(parts, devices // 2, *dims.shape[2:]) for dims in (packed, lined))
    columns, slopes = held(cuts, devices, rows * rows // (TILE * cuts), TILE), held(cuts, devices, half // cuts, 2 * rows)
    returned = held(devices, half, 2 * rows)
    table = pltpu.VMEM((2, 2 * inner, 2 * inner), jnp.bfloat16)
    pair, one = held(outer, 2 * rows, inner), held(outer, rows, inner)
    small = held(devices, 1, TILE)
    halved = pltpu.VMEM((outer, rows, 2 * inner), jnp.bfloat16)
    shapes = dict(
        turned=held(2 * rows, length), top=halved, low=halved, z=held(outer, rows, 2 * inner),
        strided=held(length, TILE), total=held(step, inner),
        both_p=pair, forcing_p=pair, full=pair, first=one, second=one, value=one, product=one,
        lines_in=table, cut_in=table, extra=held(rows, TILE), sided=pltpu.VMEM((2, parts, 2 * inner // parts, inner), jnp.bfloat16),
        s_field=columns, r_field=columns, s_slope=slopes, r_slope=returned,
        s_sum=packed_half, r_sum=packed_half, s_next=lined, r_next=held(devices, rows, 2 * rows),
        s_kept=packed, r_kept=packed, s_total=small, r_total=small,
        s_back=lined_half, r_back=held(devices // 2, rows, 2 * rows),
        s_product=columns, r_product=columns, s_last=slopes, r_last=returned,
        copies=pltpu.SemaphoreType.DMA((len(operands),)),
        sems=pltpu.SemaphoreType.DMA((1 + 4 * parts + 4 * cuts, 3)),
    )
    inputs = [pltpu.VMEM(operand.shape, operand.dtype) for operand in operands]

    def body(*refs):
        a, b = len(operands), len(operands) + 4
        c = b + len(operands)
        given = SimpleNamespace(refs=refs[:a], held=refs[b:c], **dict(zip(tables, refs[b:c])))
        outs = SimpleNamespace(next=refs[a], field=refs[a + 1], forcing=refs[a + 2], total=refs[a + 3])
        step_kernel(length, rows, devices, fast, cuts, parts, given, outs, SimpleNamespace(**dict(zip(shapes, refs[c:]))))

    anywhere = pl.BlockSpec(memory_space=pl.ANY)
    vmem, smem = pl.BlockSpec(memory_space=pltpu.VMEM), pl.BlockSpec(memory_space=pltpu.SMEM)
    shape = lambda *dims: jax.ShapeDtypeStruct(dims, float32)
    next_field, slabs, forcing_grad, total = pl.pallas_call(
        body,
        out_shape=(shape(rows, length), shape(outer, rows, inner), shape(2, rows, length), shape(1, TILE)),
        in_specs=[pl.BlockSpec(memory_space=pltpu.HBM)] * len(operands),
        out_specs=(vmem, vmem, vmem, vmem),
        scratch_shapes=inputs + list(shapes.values()),
        compiler_params=pltpu.CompilerParams(vmem_limit_bytes=34 * 2**20, has_side_effects=True, collective_id=0),
        cost_estimate=pl.CostEstimate(flops=6 * 10**10, bytes_accessed=4 * 2**20, transcendentals=0),
    )(*[pltpu.with_memory_space_constraint(one, pltpu.HBM) for one in operands])
    return pl.pallas_call(
        functools.partial(tail_kernel, length, rows),
        out_shape=(shape(rows, length), shape(rows, length), shape(2, rows, length), shape(1, 1)),
        in_specs=[vmem] * 4,
        out_specs=(anywhere, anywhere, anywhere, smem),
        scratch_shapes=[held(length, TILE), held(rows, length), pltpu.SemaphoreType.DMA((3,))],
        compiler_params=pltpu.CompilerParams(vmem_limit_bytes=8 * 2**20),
        cost_estimate=pl.CostEstimate(flops=10**9, bytes_accessed=4 * 2**20, transcendentals=0),
    )(next_field, slabs, forcing_grad, total)


def tail_kernel(length, rows, next_field, slabs, forcing_grad, total, next_out, field_out, forcing_out, total_out, strided, held, sems):
    piece = Pieces(length, rows)
    copies = [
        pltpu.make_async_copy(next_field, next_out, sems.at[0]),
        pltpu.make_async_copy(forcing_grad, forcing_out, sems.at[1]),
        pltpu.make_async_copy(held, field_out, sems.at[2]),
    ]
    copies[0].start()
    copies[1].start()
    total_out[0, 0] = jnp.sum(total[0:1, 0:1])
    piece.collect(lambda k: slabs[k], strided, [held])
    copies[2].start()
    for copy in copies:
        copy.wait()


def member_step(device, field, target, forcing_p, devices, rows, length):
    outer, inner = split_length(length)
    half = rows // 2
    float32 = jnp.float32
    shape = lambda *dims: jax.ShapeDtypeStruct(dims, float32)
    kept_blocks = shape(devices, rows * rows // TILE, TILE)
    half_blocks = shape(devices, half, 2 * rows)
    blocks = shape(devices, rows, 2 * rows)
    longer = shape(devices, rows + 8, 2 * rows)
    pair, one = shape(outer, 2 * rows, inner), shape(outer, rows, inner)
    plain = shape(rows, length)
    step = math.gcd(half, 16)
    base = [
        pltpu.VMEM((2 * rows, length), float32),
        pltpu.VMEM((outer, rows, 2 * inner), jnp.bfloat16),
        pltpu.VMEM((outer, rows, 2 * inner), jnp.bfloat16),
        pltpu.VMEM((outer, rows, 2 * inner), float32),
    ]
    strided = pltpu.VMEM((length, TILE), float32)
    total = pltpu.VMEM((step, inner), float32)
    vmem = pl.BlockSpec(memory_space=pltpu.VMEM)
    smem = pl.BlockSpec(memory_space=pltpu.SMEM)

    natural, kept, lines = orders(length, rows)
    tw_natural, tw_kept, tw_lines = [jnp.asarray(twiddle_table(length, o)) for o in (natural, kept, lines)]
    matrix = lambda *args: matrix_table(length, *args)
    forward, backward = matrix(-1.0, natural, natural), matrix(1.0, natural, natural)
    kept_out, kept_in = matrix(-1.0, natural, kept)[:, :inner], matrix(1.0, kept, natural)[:, :, :inner]
    lines_in = matrix(-1.0, lines, natural)
    mirror = jnp.asarray(mirror_table(length))
    kept_lane = jnp.asarray(kept[None, :].astype(np.int32))

    def call(body, outs, scratch, *operands):
        return pl.pallas_call(
            functools.partial(body, length, rows),
            out_shape=outs,
            in_specs=[smem if operand is device else vmem for operand in operands],
            out_specs=jax.tree.map(lambda leaf: vmem, outs),
            scratch_shapes=scratch,
            compiler_params=pltpu.CompilerParams(vmem_limit_bytes=20 * 2**20),
            cost_estimate=pl.CostEstimate(flops=6 * 10**9, bytes_accessed=4 * 2**20, transcendentals=0),
        )(*operands)

    def move(value):
        return lax.all_to_all(value, axes, split_axis=0, concat_axis=0, tiled=True)

    spectral_tables = (tw_lines, lines_in, tw_natural, backward)
    slope_tables = (tw_kept, kept_out, kept_in, kept_lane)
    sent, both_p = call(start_kernel, (kept_blocks, pair), [strided], field, target)
    second = call(slope_second_kernel, one, base, both_p, *slope_tables)
    sent = call(slope_first_kernel, half_blocks, base, move(sent), *spectral_tables)
    sent, first = call(nonlinear_kernel, (kept_blocks, one), base, move(sent), both_p, second, tw_kept, kept_out)
    sent = call(next_kernel, blocks, base, device, move(sent), forcing_p, *spectral_tables, mirror)
    sent, next_field = call(
        residual_kernel, (longer, plain), base + [strided, total],
        move(sent), both_p, tw_natural, backward, forward,
    )
    sent, full, sums = call(
        misfit_kernel, (half_blocks, pair, shape(8, 2 * rows)), base,
        device, move(sent), tw_natural, forward, tw_natural, backward, mirror,
    )
    sent, value, product = call(
        joint_kernel, (kept_blocks, one, one), base, move(sent), first, second, tw_kept, kept_in
    )
    second_part = call(slope_second_kernel, one, base, product, *slope_tables)
    sent = call(slope_first_kernel, half_blocks, base, move(sent), *spectral_tables)
    field_grad = call(
        last_kernel, plain, [strided, pltpu.VMEM((outer, rows, inner), float32)], move(sent), value, second_part
    )
    return next_field, sums[0, 0], field_grad, full


def per_device(devices, fast, initial_field, target_field, forcing):
    members, rows, length = initial_field.shape
    device = lax.axis_index(axes).astype(jnp.int32).reshape(1)
    outer, inner = split_length(length)
    vmem = pl.BlockSpec(memory_space=pltpu.VMEM)
    strided = pltpu.VMEM((length, TILE), jnp.float32)

    def reorder(body, shape, operand):
        return pl.pallas_call(
            functools.partial(body, length, rows),
            out_shape=jax.ShapeDtypeStruct(shape, jnp.float32),
            in_specs=[vmem],
            out_specs=vmem,
            scratch_shapes=[strided],
        )(operand)

    if rows * rows % (TILE * 32) == 0 and TILE % rows == 0:
        results = [
            joined_step(initial_field[m], target_field[m], forcing, devices, fast, rows, length)
            for m in range(members)
        ]
        next_field = jnp.stack([one[0] for one in results])
        field_grad = jnp.stack([one[1] for one in results])
        forcing_grad = sum(one[2] for one in results)
        objective = sum(one[3].reshape(()) for one in results) / members
        return (next_field, objective, field_grad, forcing_grad)
    forcing_p = reorder(spread_kernel, (outer, 2 * rows, inner), forcing)
    results = [
        member_step(device, initial_field[m], target_field[m], forcing_p, devices, rows, length)
        for m in range(members)
    ]
    next_field = jnp.stack([one[0] for one in results])
    objective = sum(one[1] for one in results) / (members * length * length)
    field_grad = jnp.stack([one[2] for one in results])
    forcing_grad = reorder(collect_kernel, (2, rows, length), sum(one[3] for one in results))
    return (next_field, objective, field_grad, forcing_grad)


def solution(mesh):
    devices = mesh.shape["px"] * mesh.shape["py"]
    spec = P(None, axes, None)
    return jax.shard_map(
        functools.partial(per_device, devices, mesh.shape["py"]),
        mesh=mesh,
        in_specs=(spec, spec, spec),
        out_specs=(spec, P(), spec, spec),
        check_vma=False,
    )
```

```python
import functools
import math
from types import SimpleNamespace

import jax
import jax.numpy as jnp
import numpy as np
from jax import lax
from jax.experimental import pallas as pl
from jax.experimental.pallas import tpu as pltpu
from jax.sharding import PartitionSpec as P

time_step = 0.25
axes = ("px", "py")
TILE = 128


def split_length(length):
    inner = 256 if length % 256 == 0 else TILE
    return (length // inner, inner)


def small_dft(items, sign):
    count = len(items)
    if count == 1:
        return items
    evens = small_dft(items[0::2], sign)
    odds = small_dft(items[1::2], sign)
    low, high = [], []
    for k in range(count // 2):
        odd_re, odd_im = odds[k]
        if 4 * k == count:
            odd_re, odd_im = (-odd_im, odd_re) if sign > 0 else (odd_im, -odd_re)
        elif k:
            c = math.cos(2.0 * math.pi * k / count)
            s = sign * math.sin(2.0 * math.pi * k / count)
            if abs(abs(c) - abs(s)) < 1e-12:
                sc, ss = math.copysign(1.0, c), math.copysign(1.0, s)
                odd_re, odd_im = (
                    c * (odd_re - sc * ss * odd_im),
                    c * (odd_im + sc * ss * odd_re),
                )
            else:
                odd_re, odd_im = (c * odd_re - s * odd_im, c * odd_im + s * odd_re)
        even_re, even_im = evens[k]
        low.append((even_re + odd_re, even_im + odd_im))
        high.append((even_re - odd_re, even_im - odd_im))
    return low + high


def half_dft(items, sign):
    count = 2 * len(items)
    turned = []
    for j, (re, im) in enumerate(items):
        c = math.cos(2.0 * math.pi * j / count)
        s = sign * math.sin(2.0 * math.pi * j / count)
        turned.append((re, im) if j == 0 else (c * re - s * im, c * im + s * re))
    pairs = zip(small_dft(items, sign), small_dft(turned, sign))
    return [one for pair in pairs for one in pair]


def halves(value):
    top = value.astype(jnp.bfloat16)
    return top, (value - top.astype(jnp.float32)).astype(jnp.bfloat16)


def orders(length, rows):
    inner = split_length(length)[1]
    half = rows // 2
    lane = np.arange(inner)
    natural = lane
    local = lane % (inner // 2)
    line = local % half
    kept = rows * (local // half) + np.where((lane >= inner // 2) & (line == 0), half, line)
    return natural, kept, line_order(inner, rows, TILE // rows)


def line_order(inner, rows, groups):
    lane = np.arange(inner)
    tall, wide = rows // groups, inner // groups
    within = lane % wide
    return rows * (within // tall) + tall * (lane // wide) + within % tall


def twiddle_table(length, order):
    outer = split_length(length)[0]
    angle = 2.0 * np.pi * np.outer(np.arange(outer), order) / length
    return (np.stack([np.cos(angle), np.sin(angle)]) / math.sqrt(length)).astype(np.float32)


def matrix_table(length, sign, left, right):
    inner = split_length(length)[1]
    angle = 2.0 * np.pi * (np.outer(left, right) % inner) / inner
    c, s = np.cos(angle), np.sin(angle)
    full = np.block([[c, sign * s], [-sign * s, c]])
    top = full.astype(jnp.bfloat16)
    return np.stack([top, (full - top.astype(np.float64)).astype(jnp.bfloat16)])


def mirror_table(length):
    inner = split_length(length)[1]
    lane = np.arange(inner)
    both = np.zeros((2, inner, inner))
    both[0, (inner - lane) % inner, lane] = 1.0
    both[1, inner - 1 - lane, lane] = 1.0
    return both.astype(jnp.bfloat16)


class Pieces:
    def __init__(self, length, rows, turned=None, top=None, low=None, grid_out=None):
        self.length, self.rows, self.half = length, rows, rows // 2
        self.outer, self.inner = split_length(length)
        self.turned, self.top, self.low, self.z = turned, top, low, grid_out
        self.step = math.gcd(rows // 2, 16)

    def chunks(self, lines, body):
        def run(i, carry):
            body(pl.multiple_of(i * self.step, self.step))
            return carry

        lax.fori_loop(0, lines // self.step, run, 0)

    def put(self, k, at, part, value):
        lanes = pl.ds(part * self.inner, self.inner)
        top, low = halves(value)
        self.top[k, at, lanes] = top
        self.low[k, at, lanes] = low

    def get(self, k, at, part):
        return self.z[k, at, pl.ds(part * self.inner, self.inner)]

    def multiply(self, lines, matrix, real_in=False, real_out=False):
        deep = self.inner if real_in else 2 * self.inner
        wide = self.inner if real_out else 2 * self.inner
        count = self.outer * lines
        top = self.top[:, :lines, :deep].reshape(count, deep)
        low = self.low[:, :lines, :deep].reshape(count, deep)
        right_top = matrix[0, :deep, :wide]
        right_low = matrix[1, :deep, :wide]
        dot = functools.partial(jnp.dot, preferred_element_type=jnp.float32)
        total = dot(top, right_top) + dot(low, right_top) + dot(top, right_low)
        self.z[:, :lines, :wide] = total.reshape(self.outer, lines, wide)

    def twist(self, k, pair, sign, twiddle, flip=None):
        c = twiddle[0, pl.ds(k, 1), :]
        s = twiddle[1, pl.ds(k, 1), :]
        if flip is not None and k % 2:
            c, s = flip * c, flip * s
        s = s if sign > 0 else -s
        re, im = pair
        return (re * c - im * s, re * s + im * c)

    def turn_full(self, source):
        rows, blocks = self.rows, TILE // self.rows
        for t in range(self.length // TILE):
            tile = source[pl.ds(t * blocks, blocks), :rows, :].reshape(TILE, 2 * rows)
            self.turned[: 2 * rows, pl.ds(t * TILE, TILE)] = tile.T

    def turn_lines(self, source):
        rows = self.rows
        groups = TILE // rows
        blocks, wide = self.inner // rows, self.inner // groups
        for t in range(self.outer):
            tile = source[pl.ds(t * blocks, blocks), :, :].reshape(wide, TILE).T
            for h in range(groups):
                self.turned[:rows, pl.ds(t * self.inner + h * wide, wide)] = tile[h * rows : (h + 1) * rows]

    def kept_lanes(self, j):
        wide = self.inner // 2
        return j * self.inner + (wide if 2 * j >= self.outer else 0), wide

    def clear_other(self, j):
        at, wide = self.kept_lanes(j)
        other = j * self.inner + (0 if 2 * j >= self.outer else wide)
        self.turned[: 2 * self.rows, pl.ds(other, wide)] = jnp.zeros((2 * self.rows, wide), jnp.float32)

    def turn_kept(self, source):
        rows, half, blocks = self.rows, self.half, self.inner // self.rows
        for j in range(self.outer):
            at, wide = self.kept_lanes(j)
            tile = source[pl.ds(j * blocks, blocks), :, :].reshape(wide, 2 * rows)
            self.turned[: 2 * rows, pl.ds(at, wide)] = tile.T
            self.clear_other(j)

    def unpack_middle(self):
        rows, middle = self.rows, (self.outer // 2) * self.inner
        first = self.turned[rows : 2 * rows, :TILE]
        lane0 = lax.broadcasted_iota(jnp.int32, first.shape, 1) == 0
        zero = jnp.zeros_like(first)
        self.turned[:rows, pl.ds(middle, TILE)] += jnp.where(lane0, first, zero)
        self.turned[rows : 2 * rows, :TILE] = jnp.where(lane0, zero, first)

    def incoming(self, lines, sign, twiddle, matrix, real_out=False):
        def body(r0):
            items = []
            for j in range(self.outer):
                lanes = pl.ds(j * self.inner, self.inner)
                items.append((
                    self.turned[pl.ds(r0, self.step), lanes],
                    self.turned[pl.ds(lines + r0, self.step), lanes],
                ))
            for k, pair in enumerate(small_dft(items, sign)):
                re, im = self.twist(k, pair, sign, twiddle)
                self.put(k, pl.ds(r0, self.step), 0, re)
                self.put(k, pl.ds(r0, self.step), 1, im)

        self.chunks(lines, body)
        self.multiply(lines, matrix, real_out=real_out)

    def outgoing(self, lines, sign, twiddle, matrix, real_in, write):
        self.multiply(lines, matrix, real_in=real_in)

        def body(r0):
            at = pl.ds(r0, self.step)
            write(r0, small_dft([
                self.twist(k, (self.get(k, at, 0), self.get(k, at, 1)), sign, twiddle)
                for k in range(self.outer)
            ], sign))

        self.chunks(lines, body)

    def pack_middle(self, items):
        re, im = items[0]
        lane0 = lax.broadcasted_iota(jnp.int32, im.shape, 1) == 0
        return [(re, jnp.where(lane0, items[self.outer // 2][0], im))] + items[1:]

    def write_full(self, result, pack):
        rows = self.rows

        def write(r0, items):
            at = pl.ds(r0, self.step)
            for j, (re, im) in enumerate(self.pack_middle(items) if pack else items):
                for piece in range(self.inner // rows):
                    to = j * (self.inner // rows) + piece
                    lanes = slice(piece * rows, (piece + 1) * rows)
                    result[to, at, pl.ds(0, rows)] = re[:, lanes]
                    result[to, at, pl.ds(rows, rows)] = im[:, lanes]

        return write

    def pack_cut(self, slabs, results):
        rows, half, wide = self.rows, self.half, self.inner // 2
        cuts, count = len(results), half // len(results)
        groups = TILE // (2 * count)
        tall = rows // groups
        for k in range(self.outer):
            slab = slabs(k)
            for s in range(self.inner // rows):
                for q, result in enumerate(results):
                    parts = []
                    for group in range(groups):
                        for part in range(2):
                            at = part * wide + (q * (self.inner // rows) + s) * count
                            parts.append(slab[group * tall : (group + 1) * tall, at : at + count])
                    result[k * (self.inner // rows) + s] = jnp.concatenate(parts, axis=1)

    def turn_cut(self, source, lines, spans):
        blocks = self.inner // self.rows
        groups = TILE // (2 * lines)
        wide = self.inner // groups
        for t in range(spans):
            tile = source[pl.ds(t * blocks, blocks), :, :].reshape(wide, TILE).T
            for h in range(groups):
                held = tile[h * 2 * lines : (h + 1) * 2 * lines]
                self.turned[: 2 * lines, pl.ds(t * self.inner + h * wide, wide)] = held

    def turn_whole(self, source, tiles):
        rows, blocks = self.rows, TILE // self.rows
        for t in range(tiles):
            tile = source[pl.ds(t * blocks, blocks), :rows, :].reshape(TILE, 2 * rows)
            self.turned[: 2 * rows, pl.ds(t * TILE, TILE)] = tile.T

    def turn_side(self, source, base, lines, spans):
        blocks = self.inner // self.rows
        for j in range(spans):
            tile = source[pl.ds(j * blocks, blocks), pl.ds(base, lines), :].reshape(blocks * lines, 2 * self.rows)
            self.turned[: 2 * self.rows, pl.ds(j * self.inner, blocks * lines)] = tile.T

    def turn_part(self, source, base, lines, result):
        rows, wide, blocks = self.rows, self.inner // 2, self.inner // self.rows
        count = blocks * lines
        for j in range(self.outer):
            tile = source[pl.ds(j * blocks, blocks), pl.ds(base, lines), :].reshape(count, 2 * rows).T
            result[j, :, pl.ds(base * blocks, count)] = tile[:rows]
            result[j, :, pl.ds(wide + base * blocks, count)] = tile[rows:]

    def incoming_side(self, side, spans, twiddle, matrix, add, flip=None, extra=None):
        rows, inner = self.rows, self.inner
        wide = matrix.shape[2] // 2
        held = twiddle.at[:, :, pl.ds(side * wide, wide)]
        transform = small_dft if spans == self.outer else half_dft

        def body(r0):
            at = pl.ds(r0, self.step)
            items = []
            for j in range(spans):
                lanes = pl.ds(j * inner, wide)
                items.append((self.turned[at, lanes], self.turned[pl.ds(rows + r0, self.step), lanes]))
            for k, (re, im) in enumerate(transform(items, 1.0)):
                if extra is not None:
                    re = re - extra[at, :wide] if k % 2 else re + extra[at, :wide]
                for part, value in enumerate(self.twist(k, (re, im), 1.0, held, flip)):
                    top, low = halves(value)
                    self.top[k, at, pl.ds(part * wide, wide)] = top
                    self.low[k, at, pl.ds(part * wide, wide)] = low

        self.chunks(rows, body)
        deep, count = 2 * wide, self.outer * rows
        top = self.top[:, :rows, :deep].reshape(count, deep)
        low = self.low[:, :rows, :deep].reshape(count, deep)
        right_top, right_low = matrix[0, side], matrix[1, side]
        dot = functools.partial(jnp.dot, preferred_element_type=jnp.float32)
        total = dot(top, right_top) + dot(low, right_top) + dot(top, right_low)
        total = total.reshape(self.outer, rows, inner)
        if add:
            total = self.z[:, :rows, :inner] + total
        self.z[:, :rows, :inner] = total

    def first_imaginary(self, at):
        rows = self.rows
        part = self.turned[rows : 2 * rows, pl.ds(at, TILE)]
        lane0 = lax.broadcasted_iota(jnp.int32, part.shape, 1) == 0
        self.turned[rows : 2 * rows, pl.ds(at, TILE)] = jnp.where(lane0, 0.0, part)
        return jnp.where(lane0, part, 0.0)

    def incoming_half(self, lines, sign, twiddle, matrix, flip, extra=None, real_out=False):
        def body(r0):
            at = pl.ds(r0, self.step)
            items = []
            for j in range(self.outer // 2):
                lanes = pl.ds(j * self.inner, self.inner)
                items.append((self.turned[at, lanes], self.turned[pl.ds(lines + r0, self.step), lanes]))
            for k, (re, im) in enumerate(half_dft(items, sign)):
                if extra is not None:
                    re = re - extra[at, :] if k % 2 else re + extra[at, :]
                re, im = self.twist(k, (re, im), sign, twiddle, flip)
                self.put(k, at, 0, re)
                self.put(k, at, 1, im)

        self.chunks(lines, body)
        self.multiply(lines, matrix, real_out=real_out)

    def outgoing_half(self, lines, sign, twiddle, matrix, flip, write):
        self.multiply(lines, matrix)

        def body(r0):
            at = pl.ds(r0, self.step)
            write(r0, small_dft([
                self.twist(k, (self.get(k, at, 0), self.get(k, at, 1)), sign, twiddle, flip)
                for k in range(self.outer)
            ], sign)[: self.outer // 2])

        self.chunks(lines, body)

    def outgoing_sides(self, twiddle, matrix, sides, late=None):
        self.multiply(self.rows, matrix, real_in=True)
        rows, blocks, middle = self.rows, self.inner // self.rows, self.outer // 2
        lines, step = rows // len(sides), self.step
        tall = 2 * lines * rows // TILE
        for h in range(rows // tall):

            def body(i, carry, h=h):
                r0 = pl.multiple_of(i * step, step)
                at = pl.ds(h * tall + r0, step)
                items = small_dft([
                    self.twist(k, (self.get(k, at, 0), self.get(k, at, 1)), -1.0, twiddle)
                    for k in range(self.outer)
                ], -1.0)
                (low, low_im), (high, high_im) = items[0], items[middle]
                lane0 = lax.broadcasted_iota(jnp.int32, low.shape, 1) == 0
                items[0] = (low, jnp.where(lane0, high, low_im))
                items[middle] = (high, jnp.where(lane0, low, high_im))
                if late is not None:
                    items = [
                        tuple(jnp.where(late, one, other) for one, other in zip(items[middle + j], items[j]))
                        for j in range(middle)
                    ]
                for j, pair in enumerate(items):
                    for part, value in enumerate(pair):
                        to = pl.ds((2 * h + part) * lines, lines)
                        for piece in range(blocks):
                            for side, result in enumerate(sides):
                                base = piece * rows + side * lines
                                result[j * blocks + piece, pl.ds(r0, step), to] = value[:, base : base + lines]
                return carry

            lax.fori_loop(0, tall // step, body, 0)

    def outgoing_kept(self, twiddle, matrix, result):
        self.multiply(self.rows, matrix, real_in=True)
        rows, half, blocks = self.rows, self.half, self.inner // self.rows
        tall = rows * rows // TILE
        step = math.gcd(rows, 16)
        span = min(tall, step)
        for h in range(rows // max(tall, step)):

            def body(i, carry, h=h):
                r0 = i * step if isinstance(i, int) else pl.multiple_of(i * step, step)
                at = pl.ds(h * max(tall, step) + r0, step)
                items = self.pack_middle(small_dft([
                    self.twist(k, (self.get(k, at, 0), self.get(k, at, 1)), -1.0, twiddle)
                    for k in range(self.outer)
                ], -1.0))
                for j, pair in enumerate(items):
                    base = self.inner // 2 if 2 * j >= self.outer else 0
                    for piece in range(blocks):
                        lanes = slice(base + piece * half, base + (piece + 1) * half)
                        for part, value in enumerate(pair):
                            for sub in range(step // span):
                                group = h * (step // span) + sub
                                to = pl.ds(group * rows + part * half, half)
                                held = value[sub * span : (sub + 1) * span, lanes]
                                result[j * blocks + piece, pl.ds(r0, span), to] = held
                return carry

            if tall > step:
                lax.fori_loop(0, tall // step, body, 0)
            else:
                body(0, 0)

    def mirrored(self, blocks, mirror):
        dot = functools.partial(jnp.dot, preferred_element_type=jnp.float32)

        def flip(values, which):
            top, low = halves(jnp.concatenate(values, axis=0))
            return dot(top, mirror[which]) + dot(low, mirror[which])

        flat = [part for k in range(self.outer) for pair in blocks[k] for part in pair]
        per = 2 * len(blocks[0])
        low = flip(flat[:per], 0)
        high = flip(flat[per:], 1)
        out = []
        for k in range(self.outer):
            part, base = (low, 0) if k == 0 else (high, (self.outer - k - 1) * per)
            take = lambda i: part[(base + i) * 8 : (base + i + 1) * 8]
            out.append([(take(2 * i), -take(2 * i + 1)) for i in range(per // 2)])
        return out

    def pack_columns(self, slabs, result):
        rows, half, wide = self.rows, self.half, self.inner // 2
        blocks, groups = self.inner // rows, TILE // rows
        tall = rows // groups
        for k in range(self.outer):
            slab = slabs(k)
            for s in range(blocks):
                parts = []
                for group in range(groups):
                    for part in range(2):
                        at = part * wide + s * half
                        parts.append(slab[group * tall : (group + 1) * tall, at : at + half])
                result[k * blocks + s] = jnp.concatenate(parts, axis=1)

    def turn_columns(self, source, result):
        rows, wide, blocks = self.rows, self.inner // 2, self.inner // self.rows
        for j in range(self.outer):
            tile = source[pl.ds(j * blocks, blocks), :, :].reshape(wide, 2 * rows).T
            result[j, :, pl.ds(0, wide)] = tile[:rows]
            result[j, :, pl.ds(wide, wide)] = tile[rows:]

    def spread(self, first, second, strided, result):
        rows, fill = self.rows, TILE - 2 * self.rows
        for t in range(self.length // TILE):
            lanes = pl.ds(t * TILE, TILE)
            parts = [first[:, lanes], second[:, lanes]]
            if fill:
                parts.append(jnp.zeros((fill, TILE), jnp.float32))
            strided[pl.ds(t * TILE, TILE), :] = jnp.concatenate(parts, axis=0).T
        for k in range(self.outer):
            slab = strided[pl.ds(k, self.inner, stride=self.outer), :].T
            result[k] = slab[: 2 * rows, :]

    def spread_one(self, source, strided, result, base):
        rows, wide = self.rows, self.inner // 2
        tiles = self.length // (2 * TILE)
        for t in range(tiles):
            pair = [source[:, pl.ds(at * TILE, TILE)] for at in (t, t + tiles)]
            strided[pl.ds(t * TILE, TILE), :] = jnp.concatenate(pair, axis=0).T
        for k in range(self.outer):
            slab = strided[pl.ds(k, wide, stride=self.outer), :].T
            result[k, pl.ds(base, rows), pl.ds(0, wide)] = slab[:rows]
            result[k, pl.ds(base, rows), pl.ds(wide, wide)] = slab[rows:]

    def collect_one(self, slabs, strided, result):
        rows, wide = self.rows, self.inner // 2
        tiles = self.length // (2 * TILE)
        for k in range(self.outer):
            slab = slabs(k)
            pair = jnp.concatenate([slab[:, :wide], slab[:, wide:]], axis=0)
            strided[pl.ds(k, wide, stride=self.outer), :] = pair.T
        for t in range(tiles):
            block = strided[pl.ds(t * TILE, TILE), :].T
            result[:, pl.ds(t * TILE, TILE)] = block[:rows]
            result[:, pl.ds((t + tiles) * TILE, TILE)] = block[rows:]

    def collect(self, slabs, strided, results):
        rows = self.rows
        for k in range(self.outer):
            slab = slabs(k)
            fill = TILE - slab.shape[0]
            if fill:
                slab = jnp.concatenate([slab, jnp.zeros((fill, self.inner), jnp.float32)], axis=0)
            strided[pl.ds(k, self.inner, stride=self.outer), :] = slab.T
        for t in range(self.length // TILE):
            block = strided[pl.ds(t * TILE, TILE), :].T
            for i, result in enumerate(results):
                result[:, pl.ds(t * TILE, TILE)] = block[i * rows : (i + 1) * rows, :]


def signed_waves(position, count):
    signed = jnp.where(position < count // 2, position, position - count)
    waves = 4.0 * signed.astype(jnp.float32) / count
    return waves, jnp.where(position == count // 2, jnp.float32(0.0), waves)


def first_waves(piece, k):
    lanes = lax.broadcasted_iota(jnp.int32, (1, piece.inner), 1)
    return signed_waves(piece.outer * lanes + k, piece.length)


def inverse_denominator(wave_first, wave_second):
    square = wave_first * wave_first + wave_second * wave_second
    return 1.0 / (1.0 + time_step * (square * square - square))


def second_wave(piece, position):
    shape = (position.shape[0], piece.inner)
    return jnp.broadcast_to(signed_waves(position, piece.length)[0], shape)


def row_index(count, width):
    return lax.broadcasted_iota(jnp.int32, (count, width), 0)


class Links:
    def __init__(self, devices, fast):
        self.devices, self.fast = devices, fast
        self.device = lax.axis_index(axes[0]) * fast + lax.axis_index(axes[1])
        self.near = min(8, devices // 2)
        self.steps = []
        for low in range(self.near):
            step, bit = 0, 1
            while bit < self.near:
                if low // bit % 2:
                    step += bit * (1 - 2 * lax.rem(lax.div(self.device, bit), 2))
                bit *= 2
            self.steps.append(step)

    def visit(self, count, body):
        near = self.near

        def far(i, carry):
            base = self.partner(count - near * i)
            for low in reversed(range(near)):
                body(base + self.steps[low])
            return carry

        lax.fori_loop(1, count // near, far, 0)
        for low in reversed(range(1, near)):
            body(self.device + self.steps[low])

    def partner(self, i):
        total, bit = 0, 1
        while bit < self.devices:
            total += bit * lax.rem(lax.div(self.device, bit) + lax.div(i, bit), 2)
            bit *= 2
        return total

    def place(self, peer):
        return (lax.div(peer, self.fast), lax.rem(peer, self.fast))

    def greet(self):
        barrier = pltpu.get_barrier_semaphore()

        def go(peer):
            at = self.place(peer)
            pl.semaphore_signal(barrier, inc=1, device_id=at, device_id_type=pl.DeviceIdType.MESH)

        self.visit(self.devices, go)

    def meet(self):
        pl.semaphore_wait(pltpu.get_barrier_semaphore(), self.devices - 1)

    def send(self, source, target, sems, count):
        send_sem, recv_sem, own_sem = sems
        own = lax.rem(self.device, count)

        def go(peer):
            pltpu.make_async_remote_copy(
                src_ref=source(peer if count == self.devices else lax.rem(peer, count)),
                dst_ref=target(own),
                send_sem=send_sem,
                recv_sem=recv_sem,
                device_id=self.place(peer),
                device_id_type=pl.DeviceIdType.MESH,
            ).start()

        self.visit(count, go)
        pltpu.make_async_copy(source(own), target(own), own_sem).start()

    def whole(self, source, target, sems, count):
        others = pl.ds(0, count - 1)
        return pltpu.make_async_remote_copy(
            src_ref=source(others),
            dst_ref=target(others),
            send_sem=sems[0],
            recv_sem=sems[1],
            device_id=(0, 0),
            device_id_type=pl.DeviceIdType.MESH,
        )

    def receive(self, source, target, sems, count):
        own = lax.rem(self.device, count)
        pltpu.make_async_copy(source(own), target(own), sems[2]).wait()
        self.whole(source, target, sems, count).wait_recv()

    def sent(self, source, target, sems, count):
        self.whole(source, target, sems, count).wait_send()


def start_kernel(length, rows, field, target, out, both_p, *scratch):
    piece = Pieces(length, rows)
    piece.spread(field, target, scratch[0], both_p)
    piece.pack_columns(lambda k: both_p[k, pl.ds(0, rows), :], out)


def slope_second_kernel(length, rows, field_p, twiddle, out_matrix, in_matrix, kept, result, *scratch):
    piece = Pieces(length, rows, *scratch)

    def body(r0):
        at = pl.ds(r0, piece.step)
        for k in range(piece.outer):
            piece.put(k, at, 0, field_p[k, at, :])

    piece.chunks(rows, body)
    for j in range(piece.outer):
        piece.clear_other(j)

    def write(r0, items):
        for j, (re, im) in enumerate(items):
            at, wide = piece.kept_lanes(j)
            base = at - j * piece.inner
            position = j * piece.inner + kept[:, base : base + wide]
            slope = 2.0 * signed_waves(position, length)[1]
            piece.turned[pl.ds(r0, piece.step), pl.ds(at, wide)] = -slope * im[:, base : base + wide]
            piece.turned[pl.ds(rows + r0, piece.step), pl.ds(at, wide)] = slope * re[:, base : base + wide]

    piece.outgoing(rows, -1.0, twiddle, out_matrix, True, write)
    piece.incoming(rows, 1.0, twiddle, in_matrix, real_out=True)
    result[...] = piece.z[:, :, : piece.inner]


def spread_kernel(length, rows, forcing, result, strided):
    Pieces(length, rows).spread(forcing.at[0], forcing.at[1], strided, result)


def collect_kernel(length, rows, slabs, result, strided):
    piece = Pieces(length, rows)
    piece.collect(lambda k: slabs[k], strided, [result.at[i] for i in range(result.shape[0])])


def weight_of(device, r0, step, inner):
    alone = (row_index(step, inner) + r0 + device) == 0
    return jnp.where(alone, jnp.float32(1.0), jnp.float32(2.0))


def slope_first_kernel(length, rows, source, in_twiddle, in_matrix, out_twiddle, out_matrix, out, *scratch):
    piece = Pieces(length, rows, *scratch)
    half = piece.half
    piece.turn_lines(source)
    piece.incoming(half, -1.0, in_twiddle, in_matrix)

    def body(r0):
        at = pl.ds(r0, piece.step)
        for k in range(piece.outer):
            re, im = piece.get(k, at, 0), piece.get(k, at, 1)
            scale = first_waves(piece, k)[1]
            piece.put(k, at, 0, -scale * im)
            piece.put(k, at, 1, scale * re)

    piece.chunks(half, body)
    piece.outgoing(half, 1.0, out_twiddle, out_matrix, False, piece.write_full(out, False))


def edge_inverses(piece, k):
    wave_first = first_waves(piece, k)[0]
    middle = jnp.full((1, 1), piece.length // 2, jnp.int32)
    zero = jnp.zeros((1, 1), jnp.int32)
    return [inverse_denominator(wave_first, signed_waves(p, piece.length)[0]) for p in (zero, middle)]


def next_kernel(length, rows, device_ref, source, forcing, in_twiddle, in_matrix, out_twiddle, out_matrix, mirror, out, *scratch):
    device = device_ref[0]
    piece = Pieces(length, rows, *scratch)
    half, step, inner = piece.half, piece.step, piece.inner
    late = device >= (length // rows) // 2
    piece.turn_lines(source)
    piece.incoming(half, -1.0, in_twiddle, in_matrix)

    def body(r0):
        at, also = pl.ds(r0, step), pl.ds(half + r0, step)
        index = row_index(step, 1) + r0
        low_wave = second_wave(piece, device * rows + index)
        high_wave = second_wave(piece, device * rows + half + index)
        moved = jnp.logical_and(row_index(step, inner) + r0 == 0, late)
        weight = weight_of(device, r0, step, inner)
        for k in range(piece.outer):
            wave_first = first_waves(piece, k)[0]
            low = inverse_denominator(wave_first, low_wave)
            high = inverse_denominator(wave_first, high_wave)
            for part in range(2):
                own = weight * piece.get(k, at, part)
                f_low = time_step * forcing[k, pl.ds(part * rows + r0, step), :]
                f_high = time_step * forcing[k, pl.ds(part * rows + half + r0, step), :]
                piece.put(k, at, part, (f_low + jnp.where(moved, 0.0, own)) * low)
                piece.put(k, also, part, (f_high + jnp.where(moved, own, 0.0)) * high)

    piece.chunks(half, body)

    @pl.when(device == 0)
    def _():
        at = pl.ds(0, 8)
        blocks = []
        for k in range(piece.outer):
            own = tuple(piece.get(k, at, part) for part in range(2))
            full = tuple(
                own[part] + time_step * forcing[k, pl.ds(part * rows, 8), :] for part in range(2)
            )
            blocks.append([own, full])
        flipped = piece.mirrored(blocks, mirror)
        rest = pl.ds(0, 16)
        row0 = row_index(16, inner) == 0
        for k in range(piece.outer):
            zero, middle = edge_inverses(piece, k)
            for part in range(2):
                own, full = blocks[k][0][part], blocks[k][1][part]
                own_c, full_c = flipped[k][0][part], flipped[k][1][part]
                value = 0.5 * ((full + full_c) * zero + (own - own_c) * middle)
                replace(piece, k, part, value)

    piece.outgoing(rows, 1.0, out_twiddle, out_matrix, False, piece.write_full(out, False))


def replace(piece, k, part, value):
    lanes = pl.ds(part * piece.inner, piece.inner)
    row0 = row_index(16, piece.inner) == 0
    value = jnp.concatenate([value, value], axis=0)
    for held, new in zip((piece.top, piece.low), halves(value)):
        old = held[k, pl.ds(0, 16), lanes].astype(jnp.float32)
        held[k, pl.ds(0, 16), lanes] = jnp.where(row0, new.astype(jnp.float32), old).astype(jnp.bfloat16)


def misfit_kernel(length, rows, device_ref, source, in_twiddle, in_matrix, out_twiddle, out_matrix, mirror, out, full, total_out, *scratch):
    device = device_ref[0]
    piece = Pieces(length, rows, *scratch)
    half, step, inner = piece.half, piece.step, piece.inner
    late = device >= (length // rows) // 2
    piece.turn_full(source)
    piece.incoming(rows, -1.0, in_twiddle, in_matrix)

    def body(r0):
        at, also = pl.ds(r0, step), pl.ds(half + r0, step)
        index = row_index(step, 1) + r0
        low_wave = second_wave(piece, device * rows + index)
        high_wave = second_wave(piece, device * rows + half + index)
        moved = jnp.logical_and(row_index(step, inner) + r0 == 0, late)
        weight = weight_of(device, r0, step, inner)
        for k in range(piece.outer):
            wave_first = first_waves(piece, k)[0]
            low = time_step * inverse_denominator(wave_first, low_wave)
            high = time_step * inverse_denominator(wave_first, high_wave)
            for part in range(2):
                low_value = piece.get(k, at, part) * low
                high_value = piece.get(k, also, part) * high
                full[k, pl.ds(part * rows + r0, step), :] = low_value
                full[k, pl.ds(part * rows + half + r0, step), :] = high_value
                own = jnp.where(moved, high_value, low_value)
                piece.put(k, at, part, weight * own)

    piece.chunks(half, body)

    @pl.when(device == 0)
    def _():
        at = pl.ds(0, 8)
        blocks = [[(piece.get(k, at, 0), piece.get(k, at, 1))] for k in range(piece.outer)]
        flipped = piece.mirrored(blocks, mirror)
        row0 = row_index(8, inner) == 0
        for k in range(piece.outer):
            zero, middle = edge_inverses(piece, k)
            for part in range(2):
                own, own_c = blocks[k][0][part], flipped[k][0][part]
                first = (0.5 * time_step) * (own + own_c) * zero
                value = first + (0.5 * time_step) * (own - own_c) * middle
                at_full = pl.ds(part * rows, 8)
                full[k, at_full, :] = jnp.where(row0, first, full[k, at_full, :])
                replace(piece, k, part, value)

    piece.outgoing(half, 1.0, out_twiddle, out_matrix, False, piece.write_full(out, False))
    total_out[...] = jnp.sum(source[:, pl.ds(rows, 8), :], axis=0)


def nonlinear_kernel(length, rows, source, both_p, second, twiddle, out_matrix, out, first, *scratch):
    piece = Pieces(length, rows, *scratch)
    piece.turn_columns(source, first)

    def body(r0):
        at = pl.ds(r0, piece.step)
        for k in range(piece.outer):
            one, other = first[k, at, :], second[k, at, :]
            piece.put(k, at, 0, both_p[k, at, :] - (0.5 * time_step) * (one * one + other * other))

    piece.chunks(rows, body)
    piece.outgoing_kept(twiddle, out_matrix, out)


def joint_kernel(length, rows, source, first, second, twiddle, in_matrix, out, value_out, second_out, *scratch):
    piece = Pieces(length, rows, *scratch)
    piece.turn_kept(source)
    piece.unpack_middle()
    piece.incoming(rows, 1.0, twiddle, in_matrix, real_out=True)
    lanes = pl.ds(0, piece.inner)

    def body(r0):
        at = pl.ds(r0, piece.step)
        for k in range(piece.outer):
            value = piece.get(k, at, 0)
            value_out[k, at, :] = (1.0 / time_step) * value
            second_out[k, at, :] = value * second[k, at, :]
            piece.z[k, at, lanes] = value * first[k, at, :]

    piece.chunks(rows, body)
    piece.pack_columns(lambda k: piece.z[k, pl.ds(0, rows), lanes], out)


def residual_kernel(length, rows, source, both_p, twiddle, in_matrix, out_matrix, out, field_out, *scratch):
    piece = Pieces(length, rows, *scratch[:4])
    strided, total = scratch[4:]
    piece.turn_full(source)
    piece.unpack_middle()
    piece.incoming(rows, 1.0, twiddle, in_matrix, real_out=True)
    piece.collect(lambda k: piece.get(k, pl.ds(0, rows), 0), strided, [field_out])
    total[...] = jnp.zeros_like(total)

    def body(r0):
        at = pl.ds(r0, piece.step)
        for k in range(piece.outer):
            residual = piece.get(k, at, 0) - both_p[k, pl.ds(rows + r0, piece.step), :]
            total[...] += residual * residual
            piece.put(k, at, 0, residual)

    piece.chunks(rows, body)
    piece.outgoing(rows, -1.0, twiddle, out_matrix, True, piece.write_full(out, True))
    value = 0.5 * jnp.sum(total[...])
    out[:, pl.ds(rows, 8), :] = jnp.full((out.shape[0], 8, 2 * rows), value, jnp.float32)


def last_kernel(length, rows, source, value, second, field_out, strided, first):
    piece = Pieces(length, rows)
    piece.turn_columns(source, first)
    piece.collect(lambda k: first[k] + value[k] + second[k], strided, [field_out])


def step_kernel(length, rows, devices, fast, cuts, parts, inputs, outs, box):
    links = Links(devices, fast)
    device, half, part_devices = links.device, rows // 2, devices // 2
    late = device >= part_devices
    flip = jnp.where(late, -1.0, 1.0).astype(jnp.float32)
    sides, count = range(parts), rows // parts
    copies, sems = box.copies, box.sems
    work = (box.turned, box.top, box.low, box.z)
    piece = Pieces(length, rows, *work)
    step, inner, outer = piece.step, piece.inner, piece.outer
    both_p, forcing_p, full = box.both_p, box.forcing_p, box.full
    first, second, value = box.first, box.second, box.value
    strided, total = box.strided, box.total
    lanes = pl.ds(0, inner)

    loads = [
        pltpu.make_async_copy(ref, held, copies.at[i])
        for i, (ref, held) in enumerate(zip(inputs.refs, inputs.held))
    ]
    loads[0].start()
    links.greet()
    waiting = iter(loads)

    def load(count):
        for i in range(count):
            next(waiting).wait()

    at_all = lambda ref: lambda e: ref.at[e]
    at_lines = lambda ref, base, count: lambda e: ref.at[e, pl.ds(base, count)]
    order = []

    def send(source, target, count=devices):
        i = len(order)
        order.append((source, target, (sems.at[i, 0], sems.at[i, 1], sems.at[i, 2]), count))
        links.send(*order[-1])
        return order[-1]

    def receive(*moves):
        for move in moves:
            links.receive(*move)

    tw_natural, tw_kept, tw_lines, tw_cut, tw_sided = (inputs.twiddles.at[i] for i in range(5))
    forward, backward, mirror = inputs.forward, inputs.backward, inputs.mirror
    kept_out, kept_in, kept = inputs.kept_out, inputs.kept_in, inputs.kept
    lines_in, cut_in = box.lines_in, box.cut_in
    if parts == 2 * cuts:
        tw_lines, lines_in = tw_cut, cut_in

    def permute_rows(groups, result):
        tall, blocks = rows // groups, inner // rows
        for p in range(2):
            for part in range(2):
                for group in range(groups):
                    for s in range(blocks):
                        at = part * inner + group * (inner // groups) + s * tall
                        source = part * inner + s * rows + group * tall
                        result[p, pl.ds(at, tall), :] = forward[p, pl.ds(source, tall), :]

    def slope_first(source, out, lines):
        piece.turn_cut(source, lines, outer)
        piece.incoming(lines, -1.0, tw_cut, cut_in)

        def body(r0):
            at = pl.ds(r0, step)
            for k in range(outer):
                re, im = piece.get(k, at, 0), piece.get(k, at, 1)
                scale = first_waves(piece, k)[1]
                piece.put(k, at, 0, -scale * im)
                piece.put(k, at, 1, scale * re)

        piece.chunks(lines, body)
        piece.outgoing(lines, 1.0, tw_natural, backward, False, piece.write_full(out, False))

    def slope_second(source, out):
        slope_second_kernel(length, rows, source, tw_kept, kept_out, kept_in, kept, out, *work)

    def send_columns(source, target):
        return [send(at_all(source.at[q]), at_all(target.at[q])) for q in range(cuts)]

    def turn_slopes(moves, source, back, target):
        size, result = half // cuts, []
        for q, move in enumerate(moves):
            receive(move)
            slope_first(source.at[q], back.at[q], size)
            result.append(send(at_all(back.at[q]), at_lines(target, q * size, size)))
        return result

    def lines_of(side, r0):
        line = row_index(step, 1) + r0 + side * count
        alone = (row_index(step, inner) + r0 + side * count + lax.rem(device, part_devices)) == 0
        return second_wave(piece, device * rows + line), jnp.where(alone, jnp.float32(1.0), jnp.float32(2.0))

    def edges(k):
        wave = first_waves(piece, k)[0]
        middle = jnp.full((1, 1), length // 2, jnp.int32)
        mine, theirs = jnp.where(late, middle, 0), jnp.where(late, 0, middle)
        return [inverse_denominator(wave, signed_waves(p, length)[0]) for p in (mine, theirs)]

    load(1)
    for copy in loads[1:]:
        copy.start()
    piece.spread_one(inputs.field, strided, both_p, 0)
    piece.pack_cut(lambda k: both_p[k, pl.ds(0, rows), :], [box.s_field.at[q] for q in range(cuts)])
    links.meet()
    m_field = send_columns(box.s_field, box.r_field)

    load(len(loads) - 1)
    piece.spread_one(inputs.target, strided, both_p, rows)
    if parts != 2 * cuts:
        permute_rows(TILE * parts // (2 * rows), lines_in)
    permute_rows(TILE * cuts // rows, cut_in)
    for side in sides:
        for p in range(2):
            for part in range(2):
                for s in range(inner // rows):
                    at = part * (inner // parts) + s * count
                    source = part * inner + s * rows + side * count
                    box.sided[p, side, pl.ds(at, count), :] = backward[p, pl.ds(source, count), :inner]
    slope_second(both_p, second)
    m_slope = turn_slopes(m_field, box.r_field, box.s_slope, box.r_slope)
    piece.spread(inputs.forcing.at[0], inputs.forcing.at[1], strided, forcing_p)

    for q in range(cuts):
        receive(m_slope[q])
        piece.turn_part(box.r_slope, q * half // cuts, half // cuts, first)

    def nonlinear(r0):
        at = pl.ds(r0, step)
        for k in range(outer):
            one, other = first[k, at, :], second[k, at, :]
            piece.put(k, at, 0, both_p[k, at, :] - (0.5 * time_step) * (one * one + other * other))

    piece.chunks(rows, nonlinear)
    piece.outgoing_sides(tw_natural, forward, [box.s_sum.at[side] for side in sides], late)
    backwards = sides[::-1]
    m_sum = [send(at_all(box.s_sum.at[side]), at_all(box.r_sum.at[side]), part_devices) for side in backwards]

    def divide(side):
        def body(r0):
            at = pl.ds(r0, step)
            wave, weight = lines_of(side, r0)
            for k in range(outer):
                scale = inverse_denominator(first_waves(piece, k)[0], wave)
                for part in range(2):
                    forced = time_step * forcing_p[k, pl.ds(part * rows + side * count + r0, step), :]
                    piece.put(k, at, part, (weight * piece.get(k, at, part) + forced) * scale)

        piece.chunks(count, body)
        if side:
            return

        @pl.when(lax.rem(device, part_devices) == 0)
        def _():
            at = pl.ds(0, 8)
            blocks = []
            for k in range(outer):
                own = tuple(piece.get(k, at, part) for part in range(2))
                joined = tuple(own[part] + time_step * forcing_p[k, pl.ds(part * rows, 8), :] for part in range(2))
                blocks.append([own, joined])
            flipped = piece.mirrored(blocks, mirror)
            for k in range(outer):
                mine, theirs = edges(k)
                for part in range(2):
                    own, joined = blocks[k][0][part], blocks[k][1][part]
                    own_c, joined_c = flipped[k][0][part], flipped[k][1][part]
                    replace(piece, k, part, 0.5 * ((joined + joined_c) * mine + (own - own_c) * theirs))

    m_next = []
    for side, move in zip(backwards, m_sum):
        receive(move)
        piece.turn_cut(box.r_sum.at[side], count, outer // 2)
        piece.incoming_half(count, -1.0, tw_lines, lines_in, flip)
        divide(side)
        sent = box.s_next.at[side]
        piece.outgoing(count, 1.0, tw_natural, backward, False, piece.write_full(sent, False))
        m_next.append(send(at_all(sent), at_lines(box.r_next, side * count, count)))

    for side, move in zip(backwards, m_next):
        receive(move)
        piece.turn_side(box.r_next, side * count, count, outer)
        if side == 0:
            low, high = piece.first_imaginary(0), piece.first_imaginary(length // 2)
            piece.turned[:rows, pl.ds(0, TILE)] += high
            piece.turned[:rows, pl.ds(length // 2, TILE)] += low
        piece.incoming_side(side, outer, tw_sided, box.sided, side != backwards[0])
    total[...] = jnp.zeros_like(total)

    def misfit(r0):
        at = pl.ds(r0, step)
        for k in range(outer):
            now = piece.get(k, at, 0)
            value[k, at, :] = now
            residual = now - both_p[k, pl.ds(rows + r0, step), :]
            total[...] += residual * residual
            piece.put(k, at, 0, residual)

    piece.chunks(rows, misfit)
    piece.outgoing_sides(tw_natural, forward, [box.s_kept.at[side] for side in sides])
    m_kept = [send(at_all(box.s_kept.at[side]), at_all(box.r_kept.at[side])) for side in sides]
    box.s_total[...] = jnp.full(box.s_total.shape, 0.5 * jnp.sum(total[...]), jnp.float32)
    piece.collect_one(lambda k: value[k], strided, outs.next)

    def adjoint(side):
        def body(r0):
            at = pl.ds(r0, step)
            wave, weight = lines_of(side, r0)
            for k in range(outer):
                scale = time_step * inverse_denominator(first_waves(piece, k)[0], wave)
                for part in range(2):
                    own = piece.get(k, at, part) * scale
                    full[k, pl.ds(part * rows + side * count + r0, step), :] = own
                    piece.put(k, at, part, weight * own)

        piece.chunks(count, body)
        if side:
            return

        @pl.when(lax.rem(device, part_devices) == 0)
        def _():
            at = pl.ds(0, 8)
            blocks = [[(piece.get(k, at, 0), piece.get(k, at, 1))] for k in range(outer)]
            flipped = piece.mirrored(blocks, mirror)
            row0 = row_index(8, inner) == 0
            for k in range(outer):
                mine, theirs = edges(k)
                for part in range(2):
                    own, own_c = blocks[k][0][part], flipped[k][0][part]
                    line = (0.5 * time_step) * (own + own_c) * mine
                    at_full = pl.ds(part * rows, 8)
                    full[k, at_full, :] = jnp.where(row0, line, full[k, at_full, :])
                    replace(piece, k, part, line + (0.5 * time_step) * (own - own_c) * theirs)

    m_back = []
    for side in sides:
        receive(m_kept[side])
        piece.turn_cut(box.r_kept.at[side], count, outer)
        piece.incoming(count, -1.0, tw_lines, lines_in)
        adjoint(side)
        sent = box.s_back.at[side]
        piece.outgoing_half(count, 1.0, tw_natural, backward, flip, piece.write_full(sent, False))
        m_back.append(send(at_all(sent), at_lines(box.r_back, side * count, count), part_devices))

    m_total = send(at_all(box.s_total), at_all(box.r_total))
    for side in sides:
        receive(m_back[side])
        piece.turn_side(box.r_back, side * count, count, outer // 2)
        if side == 0:
            box.extra[...] = piece.first_imaginary(0)
        piece.incoming_side(side, outer // 2, tw_sided, box.sided, side > 0, flip, None if side else box.extra)

    def products(r0):
        at = pl.ds(r0, step)
        for k in range(outer):
            now = piece.get(k, at, 0)
            value[k, at, :] = (1.0 / time_step) * now
            box.product[k, at, :] = now * second[k, at, :]
            piece.z[k, at, lanes] = now * first[k, at, :]

    piece.chunks(rows, products)
    piece.pack_cut(lambda k: piece.z[k, pl.ds(0, rows), lanes], [box.s_product.at[q] for q in range(cuts)])
    m_product = send_columns(box.s_product, box.r_product)
    slope_second(box.product, second)
    for k in range(outer):
        value[k] = value[k] + second[k]
    m_last = turn_slopes(m_product, box.r_product, box.s_last, box.r_last)

    piece.collect(lambda k: full[k], strided, [outs.forcing.at[i] for i in range(2)])
    receive(m_total)
    outs.total[...] = jnp.sum(box.r_total[...], axis=0) / (length * length)

    for q in range(cuts):
        receive(m_last[q])
        piece.turn_part(box.r_last, q * half // cuts, half // cuts, first)
    for k in range(outer):
        outs.field[k] = first[k] + value[k]
    for move in order:
        links.sent(*move)


def joined_step(field, target, forcing, devices, fast, rows, length):
    outer, inner = split_length(length)
    half, step, cuts = rows // 2, math.gcd(rows // 2, 16), 2
    parts = 2
    natural, kept = orders(length, rows)[:2]
    lines = line_order(inner, rows, TILE * parts // (2 * rows))
    cut = line_order(inner, rows, TILE * cuts // rows)
    sided = natural.reshape(inner // rows, parts, rows // parts).transpose(1, 0, 2).reshape(inner)
    matrix = lambda *args: matrix_table(length, *args)
    tables = dict(
        field=field, target=target,
        twiddles=np.stack([twiddle_table(length, o) for o in (natural, kept, lines, cut, sided)]),
        kept=kept[None, :].astype(np.int32),
        kept_out=matrix(-1.0, natural, kept)[:, :inner],
        kept_in=matrix(1.0, kept, natural)[:, :, :inner],
        forcing=forcing,
        backward=matrix(1.0, natural, natural),
        forward=matrix(-1.0, natural, natural),
        mirror=mirror_table(length),
    )
    operands = [jnp.asarray(table) for table in tables.values()]
    float32 = jnp.float32
    held = lambda *dims: pltpu.VMEM(dims, float32)
    packed = held(parts, devices, 2 * rows * rows // (parts * TILE), TILE)
    lined = held(parts, devices, rows // parts, 2 * rows)
    packed_half, lined_half = (held(parts, devices // 2, *dims.shape[2:]) for dims in (packed, lined))
    columns, slopes = held(cuts, devices, rows * rows // (TILE * cuts), TILE), held(cuts, devices, half // cuts, 2 * rows)
    returned = held(devices, half, 2 * rows)
    table = pltpu.VMEM((2, 2 * inner, 2 * inner), jnp.bfloat16)
    pair, one = held(outer, 2 * rows, inner), held(outer, rows, inner)
    small = held(devices, 1, TILE)
    halved = pltpu.VMEM((outer, rows, 2 * inner), jnp.bfloat16)
    shapes = dict(
        turned=held(2 * rows, length), top=halved, low=halved, z=held(outer, rows, 2 * inner),
        strided=held(length, TILE), total=held(step, inner),
        both_p=pair, forcing_p=pair, full=pair, first=one, second=one, value=one, product=one,
        lines_in=table, cut_in=table, extra=held(rows, TILE), sided=pltpu.VMEM((2, parts, 2 * inner // parts, inner), jnp.bfloat16),
        s_field=columns, r_field=columns, s_slope=slopes, r_slope=returned,
        s_sum=packed_half, r_sum=packed_half, s_next=lined, r_next=held(devices, rows, 2 * rows),
        s_kept=packed, r_kept=packed, s_total=small, r_total=small,
        s_back=lined_half, r_back=held(devices // 2, rows, 2 * rows),
        s_product=columns, r_product=columns, s_last=slopes, r_last=returned,
        copies=pltpu.SemaphoreType.DMA((len(operands),)),
        sems=pltpu.SemaphoreType.DMA((1 + 4 * parts + 4 * cuts, 3)),
    )
    inputs = [pltpu.VMEM(operand.shape, operand.dtype) for operand in operands]

    def body(*refs):
        a, b = len(operands), len(operands) + 4
        c = b + len(operands)
        given = SimpleNamespace(refs=refs[:a], held=refs[b:c], **dict(zip(tables, refs[b:c])))
        outs = SimpleNamespace(next=refs[a], field=refs[a + 1], forcing=refs[a + 2], total=refs[a + 3])
        step_kernel(length, rows, devices, fast, cuts, parts, given, outs, SimpleNamespace(**dict(zip(shapes, refs[c:]))))

    anywhere = pl.BlockSpec(memory_space=pl.ANY)
    vmem, smem = pl.BlockSpec(memory_space=pltpu.VMEM), pl.BlockSpec(memory_space=pltpu.SMEM)
    shape = lambda *dims: jax.ShapeDtypeStruct(dims, float32)
    next_field, slabs, forcing_grad, total = pl.pallas_call(
        body,
        out_shape=(shape(rows, length), shape(outer, rows, inner), shape(2, rows, length), shape(1, TILE)),
        in_specs=[pl.BlockSpec(memory_space=pltpu.HBM)] * len(operands),
        out_specs=(vmem, vmem, vmem, vmem),
        scratch_shapes=inputs + list(shapes.values()),
        compiler_params=pltpu.CompilerParams(vmem_limit_bytes=34 * 2**20, has_side_effects=True, collective_id=0),
        cost_estimate=pl.CostEstimate(flops=6 * 10**10, bytes_accessed=4 * 2**20, transcendentals=0),
    )(*[pltpu.with_memory_space_constraint(one, pltpu.HBM) for one in operands])
    return pl.pallas_call(
        functools.partial(tail_kernel, length, rows),
        out_shape=(shape(rows, length), shape(rows, length), shape(2, rows, length), shape(1, 1)),
        in_specs=[vmem] * 4,
        out_specs=(anywhere, anywhere, anywhere, smem),
        scratch_shapes=[held(length, TILE), held(rows, length), pltpu.SemaphoreType.DMA((3,))],
        compiler_params=pltpu.CompilerParams(vmem_limit_bytes=8 * 2**20),
        cost_estimate=pl.CostEstimate(flops=10**9, bytes_accessed=4 * 2**20, transcendentals=0),
    )(next_field, slabs, forcing_grad, total)


def tail_kernel(length, rows, next_field, slabs, forcing_grad, total, next_out, field_out, forcing_out, total_out, strided, held, sems):
    piece = Pieces(length, rows)
    copies = [
        pltpu.make_async_copy(next_field, next_out, sems.at[0]),
        pltpu.make_async_copy(forcing_grad, forcing_out, sems.at[1]),
        pltpu.make_async_copy(held, field_out, sems.at[2]),
    ]
    copies[0].start()
    copies[1].start()
    total_out[0, 0] = jnp.sum(total[0:1, 0:1])
    piece.collect_one(lambda k: slabs[k], strided, held)
    copies[2].start()
    for copy in copies:
        copy.wait()


def member_step(device, field, target, forcing_p, devices, rows, length):
    outer, inner = split_length(length)
    half = rows // 2
    float32 = jnp.float32
    shape = lambda *dims: jax.ShapeDtypeStruct(dims, float32)
    kept_blocks = shape(devices, rows * rows // TILE, TILE)
    half_blocks = shape(devices, half, 2 * rows)
    blocks = shape(devices, rows, 2 * rows)
    longer = shape(devices, rows + 8, 2 * rows)
    pair, one = shape(outer, 2 * rows, inner), shape(outer, rows, inner)
    plain = shape(rows, length)
    step = math.gcd(half, 16)
    base = [
        pltpu.VMEM((2 * rows, length), float32),
        pltpu.VMEM((outer, rows, 2 * inner), jnp.bfloat16),
        pltpu.VMEM((outer, rows, 2 * inner), jnp.bfloat16),
        pltpu.VMEM((outer, rows, 2 * inner), float32),
    ]
    strided = pltpu.VMEM((length, TILE), float32)
    total = pltpu.VMEM((step, inner), float32)
    vmem = pl.BlockSpec(memory_space=pltpu.VMEM)
    smem = pl.BlockSpec(memory_space=pltpu.SMEM)

    natural, kept, lines = orders(length, rows)
    tw_natural, tw_kept, tw_lines = [jnp.asarray(twiddle_table(length, o)) for o in (natural, kept, lines)]
    matrix = lambda *args: matrix_table(length, *args)
    forward, backward = matrix(-1.0, natural, natural), matrix(1.0, natural, natural)
    kept_out, kept_in = matrix(-1.0, natural, kept)[:, :inner], matrix(1.0, kept, natural)[:, :, :inner]
    lines_in = matrix(-1.0, lines, natural)
    mirror = jnp.asarray(mirror_table(length))
    kept_lane = jnp.asarray(kept[None, :].astype(np.int32))

    def call(body, outs, scratch, *operands):
        return pl.pallas_call(
            functools.partial(body, length, rows),
            out_shape=outs,
            in_specs=[smem if operand is device else vmem for operand in operands],
            out_specs=jax.tree.map(lambda leaf: vmem, outs),
            scratch_shapes=scratch,
            compiler_params=pltpu.CompilerParams(vmem_limit_bytes=20 * 2**20),
            cost_estimate=pl.CostEstimate(flops=6 * 10**9, bytes_accessed=4 * 2**20, transcendentals=0),
        )(*operands)

    def move(value):
        return lax.all_to_all(value, axes, split_axis=0, concat_axis=0, tiled=True)

    spectral_tables = (tw_lines, lines_in, tw_natural, backward)
    slope_tables = (tw_kept, kept_out, kept_in, kept_lane)
    sent, both_p = call(start_kernel, (kept_blocks, pair), [strided], field, target)
    second = call(slope_second_kernel, one, base, both_p, *slope_tables)
    sent = call(slope_first_kernel, half_blocks, base, move(sent), *spectral_tables)
    sent, first = call(nonlinear_kernel, (kept_blocks, one), base, move(sent), both_p, second, tw_kept, kept_out)
    sent = call(next_kernel, blocks, base, device, move(sent), forcing_p, *spectral_tables, mirror)
    sent, next_field = call(
        residual_kernel, (longer, plain), base + [strided, total],
        move(sent), both_p, tw_natural, backward, forward,
    )
    sent, full, sums = call(
        misfit_kernel, (half_blocks, pair, shape(8, 2 * rows)), base,
        device, move(sent), tw_natural, forward, tw_natural, backward, mirror,
    )
    sent, value, product = call(
        joint_kernel, (kept_blocks, one, one), base, move(sent), first, second, tw_kept, kept_in
    )
    second_part = call(slope_second_kernel, one, base, product, *slope_tables)
    sent = call(slope_first_kernel, half_blocks, base, move(sent), *spectral_tables)
    field_grad = call(
        last_kernel, plain, [strided, pltpu.VMEM((outer, rows, inner), float32)], move(sent), value, second_part
    )
    return next_field, sums[0, 0], field_grad, full


def per_device(devices, fast, initial_field, target_field, forcing):
    members, rows, length = initial_field.shape
    device = lax.axis_index(axes).astype(jnp.int32).reshape(1)
    outer, inner = split_length(length)
    vmem = pl.BlockSpec(memory_space=pltpu.VMEM)
    strided = pltpu.VMEM((length, TILE), jnp.float32)

    def reorder(body, shape, operand):
        return pl.pallas_call(
            functools.partial(body, length, rows),
            out_shape=jax.ShapeDtypeStruct(shape, jnp.float32),
            in_specs=[vmem],
            out_specs=vmem,
            scratch_shapes=[strided],
        )(operand)

    if 2 * rows == TILE and inner == 2 * TILE:
        results = [
            joined_step(initial_field[m], target_field[m], forcing, devices, fast, rows, length)
            for m in range(members)
        ]
        next_field = jnp.stack([one[0] for one in results])
        field_grad = jnp.stack([one[1] for one in results])
        forcing_grad = sum(one[2] for one in results)
        objective = sum(one[3].reshape(()) for one in results) / members
        return (next_field, objective, field_grad, forcing_grad)
    forcing_p = reorder(spread_kernel, (outer, 2 * rows, inner), forcing)
    results = [
        member_step(device, initial_field[m], target_field[m], forcing_p, devices, rows, length)
        for m in range(members)
    ]
    next_field = jnp.stack([one[0] for one in results])
    objective = sum(one[1] for one in results) / (members * length * length)
    field_grad = jnp.stack([one[2] for one in results])
    forcing_grad = reorder(collect_kernel, (2, rows, length), sum(one[3] for one in results))
    return (next_field, objective, field_grad, forcing_grad)


def solution(mesh):
    devices = mesh.shape["px"] * mesh.shape["py"]
    spec = P(None, axes, None)
    return jax.shard_map(
        functools.partial(per_device, devices, mesh.shape["py"]),
        mesh=mesh,
        in_specs=(spec, spec, spec),
        out_specs=(spec, P(), spec, spec),
        check_vma=False,
    )
```
